8 devices in a mesh: dp: 1 (over z), tp: 8 (over y, x, core).
Axes of the slice: x: 2, y: 2, z: 1, core: 2. Of those that a mesh axis runs over, the one named last changes fastest.
Arguments:
- tokens: bfloat16 [1, 4096, 3584], P('dp', 'tp')
- start_pos: int32 [1], P('dp')
- cos_tab: float32 [1, 4096, 256], P('dp')
- sin_tab: float32 [1, 4096, 256], P('dp')
- key_cache: bfloat16 [2, 1, 4096, 8, 256], P(None, 'dp', None, 'tp')
- value_cache: bfloat16 [2, 1, 4096, 8, 256], P(None, 'dp', None, 'tp')
- slot_pos: int32 [1, 4096], P('dp')
- norm_params: bfloat16 [2, 4, 3584], replicated
- w_q: bfloat16 [2, 3584, 4096], P(None, None, 'tp')
- b_q: bfloat16 [2, 4096], P(None, 'tp')
- w_k: bfloat16 [2, 3584, 2048], P(None, None, 'tp')
- b_k: bfloat16 [2, 2048], P(None, 'tp')
- w_v: bfloat16 [2, 3584, 2048], P(None, None, 'tp')
- b_v: bfloat16 [2, 2048], P(None, 'tp')
- w_o: bfloat16 [2, 4096, 3584], P(None, 'tp')
- b_o: bfloat16 [2, 3584], replicated
- w_up: bfloat16 [2, 3584, 14336], P(None, None, 'tp')
- b_up: bfloat16 [2, 14336], P(None, 'tp')
- w_down: bfloat16 [2, 14336, 3584], P(None, 'tp')
- b_down: bfloat16 [2, 3584], replicated
Outputs:
- output 1: bfloat16 [1, 4096, 3584], P('dp', 'tp')
- output 2: bfloat16 [2, 1, 4096, 8, 256], P(None, 'dp', None, 'tp')
- output 3: bfloat16 [2, 1, 4096, 8, 256], P(None, 'dp', None, 'tp')
- output 4: int32 [1, 4096], P('dp')
All inputs are finite; a program needn't handle non-finite values.
Results may differ from the reference program's by a relative error of at most 0.0194662.
Values are sent between devices in bfloat16 or wider.
A program may use at most 1 GiB of HBM per device.

```python
import jax
import jax.numpy as jnp
from jax import lax

NUM_SEQS = 1
CHUNK_LEN = 4096
MODEL_DIM = 3584
NUM_HEADS = 16
KV_HEADS = 8
HEAD_DIM = 256
FFN_DIM = 14336
WINDOW = 4096
NUM_LAYERS = 2
NORM_EPS = 1e-5
ROPE_BASE = 1000000.0


def draw_positions(start_key):
    drawn = jax.random.randint(start_key, (NUM_SEQS,), 0, 3 * WINDOW)
    start_pos = jnp.where(jnp.arange(NUM_SEQS) == 0, drawn % WINDOW, drawn).astype(jnp.int32)
    slots = jnp.arange(WINDOW)
    latest = start_pos[:, None] - 1 - (start_pos[:, None] - 1 - slots[None, :]) % WINDOW
    slot_pos = jnp.where(latest >= 0, latest, -1).astype(jnp.int32)
    return start_pos, slot_pos


def rotary_tables(start_pos):
    positions = (start_pos[:, None] + jnp.arange(CHUNK_LEN)[None, :]).astype(jnp.float32)
    inv_freq = ROPE_BASE ** (-jnp.arange(0, HEAD_DIM, 2).astype(jnp.float32) / HEAD_DIM)
    angles = positions[:, :, None] * inv_freq[None, None, :]
    angles = jnp.concatenate([angles, angles], axis=-1)
    return jnp.cos(angles), jnp.sin(angles)


def normal_draw(key, shape, scale):
    return (jax.random.normal(key, shape, jnp.float32) * scale).astype(jnp.bfloat16)


def setup_inputs(seed: int = 0, part: int = 0) -> dict:
    part_keys = jax.random.split(jax.random.fold_in(jax.random.key(seed), part), 4)
    weight_keys = jax.random.split(jax.random.key(seed + 1), 13)
    start_pos, slot_pos = draw_positions(part_keys[1])
    cos_tab, sin_tab = rotary_tables(start_pos)
    cache_shape = (NUM_LAYERS, NUM_SEQS, WINDOW, KV_HEADS, HEAD_DIM)
    q_width = NUM_HEADS * HEAD_DIM
    kv_width = KV_HEADS * HEAD_DIM
    norm_base = jnp.array([1.0, 0.0, 1.0, 0.0], jnp.float32)[None, :, None]
    norm_spread = jnp.array([0.25, 0.2, 0.25, 0.2], jnp.float32)[None, :, None]
    norm_noise = jax.random.normal(weight_keys[0], (NUM_LAYERS, 4, MODEL_DIM), jnp.float32)
    return {
        'tokens': normal_draw(part_keys[0], (NUM_SEQS, CHUNK_LEN, MODEL_DIM), 1.0),
        'start_pos': start_pos,
        'cos_tab': cos_tab,
        'sin_tab': sin_tab,
        'key_cache': normal_draw(part_keys[2], cache_shape, 1.0),
        'value_cache': normal_draw(part_keys[3], cache_shape, 1.0),
        'slot_pos': slot_pos,
        'norm_params': (norm_base + norm_spread * norm_noise).astype(jnp.bfloat16),
        'w_q': normal_draw(weight_keys[1], (NUM_LAYERS, MODEL_DIM, q_width), 2.5 * MODEL_DIM ** -0.5),
        'b_q': normal_draw(weight_keys[2], (NUM_LAYERS, q_width), 0.5),
        'w_k': normal_draw(weight_keys[3], (NUM_LAYERS, MODEL_DIM, kv_width), MODEL_DIM ** -0.5),
        'b_k': normal_draw(weight_keys[4], (NUM_LAYERS, kv_width), 0.5),
        'w_v': normal_draw(weight_keys[5], (NUM_LAYERS, MODEL_DIM, kv_width), MODEL_DIM ** -0.5),
        'b_v': normal_draw(weight_keys[6], (NUM_LAYERS, kv_width), 0.5),
        'w_o': normal_draw(weight_keys[7], (NUM_LAYERS, q_width, MODEL_DIM), 2.0 * q_width ** -0.5),
        'b_o': normal_draw(weight_keys[8], (NUM_LAYERS, MODEL_DIM), 0.3),
        'w_up': normal_draw(weight_keys[9], (NUM_LAYERS, MODEL_DIM, FFN_DIM), MODEL_DIM ** -0.5),
        'b_up': normal_draw(weight_keys[10], (NUM_LAYERS, FFN_DIM), 0.5),
        'w_down': normal_draw(weight_keys[11], (NUM_LAYERS, FFN_DIM, MODEL_DIM), FFN_DIM ** -0.5),
        'b_down': normal_draw(weight_keys[12], (NUM_LAYERS, MODEL_DIM), 0.3),
    }


def layer_norm(hidden, gain, shift):
    values = hidden.astype(jnp.float32)
    centered = values - jnp.mean(values, axis=-1, keepdims=True)
    variance = jnp.mean(centered * centered, axis=-1, keepdims=True)
    scaled = centered * lax.rsqrt(variance + NORM_EPS)
    return (scaled * gain.astype(jnp.float32) + shift.astype(jnp.float32)).astype(jnp.bfloat16)


def apply_rotary(values, cos_b, sin_b):
    half = values.shape[-1] // 2
    turned = jnp.concatenate([-values[..., half:], values[..., :half]], axis=-1)
    return (values * cos_b + turned * sin_b).astype(jnp.bfloat16)


def attend_group(group_in, old_ok, new_ok):
    query, key_new, value_new, cache_k, cache_v = group_in
    scale = HEAD_DIM ** -0.5
    score_old = jnp.einsum('gcd,wd->gcw', query.astype(jnp.float32), cache_k.astype(jnp.float32)) * scale
    score_new = jnp.einsum('gcd,jd->gcj', query.astype(jnp.float32), key_new.astype(jnp.float32)) * scale
    score_old = jnp.where(old_ok[None], score_old, -jnp.inf)
    score_new = jnp.where(new_ok[None], score_new, -jnp.inf)
    top = jnp.maximum(jnp.max(score_old, axis=-1, keepdims=True), jnp.max(score_new, axis=-1, keepdims=True))
    exp_old = jnp.exp(score_old - top)
    exp_new = jnp.exp(score_new - top)
    total = jnp.sum(exp_old, axis=-1, keepdims=True) + jnp.sum(exp_new, axis=-1, keepdims=True)
    mixed = jnp.einsum('gcw,wd->gcd', exp_old.astype(jnp.bfloat16).astype(jnp.float32), cache_v.astype(jnp.float32))
    mixed = mixed + jnp.einsum('gcj,jd->gcd', exp_new.astype(jnp.bfloat16).astype(jnp.float32), value_new.astype(jnp.float32))
    return (mixed / total).astype(jnp.bfloat16)


def attend_sequence(seq_inputs):
    query, key_new, value_new, cache_k, cache_v, held_pos, first_pos = seq_inputs
    positions = first_pos + jnp.arange(CHUNK_LEN)
    old_ok = (held_pos[None, :] >= 0) & (held_pos[None, :] > positions[:, None] - WINDOW) & (held_pos[None, :] <= positions[:, None])
    new_ok = jnp.arange(CHUNK_LEN)[None, :] <= jnp.arange(CHUNK_LEN)[:, None]
    grouped = query.reshape(CHUNK_LEN, KV_HEADS, NUM_HEADS // KV_HEADS, HEAD_DIM).transpose(1, 2, 0, 3)
    per_group = lax.map(lambda group_in: attend_group(group_in, old_ok, new_ok), (grouped, key_new.transpose(1, 0, 2), value_new.transpose(1, 0, 2), cache_k.transpose(1, 0, 2), cache_v.transpose(1, 0, 2)))
    return per_group.transpose(2, 0, 1, 3).reshape(CHUNK_LEN, NUM_HEADS * HEAD_DIM)


def reference(tokens, start_pos, cos_tab, sin_tab, key_cache, value_cache, slot_pos, norm_params, w_q, b_q, w_k, b_k, w_v, b_v, w_o, b_o, w_up, b_up, w_down, b_down):
    positions = start_pos[:, None] + jnp.arange(CHUNK_LEN)[None, :]
    slots = positions % WINDOW
    rows = jnp.arange(NUM_SEQS)[:, None]
    cos_b = cos_tab[:, :, None, :]
    sin_b = sin_tab[:, :, None, :]
    tok_count = NUM_SEQS * CHUNK_LEN

    def layer_step(hidden, layer_in):
        cache_k, cache_v, norms, proj_q, bias_q, proj_k, bias_k, proj_v, bias_v, proj_o, bias_o, proj_up, bias_up, proj_down, bias_down = layer_in
        normed = layer_norm(hidden, norms[0], norms[1]).reshape(tok_count, MODEL_DIM)
        query = jnp.dot(normed, proj_q, preferred_element_type=jnp.float32) + bias_q.astype(jnp.float32)
        query = apply_rotary(query.reshape(NUM_SEQS, CHUNK_LEN, NUM_HEADS, HEAD_DIM), cos_b, sin_b)
        key_new = jnp.dot(normed, proj_k, preferred_element_type=jnp.float32) + bias_k.astype(jnp.float32)
        key_new = apply_rotary(key_new.reshape(NUM_SEQS, CHUNK_LEN, KV_HEADS, HEAD_DIM), cos_b, sin_b)
        value_new = (jnp.dot(normed, proj_v, preferred_element_type=jnp.float32) + bias_v.astype(jnp.float32)).astype(jnp.bfloat16)
        value_new = value_new.reshape(NUM_SEQS, CHUNK_LEN, KV_HEADS, HEAD_DIM)
        mixed = lax.map(attend_sequence, (query, key_new, value_new, cache_k, cache_v, slot_pos, start_pos))
        attended = jnp.dot(mixed.reshape(tok_count, NUM_HEADS * HEAD_DIM), proj_o, preferred_element_type=jnp.float32)
        middle = (hidden.astype(jnp.float32) + attended.reshape(NUM_SEQS, CHUNK_LEN, MODEL_DIM) + bias_o.astype(jnp.float32)).astype(jnp.bfloat16)
        normed = layer_norm(middle, norms[2], norms[3]).reshape(tok_count, MODEL_DIM)
        lifted = jnp.dot(normed, proj_up, preferred_element_type=jnp.float32) + bias_up.astype(jnp.float32)
        active = jax.nn.gelu(lifted, approximate=True).astype(jnp.bfloat16)
        lowered = jnp.dot(active, proj_down, preferred_element_type=jnp.float32).reshape(NUM_SEQS, CHUNK_LEN, MODEL_DIM)
        layer_out = (middle.astype(jnp.float32) + lowered + bias_down.astype(jnp.float32)).astype(jnp.bfloat16)
        new_k = cache_k.at[rows, slots].set(key_new)
        new_v = cache_v.at[rows, slots].set(value_new)
        return layer_out, (new_k, new_v)

    final, (key_out, value_out) = lax.scan(layer_step, tokens, (key_cache, value_cache, norm_params, w_q, b_q, w_k, b_k, w_v, b_v, w_o, b_o, w_up, b_up, w_down, b_down))
    pos_out = slot_pos.at[rows, slots].set(positions.astype(jnp.int32))
    return final, key_out, value_out, pos_out
```

```python
import functools

import jax
import jax.numpy as jnp
from jax import lax
from jax.experimental import pallas as pl
from jax.experimental.pallas import tpu as pltpu
from jax.sharding import PartitionSpec as P

NORM_EPS = 1e-5
LOG2E = 1.4426950408889634
CHUNKS = 4
KEY_TILE = 512
LANES = 128
COLS = 256
WEIGHT_SLOTS = 6
VMEM_LIMIT = 60 * 1024 * 1024
BF16 = jnp.bfloat16
F32 = jnp.float32


ANY = pl.BlockSpec(memory_space=pl.ANY)
SMEM = pl.BlockSpec(memory_space=pltpu.SMEM)
VMEM = pl.BlockSpec(memory_space=pltpu.VMEM)


def layer_norm(hidden, gain, shift):
    values = hidden.astype(F32)
    centered = values - jnp.mean(values, axis=-1, keepdims=True)
    variance = jnp.mean(centered * centered, axis=-1, keepdims=True)
    scaled = centered * lax.rsqrt(variance + NORM_EPS)
    return (scaled * gain.astype(F32) + shift.astype(F32)).astype(BF16)


def gelu_tanh(x):
    inner = 0.7978845608028654 * (x + 0.044715 * (x * x * x))
    return 0.5 * x * (1.0 + jnp.tanh(inner))


def piece_rows(rows):
    half = rows // 2
    return ((0, rows), (rows, rows), (2 * rows, rows), (3 * rows, half), (3 * rows + half, half))


def part_rows(rows):
    half = rows // 2
    return ((0, rows),) + tuple((rows + n * half, half) for n in range(6))


def load_pieces(pieces, dst, sem, rows):
    copies = [pltpu.make_async_copy(p, dst.at[pl.ds(s, n)], sem) for p, (s, n) in zip(pieces, piece_rows(rows))]
    for copy in copies:
        copy.start()
    return copies


def store_parts(src, parts, sem, rows):
    copies = [pltpu.make_async_copy(src.at[pl.ds(s, n)], p, sem) for p, (s, n) in zip(parts, part_rows(rows))]
    for copy in copies:
        copy.start()
    for copy in copies:
        copy.wait()


def qkv_kernel(layer, chunk_id, chunks, dims, scal, *refs):
    rows, model, hd = dims
    pieces = refs[:5]
    cos, sin = refs[5:7]
    sides = (refs[7:10], refs[10:13])
    biases = (refs[13:16], refs[16:19])
    q_out, kv_out = refs[19:21]
    x_s, cos_s, sin_s, w_s, b_s, r_s, o_s, x_sem, t_sem, w_sem, o_sem = refs[21:]
    chip, core = scal[0], scal[1]
    block = rows * chunks
    loads = load_pieces(pieces, x_s, x_sem, rows)
    for g in range(2):
        wq, wk, wv = sides[g]
        for kind, src in enumerate((wq.at[layer, :, pl.ds(0, hd)], wq.at[layer, :, pl.ds(hd, hd)], wk.at[layer], wv.at[layer])):
            pltpu.make_async_copy(src, w_s.at[4 * g + kind], w_sem.at[4 * g + kind]).start()
    for i in range(4):
        start = (jnp.bitwise_xor(chip, i) * 2 + core) * block + chunk_id * rows
        start = pl.multiple_of(start, rows)
        for tab, dst in ((cos, cos_s), (sin, sin_s)):
            copy = pltpu.make_async_copy(tab.at[pl.ds(start, rows)], dst.at[pl.ds(i * rows, rows)], t_sem)
            copy.start()
            loads.append(copy)
    for g in range(2):
        bq, bk, bv = biases[g]
        for kind, val in enumerate((bq[layer:layer + 1, :hd], bq[layer:layer + 1, hd:], bk[layer:layer + 1, :], bv[layer:layer + 1, :])):
            b_s[4 * g + kind] = val.astype(F32)
    for copy in loads:
        copy.wait()

    def out_copy(h, kind, side, is_q):
        if is_q:
            return pltpu.make_async_copy(o_s.at[h], q_out.at[side, :, kind], o_sem.at[h])
        return pltpu.make_async_copy(o_s.at[h], kv_out.at[kind - 2, side], o_sem.at[h])

    def head(h, carry):
        side, kind = h // 4, h % 4
        pltpu.make_async_copy(w_s.at[h], w_s.at[h], w_sem.at[h]).wait()
        r_s[...] = jnp.dot(x_s[...], w_s[h], preferred_element_type=F32) + b_s[h]

        @pl.when(kind != 3)
        def _():
            u = r_s[...]
            turned = jnp.concatenate([-u[:, hd // 2:], u[:, :hd // 2]], axis=1)
            o_s[h] = (u * cos_s[...] + turned * sin_s[...]).astype(BF16).reshape(4, rows, hd)

        @pl.when(kind == 3)
        def _():
            o_s[h] = r_s[...].astype(BF16).reshape(4, rows, hd)

        @pl.when(kind < 2)
        def _():
            out_copy(h, kind, side, True).start()

        @pl.when(kind >= 2)
        def _():
            out_copy(h, kind, side, False).start()

        return carry

    lax.fori_loop(0, 8, head, 0)
    for h in range(8):
        out_copy(h, h % 4, h // 4, h % 4 < 2).wait()


def run_qkv(layer, chunk_id, chunks, scal, pieces, cos, sin, own, peer, own_b, peer_b):
    rows, model = pieces[0].shape
    hd = cos.shape[1]
    dims = (rows, model, hd)
    flops = 2 * 4 * rows * model * 8 * hd
    return pl.pallas_call(
        functools.partial(qkv_kernel, layer, chunk_id, chunks, dims),
        out_shape=(jax.ShapeDtypeStruct((2, 4, 2, rows, hd), BF16), jax.ShapeDtypeStruct((2, 2, 4, rows, hd), BF16)),
        in_specs=[SMEM] + [ANY] * 13 + [VMEM] * 6,
        out_specs=(ANY, ANY),
        scratch_shapes=[
            pltpu.VMEM((4 * rows, model), BF16),
            pltpu.VMEM((4 * rows, hd), F32),
            pltpu.VMEM((4 * rows, hd), F32),
            pltpu.VMEM((8, model, hd), BF16),
            pltpu.VMEM((8, 1, hd), F32),
            pltpu.VMEM((4 * rows, hd), F32),
            pltpu.VMEM((8, 4, rows, hd), BF16),
            pltpu.SemaphoreType.DMA,
            pltpu.SemaphoreType.DMA,
            pltpu.SemaphoreType.DMA((8,)),
            pltpu.SemaphoreType.DMA((8,)),
        ],
        compiler_params=pltpu.CompilerParams(vmem_limit_bytes=VMEM_LIMIT),
        cost_estimate=pl.CostEstimate(flops=flops, bytes_accessed=20_000_000, transcendentals=0),
        name=f"qkv_l{layer}",
    )(scal, *pieces, cos, sin, *own, *peer, *own_b, *peer_b)


def attn_kernel(layer, chunk_id, chunks, dims, emit, scal, *refs):
    rows, model, hd, window = dims
    nkv = 2 * chunks
    q = refs[0]
    kv_new = (refs[1:1 + chunks], refs[1 + chunks:1 + nkv])
    caches = (refs[1 + nkv:3 + nkv], refs[3 + nkv:5 + nkv])
    wo = refs[5 + nkv:7 + nkv]
    outs = refs[7 + nkv:14 + nkv]
    rest = refs[14 + nkv:]
    if emit:
        fresh, rest = rest[:2], rest[2:]
    kv_s, q_s, mix_s, wo_s, out_s, m_s, l_s, acc_s, kv_sem, q_sem, w_sem, o_sem, f_sem = rest
    chip, core, start_pos = scal[0], scal[1], scal[2]
    block = rows * chunks
    tall = 2 * rows
    tile = min(KEY_TILE, window)
    scale = LOG2E * hd ** -0.5
    loads = []
    for g in range(2):
        mine = []
        for kv in range(2):
            mine.append(pltpu.make_async_copy(caches[g][kv].at[layer], kv_s.at[g, kv], kv_sem.at[g]))
            for c in range(chunks):
                for src_core in range(2):
                    part = kv_new[src_core][c].at[kv, g if src_core == 0 else 1 - g]
                    who = core if src_core == 0 else 1 - core
                    for i in range(4):
                        at = (jnp.bitwise_xor(chip, i) * 2 + who) * block + c * rows
                        at = pl.multiple_of(at, rows)
                        mine.append(pltpu.make_async_copy(part.at[i], kv_s.at[g, 2 + kv, pl.ds(at, rows)], kv_sem.at[g]))
        for copy in mine:
            copy.start()
        loads.append(mine)
        if g == 0:
            q_load = pltpu.make_async_copy(q, q_s, q_sem)
            q_load.start()
    w_loads = [pltpu.make_async_copy(wo[g].at[layer], wo_s.at[pl.ds(g * 2 * hd, 2 * hd)], w_sem) for g in range(2)]
    for copy in w_loads:
        copy.start()
    q_load.wait()
    first_slot = lax.rem(start_pos, window)

    def attend(g, i):
        j0 = (jnp.bitwise_xor(chip, i) * 2 + core) * block + chunk_id * rows
        queries = q_s[g, i].reshape(tall, hd)
        m_s[...] = jnp.full_like(m_s, -jnp.inf)
        l_s[...] = jnp.zeros_like(l_s)
        acc_s[...] = jnp.zeros_like(acc_s)
        row = lax.rem(lax.broadcasted_iota(jnp.int32, (tall, 1), 0), rows) + j0
        col = lax.broadcasted_iota(jnp.int32, (1, tile), 1)

        def step(which, at, mask):
            keys = kv_s[g, which, pl.ds(at, tile), :]
            values = kv_s[g, which + 1, pl.ds(at, tile), :]
            s = lax.dot_general(queries, keys, (((1,), (1,)), ((), ())), preferred_element_type=F32) * scale
            if mask is not None:
                s = jnp.where(mask, s, -jnp.inf)
            m_prev = m_s[...]
            m_next = jnp.maximum(m_prev, jnp.max(s, axis=1, keepdims=True))
            p = jnp.exp2(s - jnp.concatenate([m_next] * (tile // LANES), axis=1))
            alpha = jnp.exp2(m_prev - m_next)
            total = l_s[...] * alpha
            for n in range(tile // LANES):
                total = total + p[:, n * LANES:(n + 1) * LANES]
            l_s[...] = total
            m_s[...] = m_next
            mixed = jnp.dot(p.astype(BF16), values, preferred_element_type=F32)
            acc_s[...] = acc_s[...] * jnp.concatenate([alpha] * (hd // LANES), axis=1) + mixed

        diag = j0 // tile
        step(2, pl.multiple_of(diag * tile, tile), col + diag * tile <= row)

        def new_tile(t, carry):
            step(2, pl.multiple_of(t * tile, tile), None)
            return carry

        lax.fori_loop(0, diag, new_tile, 0)
        floor = window - 1 - start_pos
        low = jnp.maximum(j0, floor)
        high = jnp.maximum(j0 + rows - 1, floor)

        def old_tile(t, carry):
            at = pl.multiple_of(t * tile, tile)
            i_min = lax.rem(at - first_slot + window, window)
            wraps = i_min + tile > window
            i_max = jnp.where(wraps, window - 1, i_min + tile - 1)
            full = jnp.logical_and(jnp.logical_not(wraps), i_min > high)

            @pl.when(full)
            def _():
                step(0, at, None)

            @pl.when(jnp.logical_and(jnp.logical_not(full), i_max > low))
            def _():
                age = lax.rem(col + (at - first_slot + window), window)
                step(0, at, age > jnp.maximum(row, floor))

            return carry

        lax.fori_loop(0, window // tile, old_tile, 0)
        total = jnp.sum(l_s[...], axis=1, keepdims=True)
        out = (acc_s[...] / total).astype(BF16)
        at = pl.multiple_of(i * rows, rows)
        for h in range(2):
            mix_s[g, h, pl.ds(at, rows), :] = out[h * rows:(h + 1) * rows]

    for g in range(2):
        for copy in loads[g]:
            copy.wait()
        if emit and g == 0:
            stores = [pltpu.make_async_copy(kv_s.at[0, 2 + kv], fresh[kv], f_sem) for kv in range(2)]
            for copy in stores:
                copy.start()
        lax.fori_loop(0, 4, lambda i, carry: (attend(g, i), carry)[1], 0)
    for copy in w_loads:
        copy.wait()
    mixed = jnp.concatenate([mix_s[g, h] for g in range(2) for h in range(2)], axis=1)

    def project(n, carry):
        at = pl.multiple_of(n * COLS, COLS)
        out_s[:, pl.ds(at, COLS)] = jnp.dot(mixed, wo_s[:, pl.ds(at, COLS)], preferred_element_type=F32).astype(BF16)
        return carry

    lax.fori_loop(0, model // COLS, project, 0)
    store_parts(out_s, outs, o_sem, rows)
    if emit:
        for copy in stores:
            copy.wait()


def part_shapes(rows, model):
    return tuple(jax.ShapeDtypeStruct((n, model), BF16) for _, n in part_rows(rows))


def run_attn(layer, chunk_id, chunks, scal, q, kv_own, kv_peer, caches, wo, emit):
    rows, hd = q.shape[-2:]
    model = wo[0].shape[2]
    window = caches[0].shape[1]
    dims = (rows, model, hd, window)
    out_shape = part_shapes(rows, model)
    if emit:
        out_shape = out_shape + (jax.ShapeDtypeStruct((window, hd), BF16),) * 2
    flops = 4 * 4 * rows * 4 * window * hd + 2 * 4 * rows * 4 * hd * model
    return pl.pallas_call(
        functools.partial(attn_kernel, layer, chunk_id, chunks, dims, emit),
        out_shape=out_shape,
        in_specs=[SMEM] + [ANY] * (7 + 2 * chunks),
        out_specs=(ANY,) * len(out_shape),
        scratch_shapes=[
            pltpu.VMEM((2, 4, window, hd), BF16),
            pltpu.VMEM((2, 4, 2, rows, hd), BF16),
            pltpu.VMEM((2, 2, 4 * rows, hd), BF16),
            pltpu.VMEM((4 * hd, model), BF16),
            pltpu.VMEM((4 * rows, model), BF16),
            pltpu.VMEM((2 * rows, LANES), F32),
            pltpu.VMEM((2 * rows, LANES), F32),
            pltpu.VMEM((2 * rows, hd), F32),
            pltpu.SemaphoreType.DMA((2,)),
            pltpu.SemaphoreType.DMA,
            pltpu.SemaphoreType.DMA,
            pltpu.SemaphoreType.DMA,
            pltpu.SemaphoreType.DMA,
        ],
        compiler_params=pltpu.CompilerParams(vmem_limit_bytes=VMEM_LIMIT),
        cost_estimate=pl.CostEstimate(flops=flops, bytes_accessed=30_000_000, transcendentals=16 * rows * window),
        name=f"attn_l{layer}",
    )(scal, q, *kv_own, *kv_peer, *caches, *wo)


def mlp_kernel(layer, dims, *refs):
    rows, model, ffn = dims
    pieces = refs[:5]
    up = refs[5:7]
    down = refs[7:9]
    bias = refs[9:11]
    outs = refs[11:18]
    x_s, act_s, out_s, w_s, b_s, x_sem, w_sem, o_sem = refs[18:]
    n_up = ffn // COLS
    n_down = model // COLS
    steps = 2 * n_up + n_down
    loads = load_pieces(pieces, x_s, x_sem, rows)

    def fetch(n):
        slot = lax.rem(n, WEIGHT_SLOTS)
        for side in range(2):
            @pl.when(jnp.logical_and(n >= side * n_up, n < (side + 1) * n_up))
            def _():
                at = pl.multiple_of((n - side * n_up) * COLS, COLS)
                pltpu.make_async_copy(up[side].at[layer, :, pl.ds(at, COLS)], w_s.at[slot], w_sem.at[slot]).start()

        @pl.when(jnp.logical_and(n >= 2 * n_up, n < steps))
        def _():
            at = pl.multiple_of((n - 2 * n_up) * COLS, COLS)
            for side in range(2):
                pltpu.make_async_copy(down[side].at[layer, :, pl.ds(at, COLS)], w_s.at[slot, pl.ds(side * ffn, ffn)], w_sem.at[slot]).start()

    def landed(n):
        slot = lax.rem(n, WEIGHT_SLOTS)
        pltpu.make_async_copy(w_s.at[slot], w_s.at[slot], w_sem.at[slot]).wait()
        return slot

    for n in range(WEIGHT_SLOTS - 1):
        fetch(jnp.int32(n))
    for side in range(2):
        for n in range(n_up):
            b_s[side * n_up + n] = bias[side][layer:layer + 1, n * COLS:(n + 1) * COLS].astype(F32)
    for copy in loads:
        copy.wait()

    def up_step(n, carry):
        slot = landed(n)
        fetch(n + WEIGHT_SLOTS - 1)
        lifted = jnp.dot(x_s[...], w_s[slot], preferred_element_type=F32) + b_s[n]
        at = pl.multiple_of(n * COLS, COLS)
        act_s[:, pl.ds(at, COLS)] = gelu_tanh(lifted).astype(BF16)
        return carry

    lax.fori_loop(0, 2 * n_up, up_step, 0)

    def down_step(n, carry):
        slot = landed(n)
        fetch(n + WEIGHT_SLOTS - 1)
        at = pl.multiple_of((n - 2 * n_up) * COLS, COLS)
        out_s[:, pl.ds(at, COLS)] = jnp.dot(act_s[...], w_s[slot], preferred_element_type=F32).astype(BF16)
        return carry

    lax.fori_loop(2 * n_up, steps, down_step, 0)
    store_parts(out_s, outs, o_sem, rows)


def run_mlp(layer, pieces, up, down, bias):
    rows, model = pieces[0].shape
    ffn = up[0].shape[2]
    dims = (rows, model, ffn)
    flops = 2 * 4 * rows * model * ffn * 4
    n_up = ffn // COLS
    return pl.pallas_call(
        functools.partial(mlp_kernel, layer, dims),
        out_shape=part_shapes(rows, model),
        in_specs=[ANY] * 9 + [VMEM] * 2,
        out_specs=(ANY,) * 7,
        scratch_shapes=[
            pltpu.VMEM((4 * rows, model), BF16),
            pltpu.VMEM((4 * rows, 2 * ffn), BF16),
            pltpu.VMEM((4 * rows, model), BF16),
            pltpu.VMEM((WEIGHT_SLOTS, model, COLS), BF16),
            pltpu.VMEM((2 * n_up, 1, COLS), F32),
            pltpu.SemaphoreType.DMA,
            pltpu.SemaphoreType.DMA((WEIGHT_SLOTS,)),
            pltpu.SemaphoreType.DMA,
        ],
        compiler_params=pltpu.CompilerParams(vmem_limit_bytes=VMEM_LIMIT),
        cost_estimate=pl.CostEstimate(flops=flops, bytes_accessed=60_000_000, transcendentals=8 * rows * ffn),
        name=f"mlp_l{layer}",
    )(*pieces, *up, *down, *bias)


def solution(mesh):
    tp = mesh.shape['tp']
    row_spec = P('dp', 'tp', None)
    cache_spec = P(None, 'dp', None, 'tp', None)
    col_spec = P(None, None, 'tp')
    bias_spec = P(None, 'tp')
    in_specs = (row_spec, P('dp'), P('dp', None, None), P('dp', None, None), cache_spec, cache_spec, P('dp', None), P(), col_spec, bias_spec, col_spec, bias_spec, col_spec, bias_spec, P(None, 'tp', None), P(), col_spec, bias_spec, P(None, 'tp', None), P())
    out_specs = (row_spec, cache_spec, cache_spec, P('dp', None))

    def swap(value, bit):
        return lax.ppermute(value, 'tp', [(n, n ^ bit) for n in range(tp)])

    core_swap = functools.partial(swap, bit=1)
    x_swap = functools.partial(swap, bit=2)
    y_swap = functools.partial(swap, bit=4)

    def gather(own):
        half = own.shape[0] // 2
        bx = x_swap(own)
        by = y_swap(own)
        return own, bx, by, y_swap(bx[:half]), x_swap(by[half:])

    def scatter_sum(parts):
        own, xt, xb, yt, yb, dt, db = parts
        rx = x_swap(dt)
        ry = y_swap(db)
        top_x = x_swap(xt)
        bot_y = y_swap(yb)
        bot_x = x_swap((xb.astype(F32) + ry.astype(F32)).astype(BF16))
        top_y = y_swap((yt.astype(F32) + rx.astype(F32)).astype(BF16))
        top = top_x.astype(F32) + top_y.astype(F32)
        bot = bot_x.astype(F32) + bot_y.astype(F32)
        return own.astype(F32) + jnp.concatenate([top, bot], axis=0)

    def device_step(tokens, start_pos, cos_tab, sin_tab, key_cache, value_cache, slot_pos, norm_params, w_q, b_q, w_k, b_k, w_v, b_v, w_o, b_o, w_up, b_up, w_down, b_down):
        layers, _, window, _, hd = key_cache.shape
        own_len, model = tokens.shape[1:]
        rows = own_len // CHUNKS
        me = lax.axis_index('tp')
        scal = jnp.stack([me // 2, me % 2, start_pos[0]]).astype(jnp.int32)
        cos, sin = cos_tab[0], sin_tab[0]
        kc = key_cache.reshape(layers, window, hd)
        vc = value_cache.reshape(layers, window, hd)
        qkv_w = (w_q, w_k, w_v)
        qkv_b = (b_q, b_k, b_v)
        qkv_w_peer = tuple(core_swap(w) for w in qkv_w)
        qkv_b_peer = tuple(core_swap(b) for b in qkv_b)
        caches = (kc, vc, core_swap(kc), core_swap(vc))
        wo = (w_o, core_swap(w_o))
        up = (w_up, core_swap(w_up))
        bias_up = (b_up, core_swap(b_up))
        down = (w_down, core_swap(w_down))
        hidden = [tokens[0, c * rows:(c + 1) * rows] for c in range(CHUNKS)]
        fresh = []
        for layer in range(layers):
            gain1, shift1, gain2, shift2 = (norm_params[layer, n] for n in range(4))
            q, kv, kv_peer = [], [], []
            for c in range(CHUNKS):
                pieces = gather(layer_norm(hidden[c], gain1, shift1))
                q_c, kv_c = run_qkv(layer, c, CHUNKS, scal, pieces, cos, sin, qkv_w, qkv_w_peer, qkv_b, qkv_b_peer)
                q.append(q_c)
                kv.append(kv_c)
                kv_peer.append(core_swap(kv_c))
            middle = []
            for c in range(CHUNKS):
                got = run_attn(layer, c, CHUNKS, scal, q[c], kv, kv_peer, caches, wo, c == 0)
                if c == 0:
                    fresh.append(got[7:])
                summed = scatter_sum(got[:7])
                middle.append((hidden[c].astype(F32) + summed + b_o[layer].astype(F32)).astype(BF16))
            hidden = []
            for c in range(CHUNKS):
                pieces = gather(layer_norm(middle[c], gain2, shift2))
                summed = scatter_sum(run_mlp(layer, pieces, up, down, bias_up))
                hidden.append((middle[c].astype(F32) + summed + b_down[layer].astype(F32)).astype(BF16))
        first_slot = start_pos[0] % window

        def place(values):
            rolled = lax.dynamic_slice_in_dim(jnp.concatenate([values, values], axis=0), window - first_slot, window, axis=0)
            return rolled.reshape(1, window, 1, hd)

        key_out = jnp.stack([place(f[0]) for f in fresh])
        value_out = jnp.stack([place(f[1]) for f in fresh])
        pos_out = (start_pos[0] + (jnp.arange(window, dtype=jnp.int32) - first_slot) % window)[None]
        return jnp.concatenate(hidden, axis=0)[None], key_out, value_out, pos_out

    return jax.shard_map(device_step, mesh=mesh, in_specs=in_specs, out_specs=out_specs, check_vma=False)
```

```python
import functools

import jax
import jax.numpy as jnp
from jax import lax
from jax.experimental import pallas as pl
from jax.experimental.pallas import tpu as pltpu
from jax.sharding import PartitionSpec as P

NORM_EPS = 1e-5
LOG2E = 1.4426950408889634
CHUNKS = 4
KEY_TILE = 512
LANES = 128
WIDE = 512
ROW_BLOCK = 16
WEIGHT_SLOTS = 3
VMEM_LIMIT = 62 * 1024 * 1024
BF16 = jnp.bfloat16
F32 = jnp.float32
MESH = pl.DeviceIdType.MESH


ANY = pl.BlockSpec(memory_space=pl.ANY)
SMEM = pl.BlockSpec(memory_space=pltpu.SMEM)
VMEM = pl.BlockSpec(memory_space=pltpu.VMEM)
DMA = pltpu.SemaphoreType.DMA


def gelu_tanh(x):
    inner = 0.7978845608028654 * (x + 0.044715 * (x * x * x))
    return 0.5 * x * (1.0 + jnp.tanh(inner))


def normalized(values, gain, shift):
    centered = values - jnp.mean(values, axis=-1, keepdims=True)
    variance = jnp.mean(centered * centered, axis=-1, keepdims=True)
    return (centered * lax.rsqrt(variance + NORM_EPS) * gain + shift).astype(BF16)


class Place:
    def __init__(self):
        me = lax.axis_index('tp')
        self.core = me % 2
        self.xb = (me // 2) % 2
        self.yb = me // 4
        self.peer = me + 1 - 2 * self.core
        self.x = me + 2 - 4 * self.xb
        self.y = me + 4 - 8 * self.yb

    def member(self, i):
        xb = self.xb + (i % 2) * (1 - 2 * self.xb)
        yb = self.yb + (i // 2) * (1 - 2 * self.yb)
        return yb * 2 + xb

    def barrier(self, others):
        sem = pltpu.get_barrier_semaphore()
        for other in others:
            pl.semaphore_signal(sem, inc=1, device_id={'tp': other}, device_id_type=MESH)
        pl.semaphore_wait(sem, len(others))


def remote(src, dst, send_sem, recv_sem, other):
    return pltpu.make_async_remote_copy(src_ref=src, dst_ref=dst, send_sem=send_sem, recv_sem=recv_sem, device_id={'tp': other}, device_id_type=MESH)


class Gather:
    def __init__(self, place, x_s, send, recv, rows):
        self.place, self.x_s, self.send, self.recv, self.rows = place, x_s, send, recv, rows

    def copy(self, c, kind):
        r, h = self.rows, self.rows // 2
        src, dst, size, other = ((0, r, r, self.place.x), (0, 2 * r, r, self.place.y), (r, 3 * r, h, self.place.y), (2 * r + h, 3 * r + h, h, self.place.x))[kind]
        return remote(self.x_s.at[c, pl.ds(src, size)], self.x_s.at[c, pl.ds(dst, size)], self.send.at[c, kind], self.recv.at[c, kind], other)

    def start(self, c):
        self.copy(c, 0).start()
        self.copy(c, 1).start()

    def forward(self, c):
        self.copy(c, 0).wait_recv()
        self.copy(c, 2).start()
        self.copy(c, 1).wait_recv()
        self.copy(c, 3).start()

    def finish(self, c):
        self.copy(c, 2).wait_recv()
        self.copy(c, 3).wait_recv()

    def drain(self, c):
        for kind in range(4):
            self.copy(c, kind).wait_send()


class Scatter:
    def __init__(self, place, out_s, land_s, send, recv, rows):
        self.place, self.out_s, self.land_s, self.send, self.recv, self.rows = place, out_s, land_s, send, recv, rows

    def copy(self, c, kind):
        r, h = self.rows, self.rows // 2
        x, y = self.place.x, self.place.y
        src, dst, other = ((3 * r, 2 * r, x), (3 * r + h, 2 * r + h, y), (r, 0, x), (2 * r + h, r + h, y), (r + h, h, x), (2 * r, r, y))[kind]
        return remote(self.out_s.at[c, pl.ds(src, h)], self.land_s.at[c, pl.ds(dst, h)], self.send.at[c, kind], self.recv.at[c, kind], other)

    def start(self, c):
        for kind in range(4):
            self.copy(c, kind).start()

    def add(self, c, kind, src, dst):
        self.copy(c, kind).wait_recv()

        def block(n, carry):
            at = pl.multiple_of(n * ROW_BLOCK, ROW_BLOCK)
            mine = self.out_s[c, pl.ds(dst + at, ROW_BLOCK), :].astype(F32)
            came = self.land_s[c, pl.ds(src + at, ROW_BLOCK), :].astype(F32)
            self.out_s[c, pl.ds(dst + at, ROW_BLOCK), :] = (mine + came).astype(BF16)
            return carry

        lax.fori_loop(0, self.rows // 2 // ROW_BLOCK, block, 0)

    def relay(self, c):
        r, h = self.rows, self.rows // 2
        self.add(c, 0, 2 * r, 2 * r)
        self.copy(c, 5).start()
        self.add(c, 1, 2 * r + h, r + h)
        self.copy(c, 4).start()

    def finish(self, c):
        for kind in range(2, 6):
            self.copy(c, kind).wait_recv()

    def drain(self, c):
        for kind in range(6):
            self.copy(c, kind).wait_send()


def qkv_kernel(layer, dims, *refs):
    chunks, rows, model, hd = dims
    hidden, norms, cos, sin, wq, wk, wv, bq, bk, bv, b_peer = refs[:11]
    q_out, kv_out = refs[11:13]
    x_s, h_s, t_s, w_s, b_s, oq_s, okv_s, ag_send, ag_recv, h_sem, t_sem, w_sem, wr_send, wr_recv, q_sem, kv_sem, kr_send, kr_recv = refs[13:]
    place = Place()
    block = rows * chunks
    place.barrier((place.x, place.y, place.peer))
    gather = Gather(place, x_s, ag_send, ag_recv, rows)
    loads = [pltpu.make_async_copy(hidden.at[pl.ds(c * rows, rows)], h_s.at[c], h_sem.at[c]) for c in range(chunks)]
    for copy in loads:
        copy.start()
    places = ((wq.at[layer], 0, 0, 2 * hd), (wk.at[layer], 1, 0, hd), (wv.at[layer], 1, hd, hd))
    w_local = [pltpu.make_async_copy(src, w_s.at[t, :, pl.ds(at, n)], w_sem.at[k]) for k, (src, t, at, n) in enumerate(places)]
    w_remote = [remote(src, w_s.at[2 + t, :, pl.ds(at, n)], wr_send.at[k], wr_recv.at[k], place.peer) for k, (src, t, at, n) in enumerate(places)]
    gain = norms[layer, 0:1, :].astype(F32)
    shift = norms[layer, 1:2, :].astype(F32)

    def send_own(c):
        loads[c].wait()

        def norm_block(n, carry):
            at = pl.multiple_of(n * ROW_BLOCK, ROW_BLOCK)
            x_s[c, pl.ds(at, ROW_BLOCK), :] = normalized(h_s[c, pl.ds(at, ROW_BLOCK), :].astype(F32), gain, shift)
            return carry

        lax.fori_loop(0, rows // ROW_BLOCK, norm_block, 0)
        gather.start(c)

    def chunk_pos(c, i):
        return pl.multiple_of((place.member(i) * 2 + place.core) * block + c * rows, rows)

    def table_copies(c):
        return [pltpu.make_async_copy(tab.at[pl.ds(chunk_pos(c, i), rows)], t_s.at[c, k, pl.ds(i * rows, rows)], t_sem.at[c]) for i in range(4) for k, tab in enumerate((cos, sin))]

    send_own(0)
    send_own(1)
    for copy in w_remote + w_local:
        copy.start()
    for c in range(chunks):
        for copy in table_copies(c):
            copy.start()
    b_s[0] = bq[layer:layer + 1, :].astype(F32)
    b_s[1, :, 0:hd] = bk[layer:layer + 1, :].astype(F32)
    b_s[1, :, hd:] = bv[layer:layer + 1, :].astype(F32)
    b_s[2] = b_peer[layer:layer + 1, 0:2 * hd].astype(F32)
    b_s[3] = b_peer[layer:layer + 1, 2 * hd:4 * hd].astype(F32)
    gather.forward(0)
    send_own(2)
    gather.forward(1)
    send_own(3)

    def rope(u, c):
        turned = jnp.concatenate([-u[:, hd // 2:], u[:, :hd // 2]], axis=1)
        return (u * t_s[c, 0] + turned * t_s[c, 1]).astype(BF16).reshape(4, rows, hd)

    def q_copy(c):
        return pltpu.make_async_copy(oq_s.at[c], q_out.at[c], q_sem.at[c])

    def kv_copies(c):
        near = [pltpu.make_async_copy(okv_s.at[c, :, :, i], kv_out.at[:, :, pl.ds(chunk_pos(c, i), rows)], kv_sem.at[c]) for i in range(4)]
        far = [remote(okv_s.at[c, :, g, i], kv_out.at[:, 1 - g, pl.ds(chunk_pos(c, i), rows)], kr_send.at[c], kr_recv.at[c], place.peer) for g in range(2) for i in range(4)]
        return near, far

    def chunk(c, carry):
        pltpu.make_async_copy(t_s.at[c], t_s.at[c], t_sem.at[c]).wait()
        gather.finish(c)
        for g in range(2):
            @pl.when(c == 0)
            def _():
                for copy in ((w_local[0],) if g == 0 else ()):
                    copy.wait()
                if g == 1:
                    w_remote[0].wait_recv()

            u = jnp.dot(x_s[c], w_s[2 * g], preferred_element_type=F32) + b_s[2 * g]
            for h in range(2):
                oq_s[c, g, :, h] = rope(u[:, h * hd:(h + 1) * hd], c)

            @pl.when(c == 0)
            def _():
                for copy in (w_local[1:] if g == 0 else ()):
                    copy.wait()
                if g == 1:
                    for copy in w_remote[1:]:
                        copy.wait_recv()

            u = jnp.dot(x_s[c], w_s[2 * g + 1], preferred_element_type=F32) + b_s[2 * g + 1]
            okv_s[c, 0, g] = rope(u[:, :hd], c)
            okv_s[c, 1, g] = u[:, hd:].astype(BF16).reshape(4, rows, hd)
        q_copy(c).start()
        near, far = kv_copies(c)
        for copy in near + far:
            copy.start()

        @pl.when(c + 2 < chunks)
        def _():
            gather.forward(c + 2)

        return carry

    lax.fori_loop(0, chunks, chunk, 0)
    for copy in w_remote:
        copy.wait_send()

    def settle(c, carry):
        q_copy(c).wait()
        whole = okv_s.at[c]
        pltpu.make_async_copy(whole, whole, kv_sem.at[c]).wait()
        remote(whole, whole, kr_send.at[c], kr_recv.at[c], place.peer).wait_send()
        remote(whole, whole, kr_send.at[c], kr_recv.at[c], place.peer).wait_recv()
        gather.drain(c)
        return carry

    lax.fori_loop(0, chunks, settle, 0)


def run_qkv(layer, chunks, hidden, norms, cos, sin, weights, biases, b_peer):
    model = hidden.shape[1]
    rows = hidden.shape[0] // chunks
    hd = cos.shape[1]
    window = cos.shape[0]
    dims = (chunks, rows, model, hd)
    flops = 2 * 4 * rows * chunks * model * 8 * hd
    return pl.pallas_call(
        functools.partial(qkv_kernel, layer, dims),
        out_shape=(jax.ShapeDtypeStruct((chunks, 2, 4, 2, rows, hd), BF16), jax.ShapeDtypeStruct((2, 2, window, hd), BF16)),
        in_specs=[ANY, VMEM] + [ANY] * 5 + [VMEM] * 4,
        out_specs=(ANY, ANY),
        scratch_shapes=[
            pltpu.VMEM((chunks, 4 * rows, model), BF16),
            pltpu.VMEM((chunks, rows, model), BF16),
            pltpu.VMEM((chunks, 2, 4 * rows, hd), F32),
            pltpu.VMEM((4, model, 2 * hd), BF16),
            pltpu.VMEM((4, 1, 2 * hd), F32),
            pltpu.VMEM((chunks, 2, 4, 2, rows, hd), BF16),
            pltpu.VMEM((chunks, 2, 2, 4, rows, hd), BF16),
            DMA((chunks, 4)),
            DMA((chunks, 4)),
            DMA((chunks,)),
            DMA((chunks,)),
            DMA((3,)),
            DMA((3,)),
            DMA((3,)),
            DMA((chunks,)),
            DMA((chunks,)),
            DMA((chunks,)),
            DMA((chunks,)),
        ],
        compiler_params=pltpu.CompilerParams(vmem_limit_bytes=VMEM_LIMIT, collective_id=2 * layer, has_side_effects=True),
        cost_estimate=pl.CostEstimate(flops=4 * flops, bytes_accessed=20_000_000, transcendentals=0),
        name=f"qkv_l{layer}",
    )(hidden, norms, cos, sin, *weights, *biases, b_peer)


def attn_kernel(layer, chunk_id, dims, scal, *refs):
    chunks, rows, model, hd, window = dims
    q, kv_new = refs[:2]
    caches = (refs[2:4], refs[4:6])
    wo = refs[6:8]
    own_out, x1_out, y1_out, xb_out, yt_out = refs[8:13]
    kv_s, q_s, s_s, mix_s, wo_s, out_s, m_s, l_s, acc_s, kv_sem, q_sem, w_sem, o_sem = refs[13:]
    chip, core, start_pos = scal[0], scal[1], scal[2]
    block = rows * chunks
    tall = 2 * rows
    tile = KEY_TILE
    tiles = window // tile
    scale = LOG2E * hd ** -0.5
    q_load = pltpu.make_async_copy(q.at[chunk_id], q_s, q_sem)
    q_load.start()
    for g in range(2):
        pltpu.make_async_copy(kv_new.at[:, g], kv_s.at[g, pl.ds(2, 2)], kv_sem).start()
    for g in range(2):
        for kv in range(2):
            pltpu.make_async_copy(caches[g][kv].at[layer], kv_s.at[g, kv], kv_sem).start()
    w_loads = [pltpu.make_async_copy(wo[g].at[layer], wo_s.at[pl.ds(g * 2 * hd, 2 * hd)], w_sem) for g in range(2)]
    for copy in w_loads:
        copy.start()
    q_load.wait()
    pltpu.make_async_copy(kv_s, kv_s, kv_sem).wait()
    first_slot = lax.rem(start_pos, window)
    floor = window - 1 - start_pos

    def plan(i):
        j0 = (jnp.bitwise_xor(chip, i) * 2 + core) * block + chunk_id * rows
        low = jnp.maximum(j0, floor)
        high = jnp.maximum(j0 + rows - 1, floor)
        diag = j0 // tile
        a = (first_slot + low + 1) // tile
        b = (first_slot + window - 1) // tile
        some = low < window - 1
        t_f = jnp.minimum((first_slot + high) // tile, b)
        front = jnp.where(some, t_f - a + 1, 0)
        back = jnp.where(jnp.logical_and(some, jnp.logical_and(lax.rem(first_slot, tile) != 0, b > t_f)), 1, 0)
        whole_old = jnp.where(some, b - back - t_f, 0)
        masked = 1 + front + back
        return j0, diag, a, b, t_f, front, masked, masked + diag + whole_old

    def tile_at(p, n):
        j0, diag, a, b, t_f, front, masked, count = p
        whole = n - masked
        old = jnp.where(n < masked, jnp.where(n <= front, a + n - 1, b), t_f + 1 + whole - diag)
        new = jnp.where(n == 0, diag, whole)
        is_new = jnp.logical_or(n == 0, jnp.logical_and(whole >= 0, whole < diag))
        t = jnp.where(is_new, new, old)
        return jnp.where(is_new, 2, 0), pl.multiple_of(lax.rem(t, tiles) * tile, tile), t * tile, is_new

    def scores(i, p, n):
        which, at, _, _ = tile_at(p, n)
        for g in range(2):
            queries = q_s[g, i].reshape(tall, hd)
            s_s[g] = lax.dot_general(queries, kv_s[g, which, pl.ds(at, tile), :], (((1,), (1,)), ((), ())), preferred_element_type=F32)

    scores(0, plan(0), 0)

    def attend(i, carry):
        p = plan(i)
        j0, count, masked = p[0], p[-1], p[-2]
        following = jnp.minimum(i + 1, 3)
        p_next = plan(following)
        m_s[...] = jnp.full_like(m_s, -jnp.inf)
        l_s[...] = jnp.zeros_like(l_s)
        acc_s[...] = jnp.zeros_like(acc_s)

        def step(n, with_mask):
            which, at, place, is_new = tile_at(p, n)
            last = n + 1 == count
            nw, nat, _, _ = tile_at(p, n + 1)
            fw, fat, _, _ = tile_at(p_next, 0)
            nw = jnp.where(last, fw, nw)
            nat = pl.multiple_of(jnp.where(last, fat, nat), tile)
            ni = jnp.where(last, following, i)
            if with_mask:
                row = lax.rem(lax.broadcasted_iota(jnp.int32, (tall, 1), 0), rows) + j0
                col = lax.broadcasted_iota(jnp.int32, (1, tile), 1) + place - jnp.where(is_new, 0, first_slot)
                lo = jnp.where(is_new, -1, jnp.maximum(row, floor))
                hi = jnp.where(is_new, row, window - 1)
                mask = jnp.logical_and(col > lo, col <= hi)
            for g in range(2):
                s = s_s[g] * scale
                if with_mask:
                    s = jnp.where(mask, s, -jnp.inf)
                s_next = lax.dot_general(q_s[g, ni].reshape(tall, hd), kv_s[g, nw, pl.ds(nat, tile), :], (((1,), (1,)), ((), ())), preferred_element_type=F32)
                m_prev = m_s[g]
                m_next = jnp.maximum(m_prev, jnp.max(s, axis=1, keepdims=True))
                e = jnp.exp2(s - jnp.concatenate([m_next] * (tile // LANES), axis=1))
                alpha = jnp.exp2(m_prev - m_next)
                total = l_s[g] * alpha
                for k in range(tile // LANES):
                    total = total + e[:, k * LANES:(k + 1) * LANES]
                l_s[g] = total
                m_s[g] = m_next
                mixed = jnp.dot(e.astype(BF16), kv_s[g, which + 1, pl.ds(at, tile), :], preferred_element_type=F32)
                acc_s[g] = acc_s[g] * jnp.concatenate([alpha] * (hd // LANES), axis=1) + mixed
                s_s[g] = s_next
            return n + 1

        lax.fori_loop(0, masked, lambda n, c: (step(n, True), c)[1], 0)
        lax.fori_loop(masked, count, lambda n, c: (step(n, False), c)[1], 0)
        at = pl.multiple_of(i * rows, rows)
        for g in range(2):
            total = jnp.sum(l_s[g], axis=1, keepdims=True)
            out = (acc_s[g] / total).astype(BF16)
            for h in range(2):
                mix_s[pl.ds(at, rows), (2 * g + h) * hd:(2 * g + h + 1) * hd] = out[h * rows:(h + 1) * rows]
        return carry

    lax.fori_loop(0, 4, attend, 0)
    for copy in w_loads:
        copy.wait()

    def project(n, carry):
        at = pl.multiple_of(n * WIDE, WIDE)
        out_s[:, pl.ds(at, WIDE)] = jnp.dot(mix_s[...], wo_s[:, pl.ds(at, WIDE)], preferred_element_type=F32).astype(BF16)
        return carry

    lax.fori_loop(0, model // WIDE, project, 0)
    r, h = rows, rows // 2
    moves = ((0, r, own_out), (3 * r, h, x1_out.at[pl.ds(0, h)]), (r, h, x1_out.at[pl.ds(h, h)]), (3 * r + h, h, y1_out.at[pl.ds(0, h)]), (2 * r + h, h, y1_out.at[pl.ds(h, h)]), (r + h, h, xb_out), (2 * r, h, yt_out))
    stores = [pltpu.make_async_copy(out_s.at[pl.ds(s, n)], dst, o_sem) for s, n, dst in moves]
    for copy in stores:
        copy.start()
    for copy in stores:
        copy.wait()


def run_attn(layer, chunk_id, scal, q, kv_new, caches, wo):
    chunks, rows, hd = q.shape[0], q.shape[-2], q.shape[-1]
    model = wo[0].shape[2]
    window = caches[0].shape[1]
    dims = (chunks, rows, model, hd, window)
    half = rows // 2
    flops = 4 * 4 * rows * 4 * window * hd + 2 * 4 * rows * 4 * hd * model
    return pl.pallas_call(
        functools.partial(attn_kernel, layer, chunk_id, dims),
        out_shape=tuple(jax.ShapeDtypeStruct((n, model), BF16) for n in (rows, rows, rows, half, half)),
        in_specs=[SMEM] + [ANY] * 8,
        out_specs=(ANY,) * 5,
        scratch_shapes=[
            pltpu.VMEM((2, 4, window, hd), BF16),
            pltpu.VMEM((2, 4, 2, rows, hd), BF16),
            pltpu.VMEM((2, 2 * rows, KEY_TILE), F32),
            pltpu.VMEM((4 * rows, 4 * hd), BF16),
            pltpu.VMEM((4 * hd, model), BF16),
            pltpu.VMEM((4 * rows, model), BF16),
            pltpu.VMEM((2, 2 * rows, LANES), F32),
            pltpu.VMEM((2, 2 * rows, LANES), F32),
            pltpu.VMEM((2, 2 * rows, hd), F32),
            DMA,
            DMA,
            DMA,
            DMA,
        ],
        compiler_params=pltpu.CompilerParams(vmem_limit_bytes=VMEM_LIMIT),
        cost_estimate=pl.CostEstimate(flops=flops, bytes_accessed=30_000_000, transcendentals=16 * rows * window),
        name=f"attn_l{layer}",
    )(scal, q, kv_new, *caches, *wo)


def mlp_kernel(layer, dims, bias_at, *refs):
    chunks, rows, model, ffn = dims
    parts = [refs[5 * c:5 * c + 5] for c in range(chunks)]
    refs = refs[5 * chunks:]
    hidden, norms, b_o, b_down, b_up, b_peer = refs[:6]
    up, down = refs[6:8], refs[8:10]
    h_out = refs[10]
    x_s, out_s, land_s, act_s, w_s, mid_s, b_s, ag_send, ag_recv, rs_send, rs_recv, st_sem, w_sem, h_sem = refs[11:]
    place = Place()
    half = rows // 2
    n_up = 2 * ffn // WIDE
    n_tiles = n_up + model // WIDE
    sub = WIDE // 2
    n_sub = ffn // sub
    place.barrier((place.x, place.y))
    gather = Gather(place, x_s, ag_send, ag_recv, rows)
    scatter = Scatter(place, out_s, land_s, rs_send, rs_recv, rows)
    for c in range(chunks):
        own, r1x, r1y, a2, b1 = parts[c]
        moves = ((own, 0, rows), (r1x.at[pl.ds(half, half)], rows, half), (a2, rows + half, half), (b1, 2 * rows, half), (r1y.at[pl.ds(half, half)], 2 * rows + half, half), (hidden.at[pl.ds(c * rows, rows)], 3 * rows, rows))
        for src, at, n in moves:
            pltpu.make_async_copy(src, out_s.at[c, pl.ds(at, n)], st_sem.at[c]).start()
    gain = norms[layer, 2:3, :].astype(F32)
    shift = norms[layer, 3:4, :].astype(F32)
    bias_o = b_o[layer:layer + 1, :].astype(F32)

    def fetch(c, k):
        over = k >= n_tiles
        k = jnp.where(over, k - n_tiles, k)
        c = jnp.where(over, c + 1, c)
        slot = lax.rem(c * n_tiles + k, WEIGHT_SLOTS)

        @pl.when(c < chunks)
        def _():
            for part in range(2):
                n = 2 * k + part
                for side in range(2):
                    @pl.when(jnp.logical_and(n >= side * n_sub, n < (side + 1) * n_sub))
                    def _():
                        at = pl.multiple_of((n - side * n_sub) * sub, sub)
                        pltpu.make_async_copy(up[side].at[layer, :, pl.ds(at, sub)], w_s.at[slot, :, pl.ds(part * sub, sub)], w_sem.at[slot]).start()

            @pl.when(k >= n_up)
            def _():
                at = pl.multiple_of((k - n_up) * WIDE, WIDE)
                for side in range(2):
                    pltpu.make_async_copy(down[side].at[layer, :, pl.ds(at, WIDE)], w_s.at[slot, pl.ds(side * ffn, ffn)], w_sem.at[slot]).start()

    def landed(c, k):
        slot = lax.rem(c * n_tiles + k, WEIGHT_SLOTS)
        pltpu.make_async_copy(w_s.at[slot], w_s.at[slot], w_sem.at[slot]).wait()
        fetch(c, k + WEIGHT_SLOTS - 1)
        return slot

    def send_own(c):
        pltpu.make_async_copy(out_s.at[c], out_s.at[c], st_sem.at[c]).wait()

        def norm_block(n, carry):
            at = pl.multiple_of(n * ROW_BLOCK, ROW_BLOCK)
            total = [out_s[c, pl.ds(k * rows + at, ROW_BLOCK), :].astype(F32) for k in range(4)]
            middle = (total[3] + (total[0] + total[1] + total[2]) + bias_o).astype(BF16)
            mid_s[c, pl.ds(at, ROW_BLOCK), :] = middle
            x_s[c, pl.ds(at, ROW_BLOCK), :] = normalized(middle.astype(F32), gain, shift)
            return carry

        lax.fori_loop(0, rows // ROW_BLOCK, norm_block, 0)
        gather.start(c)

    send_own(0)
    send_own(1)
    for k in range(WEIGHT_SLOTS - 1):
        fetch(jnp.int32(0), jnp.int32(k))
    for n in range(2 * n_sub):
        src = b_up[layer:layer + 1, n * sub:(n + 1) * sub] if n < n_sub else b_peer[layer:layer + 1, bias_at + (n - n_sub) * sub:bias_at + (n - n_sub + 1) * sub]
        b_s[n // 2, :, (n % 2) * sub:(n % 2 + 1) * sub] = src.astype(F32)
    gather.forward(0)
    send_own(2)
    gather.forward(1)
    send_own(3)

    def chunk(c, carry):
        gather.finish(c)

        def up_step(k, inner):
            slot = landed(c, k)
            at = pl.multiple_of(k * WIDE, WIDE)
            for top in range(2):
                r0 = top * 2 * rows
                lifted = jnp.dot(x_s[c, r0:r0 + 2 * rows, :], w_s[slot], preferred_element_type=F32) + b_s[k]
                act_s[r0:r0 + 2 * rows, pl.ds(at, WIDE)] = gelu_tanh(lifted).astype(BF16)
            return inner

        lax.fori_loop(0, n_up, up_step, 0)

        @pl.when(c + 2 < chunks)
        def _():
            gather.forward(c + 2)

        @pl.when(c >= 2)
        def _():
            scatter.relay(c - 2)

        def down_step(k, inner):
            slot = landed(c, k)
            at = pl.multiple_of((k - n_up) * WIDE, WIDE)
            out_s[c, :, pl.ds(at, WIDE)] = jnp.dot(act_s[...], w_s[slot], preferred_element_type=F32).astype(BF16)
            return inner

        lax.fori_loop(n_up, n_tiles, down_step, 0)
        scatter.start(c)
        return carry

    lax.fori_loop(0, chunks, chunk, 0)
    bias_d = b_down[layer:layer + 1, :].astype(F32)

    def h_copy(c):
        return pltpu.make_async_copy(mid_s.at[c], h_out.at[pl.ds(pl.multiple_of(c * rows, rows), rows)], h_sem.at[c])

    def finish(c, carry):
        @pl.when(c + 2 < chunks)
        def _():
            scatter.relay(c + 2)

        scatter.finish(c)

        def block(n, inner):
            at = pl.multiple_of(n * ROW_BLOCK, ROW_BLOCK)
            total = out_s[c, pl.ds(at, ROW_BLOCK), :].astype(F32) + land_s[c, pl.ds(at, ROW_BLOCK), :].astype(F32) + land_s[c, pl.ds(rows + at, ROW_BLOCK), :].astype(F32)
            mid_s[c, pl.ds(at, ROW_BLOCK), :] = (mid_s[c, pl.ds(at, ROW_BLOCK), :].astype(F32) + total + bias_d).astype(BF16)
            return inner

        lax.fori_loop(0, rows // ROW_BLOCK, block, 0)
        h_copy(c).start()
        return carry

    lax.fori_loop(0, chunks, finish, 0)

    def settle(c, carry):
        h_copy(c).wait()
        gather.drain(c)
        scatter.drain(c)
        return carry

    lax.fori_loop(0, chunks, settle, 0)


def run_mlp(layer, parts, hidden, norms, b_o, b_down, b_up, b_peer, up, down):
    chunks = len(parts)
    model = hidden.shape[1]
    rows = hidden.shape[0] // chunks
    ffn = up[0].shape[2]
    dims = (chunks, rows, model, ffn)
    flops = 2 * 4 * rows * chunks * model * ffn * 4
    flat = [a for part in parts for a in part]
    return pl.pallas_call(
        functools.partial(mlp_kernel, layer, dims, b_peer.shape[1] - ffn),
        out_shape=jax.ShapeDtypeStruct(hidden.shape, BF16),
        in_specs=[ANY] * (len(flat) + 1) + [VMEM] * 5 + [ANY] * 4,
        out_specs=ANY,
        scratch_shapes=[
            pltpu.VMEM((chunks, 4 * rows, model), BF16),
            pltpu.VMEM((chunks, 4 * rows, model), BF16),
            pltpu.VMEM((chunks, 3 * rows, model), BF16),
            pltpu.VMEM((4 * rows, 2 * ffn), BF16),
            pltpu.VMEM((WEIGHT_SLOTS, model, WIDE), BF16),
            pltpu.VMEM((chunks, rows, model), BF16),
            pltpu.VMEM((2 * ffn // WIDE, 1, WIDE), F32),
            DMA((chunks, 4)),
            DMA((chunks, 4)),
            DMA((chunks, 6)),
            DMA((chunks, 6)),
            DMA((chunks,)),
            DMA((WEIGHT_SLOTS,)),
            DMA((chunks,)),
        ],
        compiler_params=pltpu.CompilerParams(vmem_limit_bytes=VMEM_LIMIT, collective_id=2 * layer + 1, has_side_effects=True),
        cost_estimate=pl.CostEstimate(flops=2 * flops, bytes_accessed=60_000_000, transcendentals=8 * rows * ffn),
        name=f"mlp_l{layer}",
    )(*flat, hidden, norms, b_o, b_down, b_up, b_peer, *up, *down)


def solution(mesh):
    tp = mesh.shape['tp']
    row_spec = P('dp', 'tp', None)
    cache_spec = P(None, 'dp', None, 'tp', None)
    col_spec = P(None, None, 'tp')
    bias_spec = P(None, 'tp')
    in_specs = (row_spec, P('dp'), P('dp', None, None), P('dp', None, None), cache_spec, cache_spec, P('dp', None), P(), col_spec, bias_spec, col_spec, bias_spec, col_spec, bias_spec, P(None, 'tp', None), P(), col_spec, bias_spec, P(None, 'tp', None), P())
    out_specs = (row_spec, cache_spec, cache_spec, P('dp', None))

    def swap(value, bit):
        return lax.ppermute(value, 'tp', [(n, n ^ bit) for n in range(tp)])

    core_swap = functools.partial(swap, bit=1)
    x_swap = functools.partial(swap, bit=2)
    y_swap = functools.partial(swap, bit=4)

    def added(a, b):
        return (a.astype(F32) + b.astype(F32)).astype(BF16)

    def device_step(tokens, start_pos, cos_tab, sin_tab, key_cache, value_cache, slot_pos, norm_params, w_q, b_q, w_k, b_k, w_v, b_v, w_o, b_o, w_up, b_up, w_down, b_down):
        layers, _, window, _, hd = key_cache.shape
        rows = tokens.shape[1] // CHUNKS
        half = rows // 2
        me = lax.axis_index('tp')
        scal = jnp.stack([me // 2, me % 2, start_pos[0]]).astype(jnp.int32)
        cos, sin = cos_tab[0], sin_tab[0]
        kc = key_cache.reshape(layers, window, hd)
        vc = value_cache.reshape(layers, window, hd)
        b_peer = core_swap(jnp.concatenate([b_q, b_k, b_v, b_up], axis=1))
        caches = (kc, vc, core_swap(kc), core_swap(vc))
        wo = (w_o, core_swap(w_o))
        up = (w_up, core_swap(w_up))
        down = (w_down, core_swap(w_down))
        hidden = tokens[0]
        fresh = []
        for layer in range(layers):
            q, kv = run_qkv(layer, CHUNKS, hidden, norm_params, cos, sin, (w_q, w_k, w_v), (b_q, b_k, b_v), b_peer)
            fresh.append(kv)
            parts = []
            for c in range(CHUNKS):
                own, x1, y1, xb, yt = run_attn(layer, c, scal, q, kv, caches, wo)
                r1x = x_swap(x1)
                r1y = y_swap(y1)
                a2 = x_swap(added(xb, r1y[:half]))
                b1 = y_swap(added(yt, r1x[:half]))
                parts.append((own, r1x, r1y, a2, b1))
            hidden = run_mlp(layer, parts, hidden, norm_params, b_o, b_down, b_up, b_peer, up, down)
        first_slot = start_pos[0] % window

        def place(values):
            rolled = lax.dynamic_slice_in_dim(jnp.concatenate([values, values], axis=0), window - first_slot, window, axis=0)
            return rolled.reshape(1, window, 1, hd)

        key_out = jnp.stack([place(f[0, 0]) for f in fresh])
        value_out = jnp.stack([place(f[1, 0]) for f in fresh])
        pos_out = (start_pos[0] + (jnp.arange(window, dtype=jnp.int32) - first_slot) % window)[None]
        return hidden[None], key_out, value_out, pos_out

    return jax.shard_map(device_step, mesh=mesh, in_specs=in_specs, out_specs=out_specs, check_vma=False)
```

```python
import functools

import jax
import jax.numpy as jnp
from jax import lax
from jax.experimental import pallas as pl
from jax.experimental.pallas import tpu as pltpu
from jax.sharding import PartitionSpec as P

NORM_EPS = 1e-5
LOG2E = 1.4426950408889634
CHUNKS = 4
KEY_TILE = 512
LANES = 128
WIDE = 512
ROW_BLOCK = 16
WEIGHT_SLOTS = 3
ROLL_ROWS = 256
VMEM_LIMIT = 62 * 1024 * 1024
BF16 = jnp.bfloat16
F32 = jnp.float32
MESH = pl.DeviceIdType.MESH

ANY = pl.BlockSpec(memory_space=pl.ANY)
SMEM = pl.BlockSpec(memory_space=pltpu.SMEM)
VMEM = pl.BlockSpec(memory_space=pltpu.VMEM)
DMA = pltpu.SemaphoreType.DMA


def gelu_tanh(x):
    inner = 0.7978845608028654 * (x + 0.044715 * (x * x * x))
    return 0.5 * x * (1.0 + jnp.tanh(inner))


def normalized(values, gain, shift):
    centered = values - jnp.mean(values, axis=-1, keepdims=True)
    variance = jnp.mean(centered * centered, axis=-1, keepdims=True)
    return (centered * lax.rsqrt(variance + NORM_EPS) * gain + shift).astype(BF16)


def rotate(src, dst, shift, first, last):
    window = src.shape[1]

    def tile(n, carry):
        at = pl.multiple_of(n * ROLL_ROWS, ROLL_ROWS)
        want = lax.broadcasted_iota(jnp.int32, (ROLL_ROWS, 1), 0) + (n * ROLL_ROWS + shift)
        want = jnp.where(want >= window, want - window, want)
        pick = jnp.where(lax.broadcasted_iota(jnp.int32, (1, window), 1) == want, 1.0, 0.0).astype(BF16)
        for k in range(2):
            dst[k, pl.ds(at, ROLL_ROWS), :] = jnp.dot(pick, src[k], preferred_element_type=F32).astype(BF16)
        return carry

    lax.fori_loop(first, last, tile, 0)


class Place:
    def __init__(self):
        me = lax.axis_index('tp')
        self.core = lax.rem(me, 2)
        self.xb = lax.rem(lax.div(me, 2), 2)
        self.yb = lax.div(me, 4)
        self.peer = me + 1 - 2 * self.core
        self.x = me + 2 - 4 * self.xb
        self.y = me + 4 - 8 * self.yb

    def member(self, i):
        xb = self.xb + lax.rem(i, 2) * (1 - 2 * self.xb)
        yb = self.yb + lax.div(i, 2) * (1 - 2 * self.yb)
        return yb * 2 + xb

    def barrier(self, others):
        sem = pltpu.get_barrier_semaphore()
        for other in others:
            pl.semaphore_signal(sem, inc=1, device_id={'tp': other}, device_id_type=MESH)
        pl.semaphore_wait(sem, len(others))


def remote(src, dst, send_sem, recv_sem, other):
    return pltpu.make_async_remote_copy(src_ref=src, dst_ref=dst, send_sem=send_sem, recv_sem=recv_sem, device_id={'tp': other}, device_id_type=MESH)


class Gather:
    def __init__(self, place, x_s, send, recv, rows):
        self.place, self.x_s, self.send, self.recv, self.rows = place, x_s, send, recv, rows

    def copy(self, c, kind):
        r, h = self.rows, self.rows // 2
        src, dst, size, other = ((0, r, r, self.place.x), (0, 2 * r, r, self.place.y), (r, 3 * r, h, self.place.y), (2 * r + h, 3 * r + h, h, self.place.x))[kind]
        return remote(self.x_s.at[c, pl.ds(src, size)], self.x_s.at[c, pl.ds(dst, size)], self.send.at[c, kind], self.recv.at[c, kind], other)

    def start(self, c):
        self.copy(c, 0).start()
        self.copy(c, 1).start()

    def forward(self, c):
        self.copy(c, 0).wait_recv()
        self.copy(c, 2).start()
        self.copy(c, 1).wait_recv()
        self.copy(c, 3).start()

    def finish(self, c):
        self.copy(c, 2).wait_recv()
        self.copy(c, 3).wait_recv()

    def drain(self, c):
        for kind in range(4):
            self.copy(c, kind).wait_send()


class Scatter:
    def __init__(self, place, out_s, land_s, send, recv, rows):
        self.place, self.out_s, self.land_s, self.send, self.recv, self.rows = place, out_s, land_s, send, recv, rows

    def copy(self, c, kind):
        r, h = self.rows, self.rows // 2
        x, y = self.place.x, self.place.y
        src, dst, other = ((3 * r, 2 * r, x), (3 * r + h, 2 * r + h, y), (r, 0, x), (2 * r + h, r + h, y), (r + h, h, x), (2 * r, r, y))[kind]
        return remote(self.out_s.at[c, pl.ds(src, h)], self.land_s.at[c, pl.ds(dst, h)], self.send.at[c, kind], self.recv.at[c, kind], other)

    def start(self, c):
        for kind in range(4):
            self.copy(c, kind).start()

    def add(self, c, kind, src, dst):
        self.copy(c, kind).wait_recv()

        def block(n, carry):
            at = pl.multiple_of(n * ROW_BLOCK, ROW_BLOCK)
            mine = self.out_s[c, pl.ds(dst + at, ROW_BLOCK), :].astype(F32)
            came = self.land_s[c, pl.ds(src + at, ROW_BLOCK), :].astype(F32)
            self.out_s[c, pl.ds(dst + at, ROW_BLOCK), :] = (mine + came).astype(BF16)
            return carry

        lax.fori_loop(0, self.rows // 2 // ROW_BLOCK, block, 0)

    def relay(self, c):
        r, h = self.rows, self.rows // 2
        self.add(c, 0, 2 * r, 2 * r)
        self.copy(c, 5).start()
        self.add(c, 1, 2 * r + h, r + h)
        self.copy(c, 4).start()

    def finish(self, c):
        for kind in range(2, 6):
            self.copy(c, kind).wait_recv()

    def close(self, mid_s, bias, out, o_sem, chunks, first_open):
        rows = self.rows

        def o_copy(c):
            return pltpu.make_async_copy(mid_s.at[c], out.at[pl.ds(pl.multiple_of(c * rows, rows), rows)], o_sem.at[c])

        def one(c, carry):
            @pl.when(c + first_open < chunks)
            def _():
                self.relay(c + first_open)

            self.finish(c)

            def block(n, inner):
                at = pl.multiple_of(n * ROW_BLOCK, ROW_BLOCK)
                total = self.out_s[c, pl.ds(at, ROW_BLOCK), :].astype(F32) + self.land_s[c, pl.ds(at, ROW_BLOCK), :].astype(F32) + self.land_s[c, pl.ds(rows + at, ROW_BLOCK), :].astype(F32)
                mid_s[c, pl.ds(at, ROW_BLOCK), :] = (mid_s[c, pl.ds(at, ROW_BLOCK), :].astype(F32) + total + bias).astype(BF16)
                return inner

            lax.fori_loop(0, rows // ROW_BLOCK, block, 0)
            o_copy(c).start()
            return carry

        lax.fori_loop(0, chunks, one, 0)

        def settle(c, carry):
            o_copy(c).wait()
            for kind in range(6):
                self.copy(c, kind).wait_send()
            return carry

        lax.fori_loop(0, chunks, settle, 0)


def qkv_kernel(layer, dims, scal, *refs):
    chunks, rows, model, hd, window = dims
    hidden, norms, cos, sin, wq, wk, wv, biases, b_all = refs[:9]
    pushed = refs[9:14]
    q_out, kv_mine, kv_other, cache_mine, cache_peer, wo_peer, up_peer, down_peer = refs[14:22]
    x_s, h_s, t_s, w_s, b_s, bp_s, oq_s, okv_s, raw_s, old_s, ag_send, ag_recv, h_sem, t_sem, w_sem, wr_send, wr_recv, p_send, p_recv, q_sem, kv_sem, kr_send, kr_recv, raw_sem, old_sem = refs[22:]
    place = Place()
    block = rows * chunks
    place.barrier((place.x, place.y, place.peer))
    gather = Gather(place, x_s, ag_send, ag_recv, rows)
    loads = [pltpu.make_async_copy(hidden.at[pl.ds(c * rows, rows)], h_s.at[c], h_sem.at[c]) for c in range(chunks)]
    for copy in loads:
        copy.start()
    for k in range(2):
        pltpu.make_async_copy(pushed[k].at[layer], raw_s.at[k], raw_sem).start()
    places = ((wq.at[layer], 0, 0, 2 * hd), (wk.at[layer], 1, 0, hd), (wv.at[layer], 1, hd, hd))
    w_local = [pltpu.make_async_copy(src, w_s.at[t, :, pl.ds(at, n)], w_sem.at[k]) for k, (src, t, at, n) in enumerate(places)]
    w_remote = [remote(src, w_s.at[2 + t, :, pl.ds(at, n)], wr_send.at[k], wr_recv.at[k], place.peer) for k, (src, t, at, n) in enumerate(places)]
    w_remote.append(remote(b_all, bp_s, wr_send.at[3], wr_recv.at[3], place.peer))
    landing = (wo_peer, up_peer, down_peer)
    pushes = [remote(src.at[layer], dst, p_send.at[k], p_recv.at[k], place.peer) for k, (src, dst) in enumerate(zip(pushed[2:], landing))]
    old_push = remote(old_s, cache_peer, p_send.at[3], p_recv.at[3], place.peer)
    old_store = pltpu.make_async_copy(old_s, cache_mine, old_sem)
    gain = norms[layer, 0:1, :].astype(F32)
    shift = norms[layer, 1:2, :].astype(F32)

    def send_own(c):
        loads[c].wait()

        def norm_block(n, carry):
            at = pl.multiple_of(n * ROW_BLOCK, ROW_BLOCK)
            x_s[c, pl.ds(at, ROW_BLOCK), :] = normalized(h_s[c, pl.ds(at, ROW_BLOCK), :].astype(F32), gain, shift)
            return carry

        lax.fori_loop(0, rows // ROW_BLOCK, norm_block, 0)
        gather.start(c)

    def chunk_pos(c, i):
        return pl.multiple_of((place.member(i) * 2 + place.core) * block + c * rows, rows)

    def table_copies(c):
        return [pltpu.make_async_copy(tab.at[pl.ds(chunk_pos(c, i), rows)], t_s.at[c, k, pl.ds(i * rows, rows)], t_sem.at[c]) for i in range(4) for k, tab in enumerate((cos, sin))]

    send_own(0)
    send_own(1)
    for copy in w_remote + w_local + pushes:
        copy.start()
    for c in range(chunks):
        for copy in table_copies(c):
            copy.start()
    b_s[0] = biases[layer:layer + 1, 0:2 * hd].astype(F32)
    b_s[1] = biases[layer:layer + 1, 2 * hd:4 * hd].astype(F32)
    pltpu.make_async_copy(raw_s, raw_s, raw_sem).wait()
    first_slot = lax.rem(scal[0], window)
    roll_tiles = window // ROLL_ROWS
    rotate(raw_s, old_s, first_slot, 0, roll_tiles // 3)
    gather.forward(0)
    send_own(2)
    rotate(raw_s, old_s, first_slot, roll_tiles // 3, roll_tiles)
    old_push.start()
    old_store.start()
    gather.forward(1)
    send_own(3)
    w_remote[3].wait_recv()
    b_s[2] = bp_s[layer:layer + 1, 0:2 * hd].astype(F32)
    b_s[3] = bp_s[layer:layer + 1, 2 * hd:4 * hd].astype(F32)

    def rope(u, c):
        turned = jnp.concatenate([-u[:, hd // 2:], u[:, :hd // 2]], axis=1)
        return (u * t_s[c, 0] + turned * t_s[c, 1]).astype(BF16).reshape(4, rows, hd)

    def q_copy(c):
        return pltpu.make_async_copy(oq_s.at[c], q_out.at[c], q_sem.at[c])

    def kv_copies(c):
        planes = (kv_mine, kv_other)
        near = [pltpu.make_async_copy(okv_s.at[c, :, g, i], planes[g].at[:, pl.ds(chunk_pos(c, i), rows)], kv_sem.at[c]) for g in range(2) for i in range(4)]
        far = [remote(okv_s.at[c, :, g, i], planes[1 - g].at[:, pl.ds(chunk_pos(c, i), rows)], kr_send.at[c], kr_recv.at[c], place.peer) for g in range(2) for i in range(4)]
        return near, far

    def chunk(c, carry):
        pltpu.make_async_copy(t_s.at[c], t_s.at[c], t_sem.at[c]).wait()
        gather.finish(c)
        for g in range(2):
            @pl.when(c == 0)
            def _():
                for copy in ((w_local[0],) if g == 0 else ()):
                    copy.wait()
                if g == 1:
                    w_remote[0].wait_recv()

            u = jnp.dot(x_s[c], w_s[2 * g], preferred_element_type=F32) + b_s[2 * g]
            for h in range(2):
                oq_s[c, g, :, h] = rope(u[:, h * hd:(h + 1) * hd], c)

            @pl.when(c == 0)
            def _():
                for copy in (w_local[1:] if g == 0 else ()):
                    copy.wait()
                if g == 1:
                    for copy in w_remote[1:3]:
                        copy.wait_recv()

            u = jnp.dot(x_s[c], w_s[2 * g + 1], preferred_element_type=F32) + b_s[2 * g + 1]
            okv_s[c, 0, g] = rope(u[:, :hd], c)
            okv_s[c, 1, g] = u[:, hd:].astype(BF16).reshape(4, rows, hd)
        q_copy(c).start()
        near, far = kv_copies(c)
        for copy in near + far:
            copy.start()

        @pl.when(c + 2 < chunks)
        def _():
            gather.forward(c + 2)

        return carry

    lax.fori_loop(0, chunks, chunk, 0)
    for copy in w_remote:
        copy.wait_send()

    def settle(c, carry):
        q_copy(c).wait()
        whole = okv_s.at[c]
        pltpu.make_async_copy(whole, whole, kv_sem.at[c]).wait()
        remote(whole, whole, kr_send.at[c], kr_recv.at[c], place.peer).wait_send()
        remote(whole, whole, kr_send.at[c], kr_recv.at[c], place.peer).wait_recv()
        gather.drain(c)
        return carry

    lax.fori_loop(0, chunks, settle, 0)
    for copy in pushes + [old_push]:
        copy.wait_send()
        copy.wait_recv()
    old_store.wait()


def run_qkv(layer, chunks, scal, hidden, norms, cos, sin, weights, b_all, pushed):
    model = hidden.shape[1]
    rows = hidden.shape[0] // chunks
    hd = cos.shape[1]
    window = cos.shape[0]
    dims = (chunks, rows, model, hd, window)
    flops = 2 * 4 * rows * chunks * model * 8 * hd
    shapes = [(chunks, 2, 4, 2, rows, hd)] + [(2, window, hd)] * 4 + [p.shape[1:] for p in pushed[2:]]
    return pl.pallas_call(
        functools.partial(qkv_kernel, layer, dims),
        out_shape=tuple(jax.ShapeDtypeStruct(s, BF16) for s in shapes),
        in_specs=[SMEM, ANY, VMEM] + [ANY] * 5 + [VMEM] + [ANY] * 6,
        out_specs=(ANY,) * len(shapes),
        scratch_shapes=[
            pltpu.VMEM((chunks, 4 * rows, model), BF16),
            pltpu.VMEM((chunks, rows, model), BF16),
            pltpu.VMEM((chunks, 2, 4 * rows, hd), F32),
            pltpu.VMEM((4, model, 2 * hd), BF16),
            pltpu.VMEM((4, 1, 2 * hd), F32),
            pltpu.VMEM(b_all.shape, BF16),
            pltpu.VMEM((chunks, 2, 4, 2, rows, hd), BF16),
            pltpu.VMEM((chunks, 2, 2, 4, rows, hd), BF16),
            pltpu.VMEM((2, window, hd), BF16),
            pltpu.VMEM((2, window, hd), BF16),
            DMA((chunks, 4)),
            DMA((chunks, 4)),
            DMA((chunks,)),
            DMA((chunks,)),
            DMA((3,)),
            DMA((4,)),
            DMA((4,)),
            DMA((4,)),
            DMA((4,)),
            DMA((chunks,)),
            DMA((chunks,)),
            DMA((chunks,)),
            DMA((chunks,)),
            DMA,
            DMA,
        ],
        compiler_params=pltpu.CompilerParams(vmem_limit_bytes=VMEM_LIMIT, collective_id=3 * layer, has_side_effects=True),
        cost_estimate=pl.CostEstimate(flops=4 * flops, bytes_accessed=20_000_000, transcendentals=0),
        name=f"qkv_l{layer}",
    )(scal, hidden, norms, cos, sin, *weights, b_all, b_all, *pushed)


def attn_kernel(layer, dims, scal, *refs):
    chunks, rows, model, hd, window = dims
    q, kv_mine, kv_other, cache_mine, cache_peer, wo, wo_peer, hidden, b_o = refs[:9]
    mid_out, kv_rolled = refs[9:11]
    kv_s, q_s, s_s, mix_s, wo_s, out_s, land_s, mid_s, m_s, l_s, acc_s, rs_send, rs_recv, kv_sem, q_sem, w_sem, h_sem, o_sem, f_sem = refs[11:]
    place = Place()
    start_pos = scal[0]
    block = rows * chunks
    tall = 2 * rows
    tile = KEY_TILE
    tiles = window // tile
    scale = LOG2E * hd ** -0.5
    place.barrier((place.x, place.y))
    scatter = Scatter(place, out_s, land_s, rs_send, rs_recv, rows)
    q_load = pltpu.make_async_copy(q, q_s, q_sem)
    q_load.start()
    pltpu.make_async_copy(kv_mine, kv_s.at[0, pl.ds(2, 2)], kv_sem).start()
    pltpu.make_async_copy(kv_other, kv_s.at[1, pl.ds(2, 2)], kv_sem).start()
    pltpu.make_async_copy(cache_mine, kv_s.at[0, pl.ds(0, 2)], kv_sem).start()
    pltpu.make_async_copy(cache_peer, kv_s.at[1, pl.ds(0, 2)], kv_sem).start()
    pltpu.make_async_copy(wo.at[layer], wo_s.at[pl.ds(0, 2 * hd)], w_sem).start()
    pltpu.make_async_copy(wo_peer, wo_s.at[pl.ds(2 * hd, 2 * hd)], w_sem).start()
    for c in range(chunks):
        pltpu.make_async_copy(hidden.at[pl.ds(c * rows, rows)], mid_s.at[c], h_sem).start()
    q_load.wait()
    pltpu.make_async_copy(kv_s, kv_s, kv_sem).wait()
    first_slot = lax.rem(start_pos, window)
    floor = window - 1 - start_pos

    def first_row(c, i):
        return (place.member(i) * 2 + place.core) * block + c * rows

    def tile_at(diag, n):
        is_new = jnp.logical_or(n == 0, jnp.logical_and(n >= 2, n - 2 < diag))
        t = jnp.where(n < 2, diag, jnp.where(is_new, n - 2, n - 1))
        return jnp.where(is_new, 2, 0), pl.multiple_of(t * tile, tile), is_new

    def scores(c, i, g, which, at):
        return lax.dot_general(q_s[c, g, i].reshape(tall, hd), kv_s[g, which, pl.ds(at, tile), :], (((1,), (1,)), ((), ())), preferred_element_type=F32)

    for g in range(2):
        s_s[g] = scores(0, 0, g, 2, pl.multiple_of(lax.div(first_row(0, 0), tile) * tile, tile))

    def attend(c, i):
        j0 = first_row(c, i)
        diag = lax.div(j0, tile)
        count = tiles + 1
        end = i == 3
        c_next = jnp.minimum(jnp.where(end, c + 1, c), chunks - 1)
        i_next = jnp.where(end, 0, i + 1)
        next_at = lax.div(first_row(c_next, i_next), tile) * tile
        m_s[...] = jnp.full_like(m_s, -jnp.inf)
        l_s[...] = jnp.zeros_like(l_s)
        acc_s[...] = jnp.zeros_like(acc_s)

        def step(n):
            if isinstance(n, int):
                which, at = (2, 0)[n], pl.multiple_of(diag * tile, tile)
                nw, nat, _ = (0, at, None) if n == 0 else tile_at(diag, 2)
                nc, ni = c, i
                col = lax.broadcasted_iota(jnp.int32, (1, tile), 1) + at
                row = lax.rem(lax.broadcasted_iota(jnp.int32, (tall, 1), 0), rows) + j0
                mask = col <= row if n == 0 else col > jnp.maximum(row, floor)
            else:
                which, at, is_new = tile_at(diag, n)
                last = n + 1 == count
                nw, nat, _ = tile_at(diag, n + 1)
                nw = jnp.where(last, 2, nw)
                nat = pl.multiple_of(jnp.where(last, next_at, nat), tile)
                nc = jnp.where(last, c_next, c)
                ni = jnp.where(last, i_next, i)
                col = lax.broadcasted_iota(jnp.int32, (1, tile), 1) + at
                mask = col > jnp.where(is_new, -1, floor)
            for g in range(2):
                s = jnp.where(mask, s_s[g] * scale, -jnp.inf)
                s_next = scores(nc, ni, g, nw, nat)
                m_prev = m_s[g]
                m_next = jnp.maximum(m_prev, jnp.max(s, axis=1, keepdims=True))
                e = jnp.exp2(s - jnp.concatenate([m_next] * (tile // LANES), axis=1))
                alpha = jnp.exp2(m_prev - m_next)
                total = l_s[g] * alpha
                for k in range(tile // LANES):
                    total = total + e[:, k * LANES:(k + 1) * LANES]
                l_s[g] = total
                m_s[g] = m_next
                mixed = jnp.dot(e.astype(BF16), kv_s[g, which + 1, pl.ds(at, tile), :], preferred_element_type=F32)
                acc_s[g] = acc_s[g] * jnp.concatenate([alpha] * (hd // LANES), axis=1) + mixed
                s_s[g] = s_next

        step(0)
        step(1)
        lax.fori_loop(2, count, lambda n, x: (step(n), x)[1], 0)
        at = pl.multiple_of(i * rows, rows)
        for g in range(2):
            total = jnp.sum(l_s[g], axis=1, keepdims=True)
            out = (acc_s[g] / total).astype(BF16)
            for h in range(2):
                mix_s[pl.ds(at, rows), (2 * g + h) * hd:(2 * g + h + 1) * hd] = out[h * rows:(h + 1) * rows]

    def chunk(c, carry):
        def one(i, inner):
            attend(c, i)

            @pl.when(jnp.logical_and(i == 2, c >= 1))
            def _():
                scatter.relay(c - 1)

            return inner

        lax.fori_loop(0, 4, one, 0)

        @pl.when(c == 0)
        def _():
            pltpu.make_async_copy(wo_s, wo_s, w_sem).wait()

        def project(n, inner):
            at = pl.multiple_of(n * WIDE, WIDE)
            out_s[c, :, pl.ds(at, WIDE)] = jnp.dot(mix_s[...], wo_s[:, pl.ds(at, WIDE)], preferred_element_type=F32).astype(BF16)
            return inner

        lax.fori_loop(0, model // WIDE, project, 0)
        scatter.start(c)
        return carry

    lax.fori_loop(0, chunks, chunk, 0)
    pltpu.make_async_copy(mid_s, mid_s, h_sem).wait()
    rolled = kv_s.at[1, pl.ds(0, 2)]
    rotate(kv_s.at[0, pl.ds(2, 2)], rolled, window - first_slot, 0, window // ROLL_ROWS)
    roll_store = pltpu.make_async_copy(rolled, kv_rolled, f_sem)
    roll_store.start()
    scatter.close(mid_s, b_o[layer:layer + 1, :].astype(F32), mid_out, o_sem, chunks, chunks - 1)
    roll_store.wait()


def run_attn(layer, scal, q, kv_mine, kv_other, cache_mine, cache_peer, wo, wo_peer, hidden, b_o):
    chunks, rows, hd = q.shape[0], q.shape[-2], q.shape[-1]
    model = hidden.shape[1]
    window = kv_mine.shape[1]
    dims = (chunks, rows, model, hd, window)
    flops = 4 * 4 * rows * chunks * 4 * window * hd + 2 * 4 * rows * chunks * 4 * hd * model
    return pl.pallas_call(
        functools.partial(attn_kernel, layer, dims),
        out_shape=(jax.ShapeDtypeStruct(hidden.shape, BF16), jax.ShapeDtypeStruct((2, window, hd), BF16)),
        in_specs=[SMEM] + [ANY] * 8 + [VMEM],
        out_specs=(ANY, ANY),
        scratch_shapes=[
            pltpu.VMEM((2, 4, window, hd), BF16),
            pltpu.VMEM((chunks, 2, 4, 2, rows, hd), BF16),
            pltpu.VMEM((2, 2 * rows, KEY_TILE), F32),
            pltpu.VMEM((4 * rows, 4 * hd), BF16),
            pltpu.VMEM((4 * hd, model), BF16),
            pltpu.VMEM((chunks, 4 * rows, model), BF16),
            pltpu.VMEM((chunks, 3 * rows, model), BF16),
            pltpu.VMEM((chunks, rows, model), BF16),
            pltpu.VMEM((2, 2 * rows, LANES), F32),
            pltpu.VMEM((2, 2 * rows, LANES), F32),
            pltpu.VMEM((2, 2 * rows, hd), F32),
            DMA((chunks, 6)),
            DMA((chunks, 6)),
            DMA,
            DMA,
            DMA,
            DMA,
            DMA((chunks,)),
            DMA,
        ],
        compiler_params=pltpu.CompilerParams(vmem_limit_bytes=VMEM_LIMIT, collective_id=3 * layer + 1, has_side_effects=True),
        cost_estimate=pl.CostEstimate(flops=flops, bytes_accessed=30_000_000, transcendentals=16 * rows * chunks * window),
        name=f"attn_l{layer}",
    )(scal, q, kv_mine, kv_other, cache_mine, cache_peer, wo, wo_peer, hidden, b_o)


def mlp_kernel(layer, dims, bias_at, *refs):
    chunks, rows, model, ffn = dims
    middle, norms, b_down, biases, b_all, up, down, up_peer, down_peer = refs[:9]
    h_out = refs[9]
    x_s, out_s, land_s, act_s, w_s, mid_s, b_s, bp_s, ag_send, ag_recv, rs_send, rs_recv, m_sem, w_sem, b_send, b_recv, h_sem = refs[10:]
    place = Place()
    n_up = 2 * ffn // WIDE
    n_tiles = n_up + model // WIDE
    sub = WIDE // 2
    n_sub = ffn // sub
    ups = (up.at[layer], up_peer)
    downs = (down.at[layer], down_peer)
    loads = [pltpu.make_async_copy(middle.at[pl.ds(c * rows, rows)], mid_s.at[c], m_sem.at[c]) for c in range(chunks)]
    for copy in loads:
        copy.start()
    place.barrier((place.x, place.y, place.peer))
    gather = Gather(place, x_s, ag_send, ag_recv, rows)
    scatter = Scatter(place, out_s, land_s, rs_send, rs_recv, rows)
    gain = norms[layer, 2:3, :].astype(F32)
    shift = norms[layer, 3:4, :].astype(F32)

    def fetch(c, k):
        over = k >= n_tiles
        k = jnp.where(over, k - n_tiles, k)
        c = jnp.where(over, c + 1, c)
        slot = lax.rem(c * n_tiles + k, WEIGHT_SLOTS)

        @pl.when(c < chunks)
        def _():
            for part in range(2):
                n = 2 * k + part
                for side in range(2):
                    @pl.when(jnp.logical_and(n >= side * n_sub, n < (side + 1) * n_sub))
                    def _():
                        at = pl.multiple_of((n - side * n_sub) * sub, sub)
                        pltpu.make_async_copy(ups[side].at[:, pl.ds(at, sub)], w_s.at[slot, :, pl.ds(part * sub, sub)], w_sem.at[slot]).start()

            @pl.when(k >= n_up)
            def _():
                at = pl.multiple_of((k - n_up) * WIDE, WIDE)
                for side in range(2):
                    pltpu.make_async_copy(downs[side].at[:, pl.ds(at, WIDE)], w_s.at[slot, pl.ds(side * ffn, ffn)], w_sem.at[slot]).start()

    def landed(c, k):
        slot = lax.rem(c * n_tiles + k, WEIGHT_SLOTS)
        pltpu.make_async_copy(w_s.at[slot], w_s.at[slot], w_sem.at[slot]).wait()
        fetch(c, k + WEIGHT_SLOTS - 1)
        return slot

    def send_own(c):
        loads[c].wait()

        def norm_block(n, carry):
            at = pl.multiple_of(n * ROW_BLOCK, ROW_BLOCK)
            x_s[c, pl.ds(at, ROW_BLOCK), :] = normalized(mid_s[c, pl.ds(at, ROW_BLOCK), :].astype(F32), gain, shift)
            return carry

        lax.fori_loop(0, rows // ROW_BLOCK, norm_block, 0)
        gather.start(c)

    send_own(0)
    send_own(1)
    b_push = remote(b_all, bp_s, b_send, b_recv, place.peer)
    b_push.start()
    for k in range(WEIGHT_SLOTS - 1):
        fetch(jnp.int32(0), jnp.int32(k))
    gather.forward(0)
    send_own(2)
    gather.forward(1)
    send_own(3)
    b_push.wait_recv()
    for n in range(2 * n_sub):
        src = biases if n < n_sub else bp_s
        at = bias_at + (n % n_sub) * sub
        b_s[n // 2, :, (n % 2) * sub:(n % 2 + 1) * sub] = src[layer:layer + 1, at:at + sub].astype(F32)

    def chunk(c, carry):
        gather.finish(c)

        def up_step(k, inner):
            slot = landed(c, k)
            at = pl.multiple_of(k * WIDE, WIDE)
            for top in range(2):
                r0 = top * 2 * rows
                lifted = jnp.dot(x_s[c, r0:r0 + 2 * rows, :], w_s[slot], preferred_element_type=F32) + b_s[k]
                act_s[r0:r0 + 2 * rows, pl.ds(at, WIDE)] = gelu_tanh(lifted).astype(BF16)
            return inner

        lax.fori_loop(0, n_up, up_step, 0)

        @pl.when(c + 2 < chunks)
        def _():
            gather.forward(c + 2)

        @pl.when(c >= 2)
        def _():
            scatter.relay(c - 2)

        def down_step(k, inner):
            slot = landed(c, k)
            at = pl.multiple_of((k - n_up) * WIDE, WIDE)
            out_s[c, :, pl.ds(at, WIDE)] = jnp.dot(act_s[...], w_s[slot], preferred_element_type=F32).astype(BF16)
            return inner

        lax.fori_loop(n_up, n_tiles, down_step, 0)
        scatter.start(c)
        return carry

    lax.fori_loop(0, chunks, chunk, 0)
    scatter.close(mid_s, b_down[layer:layer + 1, :].astype(F32), h_out, h_sem, chunks, chunks - 2)
    for c in range(chunks):
        gather.drain(c)
    b_push.wait_send()


def run_mlp(layer, chunks, middle, norms, b_down, b_all, up, down, up_peer, down_peer):
    model = middle.shape[1]
    rows = middle.shape[0] // chunks
    ffn = up.shape[2]
    dims = (chunks, rows, model, ffn)
    flops = 2 * 4 * rows * chunks * model * ffn * 4
    return pl.pallas_call(
        functools.partial(mlp_kernel, layer, dims, b_all.shape[1] - ffn),
        out_shape=jax.ShapeDtypeStruct(middle.shape, BF16),
        in_specs=[ANY] + [VMEM] * 3 + [ANY] * 5,
        out_specs=ANY,
        scratch_shapes=[
            pltpu.VMEM((chunks, 4 * rows, model), BF16),
            pltpu.VMEM((chunks, 4 * rows, model), BF16),
            pltpu.VMEM((chunks, 3 * rows, model), BF16),
            pltpu.VMEM((4 * rows, 2 * ffn), BF16),
            pltpu.VMEM((WEIGHT_SLOTS, model, WIDE), BF16),
            pltpu.VMEM((chunks, rows, model), BF16),
            pltpu.VMEM((2 * ffn // WIDE, 1, WIDE), F32),
            pltpu.VMEM(b_all.shape, BF16),
            DMA((chunks, 4)),
            DMA((chunks, 4)),
            DMA((chunks, 6)),
            DMA((chunks, 6)),
            DMA((chunks,)),
            DMA((WEIGHT_SLOTS,)),
            DMA,
            DMA,
            DMA((chunks,)),
        ],
        compiler_params=pltpu.CompilerParams(vmem_limit_bytes=VMEM_LIMIT, collective_id=3 * layer + 2, has_side_effects=True),
        cost_estimate=pl.CostEstimate(flops=2 * flops, bytes_accessed=60_000_000, transcendentals=8 * rows * ffn),
        name=f"mlp_l{layer}",
    )(middle, norms, b_down, b_all, b_all, up, down, up_peer, down_peer)


def solution(mesh):
    row_spec = P('dp', 'tp', None)
    cache_spec = P(None, 'dp', None, 'tp', None)
    col_spec = P(None, None, 'tp')
    bias_spec = P(None, 'tp')
    in_specs = (row_spec, P('dp'), P('dp', None, None), P('dp', None, None), cache_spec, cache_spec, P('dp', None), P(), col_spec, bias_spec, col_spec, bias_spec, col_spec, bias_spec, P(None, 'tp', None), P(), col_spec, bias_spec, P(None, 'tp', None), P())
    out_specs = (row_spec, cache_spec, cache_spec, P('dp', None))

    def device_step(tokens, start_pos, cos_tab, sin_tab, key_cache, value_cache, slot_pos, norm_params, w_q, b_q, w_k, b_k, w_v, b_v, w_o, b_o, w_up, b_up, w_down, b_down):
        layers, _, window, _, hd = key_cache.shape
        cos, sin = cos_tab[0], sin_tab[0]
        kc = key_cache.reshape(layers, window, hd)
        vc = value_cache.reshape(layers, window, hd)
        b_all = jnp.concatenate([b_q, b_k, b_v, b_up], axis=1)
        hidden = tokens[0]
        fresh = []
        for layer in range(layers):
            q, kv_mine, kv_other, cache_mine, cache_peer, wo_peer, up_peer, down_peer = run_qkv(layer, CHUNKS, start_pos, hidden, norm_params, cos, sin, (w_q, w_k, w_v), b_all, (kc, vc, w_o, w_up, w_down))
            middle, kv_rolled = run_attn(layer, start_pos, q, kv_mine, kv_other, cache_mine, cache_peer, w_o, wo_peer, hidden, b_o)
            hidden = run_mlp(layer, CHUNKS, middle, norm_params, b_down, b_all, w_up, w_down, up_peer, down_peer)
            fresh.append(kv_rolled)
        key_out = jnp.stack([f[0] for f in fresh]).reshape(key_cache.shape)
        value_out = jnp.stack([f[1] for f in fresh]).reshape(value_cache.shape)
        first_slot = start_pos[0] % window
        pos_out = (start_pos[0] + (jnp.arange(window, dtype=jnp.int32) - first_slot) % window)[None]
        return hidden[None], key_out, value_out, pos_out

    return jax.shard_map(device_step, mesh=mesh, in_specs=in_specs, out_specs=out_specs, check_vma=False)
```

```python
import functools

import jax
import jax.numpy as jnp
from jax import lax
from jax.experimental import pallas as pl
from jax.experimental.pallas import tpu as pltpu
from jax.sharding import PartitionSpec as P

NORM_EPS = 1e-5
LOG2E = 1.4426950408889634
CHUNKS = 4
KEY_TILE = 512
LANES = 128
WIDE = 512
ROW_BLOCK = 16
WEIGHT_SLOTS = 3
ROLL_ROWS = 256
EARLY = 2
LOWEST = -3.3e38
VMEM_LIMIT = 62 * 1024 * 1024
BF16 = jnp.bfloat16
F32 = jnp.float32
MESH = pl.DeviceIdType.MESH

ANY = pl.BlockSpec(memory_space=pl.ANY)
SMEM = pl.BlockSpec(memory_space=pltpu.SMEM)
VMEM = pl.BlockSpec(memory_space=pltpu.VMEM)
DMA = pltpu.SemaphoreType.DMA


def gelu_tanh(x):
    inner = 0.7978845608028654 * (x + 0.044715 * (x * x * x))
    return 0.5 * x * (1.0 + jnp.tanh(inner))


def normalized(values, gain, shift):
    centered = values - jnp.mean(values, axis=-1, keepdims=True)
    variance = jnp.mean(centered * centered, axis=-1, keepdims=True)
    return (centered * lax.rsqrt(variance + NORM_EPS) * gain + shift).astype(BF16)


def rotate(planes, dst, window, shift, first, last):
    def tile(n, carry):
        at = pl.multiple_of(n * ROLL_ROWS, ROLL_ROWS)
        want = lax.broadcasted_iota(jnp.int32, (ROLL_ROWS, 1), 0) + (n * ROLL_ROWS + shift)
        want = jnp.where(want >= window, want - window, want)
        pick = jnp.where(lax.broadcasted_iota(jnp.int32, (1, window), 1) == want, 1.0, 0.0).astype(BF16)
        for k in range(2):
            dst[k, pl.ds(at, ROLL_ROWS), :] = jnp.dot(pick, planes(k), preferred_element_type=F32).astype(BF16)
        return carry

    lax.fori_loop(first, last, tile, 0)


def reset_state(st_s, w):
    for g in range(2):
        st_s[w, g, :, 0:LANES] = jnp.full((st_s.shape[2], LANES), LOWEST, F32)
        st_s[w, g, :, LANES:] = jnp.zeros((st_s.shape[2], st_s.shape[3] - LANES), F32)


def flash_step(st_s, w, s_s, scale, mask, values, next_scores):
    for g in range(2):
        s = jnp.where(mask, s_s[g] * scale, -jnp.inf)
        s_next = next_scores(g)
        m_prev = st_s[w, g, :, 0:LANES]
        m_next = jnp.maximum(m_prev, jnp.max(s, axis=1, keepdims=True))
        e = jnp.exp2(s - jnp.concatenate([m_next] * (s.shape[1] // LANES), axis=1))
        alpha = jnp.exp2(m_prev - m_next)
        total = st_s[w, g, :, LANES:2 * LANES] * alpha
        for k in range(s.shape[1] // LANES):
            total = total + e[:, k * LANES:(k + 1) * LANES]
        st_s[w, g, :, LANES:2 * LANES] = total
        st_s[w, g, :, 0:LANES] = m_next
        mixed = jnp.dot(e.astype(BF16), values(g), preferred_element_type=F32)
        st_s[w, g, :, 2 * LANES:] = st_s[w, g, :, 2 * LANES:] * jnp.concatenate([alpha] * (mixed.shape[1] // LANES), axis=1) + mixed
        s_s[g] = s_next


def score_tile(queries, keys):
    return lax.dot_general(queries, keys, (((1,), (1,)), ((), ())), preferred_element_type=F32)


class Place:
    def __init__(self):
        me = lax.axis_index('tp')
        self.core = lax.rem(me, 2)
        self.xb = lax.rem(lax.div(me, 2), 2)
        self.yb = lax.div(me, 4)
        self.peer = me + 1 - 2 * self.core
        self.x = me + 2 - 4 * self.xb
        self.y = me + 4 - 8 * self.yb

    def member(self, i):
        xb = self.xb + lax.rem(i, 2) * (1 - 2 * self.xb)
        yb = self.yb + lax.div(i, 2) * (1 - 2 * self.yb)
        return yb * 2 + xb

    def barrier(self, others):
        sem = pltpu.get_barrier_semaphore()
        for other in others:
            pl.semaphore_signal(sem, inc=1, device_id={'tp': other}, device_id_type=MESH)
        pl.semaphore_wait(sem, len(others))


def remote(src, dst, send_sem, recv_sem, other):
    return pltpu.make_async_remote_copy(src_ref=src, dst_ref=dst, send_sem=send_sem, recv_sem=recv_sem, device_id={'tp': other}, device_id_type=MESH)


class Gather:
    def __init__(self, place, x_s, send, recv, rows):
        self.place, self.x_s, self.send, self.recv, self.rows = place, x_s, send, recv, rows

    def copy(self, c, kind):
        r, h = self.rows, self.rows // 2
        src, dst, size, other = ((0, r, r, self.place.x), (0, 2 * r, r, self.place.y), (r, 3 * r, h, self.place.y), (2 * r + h, 3 * r + h, h, self.place.x))[kind]
        return remote(self.x_s.at[c, pl.ds(src, size)], self.x_s.at[c, pl.ds(dst, size)], self.send.at[c, kind], self.recv.at[c, kind], other)

    def start(self, c):
        self.copy(c, 0).start()
        self.copy(c, 1).start()

    def forward(self, c):
        self.copy(c, 0).wait_recv()
        self.copy(c, 2).start()
        self.copy(c, 1).wait_recv()
        self.copy(c, 3).start()

    def finish(self, c):
        self.copy(c, 2).wait_recv()
        self.copy(c, 3).wait_recv()

    def drain(self, c):
        for kind in range(4):
            self.copy(c, kind).wait_send()


class Scatter:
    def __init__(self, place, out_s, land_s, send, recv, rows):
        self.place, self.out_s, self.land_s, self.send, self.recv, self.rows = place, out_s, land_s, send, recv, rows

    def copy(self, c, kind):
        r, h = self.rows, self.rows // 2
        x, y = self.place.x, self.place.y
        src, dst, other = ((3 * r, 2 * r, x), (3 * r + h, 2 * r + h, y), (r, 0, x), (2 * r + h, r + h, y), (r + h, h, x), (2 * r, r, y))[kind]
        return remote(self.out_s.at[c, pl.ds(src, h)], self.land_s.at[c, pl.ds(dst, h)], self.send.at[c, kind], self.recv.at[c, kind], other)

    def start(self, c):
        for kind in range(4):
            self.copy(c, kind).start()

    def add(self, c, kind, src, dst):
        self.copy(c, kind).wait_recv()

        def block(n, carry):
            at = pl.multiple_of(n * ROW_BLOCK, ROW_BLOCK)
            mine = self.out_s[c, pl.ds(dst + at, ROW_BLOCK), :].astype(F32)
            came = self.land_s[c, pl.ds(src + at, ROW_BLOCK), :].astype(F32)
            self.out_s[c, pl.ds(dst + at, ROW_BLOCK), :] = (mine + came).astype(BF16)
            return carry

        lax.fori_loop(0, self.rows // 2 // ROW_BLOCK, block, 0)

    def relay(self, c):
        r, h = self.rows, self.rows // 2
        self.add(c, 0, 2 * r, 2 * r)
        self.copy(c, 5).start()
        self.add(c, 1, 2 * r + h, r + h)
        self.copy(c, 4).start()

    def finish(self, c):
        for kind in range(2, 6):
            self.copy(c, kind).wait_recv()

    def close(self, mid_s, bias, out, o_sem, chunks, first_open):
        rows = self.rows

        def o_copy(c):
            return pltpu.make_async_copy(mid_s.at[c], out.at[pl.ds(pl.multiple_of(c * rows, rows), rows)], o_sem.at[c])

        def one(c, carry):
            @pl.when(c + first_open < chunks)
            def _():
                self.relay(c + first_open)

            self.finish(c)

            def block(n, inner):
                at = pl.multiple_of(n * ROW_BLOCK, ROW_BLOCK)
                total = self.out_s[c, pl.ds(at, ROW_BLOCK), :].astype(F32) + self.land_s[c, pl.ds(at, ROW_BLOCK), :].astype(F32) + self.land_s[c, pl.ds(rows + at, ROW_BLOCK), :].astype(F32)
                mid_s[c, pl.ds(at, ROW_BLOCK), :] = (mid_s[c, pl.ds(at, ROW_BLOCK), :].astype(F32) + total + bias).astype(BF16)
                return inner

            lax.fori_loop(0, rows // ROW_BLOCK, block, 0)
            o_copy(c).start()
            return carry

        lax.fori_loop(0, chunks, one, 0)

        def settle(c, carry):
            o_copy(c).wait()
            for kind in range(6):
                self.copy(c, kind).wait_send()
            return carry

        lax.fori_loop(0, chunks, settle, 0)


def qkv_kernel(layer, dims, scal, *refs):
    chunks, rows, model, hd, window = dims
    hidden, norms, cos, sin, wq, wk, wv = refs[:7]
    biases, b_push = refs[7:10], refs[10:13]
    kc, vc, wo, w_up, w_down = refs[13:18]
    q_out, kv_mine, kv_other, cache_mine, cache_peer, wo_peer, up_peer, down_peer, state = refs[18:27]
    x_s, h_s, t_s, w_s, b_s, bq_s, bk_s, bv_s, oq_s, okv_s, old_s, oldp_s, st_s, s_s = refs[27:41]
    ag_send, ag_recv, h_sem, t_sem, w_sem, wr_send, wr_recv, p_send, p_recv, q_sem, kv_sem, kr_send, kr_recv, raw_sem, old_sem, st_sem = refs[41:]
    place = Place()
    block = rows * chunks
    tall = 2 * rows
    tile = KEY_TILE
    tiles = window // tile
    scale = LOG2E * hd ** -0.5
    floor = window - 1 - scal[0]
    loads = [pltpu.make_async_copy(hidden.at[pl.ds(c * rows, rows)], h_s.at[c], h_sem.at[c]) for c in range(chunks)]
    for copy in loads:
        copy.start()
    for k, cache in enumerate((kc, vc)):
        pltpu.make_async_copy(cache.at[layer], okv_s.at[pl.ds(k * window, window)], raw_sem).start()
    place.barrier((place.x, place.y, place.peer))
    gather = Gather(place, x_s, ag_send, ag_recv, rows)
    parts = ((wq.at[layer], 0, 0, 2 * hd), (wk.at[layer], 1, 0, hd), (wv.at[layer], 1, hd, hd))
    w_local = [pltpu.make_async_copy(src, w_s.at[t, :, pl.ds(at, n)], w_sem.at[k]) for k, (src, t, at, n) in enumerate(parts)]
    w_remote = [remote(src, w_s.at[2 + t, :, pl.ds(at, n)], wr_send.at[k], wr_recv.at[k], place.peer) for k, (src, t, at, n) in enumerate(parts)]
    b_remote = [remote(src, dst, wr_send.at[3 + k], wr_recv.at[3 + k], place.peer) for k, (src, dst) in enumerate(zip(b_push, (bq_s, bk_s, bv_s)))]
    landing = (wo_peer, up_peer, down_peer)
    pushes = [remote(src.at[layer], dst, p_send.at[k], p_recv.at[k], place.peer) for k, (src, dst) in enumerate(zip((wo, w_up, w_down), landing))]
    old_push = remote(old_s, oldp_s, p_send.at[3], p_recv.at[3], place.peer)
    old_store = [pltpu.make_async_copy(src, dst, old_sem.at[k]) for k, (src, dst) in enumerate(((old_s, cache_mine), (oldp_s, cache_peer)))]
    gain = norms[layer, 0:1, :].astype(F32)
    shift = norms[layer, 1:2, :].astype(F32)

    def send_own(c):
        loads[c].wait()

        def norm_block(n, carry):
            at = pl.multiple_of(n * ROW_BLOCK, ROW_BLOCK)
            x_s[c, pl.ds(at, ROW_BLOCK), :] = normalized(h_s[c, pl.ds(at, ROW_BLOCK), :].astype(F32), gain, shift)
            return carry

        lax.fori_loop(0, rows // ROW_BLOCK, norm_block, 0)
        gather.start(c)

    def chunk_pos(c, i):
        return pl.multiple_of((place.member(i) * 2 + place.core) * block + c * rows, rows)

    def kv_row(c, kv, g):
        return ((c * 2 + kv) * 2 + g) * 4 * rows

    send_own(0)
    send_own(1)
    for copy in b_remote + w_remote + w_local + pushes:
        copy.start()
    for c in range(chunks):
        for i in range(4):
            for k, tab in enumerate((cos, sin)):
                pltpu.make_async_copy(tab.at[pl.ds(chunk_pos(c, i), rows)], t_s.at[c, k, pl.ds(i * rows, rows)], t_sem.at[c]).start()
    raw = okv_s.at[pl.ds(0, 2 * window)]
    pltpu.make_async_copy(raw, raw, raw_sem).wait()
    first_slot = lax.rem(scal[0], window)
    roll_tiles = window // ROLL_ROWS

    def raw_plane(k):
        return okv_s[k * window:(k + 1) * window, :]

    rotate(raw_plane, old_s, window, first_slot, 0, roll_tiles // 3)
    gather.forward(0)
    send_own(2)
    rotate(raw_plane, old_s, window, first_slot, roll_tiles // 3, roll_tiles)
    old_push.start()
    old_store[0].start()
    gather.forward(1)
    for copy in b_remote:
        copy.wait_recv()
    for g, (bq, bk, bv) in enumerate((biases, (bq_s, bk_s, bv_s))):
        b_s[2 * g] = bq[layer:layer + 1, :].astype(F32)
        b_s[2 * g + 1, :, 0:hd] = bk[layer:layer + 1, :].astype(F32)
        b_s[2 * g + 1, :, hd:] = bv[layer:layer + 1, :].astype(F32)

    def project(c, i0, count):
        r0, n = i0 * rows, count * rows

        def rope(u):
            turned = jnp.concatenate([-u[:, hd // 2:], u[:, :hd // 2]], axis=1)
            return (u * t_s[c, 0, r0:r0 + n, :] + turned * t_s[c, 1, r0:r0 + n, :]).astype(BF16)

        def side(g, carry):
            u = jnp.dot(x_s[c, r0:r0 + n, :], w_s[2 * g], preferred_element_type=F32) + b_s[2 * g]
            for h in range(2):
                oq_s[c, g, i0:i0 + count, h] = rope(u[:, h * hd:(h + 1) * hd]).reshape(count, rows, hd)
            u = jnp.dot(x_s[c, r0:r0 + n, :], w_s[2 * g + 1], preferred_element_type=F32) + b_s[2 * g + 1]
            okv_s[pl.ds(pl.multiple_of(kv_row(c, 0, g) + r0, rows), n), :] = rope(u[:, :hd])
            okv_s[pl.ds(pl.multiple_of(kv_row(c, 1, g) + r0, rows), n), :] = u[:, hd:].astype(BF16)
            return carry

        lax.fori_loop(0, 2, side, 0)

    def q_copy(c):
        return pltpu.make_async_copy(oq_s.at[c], q_out.at[c], q_sem.at[c])

    def kv_copies(c):
        planes = (kv_mine, kv_other)
        made = []
        for kv in range(2):
            for g in range(2):
                for i in range(4):
                    src = okv_s.at[pl.ds(pl.multiple_of(kv_row(c, kv, g) + i * rows, rows), rows)]
                    at = pl.ds(chunk_pos(c, i), rows)
                    made.append(pltpu.make_async_copy(src, planes[g].at[kv, at], kv_sem.at[c]))
                    made.append(remote(src, planes[1 - g].at[kv, at], kr_send.at[c], kr_recv.at[c], place.peer))
        return made

    def old_tile(g, kv, at):
        return (old_s, oldp_s)[g][kv, pl.ds(at, tile), :]

    def queries(c, i, g):
        return oq_s[c, g, i].reshape(tall, hd)

    def state_copy(b):
        return pltpu.make_async_copy(st_s.at[lax.rem(b, 2)], state.at[b], st_sem.at[lax.rem(b, 2)])

    def start_old(c, i):
        at = pl.multiple_of(lax.div(chunk_pos(c, i), tile) * tile, tile)
        for g in range(2):
            s_s[g] = score_tile(queries(c, i, g), old_tile(g, 0, at))

    def attend_old(c, i):
        b = c * 4 + i
        w = lax.rem(b, 2)
        j0 = chunk_pos(c, i)
        diag = lax.div(j0, tile)
        i_next = jnp.minimum(i + 1, 3)
        diag_next = lax.div(chunk_pos(c, i_next), tile)

        @pl.when(b >= 2)
        def _():
            state_copy(b - 2).wait()

        reset_state(st_s, w)

        def step(t, by_row):
            at = pl.multiple_of(t * tile, tile)
            last = t + 1 == tiles
            n_at = pl.multiple_of(jnp.where(last, diag_next, t + 1) * tile, tile)
            n_i = jnp.where(last, i_next, i)
            age = lax.broadcasted_iota(jnp.int32, (1, tile), 1) + at
            if by_row:
                row = lax.rem(lax.broadcasted_iota(jnp.int32, (tall, 1), 0), rows) + j0
                mask = age > jnp.maximum(row, floor)
            else:
                mask = age > floor
            flash_step(st_s, w, s_s, scale, mask, lambda g: old_tile(g, 1, at), lambda g: score_tile(queries(c, n_i, g), old_tile(g, 0, n_at)))

        step(diag, True)

        def younger(t, carry):
            @pl.when(t > diag)
            def _():
                step(t, False)

            return carry

        lax.fori_loop(1, tiles, younger, 0)
        state_copy(b).start()

    def chunk(c, carry):
        pltpu.make_async_copy(t_s.at[c], t_s.at[c], t_sem.at[c]).wait()

        @pl.when(c == 0)
        def _():
            for copy in w_local:
                copy.wait()
            for copy in w_remote:
                copy.wait_recv()

        project(c, 0, 3)
        gather.finish(c)
        project(c, 3, 1)
        q_copy(c).start()
        for copy in kv_copies(c):
            copy.start()

        @pl.when(c == 0)
        def _():
            old_push.wait_recv()
            old_store[1].start()

        @pl.when(lax.rem(c, 2) == 0)
        def _():
            early = lax.div(c, 2)
            start_old(early, 0)

            def one(i, inner):
                @pl.when(jnp.logical_and(c == 2, i == 3))
                def _():
                    gather.forward(3)

                attend_old(early, i)
                return inner

            lax.fori_loop(0, 4, one, 0)

        @pl.when(c == 0)
        def _():
            gather.forward(2)
            send_own(3)

        return carry

    lax.fori_loop(0, chunks, chunk, 0)
    for copy in w_remote + b_remote:
        copy.wait_send()

    def settle(c, carry):
        q_copy(c).wait()
        whole = okv_s.at[pl.ds(pl.multiple_of(kv_row(c, 0, 0), rows), 16 * rows)]
        pltpu.make_async_copy(whole, whole, kv_sem.at[c]).wait()
        remote(whole, whole, kr_send.at[c], kr_recv.at[c], place.peer).wait_send()
        remote(whole, whole, kr_send.at[c], kr_recv.at[c], place.peer).wait_recv()
        gather.drain(c)
        return carry

    lax.fori_loop(0, chunks, settle, 0)
    for copy in pushes:
        copy.wait_send()
        copy.wait_recv()
    old_push.wait_send()
    for copy in old_store:
        copy.wait()
    for b in (4 * EARLY - 2, 4 * EARLY - 1):
        state_copy(b).wait()


def run_qkv(layer, chunks, scal, hidden, norms, cos, sin, weights, biases, caches, w_o, w_up, w_down):
    model = hidden.shape[1]
    rows = hidden.shape[0] // chunks
    hd = cos.shape[1]
    window = cos.shape[0]
    dims = (chunks, rows, model, hd, window)
    flops = 2 * 4 * rows * chunks * model * 8 * hd
    shapes = [(chunks, 2, 4, 2, rows, hd)] + [(2, window, hd)] * 4 + [w.shape[1:] for w in (w_o, w_up, w_down)]
    state = (4 * EARLY, 2, 2 * rows, 2 * LANES + hd)
    return pl.pallas_call(
        functools.partial(qkv_kernel, layer, dims),
        out_shape=tuple(jax.ShapeDtypeStruct(s, BF16) for s in shapes) + (jax.ShapeDtypeStruct(state, F32),),
        in_specs=[SMEM, ANY, VMEM] + [ANY] * 5 + [VMEM] * 3 + [ANY] * 8,
        out_specs=(ANY,) * (len(shapes) + 1),
        scratch_shapes=[
            pltpu.VMEM((chunks, 4 * rows, model), BF16),
            pltpu.VMEM((chunks, rows, model), BF16),
            pltpu.VMEM((chunks, 2, 4 * rows, hd), F32),
            pltpu.VMEM((4, model, 2 * hd), BF16),
            pltpu.VMEM((4, 1, 2 * hd), F32),
        ] + [pltpu.VMEM(b.shape, BF16) for b in biases] + [
            pltpu.VMEM((chunks, 2, 4, 2, rows, hd), BF16),
            pltpu.VMEM((chunks * 16 * rows, hd), BF16),
            pltpu.VMEM((2, window, hd), BF16),
            pltpu.VMEM((2, window, hd), BF16),
            pltpu.VMEM((2,) + state[1:], F32),
            pltpu.VMEM((2, 2 * rows, KEY_TILE), F32),
            DMA((chunks, 4)),
            DMA((chunks, 4)),
            DMA((chunks,)),
            DMA((chunks,)),
            DMA((3,)),
            DMA((6,)),
            DMA((6,)),
            DMA((4,)),
            DMA((4,)),
            DMA((chunks,)),
            DMA((chunks,)),
            DMA((chunks,)),
            DMA((chunks,)),
            DMA,
            DMA((2,)),
            DMA((2,)),
        ],
        compiler_params=pltpu.CompilerParams(vmem_limit_bytes=VMEM_LIMIT, collective_id=3 * layer, has_side_effects=True),
        cost_estimate=pl.CostEstimate(flops=4 * flops, bytes_accessed=20_000_000, transcendentals=0),
        name=f"qkv_l{layer}",
    )(scal, hidden, norms, cos, sin, *weights, *biases, *biases, *caches, w_o, w_up, w_down)


def attn_kernel(layer, dims, scal, *refs):
    chunks, rows, model, hd, window = dims
    q, kv_mine, kv_other, cache_mine, cache_peer, state, wo, wo_peer, hidden, b_o = refs[:10]
    mid_out, kv_rolled = refs[10:12]
    kv_s, q_s, s_s, mix_s, wo_s, out_s, land_s, mid_s, st_s, rs_send, rs_recv, new_sem, old_sem, q_sem, w_sem, h_sem, st_sem, o_sem, f_sem = refs[12:]
    place = Place()
    start_pos = scal[0]
    block = rows * chunks
    tall = 2 * rows
    tile = KEY_TILE
    tiles = window // tile
    scale = LOG2E * hd ** -0.5
    q_load = pltpu.make_async_copy(q, q_s, q_sem)
    q_load.start()
    new = kv_s.at[:, pl.ds(2, 2)]
    old = kv_s.at[:, pl.ds(0, 2)]
    for g, src in enumerate((kv_mine, kv_other)):
        pltpu.make_async_copy(src, kv_s.at[g, pl.ds(2, 2)], new_sem).start()

    def pick(k):
        return jnp.where(k == 0, 3, jnp.where(k == 3, 0, k))

    def state_copy(b):
        return pltpu.make_async_copy(state.at[lax.div(b, 4) * 4 + pick(lax.rem(b, 4))], st_s.at[lax.rem(b, 2)], st_sem.at[lax.rem(b, 2)])

    for b in range(2):
        state_copy(jnp.int32(b)).start()
    pltpu.make_async_copy(wo.at[layer], wo_s.at[pl.ds(0, 2 * hd)], w_sem).start()
    pltpu.make_async_copy(wo_peer, wo_s.at[pl.ds(2 * hd, 2 * hd)], w_sem).start()
    for g, src in enumerate((cache_mine, cache_peer)):
        pltpu.make_async_copy(src, kv_s.at[g, pl.ds(0, 2)], old_sem).start()
    for c in range(chunks):
        pltpu.make_async_copy(hidden.at[pl.ds(c * rows, rows)], mid_s.at[c], h_sem).start()
    place.barrier((place.x, place.y))
    scatter = Scatter(place, out_s, land_s, rs_send, rs_recv, rows)
    first_slot = lax.rem(start_pos, window)
    floor = window - 1 - start_pos

    def first_row(c, i):
        return (place.member(i) * 2 + place.core) * block + c * rows

    def tile_at(diag, n):
        is_new = jnp.logical_or(n == 0, jnp.logical_and(n >= 2, n - 2 < diag))
        t = jnp.where(n < 2, diag, jnp.where(is_new, n - 2, n - 1))
        return jnp.where(is_new, 2, 0), pl.multiple_of(t * tile, tile), is_new

    def scores(c, i, g, which, at):
        return score_tile(q_s[c, g, i].reshape(tall, hd), kv_s[g, which, pl.ds(at, tile), :])

    q_load.wait()
    pltpu.make_async_copy(new, new, new_sem).wait()
    for g in range(2):
        s_s[g] = scores(0, 3, g, 2, pl.multiple_of(lax.div(first_row(0, 3), tile) * tile, tile))

    def attend(c, k):
        i = pick(k)
        b = c * 4 + k
        w = lax.rem(b, 2)
        whole = c >= EARLY
        j0 = first_row(c, i)
        diag = lax.div(j0, tile)
        count = jnp.where(whole, tiles + 1, diag + 2)
        end = k == 3
        c_next = jnp.minimum(jnp.where(end, c + 1, c), chunks - 1)
        i_next = pick(jnp.where(end, 0, k + 1))
        next_at = lax.div(first_row(c_next, i_next), tile) * tile

        @pl.when(whole)
        def _():
            reset_state(st_s, w)

        @pl.when(jnp.logical_not(whole))
        def _():
            state_copy(b).wait()

        def step(n):
            which, at, is_new = tile_at(diag, n)
            following = jnp.where(jnp.logical_and(n == 0, jnp.logical_not(whole)), 2, n + 1)
            last = following == count
            nw, nat, _ = tile_at(diag, following)
            nw = jnp.where(last, 2, nw)
            nat = pl.multiple_of(jnp.where(last, next_at, nat), tile)
            nc = jnp.where(last, c_next, c)
            ni = jnp.where(last, i_next, i)
            col = lax.broadcasted_iota(jnp.int32, (1, tile), 1) + at
            row = lax.rem(lax.broadcasted_iota(jnp.int32, (tall, 1), 0), rows) + j0
            if not isinstance(n, int):
                mask = col > jnp.where(is_new, -1, floor)
            elif n == 0:
                mask = col <= row
            else:
                mask = col > jnp.maximum(row, floor)
            flash_step(st_s, w, s_s, scale, mask, lambda g: kv_s[g, which + 1, pl.ds(at, tile), :], lambda g: scores(nc, ni, g, nw, nat))

        step(0)

        @pl.when(whole)
        def _():
            step(1)

        def further(n, carry):
            @pl.when(n < count)
            def _():
                step(n)

            return carry

        lax.fori_loop(2, tiles + 1, further, 0)
        for g in range(2):
            total = jnp.sum(st_s[w, g, :, LANES:2 * LANES], axis=1, keepdims=True)
            out = (st_s[w, g, :, 2 * LANES:] / total).astype(BF16)
            for h in range(2):
                mix_s[:, (2 * g + h) * hd:(2 * g + h + 1) * hd] = out[h * rows:(h + 1) * rows]

        @pl.when(b + 2 < 4 * EARLY)
        def _():
            state_copy(b + 2).start()

        @pl.when(b == 0)
        def _():
            pltpu.make_async_copy(wo_s, wo_s, w_sem).wait()

        r0 = pl.multiple_of(i * rows, rows)
        for n in range(model // WIDE):
            out_s[c, pl.ds(r0, rows), n * WIDE:(n + 1) * WIDE] = jnp.dot(mix_s[...], wo_s[:, n * WIDE:(n + 1) * WIDE], preferred_element_type=F32).astype(BF16)

        @pl.when(k == 0)
        def _():
            scatter.copy(c, 0).start()
            scatter.copy(c, 1).start()

        @pl.when(k == 1)
        def _():
            scatter.copy(c, 2).start()

        @pl.when(k == 2)
        def _():
            scatter.copy(c, 3).start()

    def chunk(c, carry):
        @pl.when(c == EARLY)
        def _():
            pltpu.make_async_copy(old, old, old_sem).wait()

        def one(k, inner):
            attend(c, k)

            @pl.when(jnp.logical_and(k == 1, c >= 1))
            def _():
                scatter.relay(c - 1)

            return inner

        lax.fori_loop(0, 4, one, 0)
        return carry

    lax.fori_loop(0, chunks, chunk, 0)
    pltpu.make_async_copy(mid_s, mid_s, h_sem).wait()
    rolled = kv_s.at[1, pl.ds(0, 2)]
    roll_tiles = window // ROLL_ROWS

    def new_plane(k):
        return kv_s[0, 2 + k]

    rotate(new_plane, rolled, window, window - first_slot, 0, roll_tiles // 2)
    scatter.relay(chunks - 1)
    rotate(new_plane, rolled, window, window - first_slot, roll_tiles // 2, roll_tiles)
    roll_store = pltpu.make_async_copy(rolled, kv_rolled, f_sem)
    roll_store.start()
    scatter.close(mid_s, b_o[layer:layer + 1, :].astype(F32), mid_out, o_sem, chunks, chunks)
    roll_store.wait()


def run_attn(layer, scal, q, kv_mine, kv_other, cache_mine, cache_peer, state, wo, wo_peer, hidden, b_o):
    chunks, rows, hd = q.shape[0], q.shape[-2], q.shape[-1]
    model = hidden.shape[1]
    window = kv_mine.shape[1]
    dims = (chunks, rows, model, hd, window)
    flops = 4 * 4 * rows * chunks * 4 * window * hd + 2 * 4 * rows * chunks * 4 * hd * model
    return pl.pallas_call(
        functools.partial(attn_kernel, layer, dims),
        out_shape=(jax.ShapeDtypeStruct(hidden.shape, BF16), jax.ShapeDtypeStruct((2, window, hd), BF16)),
        in_specs=[SMEM] + [ANY] * 9 + [VMEM],
        out_specs=(ANY, ANY),
        scratch_shapes=[
            pltpu.VMEM((2, 4, window, hd), BF16),
            pltpu.VMEM((chunks, 2, 4, 2, rows, hd), BF16),
            pltpu.VMEM((2, 2 * rows, KEY_TILE), F32),
            pltpu.VMEM((rows, 4 * hd), BF16),
            pltpu.VMEM((4 * hd, model), BF16),
            pltpu.VMEM((chunks, 4 * rows, model), BF16),
            pltpu.VMEM((chunks, 3 * rows, model), BF16),
            pltpu.VMEM((chunks, rows, model), BF16),
            pltpu.VMEM((2,) + state.shape[1:], F32),
            DMA((chunks, 6)),
            DMA((chunks, 6)),
            DMA,
            DMA,
            DMA,
            DMA,
            DMA,
            DMA((2,)),
            DMA((chunks,)),
            DMA,
        ],
        compiler_params=pltpu.CompilerParams(vmem_limit_bytes=VMEM_LIMIT, collective_id=3 * layer + 1, has_side_effects=True),
        cost_estimate=pl.CostEstimate(flops=flops, bytes_accessed=30_000_000, transcendentals=16 * rows * chunks * window),
        name=f"attn_l{layer}",
    )(scal, q, kv_mine, kv_other, cache_mine, cache_peer, state, wo, wo_peer, hidden, b_o)


def mlp_kernel(layer, dims, *refs):
    chunks, rows, model, ffn = dims
    middle, norms, b_down, biases, b_up, up, down, up_peer, down_peer = refs[:9]
    h_out = refs[9]
    x_s, out_s, land_s, act_s, w_s, mid_s, b_s, bp_s, ag_send, ag_recv, rs_send, rs_recv, m_sem, w_sem, b_send, b_recv, h_sem = refs[10:]
    place = Place()
    n_up = 2 * ffn // WIDE
    n_tiles = n_up + model // WIDE
    sub = WIDE // 2
    n_sub = ffn // sub
    ups = (up.at[layer], up_peer)
    downs = (down.at[layer], down_peer)
    loads = [pltpu.make_async_copy(middle.at[pl.ds(c * rows, rows)], mid_s.at[c], m_sem.at[c]) for c in range(chunks)]
    for copy in loads:
        copy.start()
    place.barrier((place.x, place.y, place.peer))
    gather = Gather(place, x_s, ag_send, ag_recv, rows)
    scatter = Scatter(place, out_s, land_s, rs_send, rs_recv, rows)
    gain = norms[layer, 2:3, :].astype(F32)
    shift = norms[layer, 3:4, :].astype(F32)

    def fetch(c, k):
        over = k >= n_tiles
        k = jnp.where(over, k - n_tiles, k)
        c = jnp.where(over, c + 1, c)
        slot = lax.rem(c * n_tiles + k, WEIGHT_SLOTS)

        @pl.when(c < chunks)
        def _():
            for part in range(2):
                n = 2 * k + part
                for side in range(2):
                    @pl.when(jnp.logical_and(n >= side * n_sub, n < (side + 1) * n_sub))
                    def _():
                        at = pl.multiple_of((n - side * n_sub) * sub, sub)
                        pltpu.make_async_copy(ups[side].at[:, pl.ds(at, sub)], w_s.at[slot, :, pl.ds(part * sub, sub)], w_sem.at[slot]).start()

            @pl.when(k >= n_up)
            def _():
                at = pl.multiple_of((k - n_up) * WIDE, WIDE)
                for side in range(2):
                    pltpu.make_async_copy(downs[side].at[:, pl.ds(at, WIDE)], w_s.at[slot, pl.ds(side * ffn, ffn)], w_sem.at[slot]).start()

    def landed(c, k):
        slot = lax.rem(c * n_tiles + k, WEIGHT_SLOTS)
        pltpu.make_async_copy(w_s.at[slot], w_s.at[slot], w_sem.at[slot]).wait()
        fetch(c, k + WEIGHT_SLOTS - 1)
        return slot

    def send_own(c):
        loads[c].wait()

        def norm_block(n, carry):
            at = pl.multiple_of(n * ROW_BLOCK, ROW_BLOCK)
            x_s[c, pl.ds(at, ROW_BLOCK), :] = normalized(mid_s[c, pl.ds(at, ROW_BLOCK), :].astype(F32), gain, shift)
            return carry

        lax.fori_loop(0, rows // ROW_BLOCK, norm_block, 0)
        gather.start(c)

    send_own(0)
    send_own(1)
    b_push = remote(b_up, bp_s, b_send, b_recv, place.peer)
    b_push.start()
    for k in range(WEIGHT_SLOTS - 1):
        fetch(jnp.int32(0), jnp.int32(k))
    gather.forward(0)
    send_own(2)
    gather.forward(1)
    send_own(3)
    b_push.wait_recv()
    for n in range(2 * n_sub):
        src = biases if n < n_sub else bp_s
        at = (n % n_sub) * sub
        b_s[n // 2, :, (n % 2) * sub:(n % 2 + 1) * sub] = src[layer:layer + 1, at:at + sub].astype(F32)

    def chunk(c, carry):
        gather.finish(c)

        def up_step(k, inner):
            slot = landed(c, k)
            at = pl.multiple_of(k * WIDE, WIDE)
            for top in range(2):
                r0 = top * 2 * rows
                lifted = jnp.dot(x_s[c, r0:r0 + 2 * rows, :], w_s[slot], preferred_element_type=F32) + b_s[k]
                act_s[r0:r0 + 2 * rows, pl.ds(at, WIDE)] = gelu_tanh(lifted).astype(BF16)
            return inner

        lax.fori_loop(0, n_up, up_step, 0)

        @pl.when(c + 2 < chunks)
        def _():
            gather.forward(c + 2)

        @pl.when(c >= 2)
        def _():
            scatter.relay(c - 2)

        def down_step(k, inner):
            slot = landed(c, k)
            at = pl.multiple_of((k - n_up) * WIDE, WIDE)
            out_s[c, :, pl.ds(at, WIDE)] = jnp.dot(act_s[...], w_s[slot], preferred_element_type=F32).astype(BF16)
            return inner

        lax.fori_loop(n_up, n_tiles, down_step, 0)
        scatter.start(c)
        return carry

    lax.fori_loop(0, chunks, chunk, 0)
    scatter.close(mid_s, b_down[layer:layer + 1, :].astype(F32), h_out, h_sem, chunks, chunks - 2)
    for c in range(chunks):
        gather.drain(c)
    b_push.wait_send()


def run_mlp(layer, chunks, middle, norms, b_down, b_up, up, down, up_peer, down_peer):
    model = middle.shape[1]
    rows = middle.shape[0] // chunks
    ffn = up.shape[2]
    dims = (chunks, rows, model, ffn)
    flops = 2 * 4 * rows * chunks * model * ffn * 4
    return pl.pallas_call(
        functools.partial(mlp_kernel, layer, dims),
        out_shape=jax.ShapeDtypeStruct(middle.shape, BF16),
        in_specs=[ANY] + [VMEM] * 3 + [ANY] * 5,
        out_specs=ANY,
        scratch_shapes=[
            pltpu.VMEM((chunks, 4 * rows, model), BF16),
            pltpu.VMEM((chunks, 4 * rows, model), BF16),
            pltpu.VMEM((chunks, 3 * rows, model), BF16),
            pltpu.VMEM((4 * rows, 2 * ffn), BF16),
            pltpu.VMEM((WEIGHT_SLOTS, model, WIDE), BF16),
            pltpu.VMEM((chunks, rows, model), BF16),
            pltpu.VMEM((2 * ffn // WIDE, 1, WIDE), F32),
            pltpu.VMEM(b_up.shape, BF16),
            DMA((chunks, 4)),
            DMA((chunks, 4)),
            DMA((chunks, 6)),
            DMA((chunks, 6)),
            DMA((chunks,)),
            DMA((WEIGHT_SLOTS,)),
            DMA,
            DMA,
            DMA((chunks,)),
        ],
        compiler_params=pltpu.CompilerParams(vmem_limit_bytes=VMEM_LIMIT, collective_id=3 * layer + 2, has_side_effects=True),
        cost_estimate=pl.CostEstimate(flops=2 * flops, bytes_accessed=60_000_000, transcendentals=8 * rows * ffn),
        name=f"mlp_l{layer}",
    )(middle, norms, b_down, b_up, b_up, up, down, up_peer, down_peer)


def solution(mesh):
    row_spec = P('dp', 'tp', None)
    cache_spec = P(None, 'dp', None, 'tp', None)
    col_spec = P(None, None, 'tp')
    bias_spec = P(None, 'tp')
    in_specs = (row_spec, P('dp'), P('dp', None, None), P('dp', None, None), cache_spec, cache_spec, P('dp', None), P(), col_spec, bias_spec, col_spec, bias_spec, col_spec, bias_spec, P(None, 'tp', None), P(), col_spec, bias_spec, P(None, 'tp', None), P())
    out_specs = (row_spec, cache_spec, cache_spec, P('dp', None))

    def device_step(tokens, start_pos, cos_tab, sin_tab, key_cache, value_cache, slot_pos, norm_params, w_q, b_q, w_k, b_k, w_v, b_v, w_o, b_o, w_up, b_up, w_down, b_down):
        layers, _, window, _, hd = key_cache.shape
        cos, sin = cos_tab[0], sin_tab[0]
        kc = key_cache.reshape(layers, window, hd)
        vc = value_cache.reshape(layers, window, hd)
        hidden = tokens[0]
        fresh = []
        for layer in range(layers):
            q, kv_mine, kv_other, cache_mine, cache_peer, wo_peer, up_peer, down_peer, state = run_qkv(layer, CHUNKS, start_pos, hidden, norm_params, cos, sin, (w_q, w_k, w_v), (b_q, b_k, b_v), (kc, vc), w_o, w_up, w_down)
            middle, kv_rolled = run_attn(layer, start_pos, q, kv_mine, kv_other, cache_mine, cache_peer, state, w_o, wo_peer, hidden, b_o)
            hidden = run_mlp(layer, CHUNKS, middle, norm_params, b_down, b_up, w_up, w_down, up_peer, down_peer)
            fresh.append(kv_rolled)
        key_out = jnp.stack([f[0] for f in fresh]).reshape(key_cache.shape)
        value_out = jnp.stack([f[1] for f in fresh]).reshape(value_cache.shape)
        first_slot = start_pos[0] % window
        pos_out = (start_pos[0] + (jnp.arange(window, dtype=jnp.int32) - first_slot) % window)[None]
        return hidden[None], key_out, value_out, pos_out

    return jax.shard_map(device_step, mesh=mesh, in_specs=in_specs, out_specs=out_specs, check_vma=False)
```

```python
import functools

import jax
import jax.numpy as jnp
from jax import lax
from jax.experimental import pallas as pl
from jax.experimental.pallas import tpu as pltpu
from jax.sharding import PartitionSpec as P

NORM_EPS = 1e-5
LOG2E = 1.4426950408889634
CHUNKS = 4
KEY_TILE = 512
LANES = 128
WIDE = 512
ROW_BLOCK = 16
PAIR = 2
GROUP = 4
WEIGHT_SLOTS = 3
ROLL_ROWS = 256
ROLL_SLOTS = 4
EARLY = 2
LOWEST = -3.3e38
VMEM_LIMIT = 67_043_328
BF16 = jnp.bfloat16
F32 = jnp.float32
MESH = pl.DeviceIdType.MESH

ANY = pl.BlockSpec(memory_space=pl.ANY)
SMEM = pl.BlockSpec(memory_space=pltpu.SMEM)
VMEM = pl.BlockSpec(memory_space=pltpu.VMEM)
DMA = pltpu.SemaphoreType.DMA


def vm(*shape, dtype=BF16):
    return pltpu.VMEM(shape, dtype)


def dma(*shape):
    return DMA(shape) if shape else DMA


def whole(ref, sem):
    pltpu.make_async_copy(ref, ref, sem).wait()


def one_row(ref, n):
    return ref[pl.ds(n, 1), :].astype(F32)


def gelu_tanh(x):
    inner = 0.7978845608028654 * (x + 0.044715 * (x * x * x))
    return 0.5 * x * (1.0 + jnp.tanh(inner))


def normalized(values, gain, shift):
    centered = values - jnp.mean(values, axis=-1, keepdims=True)
    variance = jnp.mean(centered * centered, axis=-1, keepdims=True)
    return (centered * lax.rsqrt(variance + NORM_EPS) * gain + shift).astype(BF16)


def rotate(planes, put, window, shift, first, last):
    def tile(n, carry):
        want = lax.broadcasted_iota(jnp.int32, (ROLL_ROWS, 1), 0) + (n * ROLL_ROWS + shift)
        want = jnp.where(want >= window, want - window, want)
        pick = jnp.where(lax.broadcasted_iota(jnp.int32, (1, window), 1) == want, 1.0, 0.0).astype(BF16)
        put(n, [jnp.dot(pick, planes(k), preferred_element_type=F32).astype(BF16) for k in range(PAIR)])
        return carry

    lax.fori_loop(first, last, tile, 0)


def reset_state(st_s, w):
    for g in range(PAIR):
        st_s[w, g, :, 0:LANES] = jnp.full((st_s.shape[2], LANES), LOWEST, F32)
        st_s[w, g, :, LANES:] = jnp.zeros((st_s.shape[2], st_s.shape[3] - LANES), F32)


def flash_step(st_s, w, s_s, scale, mask, values, next_scores):
    for g in range(PAIR):
        s = jnp.where(mask, s_s[g] * scale, -jnp.inf)
        s_next = next_scores(g)
        m_prev = st_s[w, g, :, 0:LANES]
        m_next = jnp.maximum(m_prev, jnp.max(s, axis=1, keepdims=True))
        e = jnp.exp2(s - jnp.concatenate([m_next] * (s.shape[1] // LANES), axis=1))
        alpha = jnp.exp2(m_prev - m_next)
        total = st_s[w, g, :, LANES:2 * LANES] * alpha
        for k in range(s.shape[1] // LANES):
            total = total + e[:, k * LANES:(k + 1) * LANES]
        st_s[w, g, :, LANES:2 * LANES] = total
        st_s[w, g, :, 0:LANES] = m_next
        mixed = jnp.dot(e.astype(BF16), values(g), preferred_element_type=F32)
        st_s[w, g, :, 2 * LANES:] = st_s[w, g, :, 2 * LANES:] * jnp.concatenate([alpha] * (mixed.shape[1] // LANES), axis=1) + mixed
        s_s[g] = s_next


def score_tile(queries, keys):
    return lax.dot_general(queries, keys, (((1,), (1,)), ((), ())), preferred_element_type=F32)


class Place:
    def __init__(self):
        me = lax.axis_index('tp')
        self.core = lax.rem(me, 2)
        self.xb = lax.rem(lax.div(me, 2), 2)
        self.yb = lax.div(me, 4)
        self.peer = me + 1 - 2 * self.core
        self.x = me + 2 - 4 * self.xb
        self.y = me + 4 - 8 * self.yb

    def member(self, i):
        xb = self.xb + lax.rem(i, 2) * (1 - 2 * self.xb)
        yb = self.yb + lax.div(i, 2) * (1 - 2 * self.yb)
        return yb * 2 + xb

    def barrier(self, others):
        sem = pltpu.get_barrier_semaphore()
        for other in others:
            pl.semaphore_signal(sem, inc=1, device_id={'tp': other}, device_id_type=MESH)
        pl.semaphore_wait(sem, len(others))


def remote(src, dst, send_sem, recv_sem, other):
    return pltpu.make_async_remote_copy(src_ref=src, dst_ref=dst, send_sem=send_sem, recv_sem=recv_sem, device_id={'tp': other}, device_id_type=MESH)


class Gather:
    def __init__(self, place, x_s, send, recv, rows):
        self.place, self.x_s, self.send, self.recv, self.rows = place, x_s, send, recv, rows

    def copy(self, c, kind):
        r, h = self.rows, self.rows // 2
        src, dst, size, other = ((0, r, r, self.place.x), (0, 2 * r, r, self.place.y), (r, 3 * r, h, self.place.y), (2 * r + h, 3 * r + h, h, self.place.x))[kind]
        return remote(self.x_s.at[c, pl.ds(src, size)], self.x_s.at[c, pl.ds(dst, size)], self.send.at[c, kind], self.recv.at[c, kind], other)

    def start(self, c):
        self.copy(c, 0).start()
        self.copy(c, 1).start()

    def forward(self, c):
        self.copy(c, 0).wait_recv()
        self.copy(c, 2).start()
        self.copy(c, 1).wait_recv()
        self.copy(c, 3).start()

    def finish(self, c):
        self.copy(c, 2).wait_recv()
        self.copy(c, 3).wait_recv()

    def drain(self, c):
        for kind in range(4):
            self.copy(c, kind).wait_send()


class Scatter:
    def __init__(self, place, out_s, land_s, send, recv, rows, shift):
        self.place, self.out_s, self.land_s, self.send, self.recv, self.rows, self.shift = place, out_s, land_s, send, recv, rows, shift

    def copy(self, c, kind):
        r, h = self.rows, self.rows // 2
        x, y = self.place.x, self.place.y
        src, dst, other = ((3 * r, 2 * r, x), (3 * r + h, 2 * r + h, y), (r, 0, x), (2 * r + h, r + h, y), (r + h, h, x), (2 * r, r, y))[kind]
        return remote(self.out_s.at[c + self.shift, pl.ds(src, h)], self.land_s.at[c, pl.ds(dst, h)], self.send.at[c, kind], self.recv.at[c, kind], other)

    def start(self, c):
        for kind in range(4):
            self.copy(c, kind).start()

    def add(self, c, kind, src, dst):
        self.copy(c, kind).wait_recv()
        slot = c + self.shift

        def block(n, carry):
            at = pl.multiple_of(n * ROW_BLOCK, ROW_BLOCK)
            mine = self.out_s[slot, pl.ds(dst + at, ROW_BLOCK), :].astype(F32)
            came = self.land_s[c, pl.ds(src + at, ROW_BLOCK), :].astype(F32)
            self.out_s[slot, pl.ds(dst + at, ROW_BLOCK), :] = (mine + came).astype(BF16)
            return carry

        lax.fori_loop(0, self.rows // 2 // ROW_BLOCK, block, 0)

    def relay(self, c, settled=None):
        r, h = self.rows, self.rows // 2
        self.add(c, 0, 2 * r, 2 * r)
        self.add(c, 1, 2 * r + h, r + h)
        if settled is not None:
            @pl.when(settled >= 0)
            def _():
                self.drain(settled)

        self.copy(c, 5).start()
        self.copy(c, 4).start()

    def finish(self, c):
        for kind in range(2, 6):
            self.copy(c, kind).wait_recv()

    def drain(self, c):
        for kind in range(6):
            self.copy(c, kind).wait_send()

    def total(self, c, at):
        own = self.out_s[c + self.shift, pl.ds(at, ROW_BLOCK), :].astype(F32)
        came = [self.land_s[c, pl.ds(k * self.rows + at, ROW_BLOCK), :].astype(F32) for k in range(PAIR)]
        return own + came[0] + came[1]


def qkv_kernel(layer, dims, scal, *refs):
    chunks, rows, model, hd, window = dims
    (hidden, norms, cos, sin, wq, wk, wv, bq, bk, bv, bq_push, bk_push, bv_push, kc, vc, wo, w_up, w_down,
     q_out, kv_mine, kv_other, cache_mine, cache_peer, wo_peer, up_peer, down_peer, state,
     x_s, h_s, t_s, w_s, b_s, bq_s, bk_s, bv_s, oq_s, okv_s, old_s, oldp_s, st_s, s_s,
     ag_send, ag_recv, h_sem, t_sem, w_sem, wr_send, wr_recv, p_send, p_recv, q_sem, kv_sem, kr_send, kr_recv, raw_sem, old_sem, st_sem) = refs
    place = Place()
    block = rows * chunks
    tall = PAIR * rows
    tile = KEY_TILE
    tiles = window // tile
    scale = LOG2E * hd ** -0.5
    floor = window - 1 - scal[0]
    loads = [pltpu.make_async_copy(hidden.at[pl.ds(c * rows, rows)], h_s.at[c], h_sem.at[c]) for c in range(chunks)]
    for copy in loads:
        copy.start()
    for k, cache in enumerate((kc, vc)):
        pltpu.make_async_copy(cache.at[layer], okv_s.at[pl.ds(k * window, window)], raw_sem).start()
    place.barrier((place.x, place.y, place.peer))
    gather = Gather(place, x_s, ag_send, ag_recv, rows)
    parts = ((wq.at[layer], 0, 0, 2 * hd), (wk.at[layer], 1, 0, hd), (wv.at[layer], 1, hd, hd))
    w_local = [pltpu.make_async_copy(src, w_s.at[t, :, pl.ds(at, n)], w_sem.at[k]) for k, (src, t, at, n) in enumerate(parts)]
    w_remote = [remote(src, w_s.at[2 + t, :, pl.ds(at, n)], wr_send.at[k], wr_recv.at[k], place.peer) for k, (src, t, at, n) in enumerate(parts)]
    b_remote = [remote(src, dst, wr_send.at[3 + k], wr_recv.at[3 + k], place.peer) for k, (src, dst) in enumerate(zip((bq_push, bk_push, bv_push), (bq_s, bk_s, bv_s)))]
    landing = (wo_peer, up_peer, down_peer)
    pushes = [remote(src.at[layer], dst, p_send.at[k], p_recv.at[k], place.peer) for k, (src, dst) in enumerate(zip((wo, w_up, w_down), landing))]
    old_push = remote(old_s, oldp_s, p_send.at[3], p_recv.at[3], place.peer)
    old_store = [pltpu.make_async_copy(src, dst, old_sem.at[k]) for k, (src, dst) in enumerate(((old_s, cache_mine), (oldp_s, cache_peer)))]
    gain = one_row(norms.at[layer], 0)
    shift = one_row(norms.at[layer], 1)

    def send_own(c):
        loads[c].wait()

        def norm_block(n, carry):
            at = pl.multiple_of(n * ROW_BLOCK, ROW_BLOCK)
            x_s[c, pl.ds(at, ROW_BLOCK), :] = normalized(h_s[c, pl.ds(at, ROW_BLOCK), :].astype(F32), gain, shift)
            return carry

        lax.fori_loop(0, rows // ROW_BLOCK, norm_block, 0)
        gather.start(c)

    def chunk_pos(c, i):
        return pl.multiple_of((place.member(i) * 2 + place.core) * block + c * rows, rows)

    def kv_row(c, kv, g):
        return pl.multiple_of(((c * PAIR + kv) * PAIR + g) * GROUP * rows, rows)

    def q_row(c, g, i):
        return pl.multiple_of(((c * PAIR + g) * GROUP + i) * tall, rows)

    send_own(0)
    send_own(1)
    for copy in b_remote + w_remote + w_local + pushes:
        copy.start()
    for c in range(chunks):
        for i in range(GROUP):
            for k, tab in enumerate((cos, sin)):
                pltpu.make_async_copy(tab.at[pl.ds(chunk_pos(c, i), rows)], t_s.at[c, k, pl.ds(i * rows, rows)], t_sem.at[c]).start()
    whole(okv_s, raw_sem)
    first_slot = lax.rem(scal[0], window)
    roll_tiles = window // ROLL_ROWS

    def raw_plane(k):
        return okv_s[k * window:(k + 1) * window, :]

    def put_old(n, turned):
        for k in range(PAIR):
            old_s[pl.ds(pl.multiple_of(k * window + n * ROLL_ROWS, ROLL_ROWS), ROLL_ROWS), :] = turned[k]

    rotate(raw_plane, put_old, window, first_slot, 0, roll_tiles // 3)
    gather.forward(0)
    send_own(2)
    rotate(raw_plane, put_old, window, first_slot, roll_tiles // 3, roll_tiles)
    old_push.start()
    old_store[0].start()
    gather.forward(1)
    for copy in b_remote:
        copy.wait_recv()
    for g, (for_q, for_k, for_v) in enumerate(((bq, bk, bv), (bq_s, bk_s, bv_s))):
        b_s[PAIR * g] = one_row(for_q, layer)
        b_s[PAIR * g + 1, :, :hd] = one_row(for_k, layer)
        b_s[PAIR * g + 1, :, hd:] = one_row(for_v, layer)

    def project(c, i0, count):
        r0, n = i0 * rows, count * rows

        def rope(u):
            turned = jnp.concatenate([-u[:, hd // 2:], u[:, :hd // 2]], axis=1)
            return (u * t_s[c, 0, r0:r0 + n, :] + turned * t_s[c, 1, r0:r0 + n, :]).astype(BF16)

        def side(g, carry):
            u = jnp.dot(x_s[c, r0:r0 + n, :], w_s[PAIR * g], preferred_element_type=F32) + b_s[PAIR * g]
            for h in range(PAIR):
                turned = rope(u[:, h * hd:(h + 1) * hd])
                for i in range(count):
                    oq_s[pl.ds(pl.multiple_of(q_row(c, g, i0 + i) + h * rows, rows), rows), :] = turned[i * rows:(i + 1) * rows]
            u = jnp.dot(x_s[c, r0:r0 + n, :], w_s[PAIR * g + 1], preferred_element_type=F32) + b_s[PAIR * g + 1]
            okv_s[pl.ds(pl.multiple_of(kv_row(c, 0, g) + r0, rows), n), :] = rope(u[:, :hd])
            okv_s[pl.ds(pl.multiple_of(kv_row(c, 1, g) + r0, rows), n), :] = u[:, hd:].astype(BF16)
            return carry

        lax.fori_loop(0, 2, side, 0)

    def q_copy(c):
        part = pl.ds(q_row(c, 0, 0), PAIR * GROUP * tall)
        return pltpu.make_async_copy(oq_s.at[part], q_out.at[part], q_sem.at[c])

    def kv_copies(c):
        planes = (kv_mine, kv_other)
        made = []
        for kv in range(PAIR):
            for g in range(PAIR):
                for i in range(GROUP):
                    src = okv_s.at[pl.ds(pl.multiple_of(kv_row(c, kv, g) + i * rows, rows), rows)]
                    at = pl.ds(pl.multiple_of(kv * window + chunk_pos(c, i), rows), rows)
                    made.append(pltpu.make_async_copy(src, planes[g].at[at], kv_sem.at[c]))
                    made.append(remote(src, planes[1 - g].at[at], kr_send.at[c], kr_recv.at[c], place.peer))
        return made

    def old_tile(g, kv, at):
        return (old_s, oldp_s)[g][pl.ds(pl.multiple_of(kv * window + at, tile), tile), :]

    def queries(c, i, g):
        return oq_s[pl.ds(q_row(c, g, i), tall), :]

    def state_copy(b):
        return pltpu.make_async_copy(st_s.at[lax.rem(b, PAIR)], state.at[b], st_sem.at[lax.rem(b, PAIR)])

    def start_old(c, i):
        at = pl.multiple_of(lax.div(chunk_pos(c, i), tile) * tile, tile)
        for g in range(PAIR):
            s_s[g] = score_tile(queries(c, i, g), old_tile(g, 0, at))

    def attend_old(c, i):
        b = c * GROUP + i
        w = lax.rem(b, PAIR)
        j0 = chunk_pos(c, i)
        diag = lax.div(j0, tile)
        i_next = jnp.minimum(i + 1, 3)
        diag_next = lax.div(chunk_pos(c, i_next), tile)

        @pl.when(b >= 2)
        def _():
            state_copy(b - 2).wait()

        reset_state(st_s, w)

        def step(t, by_row):
            at = pl.multiple_of(t * tile, tile)
            last = t + 1 == tiles
            n_at = pl.multiple_of(jnp.where(last, diag_next, t + 1) * tile, tile)
            n_i = jnp.where(last, i_next, i)
            age = lax.broadcasted_iota(jnp.int32, (1, tile), 1) + at
            if by_row:
                row = lax.rem(lax.broadcasted_iota(jnp.int32, (tall, 1), 0), rows) + j0
                mask = age > jnp.maximum(row, floor)
            else:
                mask = age > floor
            flash_step(st_s, w, s_s, scale, mask, lambda g: old_tile(g, 1, at), lambda g: score_tile(queries(c, n_i, g), old_tile(g, 0, n_at)))

        step(diag, True)

        def younger(t, carry):
            @pl.when(t > diag)
            def _():
                step(t, False)

            return carry

        lax.fori_loop(1, tiles, younger, 0)
        state_copy(b).start()

    def chunk(c, carry):
        whole(t_s.at[c], t_sem.at[c])

        @pl.when(c == 0)
        def _():
            for copy in w_local:
                copy.wait()
            for copy in w_remote:
                copy.wait_recv()

        project(c, 0, 3)
        gather.finish(c)
        project(c, 3, 1)
        q_copy(c).start()
        for copy in kv_copies(c):
            copy.start()

        @pl.when(c == 0)
        def _():
            old_push.wait_recv()
            old_store[1].start()

        @pl.when(lax.rem(c, 2) == 0)
        def _():
            early = lax.div(c, 2)
            start_old(early, 0)

            def one(i, inner):
                @pl.when(jnp.logical_and(c == 2, i == 3))
                def _():
                    gather.forward(3)

                attend_old(early, i)
                return inner

            lax.fori_loop(0, 4, one, 0)

        @pl.when(c == 0)
        def _():
            gather.forward(2)
            send_own(3)

        return carry

    lax.fori_loop(0, chunks, chunk, 0)
    for copy in w_remote + b_remote:
        copy.wait_send()

    def settle(c, carry):
        q_copy(c).wait()
        part = okv_s.at[pl.ds(kv_row(c, 0, 0), PAIR * PAIR * GROUP * rows)]
        whole(part, kv_sem.at[c])
        remote(part, part, kr_send.at[c], kr_recv.at[c], place.peer).wait_send()
        remote(part, part, kr_send.at[c], kr_recv.at[c], place.peer).wait_recv()
        gather.drain(c)
        return carry

    lax.fori_loop(0, chunks, settle, 0)
    for copy in pushes:
        copy.wait_send()
        copy.wait_recv()
    old_push.wait_send()
    for copy in old_store:
        copy.wait()
    for b in (GROUP * EARLY - 2, GROUP * EARLY - 1):
        state_copy(b).wait()


def run_qkv(layer, chunks, scal, hidden, norms, cos, sin, weights, biases, caches, w_o, w_up, w_down):
    model = hidden.shape[1]
    rows = hidden.shape[0] // chunks
    hd = cos.shape[1]
    window = cos.shape[0]
    dims = (chunks, rows, model, hd, window)
    flops = 2 * 4 * rows * chunks * model * 8 * hd
    planes = (PAIR * window, hd)
    shapes = [(chunks * PAIR * GROUP * PAIR * rows, hd)] + [planes] * 4 + [w.shape[1:] for w in (w_o, w_up, w_down)]
    state = (GROUP * EARLY, PAIR, PAIR * rows, PAIR * LANES + hd)
    return pl.pallas_call(
        functools.partial(qkv_kernel, layer, dims),
        out_shape=tuple(jax.ShapeDtypeStruct(s, BF16) for s in shapes) + (jax.ShapeDtypeStruct(state, F32),),
        in_specs=[SMEM, ANY, VMEM] + [ANY] * 5 + [VMEM] * 3 + [ANY] * 8,
        out_specs=(ANY,) * (len(shapes) + 1),
        scratch_shapes=[
            vm(chunks, GROUP * rows, model),
            vm(chunks, rows, model),
            vm(chunks, PAIR, GROUP * rows, hd, dtype=F32),
            vm(GROUP, model, PAIR * hd),
            vm(GROUP, 1, PAIR * hd, dtype=F32),
            *(vm(*b.shape) for b in biases),
            vm(*shapes[0]),
            vm(chunks * PAIR * PAIR * GROUP * rows, hd),
            vm(*planes),
            vm(*planes),
            vm(PAIR, *state[1:], dtype=F32),
            vm(PAIR, PAIR * rows, KEY_TILE, dtype=F32),
            dma(chunks, GROUP),
            dma(chunks, GROUP),
            dma(chunks),
            dma(chunks),
            dma(3),
            dma(6),
            dma(6),
            dma(GROUP),
            dma(GROUP),
            dma(chunks),
            dma(chunks),
            dma(chunks),
            dma(chunks),
            dma(),
            dma(PAIR),
            dma(PAIR),
        ],
        compiler_params=pltpu.CompilerParams(vmem_limit_bytes=VMEM_LIMIT, collective_id=PAIR * layer, has_side_effects=True),
        cost_estimate=pl.CostEstimate(flops=4 * flops, bytes_accessed=20_000_000, transcendentals=0),
        name=f"qkv_l{layer}",
    )(scal, hidden, norms, cos, sin, *weights, *biases, *biases, *caches, w_o, w_up, w_down)


def block_kernel(layer, dims, scal, *refs):
    chunks, rows, model, hd, window, ffn = dims
    (q, kv_mine, kv_other, cache_mine, cache_peer, state, wo, wo_peer, hidden, norms, b_o, b_down, b_up, b_push, up, down, up_peer, down_peer,
     h_out, kv_rolled,
     big_s, q_s, s_s, mix_s, wo_s, xo_s, land_s, mid_s, st_s, b_s, bp_s,
     r1_send, r1_recv, r2_send, r2_recv, ag_send, ag_recv, new_sem, old_sem, q_sem, wo_sem, h_sem, st_sem, w_sem, b_send, b_recv, o_sem, f_sem) = refs
    place = Place()
    start_pos = scal[0]
    block = rows * chunks
    tall = PAIR * rows
    tile = KEY_TILE
    tiles = window // tile
    scale = LOG2E * hd ** -0.5

    def region(g, new):
        return jnp.where(new, (3 - g) * window, g * window)

    def load_planes(src, base, sem):
        for k in range(PAIR):
            pltpu.make_async_copy(src.at[pl.ds(k * window, window)], big_s.at[pl.ds(base, window), pl.ds(k * hd, hd)], sem).start()

    q_rows = PAIR * GROUP * tall

    def q_copy(c):
        slot = lax.rem(c, PAIR)
        src, dst = (pl.ds(pl.multiple_of(n * q_rows, rows), q_rows) for n in (c, slot))
        return pltpu.make_async_copy(q.at[src], q_s.at[dst], q_sem.at[slot])

    q_copy(jnp.int32(0)).start()
    q_copy(jnp.int32(1)).start()
    load_planes(kv_mine, 3 * window, new_sem)
    load_planes(kv_other, PAIR * window, new_sem)

    def pick(k):
        return jnp.where(k == 0, 3, jnp.where(k == 3, 0, k))

    def state_copy(b):
        slot = lax.rem(b, PAIR)
        return pltpu.make_async_copy(state.at[lax.div(b, GROUP) * GROUP + pick(lax.rem(b, GROUP))], st_s.at[slot], st_sem.at[slot])

    for b in range(PAIR):
        state_copy(jnp.int32(b)).start()
    pltpu.make_async_copy(wo.at[layer], wo_s.at[pl.ds(0, PAIR * hd)], wo_sem).start()
    pltpu.make_async_copy(wo_peer, wo_s.at[pl.ds(PAIR * hd, PAIR * hd)], wo_sem).start()
    load_planes(cache_mine, 0, old_sem)
    load_planes(cache_peer, window, old_sem)
    for c in range(chunks):
        pltpu.make_async_copy(hidden.at[pl.ds(c * rows, rows)], mid_s.at[c], h_sem).start()
    place.barrier((place.x, place.y, place.peer))
    b_copy = remote(b_push, bp_s, b_send, b_recv, place.peer)
    b_copy.start()
    first = Scatter(place, xo_s, land_s, r1_send, r1_recv, rows, 1)
    second = Scatter(place, xo_s, land_s, r2_send, r2_recv, rows, 0)
    gather = Gather(place, xo_s, ag_send, ag_recv, rows)
    first_slot = lax.rem(start_pos, window)
    floor = window - 1 - start_pos

    def first_row(c, i):
        return (place.member(i) * PAIR + place.core) * block + c * rows

    def tile_at(diag, n):
        is_new = jnp.logical_or(n == 0, jnp.logical_and(n >= 2, n - 2 < diag))
        t = jnp.where(n < 2, diag, jnp.where(is_new, n - 2, n - 1))
        return is_new, t * tile

    def tile_of(g, is_new, at, kv):
        return big_s[pl.ds(pl.multiple_of(region(g, is_new) + at, tile), tile), kv * hd:(kv + 1) * hd]

    def scores(c, i, g, is_new, at):
        r0 = pl.multiple_of(((lax.rem(c, PAIR) * PAIR + g) * GROUP + i) * tall, rows)
        return score_tile(q_s[pl.ds(r0, tall), :], tile_of(g, is_new, at, 0))

    q_copy(jnp.int32(0)).wait()
    whole(big_s.at[pl.ds(0, PAIR * window)], new_sem)
    for g in range(PAIR):
        s_s[g] = scores(jnp.int32(0), 3, g, True, lax.div(first_row(0, 3), tile) * tile)

    def attend(c, k):
        i = pick(k)
        b = c * GROUP + k
        w = lax.rem(b, PAIR)
        late = c >= EARLY
        j0 = first_row(c, i)
        diag = lax.div(j0, tile)
        count = jnp.where(late, tiles + 1, diag + 2)
        end = k == 3
        c_next = jnp.minimum(jnp.where(end, c + 1, c), chunks - 1)
        i_next = pick(jnp.where(end, 0, k + 1))
        next_at = lax.div(first_row(c_next, i_next), tile) * tile

        @pl.when(late)
        def _():
            reset_state(st_s, w)

        @pl.when(jnp.logical_not(late))
        def _():
            state_copy(b).wait()

        def step(n):
            is_new, at = tile_at(diag, n)
            following = jnp.where(jnp.logical_and(n == 0, jnp.logical_not(late)), 2, n + 1)
            last = following == count
            new_next, at_next = tile_at(diag, following)
            new_next = jnp.logical_or(last, new_next)
            at_next = jnp.where(last, next_at, at_next)
            nc = jnp.where(last, c_next, c)
            ni = jnp.where(last, i_next, i)
            col = lax.broadcasted_iota(jnp.int32, (1, tile), 1) + at
            row = lax.rem(lax.broadcasted_iota(jnp.int32, (tall, 1), 0), rows) + j0
            if not isinstance(n, int):
                mask = col > jnp.where(is_new, -1, floor)
            elif n == 0:
                mask = col <= row
            else:
                mask = col > jnp.maximum(row, floor)
            flash_step(st_s, w, s_s, scale, mask, lambda g: tile_of(g, is_new, at, 1), lambda g: scores(nc, ni, g, new_next, at_next))

        step(0)

        @pl.when(late)
        def _():
            step(1)

        def further(n, carry):
            @pl.when(n < count)
            def _():
                step(n)

            return carry

        lax.fori_loop(2, tiles + 1, further, 0)
        for g in range(PAIR):
            total = jnp.sum(st_s[w, g, :, LANES:PAIR * LANES], axis=1, keepdims=True)
            out = (st_s[w, g, :, PAIR * LANES:] / total).astype(BF16)
            for h in range(PAIR):
                n = PAIR * g + h
                mix_s[:, n * hd:(n + 1) * hd] = out[h * rows:(h + 1) * rows]

        @pl.when(b + PAIR < GROUP * EARLY)
        def _():
            state_copy(b + PAIR).start()

        @pl.when(b == 0)
        def _():
            whole(wo_s, wo_sem)

        r0 = pl.multiple_of(i * rows, rows)
        for n in range(model // WIDE):
            cols = slice(n * WIDE, (n + 1) * WIDE)
            xo_s[c + 1, pl.ds(r0, rows), cols] = jnp.dot(mix_s[...], wo_s[:, cols], preferred_element_type=F32).astype(BF16)

        @pl.when(k == 0)
        def _():
            first.copy(c, 0).start()
            first.copy(c, 1).start()

        for kind in (2, 3):
            @pl.when(k == kind - 1)
            def _():
                first.copy(c, kind).start()

    gain = one_row(norms.at[layer], 2)
    shift = one_row(norms.at[layer], 3)
    bias_o = one_row(b_o, layer)
    bias_d = one_row(b_down, layer)

    def open_mlp(c):
        first.finish(c)

        def rows_at(n, carry):
            at = pl.multiple_of(n * ROW_BLOCK, ROW_BLOCK)
            middle = (mid_s[c, pl.ds(at, ROW_BLOCK), :].astype(F32) + first.total(c, at) + bias_o).astype(BF16)
            mid_s[c, pl.ds(at, ROW_BLOCK), :] = middle
            xo_s[c, pl.ds(at, ROW_BLOCK), :] = normalized(middle.astype(F32), gain, shift)
            return carry

        lax.fori_loop(0, rows // ROW_BLOCK, rows_at, 0)
        gather.start(c)

    def attend_chunk(c, carry):
        @pl.when(c == EARLY)
        def _():
            whole(big_s.at[pl.ds(0, PAIR * window)], old_sem)
            whole(mid_s, h_sem)

        def one(k, inner):
            @pl.when(jnp.logical_and(k == 3, c + 1 < chunks))
            def _():
                q_copy(c + 1).wait()

            attend(c, k)

            @pl.when(jnp.logical_and(k == 1, c >= 1))
            def _():
                first.relay(c - 1, c - 2)

            return inner

        lax.fori_loop(0, GROUP, one, 0)

        @pl.when(c + PAIR < chunks)
        def _():
            q_copy(c + PAIR).start()

        @pl.when(c >= 2)
        def _():
            open_mlp(c - 2)

        return carry

    lax.fori_loop(0, chunks, attend_chunk, 0)

    n_up = PAIR * ffn // WIDE
    n_tiles = n_up + model // WIDE
    sub = WIDE // PAIR
    n_sub = ffn // sub
    act = wo_s.at[pl.ds(0, GROUP * rows)]
    ups = (up.at[layer], up_peer)
    downs = (down.at[layer], down_peer)

    def slot_at(c, k):
        slot = lax.rem(c * n_tiles + k, WEIGHT_SLOTS)
        return slot, pl.multiple_of(slot * model, WIDE)

    def fetch(c, k):
        over = k >= n_tiles
        k = jnp.where(over, k - n_tiles, k)
        c = jnp.where(over, c + 1, c)
        slot, base = slot_at(c, k)

        @pl.when(c < chunks)
        def _():
            for part in range(PAIR):
                n = PAIR * k + part
                for side in range(PAIR):
                    @pl.when(jnp.logical_and(n >= side * n_sub, n < (side + 1) * n_sub))
                    def _():
                        at = pl.multiple_of((n - side * n_sub) * sub, sub)
                        pltpu.make_async_copy(ups[side].at[:, pl.ds(at, sub)], big_s.at[pl.ds(base, model), pl.ds(part * sub, sub)], w_sem.at[slot]).start()

            @pl.when(k >= n_up)
            def _():
                at = pl.multiple_of((k - n_up) * WIDE, WIDE)
                for side in range(PAIR):
                    dst = big_s.at[pl.ds(pl.multiple_of(base + side * ffn, sub), ffn)]
                    pltpu.make_async_copy(downs[side].at[:, pl.ds(at, WIDE)], dst, w_sem.at[slot]).start()

    def landed(c, k):
        slot, base = slot_at(c, k)
        whole(big_s.at[pl.ds(base, model)], w_sem.at[slot])
        fetch(c, k + WEIGHT_SLOTS - 1)
        return big_s[pl.ds(base, model), :]

    for k in range(WEIGHT_SLOTS - 1):
        fetch(jnp.int32(0), jnp.int32(k))
    roll_tiles = window // ROLL_ROWS

    def new_plane(k):
        return big_s[3 * window:, k * hd:(k + 1) * hd]

    stage = WEIGHT_SLOTS * model

    def stage_at(n):
        slot = lax.rem(n, ROLL_SLOTS)
        return slot, pl.ds(pl.multiple_of(stage + slot * ROLL_ROWS, ROLL_ROWS), ROLL_ROWS)

    def staged(n):
        slot, at = stage_at(n)
        whole(big_s.at[at], f_sem.at[slot])

    def put_new(n, turned):
        slot, at = stage_at(n)

        @pl.when(n >= ROLL_SLOTS)
        def _():
            staged(n)

        for k in range(PAIR):
            cols = slice(k * hd, (k + 1) * hd)
            big_s[at, cols] = turned[k]
            dst = pl.ds(pl.multiple_of(k * window + n * ROLL_ROWS, ROLL_ROWS), ROLL_ROWS)
            pltpu.make_async_copy(big_s.at[at, cols], kv_rolled.at[dst], f_sem.at[slot]).start()

    rotate(new_plane, put_new, window, window - first_slot, 0, roll_tiles // PAIR)
    gather.forward(0)
    rotate(new_plane, put_new, window, window - first_slot, roll_tiles // PAIR, roll_tiles)
    first.relay(chunks - 1, chunks - 2)
    b_copy.wait_recv()
    for n in range(PAIR * n_sub):
        src = b_up if n < n_sub else bp_s
        at = n % n_sub * sub
        b_s[n // PAIR, :, n % PAIR * sub:(n % PAIR + 1) * sub] = one_row(src, layer)[:, at:at + sub]
    open_mlp(2)
    gather.forward(1)
    open_mlp(3)

    def mlp_chunk(c, carry):
        gather.finish(c)

        def up_step(k, inner):
            weights = landed(c, k)
            for top in range(PAIR):
                r0 = top * tall
                lifted = jnp.dot(xo_s[c, r0:r0 + tall, :], weights, preferred_element_type=F32) + b_s[k]
                act[r0:r0 + tall, pl.ds(pl.multiple_of(k * WIDE, WIDE), WIDE)] = gelu_tanh(lifted).astype(BF16)
            return inner

        lax.fori_loop(0, n_up, up_step, 0)

        @pl.when(c + 2 < chunks)
        def _():
            gather.forward(c + 2)

        gather.drain(c)

        @pl.when(c >= 2)
        def _():
            second.relay(c - 2)

        def down_step(k, inner):
            weights = landed(c, k)
            at = pl.multiple_of((k - n_up) * WIDE, WIDE)
            xo_s[c, :, pl.ds(at, WIDE)] = jnp.dot(act[...], weights, preferred_element_type=F32).astype(BF16)
            return inner

        lax.fori_loop(n_up, n_tiles, down_step, 0)
        second.start(c)
        return carry

    lax.fori_loop(0, chunks, mlp_chunk, 0)

    def o_copy(c):
        return pltpu.make_async_copy(mid_s.at[c], h_out.at[pl.ds(pl.multiple_of(c * rows, rows), rows)], o_sem.at[c])

    def close(c, carry):
        @pl.when(c + 2 < chunks)
        def _():
            second.relay(c + 2)

        second.finish(c)

        def rows_at(n, inner):
            at = pl.multiple_of(n * ROW_BLOCK, ROW_BLOCK)
            mid_s[c, pl.ds(at, ROW_BLOCK), :] = (mid_s[c, pl.ds(at, ROW_BLOCK), :].astype(F32) + second.total(c, at) + bias_d).astype(BF16)
            return inner

        lax.fori_loop(0, rows // ROW_BLOCK, rows_at, 0)
        o_copy(c).start()
        return carry

    lax.fori_loop(0, chunks, close, 0)

    def settle(c, carry):
        o_copy(c).wait()
        second.drain(c)
        return carry

    lax.fori_loop(0, chunks, settle, 0)
    first.drain(chunks - 1)
    b_copy.wait_send()
    for n in range(ROLL_SLOTS):
        staged(n)


def run_block(layer, chunks, scal, q, kv_mine, kv_other, cache_mine, cache_peer, state, w_o, wo_peer, hidden, norms, b_o, b_down, b_up, up, down, up_peer, down_peer):
    model = hidden.shape[1]
    rows = hidden.shape[0] // chunks
    hd = q.shape[1]
    window = kv_mine.shape[0] // PAIR
    ffn = up_peer.shape[1]
    dims = (chunks, rows, model, hd, window, ffn)
    flops = 10 ** 11
    return pl.pallas_call(
        functools.partial(block_kernel, layer, dims),
        out_shape=(jax.ShapeDtypeStruct(hidden.shape, BF16), jax.ShapeDtypeStruct(kv_mine.shape, BF16)),
        in_specs=[SMEM] + [ANY] * 9 + [VMEM] * 4 + [ANY] * 5,
        out_specs=(ANY, ANY),
        scratch_shapes=[
            vm(PAIR * PAIR * window, WIDE),
            vm(q.shape[0] * PAIR // chunks, hd),
            vm(PAIR, PAIR * rows, KEY_TILE, dtype=F32),
            vm(rows, GROUP * hd),
            vm(GROUP * hd, model),
            vm(chunks + 1, GROUP * rows, model),
            vm(chunks, 3 * rows, model),
            vm(chunks, rows, model),
            vm(PAIR, *state.shape[1:], dtype=F32),
            vm(PAIR * ffn // WIDE, 1, WIDE, dtype=F32),
            vm(*b_up.shape),
            dma(chunks, 6),
            dma(chunks, 6),
            dma(chunks, 6),
            dma(chunks, 6),
            dma(chunks, GROUP),
            dma(chunks, GROUP),
            dma(),
            dma(),
            dma(PAIR),
            dma(),
            dma(),
            dma(PAIR),
            dma(WEIGHT_SLOTS),
            dma(),
            dma(),
            dma(chunks),
            dma(ROLL_SLOTS),
        ],
        compiler_params=pltpu.CompilerParams(vmem_limit_bytes=VMEM_LIMIT, collective_id=PAIR * layer + 1, has_side_effects=True),
        cost_estimate=pl.CostEstimate(flops=flops, bytes_accessed=90_000_000, transcendentals=0),
        name=f"block_l{layer}",
    )(scal, q, kv_mine, kv_other, cache_mine, cache_peer, state, w_o, wo_peer, hidden, norms, b_o, b_down, b_up, b_up, up, down, up_peer, down_peer)


def solution(mesh):
    row_spec = P('dp', 'tp', None)
    cache_spec = P(None, 'dp', None, 'tp', None)
    col_spec = P(None, None, 'tp')
    bias_spec = P(None, 'tp')
    in_specs = (row_spec, P('dp'), P('dp', None, None), P('dp', None, None), cache_spec, cache_spec, P('dp', None), P(), col_spec, bias_spec, col_spec, bias_spec, col_spec, bias_spec, P(None, 'tp', None), P(), col_spec, bias_spec, P(None, 'tp', None), P())
    out_specs = (row_spec, cache_spec, cache_spec, P('dp', None))

    def device_step(tokens, start_pos, cos_tab, sin_tab, key_cache, value_cache, slot_pos, norm_params, w_q, b_q, w_k, b_k, w_v, b_v, w_o, b_o, w_up, b_up, w_down, b_down):
        layers, _, window, _, hd = key_cache.shape
        cos, sin = cos_tab[0], sin_tab[0]
        kc = key_cache.reshape(layers, window, hd)
        vc = value_cache.reshape(layers, window, hd)
        hidden = tokens[0]
        fresh = []
        for layer in range(layers):
            q, kv_mine, kv_other, cache_mine, cache_peer, wo_peer, up_peer, down_peer, state = run_qkv(layer, CHUNKS, start_pos, hidden, norm_params, cos, sin, (w_q, w_k, w_v), (b_q, b_k, b_v), (kc, vc), w_o, w_up, w_down)
            hidden, kv_rolled = run_block(layer, CHUNKS, start_pos, q, kv_mine, kv_other, cache_mine, cache_peer, state, w_o, wo_peer, hidden, norm_params, b_o, b_down, b_up, w_up, w_down, up_peer, down_peer)
            fresh.append(kv_rolled)
        key_out = jnp.stack([f[:window] for f in fresh]).reshape(key_cache.shape)
        value_out = jnp.stack([f[window:] for f in fresh]).reshape(value_cache.shape)
        first_slot = start_pos[0] % window
        pos_out = (start_pos[0] + (jnp.arange(window, dtype=jnp.int32) - first_slot) % window)[None]
        return hidden[None], key_out, value_out, pos_out

    return jax.shard_map(device_step, mesh=mesh, in_specs=in_specs, out_specs=out_specs, check_vma=False)
```

```python
import functools

import jax
import jax.numpy as jnp
from jax import lax
from jax.experimental import pallas as pl
from jax.experimental.pallas import tpu as pltpu
from jax.sharding import PartitionSpec as P

NORM_EPS = 1e-5
LOG2E = 1.4426950408889634
CHUNKS = 4
KEY_TILE = 512
LANES = 128
WIDE = 512
ROW_BLOCK = 16
PAIR = 2
GROUP = 4
WEIGHT_SLOTS = 3
ROLL_ROWS = 256
ROLL_SLOTS = 4
EARLY = 2
LOWEST = -3.3e38
VMEM_LIMIT = 67_043_328
BF16 = jnp.bfloat16
F32 = jnp.float32
MESH = pl.DeviceIdType.MESH

ANY = pl.BlockSpec(memory_space=pl.ANY)
SMEM = pl.BlockSpec(memory_space=pltpu.SMEM)
VMEM = pl.BlockSpec(memory_space=pltpu.VMEM)
DMA = pltpu.SemaphoreType.DMA


def vm(*shape, dtype=BF16):
    return pltpu.VMEM(shape, dtype)


def dma(*shape):
    return DMA(shape) if shape else DMA


def whole(ref, sem):
    pltpu.make_async_copy(ref, ref, sem).wait()


def one_row(ref, n):
    return ref[pl.ds(n, 1), :].astype(F32)


def gelu_tanh(x):
    inner = 0.7978845608028654 * (x + 0.044715 * (x * x * x))
    return 0.5 * x * (1.0 + jnp.tanh(inner))


def normalized(values, gain, shift):
    centered = values - jnp.mean(values, axis=-1, keepdims=True)
    variance = jnp.mean(centered * centered, axis=-1, keepdims=True)
    return (centered * lax.rsqrt(variance + NORM_EPS) * gain + shift).astype(BF16)


def rotate(planes, put, window, shift, first, last):
    def tile(n, carry):
        want = lax.broadcasted_iota(jnp.int32, (ROLL_ROWS, 1), 0) + (n * ROLL_ROWS + shift)
        want = jnp.where(want >= window, want - window, want)
        pick = jnp.where(lax.broadcasted_iota(jnp.int32, (1, window), 1) == want, 1.0, 0.0).astype(BF16)
        put(n, [jnp.dot(pick, planes(k), preferred_element_type=F32).astype(BF16) for k in range(PAIR)])
        return carry

    lax.fori_loop(first, last, tile, 0)


def reset_state(st_s, w):
    for g in range(PAIR):
        st_s[w, g, :, 0:LANES] = jnp.full((st_s.shape[2], LANES), LOWEST, F32)
        st_s[w, g, :, LANES:] = jnp.zeros((st_s.shape[2], st_s.shape[3] - LANES), F32)


def flash_step(st_s, w, s_s, scale, mask, values, next_scores):
    for g in range(PAIR):
        s = jnp.where(mask, s_s[g] * scale, -jnp.inf)
        s_next = next_scores(g)
        m_prev = st_s[w, g, :, 0:LANES]
        m_next = jnp.maximum(m_prev, jnp.max(s, axis=1, keepdims=True))
        e = jnp.exp2(s - jnp.concatenate([m_next] * (s.shape[1] // LANES), axis=1))
        alpha = jnp.exp2(m_prev - m_next)
        total = st_s[w, g, :, LANES:2 * LANES] * alpha
        for k in range(s.shape[1] // LANES):
            total = total + e[:, k * LANES:(k + 1) * LANES]
        st_s[w, g, :, LANES:2 * LANES] = total
        st_s[w, g, :, 0:LANES] = m_next
        mixed = jnp.dot(e.astype(BF16), values(g), preferred_element_type=F32)
        st_s[w, g, :, 2 * LANES:] = st_s[w, g, :, 2 * LANES:] * jnp.concatenate([alpha] * (mixed.shape[1] // LANES), axis=1) + mixed
        s_s[g] = s_next


def score_tile(queries, keys):
    return lax.dot_general(queries, keys, (((1,), (1,)), ((), ())), preferred_element_type=F32)


class Place:
    def __init__(self):
        me = lax.axis_index('tp')
        self.core = lax.rem(me, 2)
        self.xb = lax.rem(lax.div(me, 2), 2)
        self.yb = lax.div(me, 4)
        self.peer = me + 1 - 2 * self.core
        self.x = me + 2 - 4 * self.xb
        self.y = me + 4 - 8 * self.yb

    def member(self, i):
        xb = self.xb + lax.rem(i, 2) * (1 - 2 * self.xb)
        yb = self.yb + lax.div(i, 2) * (1 - 2 * self.yb)
        return yb * 2 + xb

    def barrier(self, others):
        sem = pltpu.get_barrier_semaphore()
        for other in others:
            pl.semaphore_signal(sem, inc=1, device_id={'tp': other}, device_id_type=MESH)
        pl.semaphore_wait(sem, len(others))


def remote(src, dst, send_sem, recv_sem, other):
    return pltpu.make_async_remote_copy(src_ref=src, dst_ref=dst, send_sem=send_sem, recv_sem=recv_sem, device_id={'tp': other}, device_id_type=MESH)


class Gather:
    def __init__(self, place, x_s, send, recv, rows):
        self.place, self.x_s, self.send, self.recv, self.rows = place, x_s, send, recv, rows

    def copy(self, c, kind):
        r, h = self.rows, self.rows // 2
        src, dst, size, other = ((0, r, r, self.place.x), (0, 2 * r, r, self.place.y), (r, 3 * r, h, self.place.y), (2 * r + h, 3 * r + h, h, self.place.x))[kind]
        return remote(self.x_s.at[c, pl.ds(src, size)], self.x_s.at[c, pl.ds(dst, size)], self.send.at[c, kind], self.recv.at[c, kind], other)

    def start(self, c):
        self.copy(c, 0).start()
        self.copy(c, 1).start()

    def forward(self, c):
        self.copy(c, 0).wait_recv()
        self.copy(c, 2).start()
        self.copy(c, 1).wait_recv()
        self.copy(c, 3).start()

    def finish(self, c):
        self.copy(c, 2).wait_recv()
        self.copy(c, 3).wait_recv()

    def drain(self, c):
        for kind in range(4):
            self.copy(c, kind).wait_send()


class Scatter:
    def __init__(self, place, out_s, land_s, send, recv, rows, shift):
        self.place, self.out_s, self.land_s, self.send, self.recv, self.rows, self.shift = place, out_s, land_s, send, recv, rows, shift

    def copy(self, c, kind):
        r, h = self.rows, self.rows // 2
        x, y = self.place.x, self.place.y
        src, dst, other = ((3 * r, 2 * r, x), (3 * r + h, 2 * r + h, y), (r, 0, x), (2 * r + h, r + h, y), (r + h, h, x), (2 * r, r, y))[kind]
        return remote(self.out_s.at[c + self.shift, pl.ds(src, h)], self.land_s.at[c, pl.ds(dst, h)], self.send.at[c, kind], self.recv.at[c, kind], other)

    def start(self, c):
        for kind in range(4):
            self.copy(c, kind).start()

    def add(self, c, kind, src, dst):
        self.copy(c, kind).wait_recv()
        slot = c + self.shift

        def block(n, carry):
            at = pl.multiple_of(n * ROW_BLOCK, ROW_BLOCK)
            mine = self.out_s[slot, pl.ds(dst + at, ROW_BLOCK), :].astype(F32)
            came = self.land_s[c, pl.ds(src + at, ROW_BLOCK), :].astype(F32)
            self.out_s[slot, pl.ds(dst + at, ROW_BLOCK), :] = (mine + came).astype(BF16)
            return carry

        lax.fori_loop(0, self.rows // 2 // ROW_BLOCK, block, 0)

    def relay(self, c, settled=None):
        r, h = self.rows, self.rows // 2
        self.add(c, 0, 2 * r, 2 * r)
        self.add(c, 1, 2 * r + h, r + h)
        if settled is not None:
            @pl.when(settled >= 0)
            def _():
                self.drain(settled)

        self.copy(c, 5).start()
        self.copy(c, 4).start()

    def finish(self, c):
        for kind in range(2, 6):
            self.copy(c, kind).wait_recv()

    def drain(self, c):
        for kind in range(6):
            self.copy(c, kind).wait_send()

    def total(self, c, at):
        own = self.out_s[c + self.shift, pl.ds(at, ROW_BLOCK), :].astype(F32)
        came = [self.land_s[c, pl.ds(k * self.rows + at, ROW_BLOCK), :].astype(F32) for k in range(PAIR)]
        return own + came[0] + came[1]


def qkv_kernel(layer, dims, scal, *refs):
    chunks, rows, model, hd, window = dims
    (hidden, norms, cos, sin, wq, wk, wv, bq, bk, bv, bq_push, bk_push, bv_push, kc, vc, wo, w_up, w_down,
     q_out, kv_mine, kv_other, cache_mine, cache_peer, wo_peer, up_peer, down_peer, state,
     x_s, h_s, t_s, w_s, b_s, bq_s, bk_s, bv_s, oq_s, okv_s, old_s, oldp_s, st_s, s_s,
     ag_send, ag_recv, h_sem, t_sem, w_sem, wr_send, wr_recv, p_send, p_recv, q_sem, kv_sem, kr_send, kr_recv, raw_sem, old_sem, st_sem) = refs
    place = Place()
    block = rows * chunks
    tall = PAIR * rows
    tile = KEY_TILE
    tiles = window // tile
    scale = LOG2E * hd ** -0.5
    floor = window - 1 - scal[0]
    loads = [pltpu.make_async_copy(hidden.at[pl.ds(c * rows, rows)], h_s.at[c], h_sem.at[c]) for c in range(chunks)]
    for copy in loads:
        copy.start()
    for k, cache in enumerate((kc, vc)):
        pltpu.make_async_copy(cache.at[layer], okv_s.at[pl.ds(k * window, window)], raw_sem).start()
    place.barrier((place.x, place.y, place.peer))
    gather = Gather(place, x_s, ag_send, ag_recv, rows)
    parts = ((wq.at[layer], 0, 0, 2 * hd), (wk.at[layer], 1, 0, hd), (wv.at[layer], 1, hd, hd))
    w_local = [pltpu.make_async_copy(src, w_s.at[t, :, pl.ds(at, n)], w_sem.at[k]) for k, (src, t, at, n) in enumerate(parts)]
    w_remote = [remote(src, w_s.at[2 + t, :, pl.ds(at, n)], wr_send.at[k], wr_recv.at[k], place.peer) for k, (src, t, at, n) in enumerate(parts)]
    b_remote = [remote(src, dst, wr_send.at[3 + k], wr_recv.at[3 + k], place.peer) for k, (src, dst) in enumerate(zip((bq_push, bk_push, bv_push), (bq_s, bk_s, bv_s)))]
    landing = (wo_peer, up_peer, down_peer)
    pushes = [remote(src.at[layer], dst, p_send.at[k], p_recv.at[k], place.peer) for k, (src, dst) in enumerate(zip((wo, w_up, w_down), landing))]
    old_push = remote(old_s, oldp_s, p_send.at[3], p_recv.at[3], place.peer)
    old_store = [pltpu.make_async_copy(src, dst, old_sem.at[k]) for k, (src, dst) in enumerate(((old_s, cache_mine), (oldp_s, cache_peer)))]
    gain = one_row(norms.at[layer], 0)
    shift = one_row(norms.at[layer], 1)

    def send_own(c):
        loads[c].wait()

        def norm_block(n, carry):
            at = pl.multiple_of(n * ROW_BLOCK, ROW_BLOCK)
            x_s[c, pl.ds(at, ROW_BLOCK), :] = normalized(h_s[c, pl.ds(at, ROW_BLOCK), :].astype(F32), gain, shift)
            return carry

        lax.fori_loop(0, rows // ROW_BLOCK, norm_block, 0)
        gather.start(c)

    def chunk_pos(c, i):
        return pl.multiple_of((place.member(i) * 2 + place.core) * block + c * rows, rows)

    def kv_row(c, kv, g):
        return pl.multiple_of(((c * PAIR + kv) * PAIR + g) * GROUP * rows, rows)

    def q_row(c, g, i):
        return pl.multiple_of(((c * PAIR + g) * GROUP + i) * tall, rows)

    send_own(0)
    send_own(1)
    for copy in b_remote + w_remote + w_local + pushes:
        copy.start()
    for c in range(chunks):
        for i in range(GROUP):
            for k, tab in enumerate((cos, sin)):
                pltpu.make_async_copy(tab.at[pl.ds(chunk_pos(c, i), rows)], t_s.at[c, k, pl.ds(i * rows, rows)], t_sem.at[c]).start()
    whole(okv_s, raw_sem)
    first_slot = lax.rem(scal[0], window)
    roll_tiles = window // ROLL_ROWS

    def raw_plane(k):
        return okv_s[k * window:(k + 1) * window, :]

    def put_old(n, turned):
        for k in range(PAIR):
            old_s[pl.ds(pl.multiple_of(k * window + n * ROLL_ROWS, ROLL_ROWS), ROLL_ROWS), :] = turned[k]

    rotate(raw_plane, put_old, window, first_slot, 0, roll_tiles // 3)
    gather.forward(0)
    send_own(2)
    rotate(raw_plane, put_old, window, first_slot, roll_tiles // 3, roll_tiles)
    old_push.start()
    old_store[0].start()
    gather.forward(1)
    for copy in b_remote:
        copy.wait_recv()
    for g, (for_q, for_k, for_v) in enumerate(((bq, bk, bv), (bq_s, bk_s, bv_s))):
        b_s[PAIR * g] = one_row(for_q, layer)
        b_s[PAIR * g + 1, :, :hd] = one_row(for_k, layer)
        b_s[PAIR * g + 1, :, hd:] = one_row(for_v, layer)

    def project(c, i0, count):
        r0, n = i0 * rows, count * rows

        def rope(u):
            turned = jnp.concatenate([-u[:, hd // 2:], u[:, :hd // 2]], axis=1)
            return (u * t_s[c, 0, r0:r0 + n, :] + turned * t_s[c, 1, r0:r0 + n, :]).astype(BF16)

        def keys_values(g, carry):
            u = jnp.dot(x_s[c, r0:r0 + n, :], w_s[PAIR * g + 1], preferred_element_type=F32) + b_s[PAIR * g + 1]
            okv_s[pl.ds(pl.multiple_of(kv_row(c, 0, g) + r0, rows), n), :] = rope(u[:, :hd])
            okv_s[pl.ds(pl.multiple_of(kv_row(c, 1, g) + r0, rows), n), :] = u[:, hd:].astype(BF16)
            return carry

        def for_queries(g, carry):
            u = jnp.dot(x_s[c, r0:r0 + n, :], w_s[PAIR * g], preferred_element_type=F32) + b_s[PAIR * g]
            for h in range(PAIR):
                turned = rope(u[:, h * hd:(h + 1) * hd])
                for i in range(count):
                    oq_s[pl.ds(pl.multiple_of(q_row(c, g, i0 + i) + h * rows, rows), rows), :] = turned[i * rows:(i + 1) * rows]
            return carry

        lax.fori_loop(0, PAIR, keys_values, 0)
        for copy in kv_copies(c, range(i0, i0 + count)):
            copy.start()
        lax.fori_loop(0, PAIR, for_queries, 0)

    def q_copy(c):
        part = pl.ds(q_row(c, 0, 0), PAIR * GROUP * tall)
        return pltpu.make_async_copy(oq_s.at[part], q_out.at[part], q_sem.at[c])

    def kv_copies(c, blocks):
        planes = (kv_mine, kv_other)
        made = []
        for kv in range(PAIR):
            for g in range(PAIR):
                for i in blocks:
                    src = okv_s.at[pl.ds(pl.multiple_of(kv_row(c, kv, g) + i * rows, rows), rows)]
                    at = pl.ds(pl.multiple_of(kv * window + chunk_pos(c, i), rows), rows)
                    made.append(pltpu.make_async_copy(src, planes[g].at[at], kv_sem.at[c]))
                    made.append(remote(src, planes[1 - g].at[at], kr_send.at[c], kr_recv.at[c], place.peer))
        return made

    def old_tile(g, kv, at):
        return (old_s, oldp_s)[g][pl.ds(pl.multiple_of(kv * window + at, tile), tile), :]

    def queries(c, i, g):
        return oq_s[pl.ds(q_row(c, g, i), tall), :]

    def state_copy(b):
        return pltpu.make_async_copy(st_s.at[lax.rem(b, PAIR)], state.at[b], st_sem.at[lax.rem(b, PAIR)])

    def start_old(c, i):
        at = pl.multiple_of(lax.div(chunk_pos(c, i), tile) * tile, tile)
        for g in range(PAIR):
            s_s[g] = score_tile(queries(c, i, g), old_tile(g, 0, at))

    def attend_old(c, i):
        b = c * GROUP + i
        w = lax.rem(b, PAIR)
        j0 = chunk_pos(c, i)
        diag = lax.div(j0, tile)
        i_next = jnp.minimum(i + 1, 3)
        diag_next = lax.div(chunk_pos(c, i_next), tile)

        @pl.when(b >= 2)
        def _():
            state_copy(b - 2).wait()

        reset_state(st_s, w)

        def step(t, by_row):
            at = pl.multiple_of(t * tile, tile)
            last = t + 1 == tiles
            n_at = pl.multiple_of(jnp.where(last, diag_next, t + 1) * tile, tile)
            n_i = jnp.where(last, i_next, i)
            age = lax.broadcasted_iota(jnp.int32, (1, tile), 1) + at
            if by_row:
                row = lax.rem(lax.broadcasted_iota(jnp.int32, (tall, 1), 0), rows) + j0
                mask = age > jnp.maximum(row, floor)
            else:
                mask = age > floor
            flash_step(st_s, w, s_s, scale, mask, lambda g: old_tile(g, 1, at), lambda g: score_tile(queries(c, n_i, g), old_tile(g, 0, n_at)))

        step(diag, True)

        def younger(t, carry):
            @pl.when(t > diag)
            def _():
                step(t, False)

            return carry

        lax.fori_loop(1, tiles, younger, 0)
        state_copy(b).start()

    def chunk(c, carry):
        whole(t_s.at[c], t_sem.at[c])

        @pl.when(c == 0)
        def _():
            for copy in w_local:
                copy.wait()
            for copy in w_remote:
                copy.wait_recv()

        project(c, 0, 3)
        gather.finish(c)
        project(c, 3, 1)
        q_copy(c).start()

        @pl.when(c == 0)
        def _():
            old_push.wait_recv()
            old_store[1].start()

        @pl.when(lax.rem(c, 2) == 0)
        def _():
            early = lax.div(c, 2)
            start_old(early, 0)

            def one(i, inner):
                @pl.when(jnp.logical_and(c == 2, i == 3))
                def _():
                    gather.forward(3)

                attend_old(early, i)
                return inner

            lax.fori_loop(0, 4, one, 0)

        @pl.when(c == 0)
        def _():
            gather.forward(2)
            send_own(3)

        return carry

    lax.fori_loop(0, chunks, chunk, 0)
    for copy in w_remote + b_remote:
        copy.wait_send()

    def settle(c, carry):
        q_copy(c).wait()
        part = okv_s.at[pl.ds(kv_row(c, 0, 0), PAIR * PAIR * GROUP * rows)]
        whole(part, kv_sem.at[c])
        remote(part, part, kr_send.at[c], kr_recv.at[c], place.peer).wait_send()
        remote(part, part, kr_send.at[c], kr_recv.at[c], place.peer).wait_recv()
        gather.drain(c)
        return carry

    lax.fori_loop(0, chunks, settle, 0)
    for copy in pushes:
        copy.wait_send()
        copy.wait_recv()
    old_push.wait_send()
    for copy in old_store:
        copy.wait()
    for b in (GROUP * EARLY - 2, GROUP * EARLY - 1):
        state_copy(b).wait()


def run_qkv(layer, chunks, scal, hidden, norms, cos, sin, weights, biases, caches, w_o, w_up, w_down):
    model = hidden.shape[1]
    rows = hidden.shape[0] // chunks
    hd = cos.shape[1]
    window = cos.shape[0]
    dims = (chunks, rows, model, hd, window)
    flops = 2 * 4 * rows * chunks * model * 8 * hd
    planes = (PAIR * window, hd)
    shapes = [(chunks * PAIR * GROUP * PAIR * rows, hd)] + [planes] * 4 + [w.shape[1:] for w in (w_o, w_up, w_down)]
    state = (GROUP * EARLY, PAIR, PAIR * rows, PAIR * LANES + hd)
    return pl.pallas_call(
        functools.partial(qkv_kernel, layer, dims),
        out_shape=tuple(jax.ShapeDtypeStruct(s, BF16) for s in shapes) + (jax.ShapeDtypeStruct(state, F32),),
        in_specs=[SMEM, ANY, VMEM] + [ANY] * 5 + [VMEM] * 3 + [ANY] * 8,
        out_specs=(ANY,) * (len(shapes) + 1),
        scratch_shapes=[
            vm(chunks, GROUP * rows, model),
            vm(chunks, rows, model),
            vm(chunks, PAIR, GROUP * rows, hd, dtype=F32),
            vm(GROUP, model, PAIR * hd),
            vm(GROUP, 1, PAIR * hd, dtype=F32),
            *(vm(*b.shape) for b in biases),
            vm(*shapes[0]),
            vm(chunks * PAIR * PAIR * GROUP * rows, hd),
            vm(*planes),
            vm(*planes),
            vm(PAIR, *state[1:], dtype=F32),
            vm(PAIR, PAIR * rows, KEY_TILE, dtype=F32),
            dma(chunks, GROUP),
            dma(chunks, GROUP),
            dma(chunks),
            dma(chunks),
            dma(3),
            dma(6),
            dma(6),
            dma(GROUP),
            dma(GROUP),
            dma(chunks),
            dma(chunks),
            dma(chunks),
            dma(chunks),
            dma(),
            dma(PAIR),
            dma(PAIR),
        ],
        compiler_params=pltpu.CompilerParams(vmem_limit_bytes=VMEM_LIMIT, collective_id=PAIR * layer, has_side_effects=True),
        cost_estimate=pl.CostEstimate(flops=4 * flops, bytes_accessed=20_000_000, transcendentals=0),
        name=f"qkv_l{layer}",
    )(scal, hidden, norms, cos, sin, *weights, *biases, *biases, *caches, w_o, w_up, w_down)


def block_kernel(layer, dims, scal, *refs):
    chunks, rows, model, hd, window, ffn = dims
    (q, kv_mine, kv_other, cache_mine, cache_peer, state, wo, wo_peer, hidden, norms, b_o, b_down, b_up, b_push, up, down, up_peer, down_peer,
     h_out, kv_rolled,
     big_s, q_s, s_s, mix_s, wo_s, xo_s, land_s, mid_s, st_s, b_s, bp_s,
     r1_send, r1_recv, r2_send, r2_recv, ag_send, ag_recv, new_sem, old_sem, q_sem, wo_sem, h_sem, st_sem, w_sem, b_send, b_recv, o_sem, f_sem) = refs
    place = Place()
    start_pos = scal[0]
    block = rows * chunks
    tall = PAIR * rows
    tile = KEY_TILE
    tiles = window // tile
    scale = LOG2E * hd ** -0.5

    def region(g, new):
        return jnp.where(new, (3 - g) * window, g * window)

    def load_planes(src, base, sem):
        for k in range(PAIR):
            pltpu.make_async_copy(src.at[pl.ds(k * window, window)], big_s.at[pl.ds(base, window), pl.ds(k * hd, hd)], sem).start()

    q_rows = PAIR * GROUP * tall

    def q_copy(c):
        slot = lax.rem(c, PAIR)
        src, dst = (pl.ds(pl.multiple_of(n * q_rows, rows), q_rows) for n in (c, slot))
        return pltpu.make_async_copy(q.at[src], q_s.at[dst], q_sem.at[slot])

    q_copy(jnp.int32(0)).start()
    q_copy(jnp.int32(1)).start()
    load_planes(kv_mine, 3 * window, new_sem)
    load_planes(kv_other, PAIR * window, new_sem)

    chip = place.member(0)
    lowest = jnp.where(chip < 2, 1, chip)
    middle = jnp.where(jnp.logical_or(chip == 0, chip == 3), 2, 3)

    def pick(c, k):
        by_place = jnp.where(k == 0, lowest, jnp.where(k == 1, middle, 6 - lowest - middle))
        diagonal = jnp.where(k == 0, 3, k)
        return jnp.where(k == 3, 0, jnp.where(c == 0, by_place, diagonal))

    def state_copy(b):
        slot = lax.rem(b, PAIR)
        c = lax.div(b, GROUP)
        return pltpu.make_async_copy(state.at[c * GROUP + pick(c, lax.rem(b, GROUP))], st_s.at[slot], st_sem.at[slot])

    for b in range(PAIR):
        state_copy(jnp.int32(b)).start()
    pltpu.make_async_copy(wo.at[layer], wo_s.at[pl.ds(0, PAIR * hd)], wo_sem).start()
    pltpu.make_async_copy(wo_peer, wo_s.at[pl.ds(PAIR * hd, PAIR * hd)], wo_sem).start()
    load_planes(cache_mine, 0, old_sem)
    load_planes(cache_peer, window, old_sem)
    for c in range(chunks):
        pltpu.make_async_copy(hidden.at[pl.ds(c * rows, rows)], mid_s.at[c], h_sem).start()
    place.barrier((place.x, place.y, place.peer))
    b_copy = remote(b_push, bp_s, b_send, b_recv, place.peer)
    b_copy.start()
    first = Scatter(place, xo_s, land_s, r1_send, r1_recv, rows, 1)
    second = Scatter(place, xo_s, land_s, r2_send, r2_recv, rows, 0)
    gather = Gather(place, xo_s, ag_send, ag_recv, rows)
    first_slot = lax.rem(start_pos, window)
    floor = window - 1 - start_pos

    def first_row(c, i):
        return (place.member(i) * PAIR + place.core) * block + c * rows

    def tile_at(diag, n):
        is_new = jnp.logical_or(n == 0, jnp.logical_and(n >= 2, n - 2 < diag))
        t = jnp.where(n < 2, diag, jnp.where(is_new, n - 2, n - 1))
        return is_new, t * tile

    def tile_of(g, is_new, at, kv):
        return big_s[pl.ds(pl.multiple_of(region(g, is_new) + at, tile), tile), kv * hd:(kv + 1) * hd]

    def scores(c, i, g, is_new, at):
        r0 = pl.multiple_of(((lax.rem(c, PAIR) * PAIR + g) * GROUP + i) * tall, rows)
        return score_tile(q_s[pl.ds(r0, tall), :], tile_of(g, is_new, at, 0))

    q_copy(jnp.int32(0)).wait()
    whole(big_s.at[pl.ds(0, PAIR * window)], new_sem)
    for g in range(PAIR):
        s_s[g] = scores(jnp.int32(0), lowest, g, True, lax.div(first_row(0, lowest), tile) * tile)

    def attend(c, k):
        i = pick(c, k)
        b = c * GROUP + k
        w = lax.rem(b, PAIR)
        late = c >= EARLY
        j0 = first_row(c, i)
        diag = lax.div(j0, tile)
        count = jnp.where(late, tiles + 1, diag + 2)
        end = k == 3
        c_next = jnp.minimum(jnp.where(end, c + 1, c), chunks - 1)
        i_next = pick(c_next, jnp.where(end, 0, k + 1))
        next_at = lax.div(first_row(c_next, i_next), tile) * tile

        @pl.when(late)
        def _():
            reset_state(st_s, w)

        @pl.when(jnp.logical_not(late))
        def _():
            state_copy(b).wait()

        def step(n):
            is_new, at = tile_at(diag, n)
            following = jnp.where(jnp.logical_and(n == 0, jnp.logical_not(late)), 2, n + 1)
            last = following == count
            new_next, at_next = tile_at(diag, following)
            new_next = jnp.logical_or(last, new_next)
            at_next = jnp.where(last, next_at, at_next)
            nc = jnp.where(last, c_next, c)
            ni = jnp.where(last, i_next, i)
            col = lax.broadcasted_iota(jnp.int32, (1, tile), 1) + at
            row = lax.rem(lax.broadcasted_iota(jnp.int32, (tall, 1), 0), rows) + j0
            if not isinstance(n, int):
                mask = col > jnp.where(is_new, -1, floor)
            elif n == 0:
                mask = col <= row
            else:
                mask = col > jnp.maximum(row, floor)
            flash_step(st_s, w, s_s, scale, mask, lambda g: tile_of(g, is_new, at, 1), lambda g: scores(nc, ni, g, new_next, at_next))

        step(0)

        @pl.when(late)
        def _():
            step(1)

        def further(n, carry):
            @pl.when(n < count)
            def _():
                step(n)

            return carry

        lax.fori_loop(2, tiles + 1, further, 0)
        for g in range(PAIR):
            total = jnp.sum(st_s[w, g, :, LANES:PAIR * LANES], axis=1, keepdims=True)
            out = (st_s[w, g, :, PAIR * LANES:] / total).astype(BF16)
            for h in range(PAIR):
                n = PAIR * g + h
                mix_s[:, n * hd:(n + 1) * hd] = out[h * rows:(h + 1) * rows]

        @pl.when(b + PAIR < GROUP * EARLY)
        def _():
            state_copy(b + PAIR).start()

        @pl.when(b == 0)
        def _():
            whole(wo_s, wo_sem)

        r0 = pl.multiple_of(i * rows, rows)
        for n in range(model // WIDE):
            cols = slice(n * WIDE, (n + 1) * WIDE)
            xo_s[c + 1, pl.ds(r0, rows), cols] = jnp.dot(mix_s[...], wo_s[:, cols], preferred_element_type=F32).astype(BF16)

        @pl.when(i == 3)
        def _():
            first.copy(c, 0).start()
            first.copy(c, 1).start()

        for kind in (2, 3):
            @pl.when(i == kind - 1)
            def _():
                first.copy(c, kind).start()

    gain = one_row(norms.at[layer], 2)
    shift = one_row(norms.at[layer], 3)
    bias_o = one_row(b_o, layer)
    bias_d = one_row(b_down, layer)

    def open_mlp(c):
        first.finish(c)

        def rows_at(n, carry):
            at = pl.multiple_of(n * ROW_BLOCK, ROW_BLOCK)
            middle = (mid_s[c, pl.ds(at, ROW_BLOCK), :].astype(F32) + first.total(c, at) + bias_o).astype(BF16)
            mid_s[c, pl.ds(at, ROW_BLOCK), :] = middle
            xo_s[c, pl.ds(at, ROW_BLOCK), :] = normalized(middle.astype(F32), gain, shift)
            return carry

        lax.fori_loop(0, rows // ROW_BLOCK, rows_at, 0)
        gather.start(c)

    def attend_chunk(c, carry):
        @pl.when(c == EARLY)
        def _():
            whole(big_s.at[pl.ds(0, PAIR * window)], old_sem)
            whole(mid_s, h_sem)

        def one(k, inner):
            @pl.when(jnp.logical_and(k == 3, c + 1 < chunks))
            def _():
                q_copy(c + 1).wait()

            attend(c, k)

            @pl.when(jnp.logical_and(k == 1, c >= 1))
            def _():
                first.relay(c - 1, c - 2)

            return inner

        lax.fori_loop(0, GROUP, one, 0)

        @pl.when(c + PAIR < chunks)
        def _():
            q_copy(c + PAIR).start()

        @pl.when(c >= 2)
        def _():
            open_mlp(c - 2)

        return carry

    lax.fori_loop(0, chunks, attend_chunk, 0)

    n_up = PAIR * ffn // WIDE
    n_tiles = n_up + model // WIDE
    sub = WIDE // PAIR
    n_sub = ffn // sub
    act = wo_s.at[pl.ds(0, GROUP * rows)]
    ups = (up.at[layer], up_peer)
    downs = (down.at[layer], down_peer)

    def slot_at(c, k):
        slot = lax.rem(c * n_tiles + k, WEIGHT_SLOTS)
        return slot, pl.multiple_of(slot * model, WIDE)

    def fetch(c, k):
        over = k >= n_tiles
        k = jnp.where(over, k - n_tiles, k)
        c = jnp.where(over, c + 1, c)
        slot, base = slot_at(c, k)

        @pl.when(c < chunks)
        def _():
            for part in range(PAIR):
                n = PAIR * k + part
                for side in range(PAIR):
                    @pl.when(jnp.logical_and(n >= side * n_sub, n < (side + 1) * n_sub))
                    def _():
                        at = pl.multiple_of((n - side * n_sub) * sub, sub)
                        pltpu.make_async_copy(ups[side].at[:, pl.ds(at, sub)], big_s.at[pl.ds(base, model), pl.ds(part * sub, sub)], w_sem.at[slot]).start()

            @pl.when(k >= n_up)
            def _():
                at = pl.multiple_of((k - n_up) * WIDE, WIDE)
                for side in range(PAIR):
                    dst = big_s.at[pl.ds(pl.multiple_of(base + side * ffn, sub), ffn)]
                    pltpu.make_async_copy(downs[side].at[:, pl.ds(at, WIDE)], dst, w_sem.at[slot]).start()

    def landed(c, k):
        slot, base = slot_at(c, k)
        whole(big_s.at[pl.ds(base, model)], w_sem.at[slot])
        fetch(c, k + WEIGHT_SLOTS - 1)
        return big_s[pl.ds(base, model), :]

    for k in range(WEIGHT_SLOTS - 1):
        fetch(jnp.int32(0), jnp.int32(k))
    roll_tiles = window // ROLL_ROWS

    def new_plane(k):
        return big_s[3 * window:, k * hd:(k + 1) * hd]

    stage = WEIGHT_SLOTS * model

    def stage_at(n):
        slot = lax.rem(n, ROLL_SLOTS)
        return slot, pl.ds(pl.multiple_of(stage + slot * ROLL_ROWS, ROLL_ROWS), ROLL_ROWS)

    def staged(n):
        slot, at = stage_at(n)
        whole(big_s.at[at], f_sem.at[slot])

    def put_new(n, turned):
        slot, at = stage_at(n)

        @pl.when(n >= ROLL_SLOTS)
        def _():
            staged(n)

        for k in range(PAIR):
            cols = slice(k * hd, (k + 1) * hd)
            big_s[at, cols] = turned[k]
            dst = pl.ds(pl.multiple_of(k * window + n * ROLL_ROWS, ROLL_ROWS), ROLL_ROWS)
            pltpu.make_async_copy(big_s.at[at, cols], kv_rolled.at[dst], f_sem.at[slot]).start()

    rotate(new_plane, put_new, window, window - first_slot, 0, roll_tiles // PAIR)
    gather.forward(0)
    rotate(new_plane, put_new, window, window - first_slot, roll_tiles // PAIR, roll_tiles)
    first.relay(chunks - 1, chunks - 2)
    b_copy.wait_recv()
    for n in range(PAIR * n_sub):
        src = b_up if n < n_sub else bp_s
        at = n % n_sub * sub
        b_s[n // PAIR, :, n % PAIR * sub:(n % PAIR + 1) * sub] = one_row(src, layer)[:, at:at + sub]
    open_mlp(2)
    gather.forward(1)
    open_mlp(3)

    def mlp_chunk(c, carry):
        gather.finish(c)

        def up_step(k, inner):
            weights = landed(c, k)
            for top in range(PAIR):
                r0 = top * tall
                lifted = jnp.dot(xo_s[c, r0:r0 + tall, :], weights, preferred_element_type=F32) + b_s[k]
                act[r0:r0 + tall, pl.ds(pl.multiple_of(k * WIDE, WIDE), WIDE)] = gelu_tanh(lifted).astype(BF16)
            return inner

        lax.fori_loop(0, n_up, up_step, 0)

        @pl.when(c + 2 < chunks)
        def _():
            gather.forward(c + 2)

        gather.drain(c)

        @pl.when(c >= 2)
        def _():
            second.relay(c - 2)

        def down_step(k, inner):
            weights = landed(c, k)
            at = pl.multiple_of((k - n_up) * WIDE, WIDE)
            xo_s[c, :, pl.ds(at, WIDE)] = jnp.dot(act[...], weights, preferred_element_type=F32).astype(BF16)
            return inner

        lax.fori_loop(n_up, n_tiles, down_step, 0)
        second.start(c)
        return carry

    lax.fori_loop(0, chunks, mlp_chunk, 0)

    def o_copy(c):
        return pltpu.make_async_copy(mid_s.at[c], h_out.at[pl.ds(pl.multiple_of(c * rows, rows), rows)], o_sem.at[c])

    def close(c, carry):
        @pl.when(c + 2 < chunks)
        def _():
            second.relay(c + 2)

        second.finish(c)

        def rows_at(n, inner):
            at = pl.multiple_of(n * ROW_BLOCK, ROW_BLOCK)
            mid_s[c, pl.ds(at, ROW_BLOCK), :] = (mid_s[c, pl.ds(at, ROW_BLOCK), :].astype(F32) + second.total(c, at) + bias_d).astype(BF16)
            return inner

        lax.fori_loop(0, rows // ROW_BLOCK, rows_at, 0)
        o_copy(c).start()
        return carry

    lax.fori_loop(0, chunks, close, 0)

    def settle(c, carry):
        o_copy(c).wait()
        second.drain(c)
        return carry

    lax.fori_loop(0, chunks, settle, 0)
    first.drain(chunks - 1)
    b_copy.wait_send()
    for n in range(ROLL_SLOTS):
        staged(n)


def run_block(layer, chunks, scal, q, kv_mine, kv_other, cache_mine, cache_peer, state, w_o, wo_peer, hidden, norms, b_o, b_down, b_up, up, down, up_peer, down_peer):
    model = hidden.shape[1]
    rows = hidden.shape[0] // chunks
    hd = q.shape[1]
    window = kv_mine.shape[0] // PAIR
    ffn = up_peer.shape[1]
    dims = (chunks, rows, model, hd, window, ffn)
    flops = 10 ** 11
    return pl.pallas_call(
        functools.partial(block_kernel, layer, dims),
        out_shape=(jax.ShapeDtypeStruct(hidden.shape, BF16), jax.ShapeDtypeStruct(kv_mine.shape, BF16)),
        in_specs=[SMEM] + [ANY] * 9 + [VMEM] * 4 + [ANY] * 5,
        out_specs=(ANY, ANY),
        scratch_shapes=[
            vm(PAIR * PAIR * window, WIDE),
            vm(q.shape[0] * PAIR // chunks, hd),
            vm(PAIR, PAIR * rows, KEY_TILE, dtype=F32),
            vm(rows, GROUP * hd),
            vm(GROUP * hd, model),
            vm(chunks + 1, GROUP * rows, model),
            vm(chunks, 3 * rows, model),
            vm(chunks, rows, model),
            vm(PAIR, *state.shape[1:], dtype=F32),
            vm(PAIR * ffn // WIDE, 1, WIDE, dtype=F32),
            vm(*b_up.shape),
            dma(chunks, 6),
            dma(chunks, 6),
            dma(chunks, 6),
            dma(chunks, 6),
            dma(chunks, GROUP),
            dma(chunks, GROUP),
            dma(),
            dma(),
            dma(PAIR),
            dma(),
            dma(),
            dma(PAIR),
            dma(WEIGHT_SLOTS),
            dma(),
            dma(),
            dma(chunks),
            dma(ROLL_SLOTS),
        ],
        compiler_params=pltpu.CompilerParams(vmem_limit_bytes=VMEM_LIMIT, collective_id=PAIR * layer + 1, has_side_effects=True),
        cost_estimate=pl.CostEstimate(flops=flops, bytes_accessed=90_000_000, transcendentals=0),
        name=f"block_l{layer}",
    )(scal, q, kv_mine, kv_other, cache_mine, cache_peer, state, w_o, wo_peer, hidden, norms, b_o, b_down, b_up, b_up, up, down, up_peer, down_peer)


def copy_kernel(scal, *refs):
    hidden, kvs = refs[0], refs[1:-8]
    h_out, k_out, v_out, p_out, h_s, kv_s, in_sem, out_sem = refs[-8:]
    window = k_out.shape[1]
    cut = window // PAIR
    part = hidden.shape[0] // PAIR
    moves = [(hidden.at[pl.ds(n * part, part)], h_s.at[pl.ds(n * part, part)], h_out.at[pl.ds(n * part, part)]) for n in range(PAIR)]
    for layer, kv in enumerate(kvs):
        for k, out in enumerate((k_out, v_out)):
            for n in range(PAIR):
                at = pl.ds(k * window + n * cut, cut)
                moves.append((kv.at[at], kv_s.at[layer, at], out.at[layer, pl.ds(n * cut, cut)]))
    for n, (src, mid, _) in enumerate(moves):
        pltpu.make_async_copy(src, mid, in_sem.at[n]).start()
    start_pos = scal[0]
    ahead = lax.broadcasted_iota(jnp.int32, p_out.shape, 1) + (window - lax.rem(start_pos, window))
    p_out[...] = start_pos + jnp.where(ahead >= window, ahead - window, ahead)
    for n, (src, mid, dst) in enumerate(moves):
        pltpu.make_async_copy(src, mid, in_sem.at[n]).wait()
        pltpu.make_async_copy(mid, dst, out_sem.at[n]).start()
    for n, (_, mid, dst) in enumerate(moves):
        pltpu.make_async_copy(mid, dst, out_sem.at[n]).wait()


def run_copy(scal, hidden, kvs, window):
    layers, hd = len(kvs), kvs[0].shape[1]
    planes = jax.ShapeDtypeStruct((layers, window, hd), BF16)
    count = PAIR + PAIR * PAIR * layers
    return pl.pallas_call(
        copy_kernel,
        out_shape=(jax.ShapeDtypeStruct(hidden.shape, BF16), planes, planes, jax.ShapeDtypeStruct((1, window), jnp.int32)),
        in_specs=[SMEM] + [ANY] * (1 + layers),
        out_specs=(ANY, ANY, ANY, VMEM),
        scratch_shapes=[vm(*hidden.shape), vm(layers, PAIR * window, hd), dma(count), dma(count)],
        compiler_params=pltpu.CompilerParams(vmem_limit_bytes=VMEM_LIMIT),
        name="copy_out",
    )(scal, hidden, *kvs)


def solution(mesh):
    row_spec = P('dp', 'tp', None)
    cache_spec = P(None, 'dp', None, 'tp', None)
    col_spec = P(None, None, 'tp')
    bias_spec = P(None, 'tp')
    in_specs = (row_spec, P('dp'), P('dp', None, None), P('dp', None, None), cache_spec, cache_spec, P('dp', None), P(), col_spec, bias_spec, col_spec, bias_spec, col_spec, bias_spec, P(None, 'tp', None), P(), col_spec, bias_spec, P(None, 'tp', None), P())
    out_specs = (row_spec, cache_spec, cache_spec, P('dp', None))

    def device_step(tokens, start_pos, cos_tab, sin_tab, key_cache, value_cache, slot_pos, norm_params, w_q, b_q, w_k, b_k, w_v, b_v, w_o, b_o, w_up, b_up, w_down, b_down):
        layers, _, window, _, hd = key_cache.shape
        cos, sin = cos_tab[0], sin_tab[0]
        kc = key_cache.reshape(layers, window, hd)
        vc = value_cache.reshape(layers, window, hd)
        hidden = tokens[0]
        fresh = []
        for layer in range(layers):
            q, kv_mine, kv_other, cache_mine, cache_peer, wo_peer, up_peer, down_peer, state = run_qkv(layer, CHUNKS, start_pos, hidden, norm_params, cos, sin, (w_q, w_k, w_v), (b_q, b_k, b_v), (kc, vc), w_o, w_up, w_down)
            hidden, kv_rolled = run_block(layer, CHUNKS, start_pos, q, kv_mine, kv_other, cache_mine, cache_peer, state, w_o, wo_peer, hidden, norm_params, b_o, b_down, b_up, w_up, w_down, up_peer, down_peer)
            fresh.append(kv_rolled)
        hidden, key_out, value_out, pos_out = run_copy(start_pos, hidden, fresh, window)
        return hidden[None], key_out.reshape(key_cache.shape), value_out.reshape(value_cache.shape), pos_out

    return jax.shard_map(device_step, mesh=mesh, in_specs=in_specs, out_specs=out_specs, check_vma=False)
```

```python
import functools

import jax
import jax.numpy as jnp
from jax import lax
from jax.experimental import pallas as pl
from jax.experimental.pallas import tpu as pltpu
from jax.sharding import PartitionSpec as P

NORM_EPS = 1e-5
LOG2E = 1.4426950408889634
CHUNKS = 4
KEY_TILE = 512
LANES = 128
WIDE = 512
ROW_BLOCK = 16
PAIR = 2
GROUP = 4
WEIGHT_SLOTS = 3
SLOTS = 5
ROLL_ROWS = 256
ROLL_SLOTS = 4
EARLY = 2
LOWEST = -3.3e38
VMEM_LIMIT = 67_043_328
BF16 = jnp.bfloat16
F32 = jnp.float32
MESH = pl.DeviceIdType.MESH

ANY = pl.BlockSpec(memory_space=pl.ANY)
SMEM = pl.BlockSpec(memory_space=pltpu.SMEM)
VMEM = pl.BlockSpec(memory_space=pltpu.VMEM)
DMA = pltpu.SemaphoreType.DMA


def vm(*shape, dtype=BF16):
    return pltpu.VMEM(shape, dtype)


def dma(*shape):
    return DMA(shape) if shape else DMA


def whole(ref, sem):
    pltpu.make_async_copy(ref, ref, sem).wait()


def one_row(ref, n):
    return ref[pl.ds(n, 1), :].astype(F32)


def gelu_tanh(x):
    inner = 0.7978845608028654 * (x + 0.044715 * (x * x * x))
    return 0.5 * x * (1.0 + jnp.tanh(inner))


def normalized(values, gain, shift):
    centered = values - jnp.mean(values, axis=-1, keepdims=True)
    variance = jnp.mean(centered * centered, axis=-1, keepdims=True)
    return (centered * lax.rsqrt(variance + NORM_EPS) * gain + shift).astype(BF16)


def rotate(planes, put, window, shift, first, last):
    def tile(n, carry):
        want = lax.broadcasted_iota(jnp.int32, (ROLL_ROWS, 1), 0) + (n * ROLL_ROWS + shift)
        want = jnp.where(want >= window, want - window, want)
        pick = jnp.where(lax.broadcasted_iota(jnp.int32, (1, window), 1) == want, 1.0, 0.0).astype(BF16)
        put(n, [jnp.dot(pick, plane(), preferred_element_type=F32).astype(BF16) for plane in planes])
        return carry

    lax.fori_loop(first, last, tile, 0)


def reset_state(st_s, w):
    for g in range(PAIR):
        st_s[w, g, :, 0:LANES] = jnp.full((st_s.shape[2], LANES), LOWEST, F32)
        st_s[w, g, :, LANES:] = jnp.zeros((st_s.shape[2], st_s.shape[3] - LANES), F32)


def flash_step(st_s, w, s_s, scale, mask, values, next_scores):
    for g in range(PAIR):
        s = jnp.where(mask, s_s[g] * scale, -jnp.inf)
        s_next = next_scores(g)
        m_prev = st_s[w, g, :, 0:LANES]
        m_next = jnp.maximum(m_prev, jnp.max(s, axis=1, keepdims=True))
        e = jnp.exp2(s - jnp.concatenate([m_next] * (s.shape[1] // LANES), axis=1))
        alpha = jnp.exp2(m_prev - m_next)
        total = st_s[w, g, :, LANES:2 * LANES] * alpha
        for k in range(s.shape[1] // LANES):
            total = total + e[:, k * LANES:(k + 1) * LANES]
        st_s[w, g, :, LANES:2 * LANES] = total
        st_s[w, g, :, 0:LANES] = m_next
        mixed = jnp.dot(e.astype(BF16), values(g), preferred_element_type=F32)
        st_s[w, g, :, 2 * LANES:] = st_s[w, g, :, 2 * LANES:] * jnp.concatenate([alpha] * (mixed.shape[1] // LANES), axis=1) + mixed
        s_s[g] = s_next


def score_tile(queries, keys):
    return lax.dot_general(queries, keys, (((1,), (1,)), ((), ())), preferred_element_type=F32)


class Place:
    def __init__(self):
        me = lax.axis_index('tp')
        self.core = lax.rem(me, 2)
        self.xb = lax.rem(lax.div(me, 2), 2)
        self.yb = lax.div(me, 4)
        self.peer = me + 1 - 2 * self.core
        self.x = me + 2 - 4 * self.xb
        self.y = me + 4 - 8 * self.yb

    def member(self, i):
        xb = self.xb + lax.rem(i, 2) * (1 - 2 * self.xb)
        yb = self.yb + lax.div(i, 2) * (1 - 2 * self.yb)
        return yb * 2 + xb

    def barrier(self, others):
        sem = pltpu.get_barrier_semaphore()
        for other in others:
            pl.semaphore_signal(sem, inc=1, device_id={'tp': other}, device_id_type=MESH)
        pl.semaphore_wait(sem, len(others))


def remote(src, dst, send_sem, recv_sem, other):
    return pltpu.make_async_remote_copy(src_ref=src, dst_ref=dst, send_sem=send_sem, recv_sem=recv_sem, device_id={'tp': other}, device_id_type=MESH)


class Gather:
    def __init__(self, place, x_s, slot, send, recv, rows):
        self.place, self.x_s, self.slot, self.send, self.recv, self.rows = place, x_s, slot, send, recv, rows

    def copy(self, c, kind):
        r, h = self.rows, self.rows // 2
        src, dst, size, other = ((0, r, r, self.place.x), (0, 2 * r, r, self.place.y), (r, 3 * r, h, self.place.y), (2 * r + h, 3 * r + h, h, self.place.x))[kind]
        slot = self.slot(c)
        return remote(self.x_s.at[slot, pl.ds(src, size)], self.x_s.at[slot, pl.ds(dst, size)], self.send.at[c, kind], self.recv.at[c, kind], other)

    def start(self, c):
        self.copy(c, 0).start()
        self.copy(c, 1).start()

    def forward(self, c):
        self.copy(c, 0).wait_recv()
        self.copy(c, 2).start()
        self.copy(c, 1).wait_recv()
        self.copy(c, 3).start()

    def finish(self, c):
        self.copy(c, 2).wait_recv()
        self.copy(c, 3).wait_recv()

    def drain(self, c):
        for kind in range(GROUP):
            self.copy(c, kind).wait_send()


class Scatter:
    def __init__(self, place, out_s, slot, land_s, send, recv, rows):
        self.place, self.out_s, self.slot, self.land_s, self.send, self.recv, self.rows = place, out_s, slot, land_s, send, recv, rows

    def copy(self, c, kind):
        r, h = self.rows, self.rows // 2
        x, y = self.place.x, self.place.y
        src, dst, other = ((3 * r, 2 * r, x), (3 * r + h, 2 * r + h, y), (r, 0, x), (2 * r + h, r + h, y), (r + h, h, x), (2 * r, r, y))[kind]
        return remote(self.out_s.at[self.slot(c), pl.ds(src, h)], self.land_s.at[c, pl.ds(dst, h)], self.send.at[c, kind], self.recv.at[c, kind], other)

    def start(self, c):
        for kind in range(GROUP):
            self.copy(c, kind).start()

    def relay(self, c, settled):
        r, h = self.rows, self.rows // 2
        slot = self.slot(c)
        for kind, src, dst in ((0, 2 * r, 2 * r), (1, 2 * r + h, r + h)):
            self.copy(c, kind).wait_recv()

            def block(n, carry):
                at = pl.multiple_of(n * ROW_BLOCK, ROW_BLOCK)
                mine = self.out_s[slot, pl.ds(dst + at, ROW_BLOCK), :].astype(F32)
                came = self.land_s[c, pl.ds(src + at, ROW_BLOCK), :].astype(F32)
                self.out_s[slot, pl.ds(dst + at, ROW_BLOCK), :] = (mine + came).astype(BF16)
                return carry

            lax.fori_loop(0, h // ROW_BLOCK, block, 0)

        @pl.when(settled >= 0)
        def _():
            self.drain(settled)

        self.copy(c, 5).start()
        self.copy(c, 4).start()

    def finish(self, c):
        for kind in range(2, 6):
            self.copy(c, kind).wait_recv()

    def drain(self, c):
        for kind in range(6):
            self.copy(c, kind).wait_send()

    def total(self, c, at):
        own = self.out_s[self.slot(c), pl.ds(at, ROW_BLOCK), :].astype(F32)
        came = [self.land_s[c, pl.ds(k * self.rows + at, ROW_BLOCK), :].astype(F32) for k in range(PAIR)]
        return own + came[0] + came[1]


def step_kernel(dims, scal, *refs):
    layers, chunks, rows, model, hd, window, ffn = dims
    (tokens, norms, cos, sin, wq, wk, wv, bq, bk, bv, bu, bq_push, bk_push, bv_push, bu_push, kc, vc, wo, up, down, b_o, b_down,
     h_out, kv_rolled, q_hbm, state, qkv_peer, wo_peer, up_peer, down_peer,
     big_s, q_s, t_s, s_s, wo_s, xo_s, land_s, mid_s, st_s, ba_s, bm_s, bq_s, bk_s, bv_s, bu_s,
     a1_send, a1_recv, a2_send, a2_recv, r1_send, r1_recv, r2_send, r2_recv, old_send, old_recv, kv_send, kv_recv, p_send, p_recv, b_send, b_recv,
     h_sem, t_sem, raw_sem, wa_sem, wo_sem, wm_sem, q_sem, st_sem, f_sem, ready) = refs
    place = Place()
    start_pos = scal[0]
    first_slot = lax.rem(start_pos, window)
    floor = window - 1 - start_pos
    block = rows * chunks
    tall = PAIR * rows
    tile = KEY_TILE
    tiles = window // tile
    scale = LOG2E * hd ** -0.5
    deep = GROUP * hd
    q_rows = PAIR * GROUP * tall
    last_chunk = chunks - 1
    roll_tiles = window // ROLL_ROWS

    def here(rows_from, count):
        return pl.ds(pl.multiple_of(rows_from, rows), count)

    def position(c, i):
        return (place.member(i) * PAIR + place.core) * block + c * rows

    def region(g, new):
        return jnp.where(new, (3 - g) * window, g * window)

    def q_row(c, g, i):
        return ((lax.rem(c, PAIR) * PAIR + g) * GROUP + i) * tall

    def tile_of(g, new, at, kv):
        return big_s[pl.ds(pl.multiple_of(region(g, new) + at, tile), tile), kv * hd:(kv + 1) * hd]

    def scores(c, i, g, new, at):
        return score_tile(q_s[here(q_row(c, g, i), tall), :], tile_of(g, new, at, 0))

    def row_blocks(body):
        def one(n, carry):
            body(pl.ds(pl.multiple_of(n * ROW_BLOCK, ROW_BLOCK), ROW_BLOCK), n * ROW_BLOCK)
            return carry

        lax.fori_loop(0, rows // ROW_BLOCK, one, 0)

    def q_move(c, out):
        inner, outer = q_s.at[here(lax.rem(c, PAIR) * q_rows, q_rows)], q_hbm.at[here(c * q_rows, q_rows)]
        sem = q_sem.at[lax.rem(c, PAIR)]
        return pltpu.make_async_copy(inner, outer, sem) if out else pltpu.make_async_copy(outer, inner, sem)

    def raw_copy(layer, k):
        return pltpu.make_async_copy((kc, vc)[k].at[layer], q_s, raw_sem)

    def table_copies(c):
        return [pltpu.make_async_copy(tab.at[here(position(c, i), rows)], t_s.at[k, pl.ds(i * rows, rows)], t_sem) for i in range(GROUP) for k, tab in enumerate((cos, sin))]

    def pushes(layer, some=slice(None)):
        pairs = ((wk, qkv_peer.at[layer, :, pl.ds(PAIR * hd, hd)]), (wv, qkv_peer.at[layer, :, pl.ds(3 * hd, hd)]), (wq, qkv_peer.at[layer, :, pl.ds(0, PAIR * hd)]),
                 (wo, wo_peer.at[layer]), (up, up_peer.at[layer]), (down, down_peer.at[layer]))
        return [remote(src.at[layer], dst, p_send.at[layer, k], p_recv.at[layer, k], place.peer) for k, (src, dst) in list(enumerate(pairs))[some]]

    def norm_into(layer, which, c, slot):
        gain, shift = one_row(norms.at[layer], which), one_row(norms.at[layer], which + 1)

        def body(at, _):
            xo_s[slot, at, :] = normalized(mid_s[c, at, :].astype(F32), gain, shift)

        row_blocks(body)

    def slot_of(layer, ahead):
        return lambda c: lax.rem(c + (SLOTS - layer + ahead), SLOTS)

    spot = [slot_of(layer, 0) for layer in range(layers)]
    spare = [(SLOTS - 1 - layer) % SLOTS for layer in range(layers)]
    gather1 = [Gather(place, xo_s, spot[layer], a1_send, a1_recv, rows) for layer in range(layers)]
    h_loads = [pltpu.make_async_copy(tokens.at[pl.ds(c * rows, rows)], mid_s.at[c], h_sem.at[c]) for c in range(chunks)]
    for copy in h_loads:
        copy.start()
    raw_copy(0, 0).start()
    place.barrier((place.x, place.y, place.peer))

    def lead(layer, c):
        if layer == 0:
            h_loads[c].wait()
            norm_into(0, 0, c, spot[0](c))
        gather1[layer].start(c)

    lead(0, 0)
    lead(0, 1)
    b_copies = [remote(src, dst, b_send.at[k], b_recv.at[k], place.peer) for k, (src, dst) in enumerate(((bq_push, bq_s), (bk_push, bk_s), (bv_push, bv_s), (bu_push, bu_s)))]
    for copy in b_copies + pushes(0):
        copy.start()
    for copy in b_copies:
        copy.wait_recv()

    def project_phase(layer):
        gather = gather1[layer]
        base_new = [region(g, True) for g in range(PAIR)]
        old_push = remote(big_s.at[pl.ds(0, window)], big_s.at[pl.ds(window, window)], old_send, old_recv, place.peer)
        n_passes = chunks + 1

        def wa_fetch(n):
            t = lax.rem(n, GROUP)
            slot = lax.rem(n, PAIR)
            dst = pl.ds(pl.multiple_of(slot * model, tile), model)
            sem = wa_sem.at[slot]
            sources = (((wk.at[layer], 0, hd), (wv.at[layer], hd, hd)), ((qkv_peer.at[layer, :, pl.ds(PAIR * hd, PAIR * hd)], 0, PAIR * hd),),
                       ((wq.at[layer], 0, PAIR * hd),), ((qkv_peer.at[layer, :, pl.ds(0, PAIR * hd)], 0, PAIR * hd),))
            for k, made in enumerate(sources):
                @pl.when(jnp.logical_and(t == k, n < n_passes * GROUP))
                def _():
                    for src, at, width in made:
                        pltpu.make_async_copy(src, wo_s.at[dst, pl.ds(at, width)], sem).start()

        def wa_landed(n):
            slot = lax.rem(n, PAIR)
            at = pl.ds(pl.multiple_of(slot * model, tile), model)
            whole(wo_s.at[at], wa_sem.at[slot])
            wa_fetch(n + 1)
            return at

        def kv_copies(c, i):
            at = position(c, i)
            return [remote(big_s.at[here(base_new[g] + at, rows)], big_s.at[here(base_new[1 - g] + at, rows)], kv_send.at[c], kv_recv.at[c], place.peer) for g in range(PAIR)]

        wa_fetch(jnp.int32(0))
        for copy in table_copies(0):
            copy.start()

        def put_old(k):
            def put(n, turned):
                big_s[pl.ds(pl.multiple_of(n * ROLL_ROWS, ROLL_ROWS), ROLL_ROWS), k * hd:(k + 1) * hd] = turned[0]

            return put

        raw = [lambda: q_s[...]]
        raw_copy(layer, 0).wait()
        rotate(raw, put_old(0), window, first_slot, 0, roll_tiles)
        raw_copy(layer, 1).start()
        gather.forward(0)
        lead(layer, 2)
        raw_copy(layer, 1).wait()
        rotate(raw, put_old(1), window, first_slot, 0, roll_tiles)
        if layer > 0:
            pl.semaphore_wait(ready, 1)
        old_push.start()
        gather.forward(1)
        for g, (for_q, for_k, for_v) in enumerate(((bq, bk, bv), (bq_s, bk_s, bv_s))):
            ba_s[PAIR * g] = one_row(for_q, layer)
            ba_s[PAIR * g + 1, :, :hd] = one_row(for_k, layer)
            ba_s[PAIR * g + 1, :, hd:] = one_row(for_v, layer)
        for copy in pushes(layer, slice(0, 3)):
            copy.wait_recv()

        def state_copy(b):
            return pltpu.make_async_copy(st_s.at[lax.rem(b, PAIR)], state.at[b], st_sem.at[lax.rem(b, PAIR)])

        def attend_old(c, i):
            b = c * GROUP + i
            w = lax.rem(b, PAIR)
            j0 = position(c, i)
            diag = lax.div(j0, tile)
            i_next = jnp.minimum(i + 1, GROUP - 1)
            diag_next = lax.div(position(c, i_next), tile)

            @pl.when(b >= PAIR)
            def _():
                state_copy(b - PAIR).wait()

            reset_state(st_s, w)

            def step(t, by_row):
                at = t * tile
                last = t + 1 == tiles
                at_next = jnp.where(last, diag_next, t + 1) * tile
                n_i = jnp.where(last, i_next, i)
                age = lax.broadcasted_iota(jnp.int32, (1, tile), 1) + at
                if by_row:
                    row = lax.rem(lax.broadcasted_iota(jnp.int32, (tall, 1), 0), rows) + j0
                    mask = age > jnp.maximum(row, floor)
                else:
                    mask = age > floor
                flash_step(st_s, w, s_s, scale, mask, lambda g: tile_of(g, False, at, 1), lambda g: scores(c, n_i, g, False, at_next))

            step(diag, True)

            def younger(t, carry):
                @pl.when(t > diag)
                def _():
                    step(t, False)

                return carry

            lax.fori_loop(1, tiles, younger, 0)
            state_copy(b).start()

        def one_pass(p, carry):
            c = jnp.minimum(p, last_chunk)
            upper = p != n_passes - 1
            lower = p != n_passes - PAIR

            @pl.when(upper)
            def _():
                whole(t_s, t_sem)

            @pl.when(lower)
            def _():
                gather.finish(c)

            slot = spot[layer](c)

            def rope(u, i):
                turned = jnp.concatenate([-u[:, hd // 2:], u[:, :hd // 2]], axis=1)
                return (u * t_s[0, i * rows:(i + 1) * rows, :] + turned * t_s[1, i * rows:(i + 1) * rows, :]).astype(BF16)

            parts = ((upper, 0, GROUP - 1), (lower, GROUP - 1, 1))

            def keys_values(g, inner):
                at = wa_landed(p * GROUP + g)
                for wanted, i0, count in parts:
                    @pl.when(wanted)
                    def _():
                        r0, n = i0 * rows, count * rows
                        u = jnp.dot(xo_s[slot, r0:r0 + n, :], wo_s[at, :], preferred_element_type=F32) + ba_s[PAIR * g + 1]
                        for i in range(count):
                            to = here(region(g, True) + position(c, i0 + i), rows)
                            part = u[i * rows:(i + 1) * rows]
                            big_s[to, :hd] = rope(part[:, :hd], i0 + i)
                            big_s[to, hd:] = part[:, hd:].astype(BF16)
                return inner

            lax.fori_loop(0, PAIR, keys_values, 0)
            for i in range(GROUP):
                @pl.when(upper if i < GROUP - 1 else lower)
                def _():
                    for copy in kv_copies(c, i):
                        copy.start()

            @pl.when(jnp.logical_and(upper, c >= PAIR))
            def _():
                q_move(c - PAIR, True).wait()

            def for_queries(g, inner):
                at = wa_landed(p * GROUP + PAIR + g)
                for wanted, i0, count in parts:
                    @pl.when(wanted)
                    def _():
                        r0, n = i0 * rows, count * rows
                        u = jnp.dot(xo_s[slot, r0:r0 + n, :], wo_s[at, :], preferred_element_type=F32) + ba_s[PAIR * g]
                        for h in range(PAIR):
                            for i in range(count):
                                part = u[i * rows:(i + 1) * rows, h * hd:(h + 1) * hd]
                                q_s[here(q_row(c, g, i0 + i) + h * rows, rows), :] = rope(part, i0 + i)
                return inner

            lax.fori_loop(0, PAIR, for_queries, 0)

            @pl.when(lower)
            def _():
                q_move(c, True).start()

            @pl.when(c < last_chunk)
            def _():
                for copy in table_copies(c + 1):
                    copy.start()

            @pl.when(p == 0)
            def _():
                old_push.wait_recv()

            @pl.when(jnp.logical_or(p == 0, p == 2))
            def _():
                early = lax.div(p, 2)
                for g in range(PAIR):
                    s_s[g] = scores(early, 0, g, False, lax.div(position(early, 0), tile) * tile)

                def one(i, inner):
                    @pl.when(jnp.logical_and(p == 2, i == 3))
                    def _():
                        gather.forward(3)

                    attend_old(early, i)
                    return inner

                lax.fori_loop(0, GROUP, one, 0)

            @pl.when(p == 0)
            def _():
                gather.forward(2)
                lead(layer, 3)

            @pl.when(p == 2)
            def _():
                q_move(2, True).wait()
                q_move(0, False).start()

            return carry

        lax.fori_loop(0, n_passes, one_pass, 0)
        q_move(last_chunk, True).wait()
        q_move(1, False).start()
        whole_chunk = big_s.at[pl.ds(0, PAIR * GROUP * rows)]
        kv_all = [remote(whole_chunk, whole_chunk, kv_send.at[c], kv_recv.at[c], place.peer) for c in range(chunks)]
        for copy in kv_all:
            copy.wait_recv()
        for copy in kv_all + [old_push]:
            copy.wait_send()
        for b in range(GROUP * EARLY - PAIR, GROUP * EARLY):
            state_copy(jnp.int32(b)).wait()
        for c in range(chunks):
            gather.drain(c)

    def block_phase(layer):
        onward = layer + 1 < layers
        gather = Gather(place, xo_s, spot[layer], a2_send, a2_recv, rows)
        first = Scatter(place, xo_s, slot_of(layer, 1), land_s, r1_send, r1_recv, rows)
        second = Scatter(place, xo_s, spot[layer], land_s, r2_send, r2_recv, rows)
        pushes(layer, slice(3, 4))[0].wait_recv()
        n_out = model // WIDE
        for n in range(n_out):
            for k, src in enumerate((wo, wo_peer)):
                pltpu.make_async_copy(src.at[layer, :, pl.ds(n * WIDE, WIDE)], wo_s.at[pl.ds(n * deep + k * PAIR * hd, PAIR * hd)], wo_sem).start()
        if onward:
            for copy in pushes(layer + 1):
                copy.start()

        def pick(k):
            return jnp.where(k == 0, 3, jnp.where(k == 3, 0, k))

        def state_copy(b):
            slot = lax.rem(b, PAIR)
            return pltpu.make_async_copy(state.at[lax.div(b, GROUP) * GROUP + pick(lax.rem(b, GROUP))], st_s.at[slot], st_sem.at[slot])

        for b in range(PAIR):
            state_copy(jnp.int32(b)).start()

        def tile_at(diag, n):
            is_new = jnp.logical_or(n == 0, jnp.logical_and(n >= 2, n - 2 < diag))
            t = jnp.where(n < 2, diag, jnp.where(is_new, n - 2, n - 1))
            return is_new, t * tile

        q_move(jnp.int32(0), False).wait()
        for g in range(PAIR):
            s_s[g] = scores(jnp.int32(0), 3, g, True, lax.div(position(0, 3), tile) * tile)

        def attend(c, k):
            i = pick(k)
            b = c * GROUP + k
            w = lax.rem(b, PAIR)
            late = c >= EARLY
            j0 = position(c, i)
            diag = lax.div(j0, tile)
            count = jnp.where(late, tiles + 1, diag + 2)
            end = k == 3
            c_next = jnp.minimum(jnp.where(end, c + 1, c), last_chunk)
            i_next = pick(jnp.where(end, 0, k + 1))
            next_at = lax.div(position(c_next, i_next), tile) * tile

            @pl.when(late)
            def _():
                reset_state(st_s, w)

            @pl.when(jnp.logical_not(late))
            def _():
                state_copy(b).wait()

            def step(n):
                is_new, at = tile_at(diag, n)
                following = jnp.where(jnp.logical_and(n == 0, jnp.logical_not(late)), 2, n + 1)
                last = following == count
                new_next, at_next = tile_at(diag, following)
                new_next = jnp.logical_or(last, new_next)
                at_next = jnp.where(last, next_at, at_next)
                nc = jnp.where(last, c_next, c)
                ni = jnp.where(last, i_next, i)
                col = lax.broadcasted_iota(jnp.int32, (1, tile), 1) + at
                row = lax.rem(lax.broadcasted_iota(jnp.int32, (tall, 1), 0), rows) + j0
                if not isinstance(n, int):
                    mask = col > jnp.where(is_new, -1, floor)
                elif n == 0:
                    mask = col <= row
                else:
                    mask = col > jnp.maximum(row, floor)
                flash_step(st_s, w, s_s, scale, mask, lambda g: tile_of(g, is_new, at, 1), lambda g: scores(nc, ni, g, new_next, at_next))

            step(0)

            @pl.when(late)
            def _():
                step(1)

            def further(n, carry):
                @pl.when(n < count)
                def _():
                    step(n)

                return carry

            lax.fori_loop(2, tiles + 1, further, 0)
            slot = first.slot(c)
            for g in range(PAIR):
                total = jnp.sum(st_s[w, g, :, LANES:PAIR * LANES], axis=1, keepdims=True)
                out = (st_s[w, g, :, PAIR * LANES:] / total).astype(BF16)
                for h in range(PAIR):
                    n = PAIR * g + h
                    xo_s[slot, :rows, n * hd:(n + 1) * hd] = out[h * rows:(h + 1) * rows]

            @pl.when(b + PAIR < GROUP * EARLY)
            def _():
                state_copy(b + PAIR).start()

            @pl.when(b == 0)
            def _():
                whole(wo_s, wo_sem)

            to = here(i * rows, rows)

            def summed(n):
                return jnp.dot(xo_s[slot, :rows, :deep], wo_s[n * deep:(n + 1) * deep, :], preferred_element_type=F32).astype(BF16)

            held = deep // WIDE
            for n in range(held, n_out):
                xo_s[slot, to, n * WIDE:(n + 1) * WIDE] = summed(n)
            for n, part in enumerate([summed(n) for n in range(held)]):
                xo_s[slot, to, n * WIDE:(n + 1) * WIDE] = part

            @pl.when(i == 3)
            def _():
                first.copy(c, 0).start()
                first.copy(c, 1).start()

            for kind in (2, 3):
                @pl.when(i == kind - 1)
                def _():
                    first.copy(c, kind).start()

        bias_o, bias_d = one_row(b_o, layer), one_row(b_down, layer)

        def open_mlp(c):
            first.finish(c)

            def body(at, n):
                mid_s[c, at, :] = (mid_s[c, at, :].astype(F32) + first.total(c, n) + bias_o).astype(BF16)

            row_blocks(body)
            norm_into(layer, 2, c, spot[layer](c))
            gather.start(c)

        def attend_chunk(c, carry):
            def one(k, inner):
                @pl.when(jnp.logical_and(k == 3, c + 1 < chunks))
                def _():
                    q_move(c + 1, False).wait()

                attend(c, k)

                @pl.when(jnp.logical_and(k == 1, c >= 1))
                def _():
                    first.relay(c - 1, c - 2)

                return inner

            lax.fori_loop(0, GROUP, one, 0)

            @pl.when(c + PAIR < chunks)
            def _():
                q_move(c + PAIR, False).start()

            @pl.when(c >= 2)
            def _():
                open_mlp(c - 2)

            return carry

        lax.fori_loop(0, chunks, attend_chunk, 0)
        if onward:
            raw_copy(layer + 1, 0).start()
        for copy in pushes(layer, slice(4, None)):
            copy.wait_recv()
        n_up = PAIR * ffn // WIDE
        n_tiles = n_up + n_out
        sub = WIDE // PAIR
        n_sub = ffn // sub
        act = xo_s.at[spare[layer]]

        def slot_at(c, k):
            slot = lax.rem(c * n_tiles + k, WEIGHT_SLOTS)
            return slot, pl.multiple_of(slot * model, WIDE)

        def fetch(c, k):
            over = k >= n_tiles
            k = jnp.where(over, k - n_tiles, k)
            c = jnp.where(over, c + 1, c)
            slot, base = slot_at(c, k)

            @pl.when(c < chunks)
            def _():
                for part in range(PAIR):
                    n = PAIR * k + part
                    for side, src in enumerate((up, up_peer)):
                        @pl.when(jnp.logical_and(n >= side * n_sub, n < (side + 1) * n_sub))
                        def _():
                            at = pl.multiple_of((n - side * n_sub) * sub, sub)
                            pltpu.make_async_copy(src.at[layer, :, pl.ds(at, sub)], big_s.at[pl.ds(base, model), pl.ds(part * sub, sub)], wm_sem.at[slot]).start()

                @pl.when(k >= n_up)
                def _():
                    at = pl.multiple_of((k - n_up) * WIDE, WIDE)
                    for side, src in enumerate((down, down_peer)):
                        dst = big_s.at[pl.ds(pl.multiple_of(base + side * ffn, sub), ffn)]
                        pltpu.make_async_copy(src.at[layer, :, pl.ds(at, WIDE)], dst, wm_sem.at[slot]).start()

        def landed(c, k):
            slot, base = slot_at(c, k)
            whole(big_s.at[pl.ds(base, model)], wm_sem.at[slot])
            fetch(c, k + WEIGHT_SLOTS - 1)
            return pl.ds(base, model)

        for k in range(WEIGHT_SLOTS - 1):
            fetch(jnp.int32(0), jnp.int32(k))
        stage = WEIGHT_SLOTS * model

        def stage_at(n):
            slot = lax.rem(n, ROLL_SLOTS)
            return slot, pl.ds(pl.multiple_of(stage + slot * ROLL_ROWS, ROLL_ROWS), ROLL_ROWS)

        def staged(n):
            slot, at = stage_at(n)
            whole(big_s.at[at], f_sem.at[slot])

        def put_new(n, turned):
            slot, at = stage_at(n)

            @pl.when(n >= ROLL_SLOTS)
            def _():
                staged(n)

            for k in range(PAIR):
                cols = slice(k * hd, (k + 1) * hd)
                big_s[at, cols] = turned[k]
                dst = pl.ds(pl.multiple_of((layer * PAIR + k) * window + n * ROLL_ROWS, ROLL_ROWS), ROLL_ROWS)
                pltpu.make_async_copy(big_s.at[at, cols], kv_rolled.at[dst], f_sem.at[slot]).start()

        fresh = [lambda k=k: big_s[3 * window:, k * hd:(k + 1) * hd] for k in range(PAIR)]
        rotate(fresh, put_new, window, window - first_slot, 0, roll_tiles // PAIR)
        gather.forward(0)
        rotate(fresh, put_new, window, window - first_slot, roll_tiles // PAIR, roll_tiles)
        for n in range(PAIR * n_sub):
            src = bu if n < n_sub else bu_s
            at = n % n_sub * sub
            bm_s[n // PAIR, :, n % PAIR * sub:(n % PAIR + 1) * sub] = one_row(src, layer)[:, at:at + sub]
        first.relay(last_chunk, last_chunk - 1)
        open_mlp(2)
        gather.forward(1)
        open_mlp(3)
        first.drain(last_chunk)
        for n in range(ROLL_SLOTS):
            staged(n)

        def mlp_chunk(c, carry):
            gather.finish(c)
            slot = spot[layer](c)

            def up_step(k, inner):
                at = landed(c, k)
                for top in range(PAIR):
                    r0 = top * tall
                    lifted = jnp.dot(xo_s[slot, r0:r0 + tall, :], big_s[at, :], preferred_element_type=F32) + bm_s[k]
                    act[r0:r0 + tall, pl.ds(pl.multiple_of(k * WIDE, WIDE), WIDE)] = gelu_tanh(lifted).astype(BF16)
                return inner

            lax.fori_loop(0, n_up, up_step, 0)

            @pl.when(c + 2 < chunks)
            def _():
                gather.forward(c + 2)

            gather.drain(c)

            @pl.when(c >= 2)
            def _():
                second.relay(c - 2, c - 3)

            def down_step(k, inner):
                at = landed(c, k)
                xo_s[slot, :, pl.ds(pl.multiple_of((k - n_up) * WIDE, WIDE), WIDE)] = jnp.dot(act[...], big_s[at, :], preferred_element_type=F32).astype(BF16)
                return inner

            lax.fori_loop(n_up, n_tiles, down_step, 0)
            second.start(c)
            return carry

        lax.fori_loop(0, chunks, mlp_chunk, 0)
        if onward:
            pl.semaphore_signal(ready, inc=1, device_id={'tp': place.peer}, device_id_type=MESH)

        def o_copy(c):
            return pltpu.make_async_copy(mid_s.at[c], h_out.at[here(c * rows, rows)], h_sem.at[c])

        second.relay(2, 1)
        second.relay(3, 2)

        def close(c, carry):
            second.finish(c)

            def body(at, n):
                mid_s[c, at, :] = (mid_s[c, at, :].astype(F32) + second.total(c, n) + bias_d).astype(BF16)

            row_blocks(body)
            if onward:
                norm_into(layer + 1, 0, c, spot[layer + 1](c))

                @pl.when(c < 2)
                def _():
                    lead(layer + 1, c)
            else:
                o_copy(c).start()
            return carry

        lax.fori_loop(0, chunks, close, 0)
        second.drain(last_chunk)
        if not onward:
            for c in range(chunks):
                o_copy(c).wait()

    for layer in range(layers):
        project_phase(layer)
        block_phase(layer)
    for copy in b_copies:
        copy.wait_send()
    for layer in range(layers):
        for copy in pushes(layer):
            copy.wait_send()


def run_step(chunks, scal, tokens, norms, cos, sin, weights, biases, caches, w_o, w_up, w_down, b_o, b_down):
    model = tokens.shape[1]
    rows = tokens.shape[0] // chunks
    layers, window, hd = caches[0].shape
    ffn = w_up.shape[2]
    dims = (layers, chunks, rows, model, hd, window, ffn)
    state = (GROUP * EARLY, PAIR, PAIR * rows, PAIR * LANES + hd)
    out = [tokens.shape, (layers * PAIR * window, hd), (chunks * PAIR * GROUP * PAIR * rows, hd), (layers, model, GROUP * hd), w_o.shape, w_up.shape, w_down.shape]
    out = [jax.ShapeDtypeStruct(o, BF16) for o in out]
    out.insert(3, jax.ShapeDtypeStruct(state, F32))
    few = [dma(*n) for n in ((chunks,), (), (), (PAIR,), (), (WEIGHT_SLOTS,), (PAIR,), (PAIR,), (ROLL_SLOTS,))]
    return pl.pallas_call(
        functools.partial(step_kernel, dims),
        out_shape=tuple(out),
        in_specs=[SMEM, ANY, VMEM] + [ANY] * 5 + [VMEM] * 4 + [ANY] * 9 + [VMEM] * 2,
        out_specs=(ANY,) * len(out),
        scratch_shapes=[
            vm(PAIR * PAIR * window, WIDE),
            vm(window, hd),
            vm(PAIR, GROUP * rows, hd, dtype=F32),
            vm(PAIR, PAIR * rows, KEY_TILE, dtype=F32),
            vm(PAIR * model, WIDE),
            vm(SLOTS, GROUP * rows, model),
            vm(chunks, 3 * rows, model),
            vm(chunks, rows, model),
            vm(PAIR, *state[1:], dtype=F32),
            vm(GROUP, 1, PAIR * hd, dtype=F32),
            vm(PAIR * ffn // WIDE, 1, WIDE, dtype=F32),
            *(vm(*b.shape) for b in biases),
            *(dma(chunks, GROUP) for _ in range(GROUP)),
            *(dma(chunks, 6) for _ in range(GROUP)),
            dma(),
            dma(),
            dma(chunks),
            dma(chunks),
            dma(layers, 6),
            dma(layers, 6),
            dma(GROUP),
            dma(GROUP),
            *few,
            pltpu.SemaphoreType.REGULAR,
        ],
        compiler_params=pltpu.CompilerParams(vmem_limit_bytes=VMEM_LIMIT, collective_id=0, has_side_effects=True),
        name="step",
    )(scal, tokens, norms, cos, sin, *weights, *biases, *biases, *caches, w_o, w_up, w_down, b_o, b_down)


def copy_kernel(scal, *refs):
    hidden, kv, h_out, k_out, v_out, p_out, h_s, kv_s, in_sem, out_sem = refs
    window = k_out.shape[1]
    cut = window // PAIR
    part = hidden.shape[0] // PAIR
    moves = [(hidden.at[pl.ds(n * part, part)], h_s.at[pl.ds(n * part, part)], h_out.at[pl.ds(n * part, part)]) for n in range(PAIR)]
    for layer in range(k_out.shape[0]):
        for k, out in enumerate((k_out, v_out)):
            for n in range(PAIR):
                at = pl.ds((layer * PAIR + k) * window + n * cut, cut)
                moves.append((kv.at[at], kv_s.at[at], out.at[layer, pl.ds(n * cut, cut)]))
    for n, (src, mid, _) in enumerate(moves):
        pltpu.make_async_copy(src, mid, in_sem.at[n]).start()
    start_pos = scal[0]
    ahead = lax.broadcasted_iota(jnp.int32, p_out.shape, 1) + (window - lax.rem(start_pos, window))
    p_out[...] = start_pos + jnp.where(ahead >= window, ahead - window, ahead)
    for n, (src, mid, dst) in enumerate(moves):
        pltpu.make_async_copy(src, mid, in_sem.at[n]).wait()
        pltpu.make_async_copy(mid, dst, out_sem.at[n]).start()
    for n, (_, mid, dst) in enumerate(moves):
        pltpu.make_async_copy(mid, dst, out_sem.at[n]).wait()


def run_copy(scal, hidden, kv, layers, window):
    hd = kv.shape[1]
    planes = jax.ShapeDtypeStruct((layers, window, hd), BF16)
    count = PAIR + PAIR * PAIR * layers
    return pl.pallas_call(
        copy_kernel,
        out_shape=(jax.ShapeDtypeStruct(hidden.shape, BF16), planes, planes, jax.ShapeDtypeStruct((1, window), jnp.int32)),
        in_specs=[SMEM, ANY, ANY],
        out_specs=(ANY, ANY, ANY, VMEM),
        scratch_shapes=[vm(*hidden.shape), vm(*kv.shape), dma(count), dma(count)],
        compiler_params=pltpu.CompilerParams(vmem_limit_bytes=VMEM_LIMIT),
        name="copy_out",
    )(scal, hidden, kv)


def solution(mesh):
    row_spec = P('dp', 'tp', None)
    cache_spec = P(None, 'dp', None, 'tp', None)
    col_spec = P(None, None, 'tp')
    bias_spec = P(None, 'tp')
    in_specs = (row_spec, P('dp'), P('dp', None, None), P('dp', None, None), cache_spec, cache_spec, P('dp', None), P(), col_spec, bias_spec, col_spec, bias_spec, col_spec, bias_spec, P(None, 'tp', None), P(), col_spec, bias_spec, P(None, 'tp', None), P())
    out_specs = (row_spec, cache_spec, cache_spec, P('dp', None))

    def device_step(tokens, start_pos, cos_tab, sin_tab, key_cache, value_cache, slot_pos, norm_params, w_q, b_q, w_k, b_k, w_v, b_v, w_o, b_o, w_up, b_up, w_down, b_down):
        layers, _, window, _, hd = key_cache.shape
        caches = tuple(cache.reshape(layers, window, hd) for cache in (key_cache, value_cache))
        made = run_step(CHUNKS, start_pos, tokens[0], norm_params, cos_tab[0], sin_tab[0], (w_q, w_k, w_v), (b_q, b_k, b_v, b_up), caches, w_o, w_up, w_down, b_o, b_down)
        hidden, key_out, value_out, pos_out = run_copy(start_pos, made[0], made[1], layers, window)
        return hidden[None], key_out.reshape(key_cache.shape), value_out.reshape(value_cache.shape), pos_out

    return jax.shard_map(device_step, mesh=mesh, in_specs=in_specs, out_specs=out_specs, check_vma=False)
```

```python
import functools

import jax
import jax.numpy as jnp
from jax import lax
from jax.experimental import pallas as pl
from jax.experimental.pallas import tpu as pltpu
from jax.sharding import PartitionSpec as P

NORM_EPS = 1e-5
LOG2E = 1.4426950408889634
CHUNKS = 4
KEY_TILE = 512
LANES = 128
WIDE = 512
ROW_BLOCK = 16
PAIR = 2
GROUP = 4
WEIGHT_SLOTS = 3
SLOTS = 5
ROLL_ROWS = 256
ROLL_SLOTS = 4
EARLY = 2
LOWEST = -3.3e38
VMEM_LIMIT = 67_043_328
BF16 = jnp.bfloat16
F32 = jnp.float32
MESH = pl.DeviceIdType.MESH

ANY = pl.BlockSpec(memory_space=pl.ANY)
SMEM = pl.BlockSpec(memory_space=pltpu.SMEM)
VMEM = pl.BlockSpec(memory_space=pltpu.VMEM)
DMA = pltpu.SemaphoreType.DMA


def vm(*shape, dtype=BF16):
    return pltpu.VMEM(shape, dtype)


def dma(*shape):
    return DMA(shape) if shape else DMA


def whole(ref, sem):
    pltpu.make_async_copy(ref, ref, sem).wait()


def one_row(ref, n):
    return ref[pl.ds(n, 1), :].astype(F32)


def gelu_tanh(x):
    inner = 0.7978845608028654 * (x + 0.044715 * (x * x * x))
    return 0.5 * x * (1.0 + jnp.tanh(inner))


def normalized(values, gain, shift):
    centered = values - jnp.mean(values, axis=-1, keepdims=True)
    variance = jnp.mean(centered * centered, axis=-1, keepdims=True)
    return (centered * lax.rsqrt(variance + NORM_EPS) * gain + shift).astype(BF16)


def rotate(planes, put, window, shift, first, last):
    def tile(n, carry):
        want = lax.broadcasted_iota(jnp.int32, (ROLL_ROWS, 1), 0) + (n * ROLL_ROWS + shift)
        want = jnp.where(want >= window, want - window, want)
        pick = jnp.where(lax.broadcasted_iota(jnp.int32, (1, window), 1) == want, 1.0, 0.0).astype(BF16)
        put(n, [jnp.dot(pick, plane(), preferred_element_type=F32).astype(BF16) for plane in planes])
        return carry

    lax.fori_loop(first, last, tile, 0)


def reset_state(st_s, w):
    for g in range(PAIR):
        st_s[w, g, :, 0:LANES] = jnp.full((st_s.shape[2], LANES), LOWEST, F32)
        st_s[w, g, :, LANES:] = jnp.zeros((st_s.shape[2], st_s.shape[3] - LANES), F32)


def flash_step(st_s, w, s_s, scale, mask, values, next_scores):
    for g in range(PAIR):
        s = jnp.where(mask, s_s[g] * scale, -jnp.inf)
        s_next = next_scores(g)
        m_prev = st_s[w, g, :, 0:LANES]
        m_next = jnp.maximum(m_prev, jnp.max(s, axis=1, keepdims=True))
        e = jnp.exp2(s - jnp.concatenate([m_next] * (s.shape[1] // LANES), axis=1))
        alpha = jnp.exp2(m_prev - m_next)
        total = st_s[w, g, :, LANES:2 * LANES] * alpha
        for k in range(s.shape[1] // LANES):
            total = total + e[:, k * LANES:(k + 1) * LANES]
        st_s[w, g, :, LANES:2 * LANES] = total
        st_s[w, g, :, 0:LANES] = m_next
        mixed = jnp.dot(e.astype(BF16), values(g), preferred_element_type=F32)
        st_s[w, g, :, 2 * LANES:] = st_s[w, g, :, 2 * LANES:] * jnp.concatenate([alpha] * (mixed.shape[1] // LANES), axis=1) + mixed
        s_s[g] = s_next


def score_tile(queries, keys):
    return lax.dot_general(queries, keys, (((1,), (1,)), ((), ())), preferred_element_type=F32)


class Place:
    def __init__(self):
        me = lax.axis_index('tp')
        self.core = lax.rem(me, 2)
        self.xb = lax.rem(lax.div(me, 2), 2)
        self.yb = lax.div(me, 4)
        self.peer = me + 1 - 2 * self.core
        self.x = me + 2 - 4 * self.xb
        self.y = me + 4 - 8 * self.yb

    def member(self, i):
        xb = self.xb + lax.rem(i, 2) * (1 - 2 * self.xb)
        yb = self.yb + lax.div(i, 2) * (1 - 2 * self.yb)
        return yb * 2 + xb

    def barrier(self, others):
        sem = pltpu.get_barrier_semaphore()
        for other in others:
            pl.semaphore_signal(sem, inc=1, device_id={'tp': other}, device_id_type=MESH)
        pl.semaphore_wait(sem, len(others))


def remote(src, dst, send_sem, recv_sem, other):
    return pltpu.make_async_remote_copy(src_ref=src, dst_ref=dst, send_sem=send_sem, recv_sem=recv_sem, device_id={'tp': other}, device_id_type=MESH)


class Gather:
    def __init__(self, place, x_s, slot, send, recv, rows):
        self.place, self.x_s, self.slot, self.send, self.recv, self.rows = place, x_s, slot, send, recv, rows

    def copy(self, c, kind):
        r, h = self.rows, self.rows // 2
        x, y = self.place.x, self.place.y
        src, dst, other = ((0, r, x), (h, 2 * r + h, y), (h, r + h, x), (0, 2 * r, y), (r, 3 * r, y), (2 * r + h, 3 * r + h, x))[kind]
        slot = self.slot(c)
        return remote(self.x_s.at[slot, pl.ds(src, h)], self.x_s.at[slot, pl.ds(dst, h)], self.send.at[c, kind], self.recv.at[c, kind], other)

    def start(self, c):
        for kind in range(4):
            self.copy(c, kind).start()

    def forward(self, c):
        for kind in range(2):
            self.copy(c, kind).wait_recv()
            self.copy(c, kind + 4).start()

    def near(self, c):
        for kind in (2, 3):
            self.copy(c, kind).wait_recv()

    def finish(self, c):
        for kind in (4, 5):
            self.copy(c, kind).wait_recv()

    def drain(self, c):
        for kind in range(6):
            self.copy(c, kind).wait_send()


class Scatter:
    def __init__(self, place, out_s, slot, land_s, send, recv, rows):
        self.place, self.out_s, self.slot, self.land_s, self.send, self.recv, self.rows = place, out_s, slot, land_s, send, recv, rows

    def copy(self, c, kind):
        r, h = self.rows, self.rows // 2
        x, y = self.place.x, self.place.y
        src, dst, other = ((3 * r, 2 * r, x), (3 * r + h, 2 * r + h, y), (r, 0, x), (2 * r + h, r + h, y), (r + h, h, x), (2 * r, r, y))[kind]
        return remote(self.out_s.at[self.slot(c), pl.ds(src, h)], self.land_s.at[c, pl.ds(dst, h)], self.send.at[c, kind], self.recv.at[c, kind], other)

    def start(self, c):
        for kind in range(GROUP):
            self.copy(c, kind).start()

    def relay(self, c, settled):
        r, h = self.rows, self.rows // 2
        slot = self.slot(c)
        for kind, src, dst in ((0, 2 * r, 2 * r), (1, 2 * r + h, r + h)):
            self.copy(c, kind).wait_recv()

            def block(n, carry):
                at = pl.multiple_of(n * ROW_BLOCK, ROW_BLOCK)
                mine = self.out_s[slot, pl.ds(dst + at, ROW_BLOCK), :].astype(F32)
                came = self.land_s[c, pl.ds(src + at, ROW_BLOCK), :].astype(F32)
                self.out_s[slot, pl.ds(dst + at, ROW_BLOCK), :] = (mine + came).astype(BF16)
                return carry

            lax.fori_loop(0, h // ROW_BLOCK, block, 0)

        if settled is not None:
            @pl.when(settled >= 0)
            def _():
                self.drain(settled)

        self.copy(c, 5).start()
        self.copy(c, 4).start()

    def finish(self, c):
        for kind in range(2, 6):
            self.copy(c, kind).wait_recv()

    def drain(self, c):
        for kind in range(6):
            self.copy(c, kind).wait_send()

    def total(self, c, at):
        own = self.out_s[self.slot(c), pl.ds(at, ROW_BLOCK), :].astype(F32)
        came = [self.land_s[c, pl.ds(k * self.rows + at, ROW_BLOCK), :].astype(F32) for k in range(PAIR)]
        return own + came[0] + came[1]


def step_kernel(dims, scal, *refs):
    layers, chunks, rows, model, hd, window, ffn = dims
    (tokens, norms, cos, sin, wq, wk, wv, bq, bk, bv, bu, bq_push, bk_push, bv_push, bu_push, kc, vc, wo, up, down, b_o, b_down,
     h_out, kv_rolled, q_hbm, state, qkv_peer, wo_peer, up_peer, down_peer,
     big_s, q_s, t_s, s_s, wo_s, xo_s, land_s, mid_s, st_s, ba_s, bm_s, bq_s, bk_s, bv_s, bu_s,
     a1_send, a1_recv, a2_send, a2_recv, r1_send, r1_recv, r2_send, r2_recv, old_send, old_recv, kv_send, kv_recv, p_send, p_recv, b_send, b_recv,
     h_sem, t_sem, raw_sem, wa_sem, wo_sem, wm_sem, q_sem, st_sem, f_sem, ready) = refs
    place = Place()
    start_pos = scal[0]
    first_slot = lax.rem(start_pos, window)
    floor = window - 1 - start_pos
    block = rows * chunks
    tall = PAIR * rows
    tile = KEY_TILE
    tiles = window // tile
    scale = LOG2E * hd ** -0.5
    deep = GROUP * hd
    q_rows = PAIR * GROUP * tall
    last_chunk = chunks - 1
    roll_tiles = window // ROLL_ROWS

    def here(rows_from, count):
        return pl.ds(pl.multiple_of(rows_from, rows), count)

    def position(c, i):
        return (place.member(i) * PAIR + place.core) * block + c * rows

    def region(g, new):
        return jnp.where(new, (3 - g) * window, g * window)

    def q_row(c, g, i):
        return ((lax.rem(c, PAIR) * PAIR + g) * GROUP + i) * tall

    def tile_of(g, new, at, kv):
        return big_s[pl.ds(pl.multiple_of(region(g, new) + at, tile), tile), kv * hd:(kv + 1) * hd]

    def scores(c, i, g, new, at):
        return score_tile(q_s[here(q_row(c, g, i), tall), :], tile_of(g, new, at, 0))

    def row_blocks(body):
        def one(n, carry):
            body(pl.ds(pl.multiple_of(n * ROW_BLOCK, ROW_BLOCK), ROW_BLOCK), n * ROW_BLOCK)
            return carry

        lax.fori_loop(0, rows // ROW_BLOCK, one, 0)

    def q_move(c, out):
        inner, outer = q_s.at[here(lax.rem(c, PAIR) * q_rows, q_rows)], q_hbm.at[here(c * q_rows, q_rows)]
        sem = q_sem.at[lax.rem(c, PAIR)]
        return pltpu.make_async_copy(inner, outer, sem) if out else pltpu.make_async_copy(outer, inner, sem)

    def raw_copy(layer, k):
        return pltpu.make_async_copy((kc, vc)[k].at[layer], q_s, raw_sem)

    def table_copies(c):
        return [pltpu.make_async_copy(tab.at[here(position(c, i), rows)], t_s.at[k, pl.ds(i * rows, rows)], t_sem) for i in range(GROUP) for k, tab in enumerate((cos, sin))]

    def pushes(layer, some=slice(None)):
        pairs = ((wk, qkv_peer.at[layer, :, pl.ds(PAIR * hd, hd)]), (wv, qkv_peer.at[layer, :, pl.ds(3 * hd, hd)]), (wq, qkv_peer.at[layer, :, pl.ds(0, PAIR * hd)]),
                 (wo, wo_peer.at[layer]), (up, up_peer.at[layer]), (down, down_peer.at[layer]))
        return [remote(src.at[layer], dst, p_send.at[layer, k], p_recv.at[layer, k], place.peer) for k, (src, dst) in list(enumerate(pairs))[some]]

    def norm_into(layer, which, c, slot):
        gain, shift = one_row(norms.at[layer], which), one_row(norms.at[layer], which + 1)

        def body(at, _):
            xo_s[slot, at, :] = normalized(mid_s[c, at, :].astype(F32), gain, shift)

        row_blocks(body)

    def slot_of(layer, ahead):
        return lambda c: lax.rem(c + (SLOTS - layer + ahead), SLOTS)

    spot = [slot_of(layer, 0) for layer in range(layers)]
    spare = [(SLOTS - 1 - layer) % SLOTS for layer in range(layers)]
    gather1 = [Gather(place, xo_s, spot[layer], a1_send, a1_recv, rows) for layer in range(layers)]
    h_loads = [pltpu.make_async_copy(tokens.at[pl.ds(c * rows, rows)], mid_s.at[c], h_sem.at[c]) for c in range(chunks)]
    for copy in h_loads:
        copy.start()
    raw_copy(0, 0).start()
    place.barrier((place.x, place.y, place.peer))

    def lead(layer, c):
        if layer == 0:
            h_loads[c].wait()
            norm_into(0, 0, c, spot[0](c))
        gather1[layer].start(c)

    lead(0, 0)
    lead(0, 1)
    b_copies = [remote(src, dst, b_send.at[k], b_recv.at[k], place.peer) for k, (src, dst) in enumerate(((bq_push, bq_s), (bk_push, bk_s), (bv_push, bv_s), (bu_push, bu_s)))]
    for copy in b_copies + pushes(0):
        copy.start()
    for copy in b_copies:
        copy.wait_recv()

    def pick(k):
        return jnp.where(k == 0, 3, jnp.where(k == 3, 0, k))

    def state_move(b, out):
        slot = lax.rem(b, PAIR)
        if out:
            return pltpu.make_async_copy(st_s.at[slot], state.at[b], st_sem.at[slot])
        return pltpu.make_async_copy(state.at[lax.div(b, GROUP) * GROUP + pick(lax.rem(b, GROUP))], st_s.at[slot], st_sem.at[slot])

    def project_phase(layer):
        gather = gather1[layer]
        old_push = remote(big_s.at[pl.ds(0, window)], big_s.at[pl.ds(window, window)], old_send, old_recv, place.peer)
        n_passes = chunks + 1

        def wa_fetch(n):
            t = lax.rem(n, GROUP)
            slot = lax.rem(n, PAIR)
            dst = pl.ds(pl.multiple_of(slot * model, tile), model)
            sem = wa_sem.at[slot]
            sources = (((wk.at[layer], 0, hd), (wv.at[layer], hd, hd)), ((qkv_peer.at[layer, :, pl.ds(PAIR * hd, PAIR * hd)], 0, PAIR * hd),),
                       ((wq.at[layer], 0, PAIR * hd),), ((qkv_peer.at[layer, :, pl.ds(0, PAIR * hd)], 0, PAIR * hd),))
            for k, made in enumerate(sources):
                @pl.when(jnp.logical_and(t == k, n < n_passes * GROUP))
                def _():
                    for src, at, width in made:
                        pltpu.make_async_copy(src, wo_s.at[dst, pl.ds(at, width)], sem).start()

        def wa_landed(n):
            slot = lax.rem(n, PAIR)
            at = pl.ds(pl.multiple_of(slot * model, tile), model)
            whole(wo_s.at[at], wa_sem.at[slot])
            return at

        def kv_copy(c, i, g):
            at = position(c, i)
            return remote(big_s.at[here(region(g, True) + at, rows)], big_s.at[here(region(1 - g, True) + at, rows)], kv_send.at[c], kv_recv.at[c], place.peer)

        wa_fetch(jnp.int32(0))
        for copy in table_copies(0):
            copy.start()

        def put_old(k):
            def put(n, turned):
                big_s[pl.ds(pl.multiple_of(n * ROLL_ROWS, ROLL_ROWS), ROLL_ROWS), k * hd:(k + 1) * hd] = turned[0]

            return put

        raw = [lambda: q_s[...]]
        raw_copy(layer, 0).wait()
        rotate(raw, put_old(0), window, first_slot, 0, roll_tiles)
        raw_copy(layer, 1).start()
        gather.forward(0)
        lead(layer, 2)
        raw_copy(layer, 1).wait()
        rotate(raw, put_old(1), window, first_slot, 0, roll_tiles)
        if layer > 0:
            pl.semaphore_wait(ready, 1)
        old_push.start()
        gather.forward(1)
        for g, (for_q, for_k, for_v) in enumerate(((bq, bk, bv), (bq_s, bk_s, bv_s))):
            ba_s[PAIR * g] = one_row(for_q, layer)
            ba_s[PAIR * g + 1, :, :hd] = one_row(for_k, layer)
            ba_s[PAIR * g + 1, :, hd:] = one_row(for_v, layer)
        for copy in pushes(layer, slice(0, 3)):
            copy.wait_recv()
        wa_fetch(jnp.int32(1))

        def attend_old(c, i):
            b = c * GROUP + i
            w = lax.rem(b, PAIR)
            j0 = position(c, i)
            diag = lax.div(j0, tile)
            i_next = jnp.minimum(i + 1, GROUP - 1)
            diag_next = lax.div(position(c, i_next), tile)

            @pl.when(b >= PAIR)
            def _():
                state_move(b - PAIR, True).wait()

            reset_state(st_s, w)

            def step(t, by_row):
                at = t * tile
                last = t + 1 == tiles
                at_next = jnp.where(last, diag_next, t + 1) * tile
                n_i = jnp.where(last, i_next, i)
                age = lax.broadcasted_iota(jnp.int32, (1, tile), 1) + at
                if by_row:
                    row = lax.rem(lax.broadcasted_iota(jnp.int32, (tall, 1), 0), rows) + j0
                    mask = age > jnp.maximum(row, floor)
                else:
                    mask = age > floor
                flash_step(st_s, w, s_s, scale, mask, lambda g: tile_of(g, False, at, 1), lambda g: scores(c, n_i, g, False, at_next))

            step(diag, True)

            def younger(t, carry):
                @pl.when(t > diag)
                def _():
                    step(t, False)

                return carry

            lax.fori_loop(1, tiles, younger, 0)
            state_move(b, True).start()

        def one_pass(p, carry):
            c = jnp.minimum(p, last_chunk)
            upper = p != n_passes - 1
            lower = p != n_passes - PAIR

            @pl.when(upper)
            def _():
                whole(t_s, t_sem)
                gather.near(c)

            @pl.when(lower)
            def _():
                gather.finish(c)

            slot = spot[layer](c)

            def rope(u, i):
                turned = jnp.concatenate([-u[:, hd // 2:], u[:, :hd // 2]], axis=1)
                return (u * t_s[0, i * rows:(i + 1) * rows, :] + turned * t_s[1, i * rows:(i + 1) * rows, :]).astype(BF16)

            parts = ((upper, 0, GROUP - 1), (lower, GROUP - 1, 1))

            def keys_values(g, inner):
                at = wa_landed(p * GROUP + g)
                for wanted, i0, count in parts:
                    @pl.when(wanted)
                    def _():
                        r0, n = i0 * rows, count * rows
                        u = jnp.dot(xo_s[slot, r0:r0 + n, :], wo_s[at, :], preferred_element_type=F32) + ba_s[PAIR * g + 1]
                        for i in range(count):
                            to = here(region(g, True) + position(c, i0 + i), rows)
                            part = u[i * rows:(i + 1) * rows]
                            big_s[to, :hd] = rope(part[:, :hd], i0 + i)
                            big_s[to, hd:] = part[:, hd:].astype(BF16)
                        for i in range(i0, i0 + count):
                            kv_copy(c, i, g).start()
                wa_fetch(p * GROUP + g + PAIR)
                return inner

            lax.fori_loop(0, PAIR, keys_values, 0)

            @pl.when(jnp.logical_and(upper, c >= PAIR))
            def _():
                q_move(c - PAIR, True).wait()

            def for_queries(g, inner):
                at = wa_landed(p * GROUP + PAIR + g)
                for wanted, i0, count in parts:
                    @pl.when(wanted)
                    def _():
                        r0, n = i0 * rows, count * rows
                        u = jnp.dot(xo_s[slot, r0:r0 + n, :], wo_s[at, :], preferred_element_type=F32) + ba_s[PAIR * g]
                        for h in range(PAIR):
                            for i in range(count):
                                part = u[i * rows:(i + 1) * rows, h * hd:(h + 1) * hd]
                                q_s[here(q_row(c, g, i0 + i) + h * rows, rows), :] = rope(part, i0 + i)
                wa_fetch(p * GROUP + g + PAIR + PAIR)
                return inner

            lax.fori_loop(0, PAIR, for_queries, 0)

            @pl.when(lower)
            def _():
                q_move(c, True).start()

            @pl.when(c < last_chunk)
            def _():
                for copy in table_copies(c + 1):
                    copy.start()

            @pl.when(p == 0)
            def _():
                old_push.wait_recv()

            @pl.when(jnp.logical_or(p == 0, p == 2))
            def _():
                early = lax.div(p, 2)
                for g in range(PAIR):
                    s_s[g] = scores(early, 0, g, False, lax.div(position(early, 0), tile) * tile)

                @pl.when(p == 2)
                def _():
                    gather.forward(3)

                def one(i, inner):
                    attend_old(early, i)
                    return inner

                lax.fori_loop(0, GROUP, one, 0)

            @pl.when(p == 0)
            def _():
                gather.forward(2)
                lead(layer, 3)

            @pl.when(p == 2)
            def _():
                q_move(2, True).wait()
                q_move(0, False).start()
                for b in range(PAIR):
                    state_move(jnp.int32(GROUP * EARLY - PAIR + b), True).wait()
                    state_move(jnp.int32(b), False).start()

            return carry

        lax.fori_loop(0, n_passes, one_pass, 0)
        q_move(last_chunk, True).wait()
        q_move(1, False).start()
        whole_chunk = big_s.at[pl.ds(0, PAIR * GROUP * rows)]
        kv_all = [remote(whole_chunk, whole_chunk, kv_send.at[c], kv_recv.at[c], place.peer) for c in range(chunks)]
        for copy in kv_all:
            copy.wait_recv()
        for copy in kv_all + [old_push]:
            copy.wait_send()
        for c in range(chunks):
            gather.drain(c)

    def block_phase(layer):
        onward = layer + 1 < layers
        gather = Gather(place, xo_s, spot[layer], a2_send, a2_recv, rows)
        first = Scatter(place, xo_s, slot_of(layer, 1), land_s, r1_send, r1_recv, rows)
        second = Scatter(place, xo_s, spot[layer], land_s, r2_send, r2_recv, rows)
        pushes(layer, slice(3, 4))[0].wait_recv()
        n_out = model // WIDE
        for n in range(n_out):
            for k, src in enumerate((wo, wo_peer)):
                pltpu.make_async_copy(src.at[layer, :, pl.ds(n * WIDE, WIDE)], wo_s.at[pl.ds(n * deep + k * PAIR * hd, PAIR * hd)], wo_sem).start()
        if onward:
            for copy in pushes(layer + 1):
                copy.start()

        def tile_at(diag, n):
            is_new = jnp.logical_or(n == 0, jnp.logical_and(n >= 2, n - 2 < diag))
            t = jnp.where(n < 2, diag, jnp.where(is_new, n - 2, n - 1))
            return is_new, t * tile

        q_move(jnp.int32(0), False).wait()
        for g in range(PAIR):
            s_s[g] = scores(jnp.int32(0), 3, g, True, lax.div(position(0, 3), tile) * tile)

        def attend(c, k):
            i = pick(k)
            b = c * GROUP + k
            w = lax.rem(b, PAIR)
            late = c >= EARLY
            j0 = position(c, i)
            diag = lax.div(j0, tile)
            count = jnp.where(late, tiles + 1, diag + 2)
            end = k == 3
            c_next = jnp.minimum(jnp.where(end, c + 1, c), last_chunk)
            i_next = pick(jnp.where(end, 0, k + 1))
            next_at = lax.div(position(c_next, i_next), tile) * tile

            @pl.when(late)
            def _():
                reset_state(st_s, w)

            @pl.when(jnp.logical_not(late))
            def _():
                state_move(b, False).wait()

            def step(n):
                is_new, at = tile_at(diag, n)
                following = jnp.where(jnp.logical_and(n == 0, jnp.logical_not(late)), 2, n + 1)
                last = following == count
                new_next, at_next = tile_at(diag, following)
                new_next = jnp.logical_or(last, new_next)
                at_next = jnp.where(last, next_at, at_next)
                nc = jnp.where(last, c_next, c)
                ni = jnp.where(last, i_next, i)
                col = lax.broadcasted_iota(jnp.int32, (1, tile), 1) + at
                row = lax.rem(lax.broadcasted_iota(jnp.int32, (tall, 1), 0), rows) + j0
                if not isinstance(n, int):
                    mask = col > jnp.where(is_new, -1, floor)
                elif n == 0:
                    mask = col <= row
                else:
                    mask = col > jnp.maximum(row, floor)
                flash_step(st_s, w, s_s, scale, mask, lambda g: tile_of(g, is_new, at, 1), lambda g: scores(nc, ni, g, new_next, at_next))

            step(0)

            @pl.when(late)
            def _():
                step(1)

            def further(n, carry):
                @pl.when(n < count)
                def _():
                    step(n)

                return carry

            lax.fori_loop(2, tiles + 1, further, 0)
            slot = first.slot(c)
            for g in range(PAIR):
                total = jnp.sum(st_s[w, g, :, LANES:PAIR * LANES], axis=1, keepdims=True)
                out = (st_s[w, g, :, PAIR * LANES:] / total).astype(BF16)
                for h in range(PAIR):
                    n = PAIR * g + h
                    xo_s[slot, :rows, n * hd:(n + 1) * hd] = out[h * rows:(h + 1) * rows]

            @pl.when(b + PAIR < GROUP * EARLY)
            def _():
                state_move(b + PAIR, False).start()

            @pl.when(b == 0)
            def _():
                whole(wo_s, wo_sem)

            to = here(i * rows, rows)

            def summed(n):
                return jnp.dot(xo_s[slot, :rows, :deep], wo_s[n * deep:(n + 1) * deep, :], preferred_element_type=F32).astype(BF16)

            held = deep // WIDE
            for n in range(held, n_out):
                xo_s[slot, to, n * WIDE:(n + 1) * WIDE] = summed(n)
            for n, part in enumerate([summed(n) for n in range(held)]):
                xo_s[slot, to, n * WIDE:(n + 1) * WIDE] = part

            @pl.when(i == 3)
            def _():
                first.copy(c, 0).start()
                first.copy(c, 1).start()

            for kind in (2, 3):
                @pl.when(i == kind - 1)
                def _():
                    first.copy(c, kind).start()

        bias_o, bias_d = one_row(b_o, layer), one_row(b_down, layer)

        def open_mlp(c):
            first.finish(c)

            def body(at, n):
                mid_s[c, at, :] = (mid_s[c, at, :].astype(F32) + first.total(c, n) + bias_o).astype(BF16)

            row_blocks(body)
            norm_into(layer, 2, c, spot[layer](c))
            gather.start(c)

        def attend_chunk(c, carry):
            def one(k, inner):
                @pl.when(jnp.logical_and(k == 3, c + 1 < chunks))
                def _():
                    q_move(c + 1, False).wait()

                attend(c, k)

                @pl.when(jnp.where(c == 0, k == 3, jnp.logical_and(c >= 2, k == 0)))
                def _():
                    first.relay(jnp.maximum(c - 1, 0), c - 2)

                return inner

            lax.fori_loop(0, GROUP, one, 0)

            @pl.when(c + PAIR < chunks)
            def _():
                q_move(c + PAIR, False).start()

            @pl.when(c >= 2)
            def _():
                open_mlp(c - 2)

            return carry

        lax.fori_loop(0, chunks, attend_chunk, 0)
        if onward:
            raw_copy(layer + 1, 0).start()
        for copy in pushes(layer, slice(4, None)):
            copy.wait_recv()
        n_up = PAIR * ffn // WIDE
        n_tiles = n_up + n_out
        sub = WIDE // PAIR
        n_sub = ffn // sub
        act = xo_s.at[spare[layer]]

        def slot_at(c, k):
            slot = lax.rem(c * n_tiles + k, WEIGHT_SLOTS)
            return slot, pl.multiple_of(slot * model, WIDE)

        def fetch(c, k):
            over = k >= n_tiles
            k = jnp.where(over, k - n_tiles, k)
            c = jnp.where(over, c + 1, c)
            slot, base = slot_at(c, k)

            @pl.when(c < chunks)
            def _():
                for part in range(PAIR):
                    n = PAIR * k + part
                    for side, src in enumerate((up, up_peer)):
                        @pl.when(jnp.logical_and(n >= side * n_sub, n < (side + 1) * n_sub))
                        def _():
                            at = pl.multiple_of((n - side * n_sub) * sub, sub)
                            pltpu.make_async_copy(src.at[layer, :, pl.ds(at, sub)], big_s.at[pl.ds(base, model), pl.ds(part * sub, sub)], wm_sem.at[slot]).start()

                @pl.when(k >= n_up)
                def _():
                    at = pl.multiple_of((k - n_up) * WIDE, WIDE)
                    for side, src in enumerate((down, down_peer)):
                        dst = big_s.at[pl.ds(pl.multiple_of(base + side * ffn, sub), ffn)]
                        pltpu.make_async_copy(src.at[layer, :, pl.ds(at, WIDE)], dst, wm_sem.at[slot]).start()

        def landed(c, k):
            slot, base = slot_at(c, k)
            whole(big_s.at[pl.ds(base, model)], wm_sem.at[slot])
            fetch(c, k + WEIGHT_SLOTS - 1)
            return pl.ds(base, model)

        for k in range(WEIGHT_SLOTS - 1):
            fetch(jnp.int32(0), jnp.int32(k))
        stage = WEIGHT_SLOTS * model

        def stage_at(n):
            slot = lax.rem(n, ROLL_SLOTS)
            return slot, pl.ds(pl.multiple_of(stage + slot * ROLL_ROWS, ROLL_ROWS), ROLL_ROWS)

        def staged(n):
            slot, at = stage_at(n)
            whole(big_s.at[at], f_sem.at[slot])

        def put_new(n, turned):
            slot, at = stage_at(n)

            @pl.when(n >= ROLL_SLOTS)
            def _():
                staged(n)

            for k in range(PAIR):
                cols = slice(k * hd, (k + 1) * hd)
                big_s[at, cols] = turned[k]
                dst = pl.ds(pl.multiple_of((layer * PAIR + k) * window + n * ROLL_ROWS, ROLL_ROWS), ROLL_ROWS)
                pltpu.make_async_copy(big_s.at[at, cols], kv_rolled.at[dst], f_sem.at[slot]).start()

        fresh = [lambda k=k: big_s[3 * window:, k * hd:(k + 1) * hd] for k in range(PAIR)]
        rotate(fresh, put_new, window, window - first_slot, 0, roll_tiles // PAIR)
        gather.forward(0)
        rotate(fresh, put_new, window, window - first_slot, roll_tiles // PAIR, roll_tiles)
        for n in range(PAIR * n_sub):
            src = bu if n < n_sub else bu_s
            at = n % n_sub * sub
            bm_s[n // PAIR, :, n % PAIR * sub:(n % PAIR + 1) * sub] = one_row(src, layer)[:, at:at + sub]
        first.relay(last_chunk, last_chunk - 1)
        open_mlp(2)
        gather.forward(1)
        open_mlp(3)
        first.drain(last_chunk)
        for n in range(ROLL_SLOTS):
            staged(n)

        def mlp_chunk(c, carry):
            gather.near(c)
            gather.finish(c)
            slot = spot[layer](c)

            def up_step(k, inner):
                at = landed(c, k)
                for top in range(PAIR):
                    r0 = top * tall
                    lifted = jnp.dot(xo_s[slot, r0:r0 + tall, :], big_s[at, :], preferred_element_type=F32) + bm_s[k]
                    act[r0:r0 + tall, pl.ds(pl.multiple_of(k * WIDE, WIDE), WIDE)] = gelu_tanh(lifted).astype(BF16)
                return inner

            lax.fori_loop(0, n_up, up_step, 0)

            @pl.when(c + 2 < chunks)
            def _():
                gather.forward(c + 2)

            gather.drain(c)

            @pl.when(c >= 2)
            def _():
                second.relay(c - 2, c - 3 if onward else None)

            def down_step(k, inner):
                at = landed(c, k)
                xo_s[slot, :, pl.ds(pl.multiple_of((k - n_up) * WIDE, WIDE), WIDE)] = jnp.dot(act[...], big_s[at, :], preferred_element_type=F32).astype(BF16)
                return inner

            lax.fori_loop(n_up, n_tiles, down_step, 0)
            second.start(c)
            return carry

        lax.fori_loop(0, chunks, mlp_chunk, 0)
        if onward:
            pl.semaphore_signal(ready, inc=1, device_id={'tp': place.peer}, device_id_type=MESH)

        def o_copy(c):
            return pltpu.make_async_copy(mid_s.at[c], h_out.at[here(c * rows, rows)], h_sem.at[c])

        second.relay(2, 1 if onward else None)
        second.relay(3, 2 if onward else None)

        def close(c, carry):
            second.finish(c)

            def body(at, n):
                mid_s[c, at, :] = (mid_s[c, at, :].astype(F32) + second.total(c, n) + bias_d).astype(BF16)

            row_blocks(body)
            if onward:
                norm_into(layer + 1, 0, c, spot[layer + 1](c))

                @pl.when(c < 2)
                def _():
                    lead(layer + 1, c)
            else:
                o_copy(c).start()
            return carry

        lax.fori_loop(0, chunks, close, 0)
        if onward:
            second.drain(last_chunk)
        else:
            for c in range(chunks):
                second.drain(c)
                o_copy(c).wait()

    for layer in range(layers):
        project_phase(layer)
        block_phase(layer)
    for copy in b_copies:
        copy.wait_send()
    for layer in range(layers):
        for copy in pushes(layer):
            copy.wait_send()


def run_step(chunks, scal, tokens, norms, cos, sin, weights, biases, caches, w_o, w_up, w_down, b_o, b_down):
    model = tokens.shape[1]
    rows = tokens.shape[0] // chunks
    layers, window, hd = caches[0].shape
    ffn = w_up.shape[2]
    dims = (layers, chunks, rows, model, hd, window, ffn)
    state = (GROUP * EARLY, PAIR, PAIR * rows, PAIR * LANES + hd)
    out = [tokens.shape, (layers * PAIR * window, hd), (chunks * PAIR * GROUP * PAIR * rows, hd), (layers, model, GROUP * hd), w_o.shape, w_up.shape, w_down.shape]
    out = [jax.ShapeDtypeStruct(o, BF16) for o in out]
    out.insert(3, jax.ShapeDtypeStruct(state, F32))
    few = [dma(*n) for n in ((chunks,), (), (), (PAIR,), (), (WEIGHT_SLOTS,), (PAIR,), (PAIR,), (ROLL_SLOTS,))]
    return pl.pallas_call(
        functools.partial(step_kernel, dims),
        out_shape=tuple(out),
        in_specs=[SMEM, ANY, VMEM] + [ANY] * 5 + [VMEM] * 4 + [ANY] * 9 + [VMEM] * 2,
        out_specs=(ANY,) * len(out),
        scratch_shapes=[
            vm(PAIR * PAIR * window, WIDE),
            vm(window, hd),
            vm(PAIR, GROUP * rows, hd, dtype=F32),
            vm(PAIR, PAIR * rows, KEY_TILE, dtype=F32),
            vm(PAIR * model, WIDE),
            vm(SLOTS, GROUP * rows, model),
            vm(chunks, 3 * rows, model),
            vm(chunks, rows, model),
            vm(PAIR, *state[1:], dtype=F32),
            vm(GROUP, 1, PAIR * hd, dtype=F32),
            vm(PAIR * ffn // WIDE, 1, WIDE, dtype=F32),
            *(vm(*b.shape) for b in biases),
            *(dma(chunks, 6) for _ in range(8)),
            dma(),
            dma(),
            dma(chunks),
            dma(chunks),
            dma(layers, 6),
            dma(layers, 6),
            dma(GROUP),
            dma(GROUP),
            *few,
            pltpu.SemaphoreType.REGULAR,
        ],
        compiler_params=pltpu.CompilerParams(vmem_limit_bytes=VMEM_LIMIT, collective_id=0, has_side_effects=True),
        name="step",
    )(scal, tokens, norms, cos, sin, *weights, *biases, *biases, *caches, w_o, w_up, w_down, b_o, b_down)


def copy_kernel(scal, *refs):
    hidden, kv, h_out, k_out, v_out, p_out, h_s, kv_s, in_sem, out_sem = refs
    window = k_out.shape[1]
    cut = window // GROUP
    part = hidden.shape[0] // GROUP
    moves = [(hidden.at[pl.ds(n * part, part)], h_s.at[pl.ds(n * part, part)], h_out.at[pl.ds(n * part, part)]) for n in range(GROUP)]
    for layer in range(k_out.shape[0]):
        for k, out in enumerate((k_out, v_out)):
            for n in range(GROUP):
                at = pl.ds((layer * PAIR + k) * window + n * cut, cut)
                moves.append((kv.at[at], kv_s.at[at], out.at[layer, pl.ds(n * cut, cut)]))
    for n, (src, mid, _) in enumerate(moves):
        pltpu.make_async_copy(src, mid, in_sem.at[n]).start()
    start_pos = scal[0]
    ahead = lax.broadcasted_iota(jnp.int32, p_out.shape, 1) + (window - lax.rem(start_pos, window))
    p_out[...] = start_pos + jnp.where(ahead >= window, ahead - window, ahead)
    for n, (src, mid, dst) in enumerate(moves):
        pltpu.make_async_copy(src, mid, in_sem.at[n]).wait()
        pltpu.make_async_copy(mid, dst, out_sem.at[n]).start()
    for n, (_, mid, dst) in enumerate(moves):
        pltpu.make_async_copy(mid, dst, out_sem.at[n]).wait()


def run_copy(scal, hidden, kv, layers, window):
    hd = kv.shape[1]
    planes = jax.ShapeDtypeStruct((layers, window, hd), BF16)
    count = GROUP + PAIR * GROUP * layers
    return pl.pallas_call(
        copy_kernel,
        out_shape=(jax.ShapeDtypeStruct(hidden.shape, BF16), planes, planes, jax.ShapeDtypeStruct((1, window), jnp.int32)),
        in_specs=[SMEM, ANY, ANY],
        out_specs=(ANY, ANY, ANY, VMEM),
        scratch_shapes=[vm(*hidden.shape), vm(*kv.shape), dma(count), dma(count)],
        compiler_params=pltpu.CompilerParams(vmem_limit_bytes=VMEM_LIMIT),
        name="copy_out",
    )(scal, hidden, kv)


def solution(mesh):
    row_spec = P('dp', 'tp', None)
    cache_spec = P(None, 'dp', None, 'tp', None)
    col_spec = P(None, None, 'tp')
    bias_spec = P(None, 'tp')
    in_specs = (row_spec, P('dp'), P('dp', None, None), P('dp', None, None), cache_spec, cache_spec, P('dp', None), P(), col_spec, bias_spec, col_spec, bias_spec, col_spec, bias_spec, P(None, 'tp', None), P(), col_spec, bias_spec, P(None, 'tp', None), P())
    out_specs = (row_spec, cache_spec, cache_spec, P('dp', None))

    def device_step(tokens, start_pos, cos_tab, sin_tab, key_cache, value_cache, slot_pos, norm_params, w_q, b_q, w_k, b_k, w_v, b_v, w_o, b_o, w_up, b_up, w_down, b_down):
        layers, _, window, _, hd = key_cache.shape
        caches = tuple(cache.reshape(layers, window, hd) for cache in (key_cache, value_cache))
        made = run_step(CHUNKS, start_pos, tokens[0], norm_params, cos_tab[0], sin_tab[0], (w_q, w_k, w_v), (b_q, b_k, b_v, b_up), caches, w_o, w_up, w_down, b_o, b_down)
        hidden, key_out, value_out, pos_out = run_copy(start_pos, made[0], made[1], layers, window)
        return hidden[None], key_out.reshape(key_cache.shape), value_out.reshape(value_cache.shape), pos_out

    return jax.shard_map(device_step, mesh=mesh, in_specs=in_specs, out_specs=out_specs, check_vma=False)
```

```python
import functools

import jax
import jax.numpy as jnp
from jax import lax
from jax.experimental import pallas as pl
from jax.experimental.pallas import tpu as pltpu
from jax.sharding import PartitionSpec as P

NORM_EPS = 1e-5
LOG2E = 1.4426950408889634
CHUNKS = 4
KEY_TILE = 512
LANES = 128
WIDE = 512
ROW_BLOCK = 16
PAIR = 2
GROUP = 4
WEIGHT_SLOTS = 3
SLOTS = 5
ROLL_ROWS = 256
ROLL_SLOTS = 4
EARLY = 2
LOWEST = -3.3e38
VMEM_LIMIT = 67_043_328
BF16 = jnp.bfloat16
F32 = jnp.float32
MESH = pl.DeviceIdType.MESH

ANY = pl.BlockSpec(memory_space=pl.ANY)
SMEM = pl.BlockSpec(memory_space=pltpu.SMEM)
VMEM = pl.BlockSpec(memory_space=pltpu.VMEM)
DMA = pltpu.SemaphoreType.DMA


def vm(*shape, dtype=BF16):
    return pltpu.VMEM(shape, dtype)


def dma(*shape):
    return DMA(shape) if shape else DMA


def whole(ref, sem):
    pltpu.make_async_copy(ref, ref, sem).wait()


def one_row(ref, n):
    return ref[pl.ds(n, 1), :].astype(F32)


def gelu_tanh(x):
    inner = 0.7978845608028654 * (x + 0.044715 * (x * x * x))
    return 0.5 * x * (1.0 + jnp.tanh(inner))


def normalized(values, gain, shift):
    centered = values - jnp.mean(values, axis=-1, keepdims=True)
    variance = jnp.mean(centered * centered, axis=-1, keepdims=True)
    return (centered * lax.rsqrt(variance + NORM_EPS) * gain + shift).astype(BF16)


def rotate(planes, put, window, shift, first, last):
    def tile(n, carry):
        want = lax.broadcasted_iota(jnp.int32, (ROLL_ROWS, 1), 0) + (n * ROLL_ROWS + shift)
        want = jnp.where(want >= window, want - window, want)
        pick = jnp.where(lax.broadcasted_iota(jnp.int32, (1, window), 1) == want, 1.0, 0.0).astype(BF16)
        put(n, [jnp.dot(pick, plane(), preferred_element_type=F32).astype(BF16) for plane in planes])
        return carry

    lax.fori_loop(first, last, tile, 0)


def reset_state(st_s, w):
    for g in range(PAIR):
        st_s[w, g, :, 0:LANES] = jnp.full((st_s.shape[2], LANES), LOWEST, F32)
        st_s[w, g, :, LANES:] = jnp.zeros((st_s.shape[2], st_s.shape[3] - LANES), F32)


def flash_step(st_s, w, s_s, scale, mask, values, next_scores, width=KEY_TILE):
    for g in range(PAIR):
        s = s_s[g, :, :width] * scale
        if mask is not None:
            s = jnp.where(mask, s, -jnp.inf)
        s_next = next_scores(g)
        m_prev = st_s[w, g, :, 0:LANES]
        m_next = jnp.maximum(m_prev, jnp.max(s, axis=1, keepdims=True))
        e = jnp.exp2(s - jnp.concatenate([m_next] * (s.shape[1] // LANES), axis=1))
        alpha = jnp.exp2(m_prev - m_next)
        total = st_s[w, g, :, LANES:2 * LANES] * alpha
        for k in range(s.shape[1] // LANES):
            total = total + e[:, k * LANES:(k + 1) * LANES]
        st_s[w, g, :, LANES:2 * LANES] = total
        st_s[w, g, :, 0:LANES] = m_next
        mixed = jnp.dot(e.astype(BF16), values(g), preferred_element_type=F32)
        st_s[w, g, :, 2 * LANES:] = st_s[w, g, :, 2 * LANES:] * jnp.concatenate([alpha] * (mixed.shape[1] // LANES), axis=1) + mixed
        s_s[g, :, :s_next.shape[1]] = s_next


def score_tile(queries, keys):
    return lax.dot_general(queries, keys, (((1,), (1,)), ((), ())), preferred_element_type=F32)


class Place:
    def __init__(self):
        me = lax.axis_index('tp')
        self.core = lax.rem(me, 2)
        self.xb = lax.rem(lax.div(me, 2), 2)
        self.yb = lax.div(me, 4)
        self.peer = me + 1 - 2 * self.core
        self.x = me + 2 - 4 * self.xb
        self.y = me + 4 - 8 * self.yb

    def member(self, i):
        xb = self.xb + lax.rem(i, 2) * (1 - 2 * self.xb)
        yb = self.yb + lax.div(i, 2) * (1 - 2 * self.yb)
        return yb * 2 + xb

    def barrier(self, others):
        sem = pltpu.get_barrier_semaphore()
        for other in others:
            pl.semaphore_signal(sem, inc=1, device_id={'tp': other}, device_id_type=MESH)
        pl.semaphore_wait(sem, len(others))


def remote(src, dst, send_sem, recv_sem, other):
    return pltpu.make_async_remote_copy(src_ref=src, dst_ref=dst, send_sem=send_sem, recv_sem=recv_sem, device_id={'tp': other}, device_id_type=MESH)


class Gather:
    def __init__(self, place, x_s, slot, send, recv, rows):
        self.place, self.x_s, self.slot, self.send, self.recv, self.rows = place, x_s, slot, send, recv, rows

    def copy(self, c, kind):
        r, h = self.rows, self.rows // 2
        x, y = self.place.x, self.place.y
        src, dst, other = ((0, r, x), (h, 2 * r + h, y), (h, r + h, x), (0, 2 * r, y), (r, 3 * r, y), (2 * r + h, 3 * r + h, x))[kind]
        slot = self.slot(c)
        return remote(self.x_s.at[slot, pl.ds(src, h)], self.x_s.at[slot, pl.ds(dst, h)], self.send.at[c, kind], self.recv.at[c, kind], other)

    def start(self, c):
        for kind in range(4):
            self.copy(c, kind).start()

    def forward(self, c):
        for kind in range(2):
            self.copy(c, kind).wait_recv()
            self.copy(c, kind + 4).start()

    def near(self, c):
        for kind in (2, 3):
            self.copy(c, kind).wait_recv()

    def finish(self, c):
        for kind in (4, 5):
            self.copy(c, kind).wait_recv()

    def drain(self, c):
        for kind in range(6):
            self.copy(c, kind).wait_send()


class Scatter:
    def __init__(self, place, out_s, slot, land_s, send, recv, rows):
        self.place, self.out_s, self.slot, self.land_s, self.send, self.recv, self.rows = place, out_s, slot, land_s, send, recv, rows

    def copy(self, c, kind):
        r, h = self.rows, self.rows // 2
        x, y = self.place.x, self.place.y
        src, dst, other = ((3 * r, 2 * r, x), (3 * r + h, 2 * r + h, y), (r, 0, x), (2 * r + h, r + h, y), (r + h, h, x), (2 * r, r, y))[kind]
        return remote(self.out_s.at[self.slot(c), pl.ds(src, h)], self.land_s.at[c, pl.ds(dst, h)], self.send.at[c, kind], self.recv.at[c, kind], other)

    def start(self, c):
        for kind in range(GROUP):
            self.copy(c, kind).start()

    def relay(self, c, settled):
        r, h = self.rows, self.rows // 2
        slot = self.slot(c)
        for kind, src, dst in ((0, 2 * r, 2 * r), (1, 2 * r + h, r + h)):
            self.copy(c, kind).wait_recv()

            def block(n, carry):
                at = pl.multiple_of(n * ROW_BLOCK, ROW_BLOCK)
                mine = self.out_s[slot, pl.ds(dst + at, ROW_BLOCK), :].astype(F32)
                came = self.land_s[c, pl.ds(src + at, ROW_BLOCK), :].astype(F32)
                self.out_s[slot, pl.ds(dst + at, ROW_BLOCK), :] = (mine + came).astype(BF16)
                return carry

            lax.fori_loop(0, h // ROW_BLOCK, block, 0)

        if settled is not None:
            @pl.when(settled >= 0)
            def _():
                self.drain(settled)

        self.copy(c, 5).start()
        self.copy(c, 4).start()

    def finish(self, c):
        for kind in range(2, 6):
            self.copy(c, kind).wait_recv()

    def drain(self, c):
        for kind in range(6):
            self.copy(c, kind).wait_send()

    def total(self, c, at):
        own = self.out_s[self.slot(c), pl.ds(at, ROW_BLOCK), :].astype(F32)
        came = [self.land_s[c, pl.ds(k * self.rows + at, ROW_BLOCK), :].astype(F32) for k in range(PAIR)]
        return own + came[0] + came[1]


def step_kernel(dims, scal, *refs):
    layers, chunks, rows, model, hd, window, ffn = dims
    (tokens, norms, cos, sin, wq, wk, wv, bq, bk, bv, bu, bq_push, bk_push, bv_push, bu_push, kc, vc, wo, up, down, b_o, b_down,
     h_out, kv_rolled, q_hbm, state, qkv_peer, wo_peer, up_peer, down_peer,
     big_s, q_s, t_s, s_s, wo_s, xo_s, land_s, mid_s, st_s, ba_s, bm_s, bq_s, bk_s, bv_s, bu_s,
     a1_send, a1_recv, a2_send, a2_recv, r1_send, r1_recv, r2_send, r2_recv, old_send, old_recv, kv_send, kv_recv, p_send, p_recv, b_send, b_recv,
     h_sem, t_sem, raw_sem, wa_sem, wo_sem, wm_sem, q_sem, st_sem, f_sem, ready) = refs
    place = Place()
    start_pos = scal[0]
    first_slot = lax.rem(start_pos, window)
    floor = window - 1 - start_pos
    block = rows * chunks
    tall = PAIR * rows
    tile = KEY_TILE
    tiles = window // tile
    scale = LOG2E * hd ** -0.5
    deep = GROUP * hd
    q_rows = PAIR * GROUP * tall
    last_chunk = chunks - 1
    roll_tiles = window // ROLL_ROWS

    def here(rows_from, count):
        return pl.ds(pl.multiple_of(rows_from, rows), count)

    def position(c, i):
        return (place.member(i) * PAIR + place.core) * block + c * rows

    def region(g, new):
        return jnp.where(new, (3 - g) * window, g * window)

    def q_row(c, g, i):
        return ((lax.rem(c, PAIR) * PAIR + g) * GROUP + i) * tall

    def tile_of(g, new, at, kv):
        return big_s[pl.ds(pl.multiple_of(region(g, new) + at, tile), tile), kv * hd:(kv + 1) * hd]

    def scores(c, i, g, new, at):
        return score_tile(q_s[here(q_row(c, g, i), tall), :], tile_of(g, new, at, 0))

    def row_blocks(body, first=0, last=rows):
        def one(n, carry):
            body(pl.ds(pl.multiple_of(n * ROW_BLOCK, ROW_BLOCK), ROW_BLOCK), n * ROW_BLOCK)
            return carry

        lax.fori_loop(first // ROW_BLOCK, last // ROW_BLOCK, one, 0)

    def q_move(c, out):
        inner, outer = q_s.at[here(lax.rem(c, PAIR) * q_rows, q_rows)], q_hbm.at[here(c * q_rows, q_rows)]
        sem = q_sem.at[lax.rem(c, PAIR)]
        return pltpu.make_async_copy(inner, outer, sem) if out else pltpu.make_async_copy(outer, inner, sem)

    def raw_copy(layer, k):
        return pltpu.make_async_copy((kc, vc)[k].at[layer], q_s, raw_sem)

    def table_copies(c):
        return [pltpu.make_async_copy(tab.at[here(position(c, i), rows)], t_s.at[k, pl.ds(i * rows, rows)], t_sem) for i in range(GROUP) for k, tab in enumerate((cos, sin))]

    def pushes(layer, some=slice(None)):
        pairs = ((wk, qkv_peer.at[layer, :, pl.ds(PAIR * hd, hd)]), (wv, qkv_peer.at[layer, :, pl.ds(3 * hd, hd)]), (wq, qkv_peer.at[layer, :, pl.ds(0, PAIR * hd)]),
                 (wo, wo_peer.at[layer]), (up, up_peer.at[layer]), (down, down_peer.at[layer]))
        return [remote(src.at[layer], dst, p_send.at[layer, k], p_recv.at[layer, k], place.peer) for k, (src, dst) in list(enumerate(pairs))[some]]

    def norm_into(layer, which, c, slot, *span):
        gain, shift = one_row(norms.at[layer], which), one_row(norms.at[layer], which + 1)

        def body(at, _):
            xo_s[slot, at, :] = normalized(mid_s[c, at, :].astype(F32), gain, shift)

        row_blocks(body, *span)

    def slot_of(layer, ahead):
        return lambda c: lax.rem(c + (SLOTS - layer + ahead), SLOTS)

    spot = [slot_of(layer, 0) for layer in range(layers)]
    spare = [(SLOTS - 1 - layer) % SLOTS for layer in range(layers)]
    gather1 = [Gather(place, xo_s, spot[layer], a1_send, a1_recv, rows) for layer in range(layers)]
    h_loads = [pltpu.make_async_copy(tokens.at[pl.ds(c * rows, rows)], mid_s.at[c], h_sem.at[c]) for c in range(chunks)]
    for copy in h_loads:
        copy.start()
    raw_copy(0, 0).start()
    place.barrier((place.x, place.y, place.peer))

    def lead(layer, c):
        if layer == 0:
            h_loads[c].wait()
        if layer == 0 and c == 0:
            for k in range(PAIR):
                norm_into(0, 0, c, spot[0](c), k * rows // PAIR, (k + 1) * rows // PAIR)
                for kind in (k, 3 - k):
                    gather1[0].copy(c, kind).start()
            return
        if layer == 0:
            norm_into(0, 0, c, spot[0](c))
        gather1[layer].start(c)

    lead(0, 0)
    lead(0, 1)
    b_copies = [remote(src, dst, b_send.at[k], b_recv.at[k], place.peer) for k, (src, dst) in enumerate(((bq_push, bq_s), (bk_push, bk_s), (bv_push, bv_s), (bu_push, bu_s)))]
    for copy in b_copies + pushes(0):
        copy.start()
    for copy in b_copies:
        copy.wait_recv()

    def pick(k):
        return jnp.where(k == 0, 3, jnp.where(k == 3, 0, k))

    def state_move(b, out):
        slot = lax.rem(b, PAIR)
        if out:
            return pltpu.make_async_copy(st_s.at[slot], state.at[b], st_sem.at[slot])
        return pltpu.make_async_copy(state.at[lax.div(b, GROUP) * GROUP + pick(lax.rem(b, GROUP))], st_s.at[slot], st_sem.at[slot])

    def project_phase(layer):
        gather = gather1[layer]
        old_push = remote(big_s.at[pl.ds(0, window)], big_s.at[pl.ds(window, window)], old_send, old_recv, place.peer)
        n_passes = PAIR * chunks

        def wa_fetch(n):
            t = lax.rem(n, GROUP)
            slot = lax.rem(n, PAIR)
            dst = pl.ds(pl.multiple_of(slot * model, tile), model)
            sem = wa_sem.at[slot]
            sources = (((wk.at[layer], 0, hd), (wv.at[layer], hd, hd)), ((qkv_peer.at[layer, :, pl.ds(PAIR * hd, PAIR * hd)], 0, PAIR * hd),),
                       ((wq.at[layer], 0, PAIR * hd),), ((qkv_peer.at[layer, :, pl.ds(0, PAIR * hd)], 0, PAIR * hd),))
            for k, made in enumerate(sources):
                @pl.when(jnp.logical_and(t == k, n < n_passes * GROUP))
                def _():
                    for src, at, width in made:
                        pltpu.make_async_copy(src, wo_s.at[dst, pl.ds(at, width)], sem).start()

        def wa_landed(n):
            slot = lax.rem(n, PAIR)
            at = pl.ds(pl.multiple_of(slot * model, tile), model)
            whole(wo_s.at[at], wa_sem.at[slot])
            return at

        def kv_copy(c, i, g):
            at = position(c, i)
            return remote(big_s.at[here(region(g, True) + at, rows)], big_s.at[here(region(1 - g, True) + at, rows)], kv_send.at[c], kv_recv.at[c], place.peer)

        whole_chunk = big_s.at[pl.ds(0, PAIR * GROUP * rows)]
        kv_all = [remote(whole_chunk, whole_chunk, kv_send.at[c], kv_recv.at[c], place.peer) for c in range(chunks)]
        wa_fetch(jnp.int32(0))
        for copy in table_copies(0):
            copy.start()

        def put_old(k):
            def put(n, turned):
                big_s[pl.ds(pl.multiple_of(n * ROLL_ROWS, ROLL_ROWS), ROLL_ROWS), k * hd:(k + 1) * hd] = turned[0]

            return put

        raw = [lambda: q_s[...]]
        raw_copy(layer, 0).wait()
        rotate(raw, put_old(0), window, first_slot, 0, roll_tiles)
        raw_copy(layer, 1).start()
        gather.forward(0)
        lead(layer, 2)
        raw_copy(layer, 1).wait()
        rotate(raw, put_old(1), window, first_slot, 0, roll_tiles)
        if layer > 0:
            pl.semaphore_wait(ready, 1)
        old_push.start()
        gather.forward(1)
        for g, (for_q, for_k, for_v) in enumerate(((bq, bk, bv), (bq_s, bk_s, bv_s))):
            ba_s[PAIR * g] = one_row(for_q, layer)
            ba_s[PAIR * g + 1, :, :hd] = one_row(for_k, layer)
            ba_s[PAIR * g + 1, :, hd:] = one_row(for_v, layer)
        for copy in pushes(layer, slice(0, 3)):
            copy.wait_recv()
        wa_fetch(jnp.int32(1))

        def attend_old(c, i):
            b = c * GROUP + i
            w = lax.rem(b, PAIR)
            j0 = position(c, i)
            diag = lax.div(j0, tile)
            i_next = jnp.where(i < 2, i + 1, i)
            diag_next = lax.div(position(c, i_next), tile)

            @pl.when(b >= PAIR)
            def _():
                state_move(b - PAIR, True).wait()

            reset_state(st_s, w)

            def step(t, by_row):
                at = t * tile
                last = t + 1 == tiles
                at_next = jnp.where(last, diag_next, t + 1) * tile
                n_i = jnp.where(last, i_next, i)
                age = lax.broadcasted_iota(jnp.int32, (1, tile), 1) + at
                if by_row:
                    row = lax.rem(lax.broadcasted_iota(jnp.int32, (tall, 1), 0), rows) + j0
                    mask = age > jnp.maximum(row, floor)
                else:
                    mask = age > floor
                flash_step(st_s, w, s_s, scale, mask, lambda g: tile_of(g, False, at, 1), lambda g: scores(c, n_i, g, False, at_next))

            step(diag, True)

            def younger(t, carry):
                @pl.when(t > diag)
                def _():
                    step(t, False)

                return carry

            lax.fori_loop(1, tiles, younger, 0)
            state_move(b, True).start()

        def one_pass(p, carry):
            c = lax.div(p, PAIR)
            lower = lax.rem(p, PAIR) == 1
            upper = jnp.logical_not(lower)

            @pl.when(upper)
            def _():
                whole(t_s, t_sem)
                gather.near(c)

            @pl.when(lower)
            def _():
                gather.finish(c)

            slot = spot[layer](c)

            def rope(u, i):
                turned = jnp.concatenate([-u[:, hd // 2:], u[:, :hd // 2]], axis=1)
                return (u * t_s[0, i * rows:(i + 1) * rows, :] + turned * t_s[1, i * rows:(i + 1) * rows, :]).astype(BF16)

            parts = ((upper, 0, GROUP - 1), (lower, GROUP - 1, 1))

            def keys_values(g, inner):
                at = wa_landed(p * GROUP + g)
                for wanted, i0, count in parts:
                    @pl.when(wanted)
                    def _():
                        r0, n = i0 * rows, count * rows
                        u = jnp.dot(xo_s[slot, r0:r0 + n, :], wo_s[at, :], preferred_element_type=F32) + ba_s[PAIR * g + 1]
                        for i in range(count):
                            to = here(region(g, True) + position(c, i0 + i), rows)
                            part = u[i * rows:(i + 1) * rows]
                            big_s[to, :hd] = rope(part[:, :hd], i0 + i)
                            big_s[to, hd:] = part[:, hd:].astype(BF16)
                        for i in range(i0, i0 + count):
                            kv_copy(c, i, g).start()
                wa_fetch(p * GROUP + g + PAIR)
                return inner

            lax.fori_loop(0, PAIR, keys_values, 0)

            @pl.when(jnp.logical_and(upper, c >= PAIR))
            def _():
                q_move(c - PAIR, True).wait()

            def for_queries(g, inner):
                at = wa_landed(p * GROUP + PAIR + g)
                for wanted, i0, count in parts:
                    @pl.when(wanted)
                    def _():
                        r0, n = i0 * rows, count * rows
                        u = jnp.dot(xo_s[slot, r0:r0 + n, :], wo_s[at, :], preferred_element_type=F32) + ba_s[PAIR * g]
                        for h in range(PAIR):
                            for i in range(count):
                                part = u[i * rows:(i + 1) * rows, h * hd:(h + 1) * hd]
                                q_s[here(q_row(c, g, i0 + i) + h * rows, rows), :] = rope(part, i0 + i)
                wa_fetch(p * GROUP + g + PAIR + PAIR)
                return inner

            lax.fori_loop(0, PAIR, for_queries, 0)

            @pl.when(lower)
            def _():
                q_move(c, True).start()

            @pl.when(jnp.logical_and(lower, c < last_chunk))
            def _():
                for copy in table_copies(c + 1):
                    copy.start()

            @pl.when(p == 0)
            def _():
                old_push.wait_recv()

            @pl.when(p == 2)
            def _():
                gather.forward(2)
                lead(layer, 3)

            @pl.when(c < EARLY)
            def _():
                i0 = jnp.where(lower, 3, 0)
                for g in range(PAIR):
                    s_s[g] = scores(c, i0, g, False, lax.div(position(c, i0), tile) * tile)

                def one(i, inner):
                    @pl.when((i == 3) == lower)
                    def _():
                        attend_old(c, i)

                    return inner

                lax.fori_loop(0, GROUP, one, 0)

            @pl.when(p == n_passes - 3)
            def _():
                gather.forward(3)
                q_move(2, True).wait()
                q_move(0, False).start()
                for b in range(PAIR):
                    state_move(jnp.int32(GROUP * EARLY - PAIR + b), True).wait()
                    state_move(jnp.int32(b), False).start()
                for copy in kv_all[:3]:
                    copy.wait_recv()
                q_move(0, False).wait()
                state_move(jnp.int32(0), False).wait()
                diag = lax.div(position(0, 3), tile)
                width = 3 * rows

                def keys(g, t, kv):
                    return big_s[here(region(g, True) + t * tile, width), kv * hd:(kv + 1) * hd]

                def ahead(t):
                    return [score_tile(q_s[here(q_row(0, g, 3), tall), :], keys(g, t, 0)) for g in range(PAIR)]

                for g, part in enumerate(ahead(0)):
                    s_s[g, :, :width] = part

                def earlier(t, inner):
                    @pl.when(t < diag)
                    def _():
                        nxt = jnp.minimum(t + 1, tiles - 1)
                        flash_step(st_s, 0, s_s, scale, None, lambda g: keys(g, t, 1), lambda g: score_tile(q_s[here(q_row(0, g, 3), tall), :], keys(g, nxt, 0)), width)

                    return inner

                lax.fori_loop(0, tiles - 1, earlier, 0)

            return carry

        lax.fori_loop(0, n_passes, one_pass, 0)
        q_move(last_chunk, True).wait()
        q_move(1, False).start()
        kv_all[3].wait_recv()
        for copy in kv_all + [old_push]:
            copy.wait_send()
        for c in range(chunks):
            gather.drain(c)

    def block_phase(layer):
        onward = layer + 1 < layers
        gather = Gather(place, xo_s, spot[layer], a2_send, a2_recv, rows)
        first = Scatter(place, xo_s, slot_of(layer, 1), land_s, r1_send, r1_recv, rows)
        second = Scatter(place, xo_s, spot[layer], land_s, r2_send, r2_recv, rows)
        pushes(layer, slice(3, 4))[0].wait_recv()
        n_out = model // WIDE
        for n in range(n_out):
            for k, src in enumerate((wo, wo_peer)):
                pltpu.make_async_copy(src.at[layer, :, pl.ds(n * WIDE, WIDE)], wo_s.at[pl.ds(n * deep + k * PAIR * hd, PAIR * hd)], wo_sem).start()
        if onward:
            for copy in pushes(layer + 1):
                copy.start()

        def tile_at(diag, n):
            is_new = jnp.logical_or(n == 0, jnp.logical_and(n >= 2, n - 2 < diag))
            t = jnp.where(n < 2, diag, jnp.where(is_new, n - 2, n - 1))
            return is_new, t * tile

        for g in range(PAIR):
            s_s[g] = scores(jnp.int32(0), 3, g, True, lax.div(position(0, 3), tile) * tile)

        def attend(c, k):
            i = pick(k)
            b = c * GROUP + k
            w = lax.rem(b, PAIR)
            late = c >= EARLY
            j0 = position(c, i)
            diag = lax.div(j0, tile)
            count = jnp.where(b == 0, 2, jnp.where(late, tiles + 1, diag + 2))
            end = k == 3
            c_next = jnp.minimum(jnp.where(end, c + 1, c), last_chunk)
            i_next = pick(jnp.where(end, 0, k + 1))
            next_at = lax.div(position(c_next, i_next), tile) * tile

            @pl.when(late)
            def _():
                reset_state(st_s, w)

            @pl.when(jnp.logical_and(jnp.logical_not(late), b > 0))
            def _():
                state_move(b, False).wait()

            def step(n):
                is_new, at = tile_at(diag, n)
                following = jnp.where(jnp.logical_and(n == 0, jnp.logical_not(late)), 2, n + 1)
                last = following == count
                new_next, at_next = tile_at(diag, following)
                new_next = jnp.logical_or(last, new_next)
                at_next = jnp.where(last, next_at, at_next)
                nc = jnp.where(last, c_next, c)
                ni = jnp.where(last, i_next, i)
                col = lax.broadcasted_iota(jnp.int32, (1, tile), 1) + at
                row = lax.rem(lax.broadcasted_iota(jnp.int32, (tall, 1), 0), rows) + j0
                if not isinstance(n, int):
                    mask = col > jnp.where(is_new, -1, floor)
                elif n == 0:
                    mask = col <= row
                else:
                    mask = col > jnp.maximum(row, floor)
                flash_step(st_s, w, s_s, scale, mask, lambda g: tile_of(g, is_new, at, 1), lambda g: scores(nc, ni, g, new_next, at_next))

            step(0)

            @pl.when(late)
            def _():
                step(1)

            def last_keys(u, carry):
                @pl.when(jnp.logical_and(b == 0, u * GROUP < diag))
                def _():
                    def gathered(g, kv):
                        cols = slice(kv * hd, (kv + 1) * hd)
                        return jnp.concatenate([big_s[here(region(g, True) + (u * GROUP + n + 1) * tile - rows, rows), cols] for n in range(GROUP)], axis=0)

                    for g in range(PAIR):
                        s_s[g] = score_tile(q_s[here(q_row(c, g, i), tall), :], gathered(g, 0))
                    seen = lax.broadcasted_iota(jnp.int32, (1, tile), 1) < (diag - u * GROUP) * rows
                    flash_step(st_s, w, s_s, scale, seen, lambda g: gathered(g, 1), lambda g: scores(c_next, i_next, g, True, next_at))

                return carry

            lax.fori_loop(0, PAIR, last_keys, 0)

            def further(n, carry):
                @pl.when(n < count)
                def _():
                    step(n)

                return carry

            lax.fori_loop(2, tiles + 1, further, 0)
            slot = first.slot(c)
            for g in range(PAIR):
                total = jnp.sum(st_s[w, g, :, LANES:PAIR * LANES], axis=1, keepdims=True)
                out = (st_s[w, g, :, PAIR * LANES:] / total).astype(BF16)
                for h in range(PAIR):
                    n = PAIR * g + h
                    xo_s[slot, :rows, n * hd:(n + 1) * hd] = out[h * rows:(h + 1) * rows]

            @pl.when(b + PAIR < GROUP * EARLY)
            def _():
                state_move(b + PAIR, False).start()

            @pl.when(b == 0)
            def _():
                whole(wo_s, wo_sem)

            to = here(i * rows, rows)

            def summed(n):
                return jnp.dot(xo_s[slot, :rows, :deep], wo_s[n * deep:(n + 1) * deep, :], preferred_element_type=F32).astype(BF16)

            held = deep // WIDE
            for n in range(held, n_out):
                xo_s[slot, to, n * WIDE:(n + 1) * WIDE] = summed(n)
            for n, part in enumerate([summed(n) for n in range(held)]):
                xo_s[slot, to, n * WIDE:(n + 1) * WIDE] = part

            @pl.when(i == 3)
            def _():
                first.copy(c, 0).start()
                first.copy(c, 1).start()

            for kind in (2, 3):
                @pl.when(i == kind - 1)
                def _():
                    first.copy(c, kind).start()

        bias_o, bias_d = one_row(b_o, layer), one_row(b_down, layer)

        def open_mlp(c):
            first.finish(c)

            def body(at, n):
                mid_s[c, at, :] = (mid_s[c, at, :].astype(F32) + first.total(c, n) + bias_o).astype(BF16)

            row_blocks(body)
            norm_into(layer, 2, c, spot[layer](c))
            gather.start(c)

        def attend_chunk(c, carry):
            def one(k, inner):
                @pl.when(jnp.logical_and(k == 3, c + 1 < chunks))
                def _():
                    q_move(c + 1, False).wait()

                attend(c, k)

                @pl.when(jnp.where(c == 0, k == 3, jnp.logical_and(c >= 2, k == 0)))
                def _():
                    first.relay(jnp.maximum(c - 1, 0), c - 2)

                return inner

            lax.fori_loop(0, GROUP, one, 0)

            @pl.when(c + PAIR < chunks)
            def _():
                q_move(c + PAIR, False).start()

            @pl.when(c >= 2)
            def _():
                open_mlp(c - 2)

            return carry

        lax.fori_loop(0, chunks, attend_chunk, 0)
        if onward:
            raw_copy(layer + 1, 0).start()
        for copy in pushes(layer, slice(4, None)):
            copy.wait_recv()
        n_up = PAIR * ffn // WIDE
        n_tiles = n_up + n_out
        sub = WIDE // PAIR
        n_sub = ffn // sub
        act = xo_s.at[spare[layer]]

        def slot_at(c, k):
            slot = lax.rem(c * n_tiles + k, WEIGHT_SLOTS)
            return slot, pl.multiple_of(slot * model, WIDE)

        def fetch(c, k):
            over = k >= n_tiles
            k = jnp.where(over, k - n_tiles, k)
            c = jnp.where(over, c + 1, c)
            slot, base = slot_at(c, k)

            @pl.when(c < chunks)
            def _():
                for part in range(PAIR):
                    n = PAIR * k + part
                    for side, src in enumerate((up, up_peer)):
                        @pl.when(jnp.logical_and(n >= side * n_sub, n < (side + 1) * n_sub))
                        def _():
                            at = pl.multiple_of((n - side * n_sub) * sub, sub)
                            pltpu.make_async_copy(src.at[layer, :, pl.ds(at, sub)], big_s.at[pl.ds(base, model), pl.ds(part * sub, sub)], wm_sem.at[slot]).start()

                @pl.when(k >= n_up)
                def _():
                    at = pl.multiple_of((k - n_up) * WIDE, WIDE)
                    for side, src in enumerate((down, down_peer)):
                        dst = big_s.at[pl.ds(pl.multiple_of(base + side * ffn, sub), ffn)]
                        pltpu.make_async_copy(src.at[layer, :, pl.ds(at, WIDE)], dst, wm_sem.at[slot]).start()

        def landed(c, k):
            slot, base = slot_at(c, k)
            whole(big_s.at[pl.ds(base, model)], wm_sem.at[slot])
            fetch(c, k + WEIGHT_SLOTS - 1)
            return pl.ds(base, model)

        for k in range(WEIGHT_SLOTS - 1):
            fetch(jnp.int32(0), jnp.int32(k))
        stage = WEIGHT_SLOTS * model

        def stage_at(n):
            slot = lax.rem(n, ROLL_SLOTS)
            return slot, pl.ds(pl.multiple_of(stage + slot * ROLL_ROWS, ROLL_ROWS), ROLL_ROWS)

        def staged(n):
            slot, at = stage_at(n)
            whole(big_s.at[at], f_sem.at[slot])

        def put_new(n, turned):
            slot, at = stage_at(n)

            @pl.when(n >= ROLL_SLOTS)
            def _():
                staged(n)

            for k in range(PAIR):
                cols = slice(k * hd, (k + 1) * hd)
                big_s[at, cols] = turned[k]
                dst = pl.ds(pl.multiple_of((layer * PAIR + k) * window + n * ROLL_ROWS, ROLL_ROWS), ROLL_ROWS)
                pltpu.make_async_copy(big_s.at[at, cols], kv_rolled.at[dst], f_sem.at[slot]).start()

        fresh = [lambda k=k: big_s[3 * window:, k * hd:(k + 1) * hd] for k in range(PAIR)]
        rotate(fresh, put_new, window, window - first_slot, 0, roll_tiles // PAIR)
        gather.forward(0)
        rotate(fresh, put_new, window, window - first_slot, roll_tiles // PAIR, roll_tiles)
        for n in range(PAIR * n_sub):
            src = bu if n < n_sub else bu_s
            at = n % n_sub * sub
            bm_s[n // PAIR, :, n % PAIR * sub:(n % PAIR + 1) * sub] = one_row(src, layer)[:, at:at + sub]
        first.relay(last_chunk, last_chunk - 1)
        open_mlp(2)
        gather.forward(1)
        open_mlp(3)
        first.drain(last_chunk)
        for n in range(ROLL_SLOTS):
            staged(n)

        def mlp_chunk(c, carry):
            gather.near(c)
            gather.finish(c)
            slot = spot[layer](c)

            def up_step(k, inner):
                at = landed(c, k)
                for top in range(PAIR):
                    r0 = top * tall
                    lifted = jnp.dot(xo_s[slot, r0:r0 + tall, :], big_s[at, :], preferred_element_type=F32) + bm_s[k]
                    act[r0:r0 + tall, pl.ds(pl.multiple_of(k * WIDE, WIDE), WIDE)] = gelu_tanh(lifted).astype(BF16)
                return inner

            lax.fori_loop(0, n_up, up_step, 0)

            @pl.when(c + 2 < chunks)
            def _():
                gather.forward(c + 2)

            gather.drain(c)

            @pl.when(c >= 2)
            def _():
                second.relay(c - 2, c - 3 if onward else None)

            def down_step(k, inner):
                at = landed(c, k)
                xo_s[slot, :, pl.ds(pl.multiple_of((k - n_up) * WIDE, WIDE), WIDE)] = jnp.dot(act[...], big_s[at, :], preferred_element_type=F32).astype(BF16)
                return inner

            lax.fori_loop(n_up, n_tiles, down_step, 0)
            second.start(c)
            return carry

        lax.fori_loop(0, chunks, mlp_chunk, 0)
        if onward:
            pl.semaphore_signal(ready, inc=1, device_id={'tp': place.peer}, device_id_type=MESH)

        def o_copy(c):
            return pltpu.make_async_copy(mid_s.at[c], h_out.at[here(c * rows, rows)], h_sem.at[c])

        second.relay(2, 1 if onward else None)
        second.relay(3, 2 if onward else None)

        def close(c, carry):
            second.finish(c)

            def body(at, n):
                mid_s[c, at, :] = (mid_s[c, at, :].astype(F32) + second.total(c, n) + bias_d).astype(BF16)

            row_blocks(body)
            if onward:
                norm_into(layer + 1, 0, c, spot[layer + 1](c))

                @pl.when(c < 2)
                def _():
                    lead(layer + 1, c)
            else:
                o_copy(c).start()
            return carry

        lax.fori_loop(0, chunks, close, 0)
        if onward:
            second.drain(last_chunk)
        else:
            for c in range(chunks):
                second.drain(c)
                o_copy(c).wait()

    for layer in range(layers):
        project_phase(layer)
        block_phase(layer)
    for copy in b_copies:
        copy.wait_send()
    for layer in range(layers):
        for copy in pushes(layer):
            copy.wait_send()


def run_step(chunks, scal, tokens, norms, cos, sin, weights, biases, caches, w_o, w_up, w_down, b_o, b_down):
    model = tokens.shape[1]
    rows = tokens.shape[0] // chunks
    layers, window, hd = caches[0].shape
    ffn = w_up.shape[2]
    dims = (layers, chunks, rows, model, hd, window, ffn)
    state = (GROUP * EARLY, PAIR, PAIR * rows, PAIR * LANES + hd)
    out = [tokens.shape, (layers * PAIR * window, hd), (chunks * PAIR * GROUP * PAIR * rows, hd), (layers, model, GROUP * hd), w_o.shape, w_up.shape, w_down.shape]
    out = [jax.ShapeDtypeStruct(o, BF16) for o in out]
    out.insert(3, jax.ShapeDtypeStruct(state, F32))
    few = [dma(*n) for n in ((chunks,), (), (), (PAIR,), (), (WEIGHT_SLOTS,), (PAIR,), (PAIR,), (ROLL_SLOTS,))]
    return pl.pallas_call(
        functools.partial(step_kernel, dims),
        out_shape=tuple(out),
        in_specs=[SMEM, ANY, VMEM] + [ANY] * 5 + [VMEM] * 4 + [ANY] * 9 + [VMEM] * 2,
        out_specs=(ANY,) * len(out),
        scratch_shapes=[
            vm(PAIR * PAIR * window, WIDE),
            vm(window, hd),
            vm(PAIR, GROUP * rows, hd, dtype=F32),
            vm(PAIR, PAIR * rows, KEY_TILE, dtype=F32),
            vm(PAIR * model, WIDE),
            vm(SLOTS, GROUP * rows, model),
            vm(chunks, 3 * rows, model),
            vm(chunks, rows, model),
            vm(PAIR, *state[1:], dtype=F32),
            vm(GROUP, 1, PAIR * hd, dtype=F32),
            vm(PAIR * ffn // WIDE, 1, WIDE, dtype=F32),
            *(vm(*b.shape) for b in biases),
            *(dma(chunks, 6) for _ in range(8)),
            dma(),
            dma(),
            dma(chunks),
            dma(chunks),
            dma(layers, 6),
            dma(layers, 6),
            dma(GROUP),
            dma(GROUP),
            *few,
            pltpu.SemaphoreType.REGULAR,
        ],
        compiler_params=pltpu.CompilerParams(vmem_limit_bytes=VMEM_LIMIT, collective_id=0, has_side_effects=True),
        name="step",
    )(scal, tokens, norms, cos, sin, *weights, *biases, *biases, *caches, w_o, w_up, w_down, b_o, b_down)


def copy_kernel(scal, *refs):
    hidden, kv, h_out, k_out, v_out, p_out, h_s, kv_s, in_sem, out_sem = refs
    window = k_out.shape[1]
    cut = window // GROUP
    part = hidden.shape[0] // GROUP
    moves = [(hidden.at[pl.ds(n * part, part)], h_s.at[pl.ds(n * part, part)], h_out.at[pl.ds(n * part, part)]) for n in range(GROUP)]
    for layer in range(k_out.shape[0]):
        for k, out in enumerate((k_out, v_out)):
            for n in range(GROUP):
                at = pl.ds((layer * PAIR + k) * window + n * cut, cut)
                moves.append((kv.at[at], kv_s.at[at], out.at[layer, pl.ds(n * cut, cut)]))
    for n, (src, mid, _) in enumerate(moves):
        pltpu.make_async_copy(src, mid, in_sem.at[n]).start()
    start_pos = scal[0]
    ahead = lax.broadcasted_iota(jnp.int32, p_out.shape, 1) + (window - lax.rem(start_pos, window))
    p_out[...] = start_pos + jnp.where(ahead >= window, ahead - window, ahead)
    for n, (src, mid, dst) in enumerate(moves):
        pltpu.make_async_copy(src, mid, in_sem.at[n]).wait()
        pltpu.make_async_copy(mid, dst, out_sem.at[n]).start()
    for n, (_, mid, dst) in enumerate(moves):
        pltpu.make_async_copy(mid, dst, out_sem.at[n]).wait()


def run_copy(scal, hidden, kv, layers, window):
    hd = kv.shape[1]
    planes = jax.ShapeDtypeStruct((layers, window, hd), BF16)
    count = GROUP + PAIR * GROUP * layers
    return pl.pallas_call(
        copy_kernel,
        out_shape=(jax.ShapeDtypeStruct(hidden.shape, BF16), planes, planes, jax.ShapeDtypeStruct((1, window), jnp.int32)),
        in_specs=[SMEM, ANY, ANY],
        out_specs=(ANY, ANY, ANY, VMEM),
        scratch_shapes=[vm(*hidden.shape), vm(*kv.shape), dma(count), dma(count)],
        compiler_params=pltpu.CompilerParams(vmem_limit_bytes=VMEM_LIMIT),
        name="copy_out",
    )(scal, hidden, kv)


def solution(mesh):
    row_spec = P('dp', 'tp', None)
    cache_spec = P(None, 'dp', None, 'tp', None)
    col_spec = P(None, None, 'tp')
    bias_spec = P(None, 'tp')
    in_specs = (row_spec, P('dp'), P('dp', None, None), P('dp', None, None), cache_spec, cache_spec, P('dp', None), P(), col_spec, bias_spec, col_spec, bias_spec, col_spec, bias_spec, P(None, 'tp', None), P(), col_spec, bias_spec, P(None, 'tp', None), P())
    out_specs = (row_spec, cache_spec, cache_spec, P('dp', None))

    def device_step(tokens, start_pos, cos_tab, sin_tab, key_cache, value_cache, slot_pos, norm_params, w_q, b_q, w_k, b_k, w_v, b_v, w_o, b_o, w_up, b_up, w_down, b_down):
        layers, _, window, _, hd = key_cache.shape
        caches = tuple(cache.reshape(layers, window, hd) for cache in (key_cache, value_cache))
        made = run_step(CHUNKS, start_pos, tokens[0], norm_params, cos_tab[0], sin_tab[0], (w_q, w_k, w_v), (b_q, b_k, b_v, b_up), caches, w_o, w_up, w_down, b_o, b_down)
        hidden, key_out, value_out, pos_out = run_copy(start_pos, made[0], made[1], layers, window)
        return hidden[None], key_out.reshape(key_cache.shape), value_out.reshape(value_cache.shape), pos_out

    return jax.shard_map(device_step, mesh=mesh, in_specs=in_specs, out_specs=out_specs, check_vma=False)
```

```python
import functools

import jax
import jax.numpy as jnp
from jax import lax
from jax.experimental import pallas as pl
from jax.experimental.pallas import tpu as pltpu
from jax.sharding import PartitionSpec as P

NORM_EPS = 1e-5
LOG2E = 1.4426950408889634
CHUNKS = 4
KEY_TILE = 512
LANES = 128
WIDE = 512
ROW_BLOCK = 16
PAIR = 2
GROUP = 4
WEIGHT_SLOTS = 3
SLOTS = 5
ROLL_ROWS = 256
ROLL_SLOTS = 4
EARLY = 7
LOWEST = -3.3e38
VMEM_LIMIT = 67_043_328
BF16 = jnp.bfloat16
F32 = jnp.float32
MESH = pl.DeviceIdType.MESH

ANY = pl.BlockSpec(memory_space=pl.ANY)
SMEM = pl.BlockSpec(memory_space=pltpu.SMEM)
VMEM = pl.BlockSpec(memory_space=pltpu.VMEM)
DMA = pltpu.SemaphoreType.DMA


def vm(*shape, dtype=BF16):
    return pltpu.VMEM(shape, dtype)


def dma(*shape):
    return DMA(shape) if shape else DMA


def whole(ref, sem):
    pltpu.make_async_copy(ref, ref, sem).wait()


def one_row(ref, n):
    return ref[pl.ds(n, 1), :].astype(F32)


def gelu_tanh(x):
    inner = 0.7978845608028654 * (x + 0.044715 * (x * x * x))
    return 0.5 * x * (1.0 + jnp.tanh(inner))


def normalized(values, gain, shift):
    centered = values - jnp.mean(values, axis=-1, keepdims=True)
    variance = jnp.mean(centered * centered, axis=-1, keepdims=True)
    return (centered * lax.rsqrt(variance + NORM_EPS) * gain + shift).astype(BF16)


def rotate(planes, put, window, shift, first, last):
    def tile(n, carry):
        want = lax.broadcasted_iota(jnp.int32, (ROLL_ROWS, 1), 0) + (n * ROLL_ROWS + shift)
        want = jnp.where(want >= window, want - window, want)
        pick = jnp.where(lax.broadcasted_iota(jnp.int32, (1, window), 1) == want, 1.0, 0.0).astype(BF16)
        put(n, [jnp.dot(pick, plane(), preferred_element_type=F32).astype(BF16) for plane in planes])
        return carry

    lax.fori_loop(first, last, tile, 0)


def reset_state(st_s, w):
    for g in range(PAIR):
        st_s[w, g, :, 0:LANES] = jnp.full((st_s.shape[2], LANES), LOWEST, F32)
        st_s[w, g, :, LANES:] = jnp.zeros((st_s.shape[2], st_s.shape[3] - LANES), F32)


def flash_step(st_s, w, s_s, scale, mask, values, next_scores):
    for g in range(PAIR):
        s = jnp.where(mask, s_s[g] * scale, -jnp.inf)
        s_next = next_scores(g)
        m_prev = st_s[w, g, :, 0:LANES]
        m_next = jnp.maximum(m_prev, jnp.max(s, axis=1, keepdims=True))
        e = jnp.exp2(s - jnp.concatenate([m_next] * (s.shape[1] // LANES), axis=1))
        alpha = jnp.exp2(m_prev - m_next)
        total = st_s[w, g, :, LANES:2 * LANES] * alpha
        for k in range(s.shape[1] // LANES):
            total = total + e[:, k * LANES:(k + 1) * LANES]
        st_s[w, g, :, LANES:2 * LANES] = total
        st_s[w, g, :, 0:LANES] = m_next
        mixed = jnp.dot(e.astype(BF16), values(g), preferred_element_type=F32)
        st_s[w, g, :, 2 * LANES:] = st_s[w, g, :, 2 * LANES:] * jnp.concatenate([alpha] * (mixed.shape[1] // LANES), axis=1) + mixed
        s_s[g] = s_next


def score_tile(queries, keys):
    return lax.dot_general(queries, keys, (((1,), (1,)), ((), ())), preferred_element_type=F32)


class Place:
    def __init__(self):
        me = lax.axis_index('tp')
        self.core = lax.rem(me, 2)
        self.xb = lax.rem(lax.div(me, 2), 2)
        self.yb = lax.div(me, 4)
        self.peer = me + 1 - 2 * self.core
        self.x = me + 2 - 4 * self.xb
        self.y = me + 4 - 8 * self.yb

    def member(self, i):
        xb = self.xb + lax.rem(i, 2) * (1 - 2 * self.xb)
        yb = self.yb + lax.div(i, 2) * (1 - 2 * self.yb)
        return yb * 2 + xb

    def barrier(self, others):
        sem = pltpu.get_barrier_semaphore()
        for other in others:
            pl.semaphore_signal(sem, inc=1, device_id={'tp': other}, device_id_type=MESH)
        pl.semaphore_wait(sem, len(others))


def remote(src, dst, send_sem, recv_sem, other):
    return pltpu.make_async_remote_copy(src_ref=src, dst_ref=dst, send_sem=send_sem, recv_sem=recv_sem, device_id={'tp': other}, device_id_type=MESH)


class Gather:
    def __init__(self, place, x_s, slot, send, recv, rows):
        self.place, self.x_s, self.slot, self.send, self.recv, self.rows = place, x_s, slot, send, recv, rows

    def copy(self, c, kind):
        r, h = self.rows, self.rows // 2
        x, y = self.place.x, self.place.y
        src, dst, other = ((0, r, x), (h, 2 * r + h, y), (h, r + h, x), (0, 2 * r, y), (r, 3 * r, y), (2 * r + h, 3 * r + h, x))[kind]
        slot = self.slot(c)
        return remote(self.x_s.at[slot, pl.ds(src, h)], self.x_s.at[slot, pl.ds(dst, h)], self.send.at[c, kind], self.recv.at[c, kind], other)

    def start(self, c):
        for kind in range(4):
            self.copy(c, kind).start()

    def forward(self, c):
        for kind in range(2):
            self.copy(c, kind).wait_recv()
            self.copy(c, kind + 4).start()

    def near(self, c):
        for kind in (2, 3):
            self.copy(c, kind).wait_recv()

    def finish(self, c):
        for kind in (4, 5):
            self.copy(c, kind).wait_recv()

    def drain(self, c):
        for kind in range(6):
            self.copy(c, kind).wait_send()


class Scatter:
    def __init__(self, place, out_s, slot, land_s, send, recv, rows):
        self.place, self.out_s, self.slot, self.land_s, self.send, self.recv, self.rows = place, out_s, slot, land_s, send, recv, rows

    def copy(self, c, kind):
        r, h = self.rows, self.rows // 2
        x, y = self.place.x, self.place.y
        src, dst, other = ((3 * r, 2 * r, x), (3 * r + h, 2 * r + h, y), (r, 0, x), (2 * r + h, r + h, y), (r + h, h, x), (2 * r, r, y))[kind]
        return remote(self.out_s.at[self.slot(c), pl.ds(src, h)], self.land_s.at[c, pl.ds(dst, h)], self.send.at[c, kind], self.recv.at[c, kind], other)

    def start(self, c):
        for kind in range(GROUP):
            self.copy(c, kind).start()

    def relay(self, c, settled):
        r, h = self.rows, self.rows // 2
        slot = self.slot(c)
        for kind, src, dst in ((0, 2 * r, 2 * r), (1, 2 * r + h, r + h)):
            self.copy(c, kind).wait_recv()

            def block(n, carry):
                at = pl.multiple_of(n * ROW_BLOCK, ROW_BLOCK)
                mine = self.out_s[slot, pl.ds(dst + at, ROW_BLOCK), :].astype(F32)
                came = self.land_s[c, pl.ds(src + at, ROW_BLOCK), :].astype(F32)
                self.out_s[slot, pl.ds(dst + at, ROW_BLOCK), :] = (mine + came).astype(BF16)
                return carry

            lax.fori_loop(0, h // ROW_BLOCK, block, 0)

        if settled is not None:
            @pl.when(settled >= 0)
            def _():
                self.drain(settled)

        self.copy(c, 5).start()
        self.copy(c, 4).start()

    def finish(self, c):
        for kind in range(2, 6):
            self.copy(c, kind).wait_recv()

    def drain(self, c):
        for kind in range(6):
            self.copy(c, kind).wait_send()

    def total(self, c, at):
        own = self.out_s[self.slot(c), pl.ds(at, ROW_BLOCK), :].astype(F32)
        came = [self.land_s[c, pl.ds(k * self.rows + at, ROW_BLOCK), :].astype(F32) for k in range(PAIR)]
        return own + came[0] + came[1]


def step_kernel(dims, scal, *refs):
    layers, chunks, rows, model, hd, window, ffn = dims
    (tokens, norms, cos, sin, wq, wk, wv, bq, bk, bv, bu, bq_push, bk_push, bv_push, bu_push, kc, vc, wo, up, down, b_o, b_down,
     h_out, kv_rolled, q_hbm, state, qkv_peer, wo_peer, up_peer, down_peer,
     big_s, q_s, t_s, s_s, wo_s, xo_s, land_s, mid_s, st_s, ba_s, bm_s, bq_s, bk_s, bv_s, bu_s,
     a1_send, a1_recv, a2_send, a2_recv, r1_send, r1_recv, r2_send, r2_recv, old_send, old_recv, kv_send, kv_recv, p_send, p_recv, b_send, b_recv,
     h_sem, t_sem, raw_sem, wa_sem, wo_sem, wm_sem, q_sem, st_sem, f_sem, ready) = refs
    place = Place()
    start_pos = scal[0]
    first_slot = lax.rem(start_pos, window)
    floor = window - 1 - start_pos
    block = rows * chunks
    tall = PAIR * rows
    tile = KEY_TILE
    tiles = window // tile
    scale = LOG2E * hd ** -0.5
    deep = GROUP * hd
    q_rows = PAIR * GROUP * tall
    last_chunk = chunks - 1
    roll_tiles = window // ROLL_ROWS

    def here(rows_from, count):
        return pl.ds(pl.multiple_of(rows_from, rows), count)

    def position(c, i):
        return (place.member(i) * PAIR + place.core) * block + c * rows

    def region(g, new):
        return jnp.where(new, (3 - g) * window, g * window)

    def q_row(c, g, i):
        return ((lax.rem(c, PAIR) * PAIR + g) * GROUP + i) * tall

    def tile_of(g, new, at, kv):
        return big_s[pl.ds(pl.multiple_of(region(g, new) + at, tile), tile), kv * hd:(kv + 1) * hd]

    def scores(c, i, g, new, at):
        return score_tile(q_s[here(q_row(c, g, i), tall), :], tile_of(g, new, at, 0))

    def row_blocks(body, first=0, last=rows):
        def one(n, carry):
            body(pl.ds(pl.multiple_of(n * ROW_BLOCK, ROW_BLOCK), ROW_BLOCK), n * ROW_BLOCK)
            return carry

        lax.fori_loop(first // ROW_BLOCK, last // ROW_BLOCK, one, 0)

    def q_move(c, out):
        inner, outer = q_s.at[here(lax.rem(c, PAIR) * q_rows, q_rows)], q_hbm.at[here(c * q_rows, q_rows)]
        sem = q_sem.at[lax.rem(c, PAIR)]
        return pltpu.make_async_copy(inner, outer, sem) if out else pltpu.make_async_copy(outer, inner, sem)

    def raw_copy(layer, k):
        return pltpu.make_async_copy((kc, vc)[k].at[layer], q_s, raw_sem)

    def table_copies(c):
        return [pltpu.make_async_copy(tab.at[here(position(c, i), rows)], t_s.at[k, pl.ds(i * rows, rows)], t_sem) for i in range(GROUP) for k, tab in enumerate((cos, sin))]

    def pushes(layer, some=slice(None)):
        pairs = ((wk, qkv_peer.at[layer, :, pl.ds(PAIR * hd, hd)]), (wv, qkv_peer.at[layer, :, pl.ds(3 * hd, hd)]), (wq, qkv_peer.at[layer, :, pl.ds(0, PAIR * hd)]),
                 (wo, wo_peer.at[layer]), (up, up_peer.at[layer]), (down, down_peer.at[layer]))
        return [remote(src.at[layer], dst, p_send.at[layer, k], p_recv.at[layer, k], place.peer) for k, (src, dst) in list(enumerate(pairs))[some]]

    def norm_into(layer, which, c, slot, *span):
        gain, shift = one_row(norms.at[layer], which), one_row(norms.at[layer], which + 1)

        def body(at, _):
            xo_s[slot, at, :] = normalized(mid_s[c, at, :].astype(F32), gain, shift)

        row_blocks(body, *span)

    def slot_of(layer, ahead):
        return lambda c: lax.rem(c + (SLOTS - layer + ahead), SLOTS)

    spot = [slot_of(layer, 0) for layer in range(layers)]
    spare = [(SLOTS - 1 - layer) % SLOTS for layer in range(layers)]
    gather1 = [Gather(place, xo_s, spot[layer], a1_send, a1_recv, rows) for layer in range(layers)]
    h_loads = [pltpu.make_async_copy(tokens.at[pl.ds(c * rows, rows)], mid_s.at[c], h_sem.at[c]) for c in range(chunks)]
    for copy in h_loads:
        copy.start()
    raw_copy(0, 0).start()
    place.barrier((place.x, place.y, place.peer))

    def lead(layer, c):
        if layer == 0:
            h_loads[c].wait()
        if layer == 0 and c == 0:
            for k in range(PAIR):
                norm_into(0, 0, c, spot[0](c), k * rows // PAIR, (k + 1) * rows // PAIR)
                for kind in (k, 3 - k):
                    gather1[0].copy(c, kind).start()
            return
        if layer == 0:
            norm_into(0, 0, c, spot[0](c))
        gather1[layer].start(c)

    lead(0, 0)
    lead(0, 1)
    b_copies = [remote(src, dst, b_send.at[k], b_recv.at[k], place.peer) for k, (src, dst) in enumerate(((bq_push, bq_s), (bk_push, bk_s), (bv_push, bv_s), (bu_push, bu_s)))]
    for copy in b_copies + pushes(0):
        copy.start()
    for copy in b_copies:
        copy.wait_recv()

    def pick(k):
        return jnp.where(k == 0, 3, jnp.where(k == 3, 0, k))

    def state_out(n, c, i):
        return pltpu.make_async_copy(st_s.at[lax.rem(n, PAIR)], state.at[c * GROUP + i], st_sem.at[lax.rem(n, PAIR)])

    def state_in(b):
        slot = lax.rem(b, PAIR)
        return pltpu.make_async_copy(state.at[lax.div(b, GROUP) * GROUP + pick(lax.rem(b, GROUP))], st_s.at[slot], st_sem.at[slot])

    def project_phase(layer):
        gather = gather1[layer]
        old_push = remote(big_s.at[pl.ds(0, window)], big_s.at[pl.ds(window, window)], old_send, old_recv, place.peer)
        n_passes = chunks + 1

        def wa_fetch(n):
            t = lax.rem(n, GROUP)
            slot = lax.rem(n, PAIR)
            dst = pl.ds(pl.multiple_of(slot * model, tile), model)
            sem = wa_sem.at[slot]
            sources = (((wk.at[layer], 0, hd), (wv.at[layer], hd, hd)), ((qkv_peer.at[layer, :, pl.ds(PAIR * hd, PAIR * hd)], 0, PAIR * hd),),
                       ((wq.at[layer], 0, PAIR * hd),), ((qkv_peer.at[layer, :, pl.ds(0, PAIR * hd)], 0, PAIR * hd),))
            for k, made in enumerate(sources):
                @pl.when(jnp.logical_and(t == k, n < n_passes * GROUP))
                def _():
                    for src, at, width in made:
                        pltpu.make_async_copy(src, wo_s.at[dst, pl.ds(at, width)], sem).start()

        def wa_landed(n):
            slot = lax.rem(n, PAIR)
            at = pl.ds(pl.multiple_of(slot * model, tile), model)
            whole(wo_s.at[at], wa_sem.at[slot])
            return at

        def kv_copy(c, i, g):
            at = position(c, i)
            return remote(big_s.at[here(region(g, True) + at, rows)], big_s.at[here(region(1 - g, True) + at, rows)], kv_send.at[c], kv_recv.at[c], place.peer)

        wa_fetch(jnp.int32(0))
        for copy in table_copies(0):
            copy.start()

        def put_old(k):
            def put(n, turned):
                big_s[pl.ds(pl.multiple_of(n * ROLL_ROWS, ROLL_ROWS), ROLL_ROWS), k * hd:(k + 1) * hd] = turned[0]

            return put

        raw = [lambda: q_s[...]]
        raw_copy(layer, 0).wait()
        rotate(raw, put_old(0), window, first_slot, 0, roll_tiles)
        raw_copy(layer, 1).start()
        gather.forward(0)
        lead(layer, 2)
        raw_copy(layer, 1).wait()
        rotate(raw, put_old(1), window, first_slot, 0, roll_tiles)
        if layer > 0:
            pl.semaphore_wait(ready, 1)
        old_push.start()
        gather.forward(1)
        for g, (for_q, for_k, for_v) in enumerate(((bq, bk, bv), (bq_s, bk_s, bv_s))):
            ba_s[PAIR * g] = one_row(for_q, layer)
            ba_s[PAIR * g + 1, :, :hd] = one_row(for_k, layer)
            ba_s[PAIR * g + 1, :, hd:] = one_row(for_v, layer)
        for copy in pushes(layer, slice(0, 3)):
            copy.wait_recv()
        wa_fetch(jnp.int32(1))

        def attend_old(c, i):
            b = c * (GROUP - 1) + i
            w = lax.rem(b, PAIR)
            j0 = position(c, i)
            diag = lax.div(j0, tile)
            i_next = jnp.minimum(i + 1, GROUP - 1)
            diag_next = lax.div(position(c, i_next), tile)

            @pl.when(b >= PAIR)
            def _():
                state_out(b - PAIR, c, i).wait()

            reset_state(st_s, w)

            def step(t, by_row):
                at = t * tile
                last = t + 1 == tiles
                at_next = jnp.where(last, diag_next, t + 1) * tile
                n_i = jnp.where(last, i_next, i)
                age = lax.broadcasted_iota(jnp.int32, (1, tile), 1) + at
                if by_row:
                    row = lax.rem(lax.broadcasted_iota(jnp.int32, (tall, 1), 0), rows) + j0
                    mask = age > jnp.maximum(row, floor)
                else:
                    mask = age > floor
                flash_step(st_s, w, s_s, scale, mask, lambda g: tile_of(g, False, at, 1), lambda g: scores(c, n_i, g, False, at_next))

            step(diag, True)

            def younger(t, carry):
                @pl.when(t > diag)
                def _():
                    step(t, False)

                return carry

            lax.fori_loop(1, tiles, younger, 0)
            state_out(b, c, i).start()

        def one_pass(p, carry):
            c = jnp.minimum(p, last_chunk)
            upper = p != n_passes - 1
            lower = p != n_passes - PAIR

            @pl.when(upper)
            def _():
                whole(t_s, t_sem)
                gather.near(c)

            @pl.when(lower)
            def _():
                gather.finish(c)

            slot = spot[layer](c)

            def rope(u, i):
                turned = jnp.concatenate([-u[:, hd // 2:], u[:, :hd // 2]], axis=1)
                return (u * t_s[0, i * rows:(i + 1) * rows, :] + turned * t_s[1, i * rows:(i + 1) * rows, :]).astype(BF16)

            parts = ((upper, 0, GROUP - 1), (lower, GROUP - 1, 1))

            def keys_values(g, inner):
                at = wa_landed(p * GROUP + g)
                for wanted, i0, count in parts:
                    @pl.when(wanted)
                    def _():
                        r0, n = i0 * rows, count * rows
                        u = jnp.dot(xo_s[slot, r0:r0 + n, :], wo_s[at, :], preferred_element_type=F32) + ba_s[PAIR * g + 1]
                        for i in range(count):
                            to = here(region(g, True) + position(c, i0 + i), rows)
                            part = u[i * rows:(i + 1) * rows]
                            big_s[to, :hd] = rope(part[:, :hd], i0 + i)
                            big_s[to, hd:] = part[:, hd:].astype(BF16)
                        for i in range(i0, i0 + count):
                            kv_copy(c, i, g).start()
                wa_fetch(p * GROUP + g + PAIR)
                return inner

            lax.fori_loop(0, PAIR, keys_values, 0)

            @pl.when(jnp.logical_and(upper, c >= PAIR))
            def _():
                q_move(c - PAIR, True).wait()

            def for_queries(g, inner):
                at = wa_landed(p * GROUP + PAIR + g)
                for wanted, i0, count in parts:
                    @pl.when(wanted)
                    def _():
                        r0, n = i0 * rows, count * rows
                        u = jnp.dot(xo_s[slot, r0:r0 + n, :], wo_s[at, :], preferred_element_type=F32) + ba_s[PAIR * g]
                        for h in range(PAIR):
                            for i in range(count):
                                part = u[i * rows:(i + 1) * rows, h * hd:(h + 1) * hd]
                                q_s[here(q_row(c, g, i0 + i) + h * rows, rows), :] = rope(part, i0 + i)
                wa_fetch(p * GROUP + g + PAIR + PAIR)
                return inner

            lax.fori_loop(0, PAIR, for_queries, 0)

            @pl.when(lower)
            def _():
                q_move(c, True).start()

            @pl.when(c < last_chunk)
            def _():
                for copy in table_copies(c + 1):
                    copy.start()

            @pl.when(p == 0)
            def _():
                old_push.wait_recv()

            @pl.when(jnp.logical_or(p == 0, p == 2))
            def _():
                early = lax.div(p, 2)
                for g in range(PAIR):
                    s_s[g] = scores(early, early, g, False, lax.div(position(early, early), tile) * tile)

                @pl.when(p == 2)
                def _():
                    gather.forward(3)

                def one(i, inner):
                    @pl.when(i >= early)
                    def _():
                        attend_old(early, i)

                    return inner

                lax.fori_loop(0, GROUP, one, 0)

            @pl.when(p == 0)
            def _():
                gather.forward(2)
                lead(layer, 3)

            @pl.when(p == 2)
            def _():
                q_move(2, True).wait()
                q_move(0, False).start()
                for b in range(PAIR):
                    state_out(jnp.int32(EARLY - PAIR + b), 0, 0).wait()
                for b in range(PAIR):
                    state_in(jnp.int32(b)).start()

            return carry

        lax.fori_loop(0, n_passes, one_pass, 0)
        whole_chunk = big_s.at[pl.ds(0, PAIR * GROUP * rows)]
        kv_all = [remote(whole_chunk, whole_chunk, kv_send.at[c], kv_recv.at[c], place.peer) for c in range(chunks)]
        for copy in kv_all:
            copy.wait_recv()
        for c in range(chunks):
            gather.drain(c)
        return kv_all + [old_push]

    def block_phase(layer, sent):
        onward = layer + 1 < layers
        gather = Gather(place, xo_s, spot[layer], a2_send, a2_recv, rows)
        first = Scatter(place, xo_s, slot_of(layer, 1), land_s, r1_send, r1_recv, rows)
        second = Scatter(place, xo_s, spot[layer], land_s, r2_send, r2_recv, rows)
        pushes(layer, slice(3, 4))[0].wait_recv()
        n_out = model // WIDE
        for n in range(n_out):
            for k, src in enumerate((wo, wo_peer)):
                pltpu.make_async_copy(src.at[layer, :, pl.ds(n * WIDE, WIDE)], wo_s.at[pl.ds(n * deep + k * PAIR * hd, PAIR * hd)], wo_sem).start()
        if onward:
            for copy in pushes(layer + 1):
                copy.start()

        def tile_at(diag, n):
            is_new = jnp.logical_or(n == 0, jnp.logical_and(n >= 2, n - 2 < diag))
            t = jnp.where(n < 2, diag, jnp.where(is_new, n - 2, n - 1))
            return is_new, t * tile

        q_move(jnp.int32(0), False).wait()
        for g in range(PAIR):
            s_s[g] = scores(jnp.int32(0), 3, g, True, lax.div(position(0, 3), tile) * tile)

        def attend(c, k):
            i = pick(k)
            b = c * GROUP + k
            w = lax.rem(b, PAIR)
            late = b >= EARLY
            j0 = position(c, i)
            diag = lax.div(j0, tile)
            count = jnp.where(late, tiles + 1, diag + 2)
            end = k == 3
            c_next = jnp.minimum(jnp.where(end, c + 1, c), last_chunk)
            i_next = pick(jnp.where(end, 0, k + 1))
            next_at = lax.div(position(c_next, i_next), tile) * tile

            @pl.when(late)
            def _():
                reset_state(st_s, w)

            @pl.when(jnp.logical_not(late))
            def _():
                state_in(b).wait()

            def step(n):
                is_new, at = tile_at(diag, n)
                following = jnp.where(jnp.logical_and(n == 0, jnp.logical_not(late)), 2, n + 1)
                last = following == count
                new_next, at_next = tile_at(diag, following)
                new_next = jnp.logical_or(last, new_next)
                at_next = jnp.where(last, next_at, at_next)
                nc = jnp.where(last, c_next, c)
                ni = jnp.where(last, i_next, i)
                col = lax.broadcasted_iota(jnp.int32, (1, tile), 1) + at
                row = lax.rem(lax.broadcasted_iota(jnp.int32, (tall, 1), 0), rows) + j0
                if not isinstance(n, int):
                    mask = col > jnp.where(is_new, -1, floor)
                elif n == 0:
                    mask = col <= row
                else:
                    mask = col > jnp.maximum(row, floor)
                flash_step(st_s, w, s_s, scale, mask, lambda g: tile_of(g, is_new, at, 1), lambda g: scores(nc, ni, g, new_next, at_next))

            step(0)

            @pl.when(late)
            def _():
                step(1)

            def further(n, carry):
                @pl.when(n < count)
                def _():
                    step(n)

                return carry

            lax.fori_loop(2, tiles + 1, further, 0)
            slot = first.slot(c)
            for g in range(PAIR):
                total = jnp.sum(st_s[w, g, :, LANES:PAIR * LANES], axis=1, keepdims=True)
                out = (st_s[w, g, :, PAIR * LANES:] / total).astype(BF16)
                for h in range(PAIR):
                    n = PAIR * g + h
                    xo_s[slot, :rows, n * hd:(n + 1) * hd] = out[h * rows:(h + 1) * rows]

            @pl.when(b + PAIR < EARLY)
            def _():
                state_in(b + PAIR).start()

            @pl.when(b == 0)
            def _():
                whole(wo_s, wo_sem)

            to = here(i * rows, rows)

            def summed(n):
                return jnp.dot(xo_s[slot, :rows, :deep], wo_s[n * deep:(n + 1) * deep, :], preferred_element_type=F32).astype(BF16)

            held = deep // WIDE
            for n in range(held, n_out):
                xo_s[slot, to, n * WIDE:(n + 1) * WIDE] = summed(n)
            for n, part in enumerate([summed(n) for n in range(held)]):
                xo_s[slot, to, n * WIDE:(n + 1) * WIDE] = part

            @pl.when(i == 3)
            def _():
                first.copy(c, 0).start()
                first.copy(c, 1).start()

            for kind in (2, 3):
                @pl.when(i == kind - 1)
                def _():
                    first.copy(c, kind).start()

        bias_o, bias_d = one_row(b_o, layer), one_row(b_down, layer)

        def open_mlp(c):
            first.finish(c)

            def body(at, n):
                mid_s[c, at, :] = (mid_s[c, at, :].astype(F32) + first.total(c, n) + bias_o).astype(BF16)

            row_blocks(body)
            norm_into(layer, 2, c, spot[layer](c))
            gather.start(c)

        def attend_chunk(c, carry):
            def one(k, inner):
                @pl.when(jnp.logical_and(k == 3, c + 1 < chunks))
                def _():
                    q_move(c + 1, False).wait()

                attend(c, k)

                @pl.when(jnp.logical_and(c == 0, k == 1))
                def _():
                    q_move(last_chunk, True).wait()
                    q_move(1, False).start()

                @pl.when(jnp.where(c == 0, k == 3, jnp.logical_and(c >= 2, k == 0)))
                def _():
                    first.relay(jnp.maximum(c - 1, 0), c - 2)

                return inner

            lax.fori_loop(0, GROUP, one, 0)

            @pl.when(c + PAIR < chunks)
            def _():
                q_move(c + PAIR, False).start()

            @pl.when(c >= 2)
            def _():
                open_mlp(c - 2)

            return carry

        lax.fori_loop(0, chunks, attend_chunk, 0)
        for copy in sent:
            copy.wait_send()
        if onward:
            raw_copy(layer + 1, 0).start()
        for copy in pushes(layer, slice(4, None)):
            copy.wait_recv()
        n_up = PAIR * ffn // WIDE
        n_tiles = n_up + n_out
        sub = WIDE // PAIR
        n_sub = ffn // sub
        act = xo_s.at[spare[layer]]

        def slot_at(c, k):
            slot = lax.rem(c * n_tiles + k, WEIGHT_SLOTS)
            return slot, pl.multiple_of(slot * model, WIDE)

        def fetch(c, k):
            over = k >= n_tiles
            k = jnp.where(over, k - n_tiles, k)
            c = jnp.where(over, c + 1, c)
            slot, base = slot_at(c, k)

            @pl.when(c < chunks)
            def _():
                for part in range(PAIR):
                    n = PAIR * k + part
                    for side, src in enumerate((up, up_peer)):
                        @pl.when(jnp.logical_and(n >= side * n_sub, n < (side + 1) * n_sub))
                        def _():
                            at = pl.multiple_of((n - side * n_sub) * sub, sub)
                            pltpu.make_async_copy(src.at[layer, :, pl.ds(at, sub)], big_s.at[pl.ds(base, model), pl.ds(part * sub, sub)], wm_sem.at[slot]).start()

                @pl.when(k >= n_up)
                def _():
                    at = pl.multiple_of((k - n_up) * WIDE, WIDE)
                    for side, src in enumerate((down, down_peer)):
                        dst = big_s.at[pl.ds(pl.multiple_of(base + side * ffn, sub), ffn)]
                        pltpu.make_async_copy(src.at[layer, :, pl.ds(at, WIDE)], dst, wm_sem.at[slot]).start()

        def landed(c, k):
            slot, base = slot_at(c, k)
            whole(big_s.at[pl.ds(base, model)], wm_sem.at[slot])
            fetch(c, k + WEIGHT_SLOTS - 1)
            return pl.ds(base, model)

        for k in range(WEIGHT_SLOTS - 1):
            fetch(jnp.int32(0), jnp.int32(k))
        stage = WEIGHT_SLOTS * model

        def stage_at(n):
            slot = lax.rem(n, ROLL_SLOTS)
            return slot, pl.ds(pl.multiple_of(stage + slot * ROLL_ROWS, ROLL_ROWS), ROLL_ROWS)

        def staged(n):
            slot, at = stage_at(n)
            whole(big_s.at[at], f_sem.at[slot])

        def put_new(n, turned):
            slot, at = stage_at(n)

            @pl.when(n >= ROLL_SLOTS)
            def _():
                staged(n)

            for k in range(PAIR):
                cols = slice(k * hd, (k + 1) * hd)
                big_s[at, cols] = turned[k]
                dst = pl.ds(pl.multiple_of((layer * PAIR + k) * window + n * ROLL_ROWS, ROLL_ROWS), ROLL_ROWS)
                pltpu.make_async_copy(big_s.at[at, cols], kv_rolled.at[dst], f_sem.at[slot]).start()

        fresh = [lambda k=k: big_s[3 * window:, k * hd:(k + 1) * hd] for k in range(PAIR)]
        rotate(fresh, put_new, window, window - first_slot, 0, roll_tiles // PAIR)
        gather.forward(0)
        rotate(fresh, put_new, window, window - first_slot, roll_tiles // PAIR, roll_tiles)
        for n in range(PAIR * n_sub):
            src = bu if n < n_sub else bu_s
            at = n % n_sub * sub
            bm_s[n // PAIR, :, n % PAIR * sub:(n % PAIR + 1) * sub] = one_row(src, layer)[:, at:at + sub]
        first.relay(last_chunk, last_chunk - 1)
        open_mlp(2)
        gather.forward(1)
        open_mlp(3)
        first.drain(last_chunk)
        for n in range(ROLL_SLOTS):
            staged(n)

        def mlp_chunk(c, carry):
            gather.near(c)
            gather.finish(c)
            slot = spot[layer](c)

            def up_step(k, inner):
                at = landed(c, k)
                for top in range(PAIR):
                    r0 = top * tall
                    lifted = jnp.dot(xo_s[slot, r0:r0 + tall, :], big_s[at, :], preferred_element_type=F32) + bm_s[k]
                    act[r0:r0 + tall, pl.ds(pl.multiple_of(k * WIDE, WIDE), WIDE)] = gelu_tanh(lifted).astype(BF16)
                return inner

            lax.fori_loop(0, n_up, up_step, 0)

            @pl.when(c + 2 < chunks)
            def _():
                gather.forward(c + 2)

            gather.drain(c)

            @pl.when(c >= 2)
            def _():
                second.relay(c - 2, c - 3 if onward else None)

            def down_step(k, inner):
                at = landed(c, k)
                xo_s[slot, :, pl.ds(pl.multiple_of((k - n_up) * WIDE, WIDE), WIDE)] = jnp.dot(act[...], big_s[at, :], preferred_element_type=F32).astype(BF16)
                return inner

            lax.fori_loop(n_up, n_tiles, down_step, 0)
            second.start(c)
            return carry

        lax.fori_loop(0, chunks, mlp_chunk, 0)
        if onward:
            pl.semaphore_signal(ready, inc=1, device_id={'tp': place.peer}, device_id_type=MESH)

        def o_copy(c):
            return pltpu.make_async_copy(mid_s.at[c], h_out.at[here(c * rows, rows)], h_sem.at[c])

        second.relay(2, 1 if onward else None)
        second.relay(3, 2 if onward else None)

        def close(c, carry):
            second.finish(c)

            def body(at, n):
                mid_s[c, at, :] = (mid_s[c, at, :].astype(F32) + second.total(c, n) + bias_d).astype(BF16)

            row_blocks(body)
            if onward:
                norm_into(layer + 1, 0, c, spot[layer + 1](c))

                @pl.when(c < 2)
                def _():
                    lead(layer + 1, c)
            else:
                o_copy(c).start()
            return carry

        lax.fori_loop(0, chunks, close, 0)
        if onward:
            second.drain(last_chunk)
        else:
            for c in range(chunks):
                second.drain(c)
                o_copy(c).wait()

    for layer in range(layers):
        block_phase(layer, project_phase(layer))
    for copy in b_copies:
        copy.wait_send()
    for layer in range(layers):
        for copy in pushes(layer):
            copy.wait_send()


def run_step(chunks, scal, tokens, norms, cos, sin, weights, biases, caches, w_o, w_up, w_down, b_o, b_down):
    model = tokens.shape[1]
    rows = tokens.shape[0] // chunks
    layers, window, hd = caches[0].shape
    ffn = w_up.shape[2]
    dims = (layers, chunks, rows, model, hd, window, ffn)
    state = (PAIR * GROUP, PAIR, PAIR * rows, PAIR * LANES + hd)
    out = [tokens.shape, (layers * PAIR * window, hd), (chunks * PAIR * GROUP * PAIR * rows, hd), (layers, model, GROUP * hd), w_o.shape, w_up.shape, w_down.shape]
    out = [jax.ShapeDtypeStruct(o, BF16) for o in out]
    out.insert(3, jax.ShapeDtypeStruct(state, F32))
    few = [dma(*n) for n in ((chunks,), (), (), (PAIR,), (), (WEIGHT_SLOTS,), (PAIR,), (PAIR,), (ROLL_SLOTS,))]
    return pl.pallas_call(
        functools.partial(step_kernel, dims),
        out_shape=tuple(out),
        in_specs=[SMEM, ANY, VMEM] + [ANY] * 5 + [VMEM] * 4 + [ANY] * 9 + [VMEM] * 2,
        out_specs=(ANY,) * len(out),
        scratch_shapes=[
            vm(PAIR * PAIR * window, WIDE),
            vm(window, hd),
            vm(PAIR, GROUP * rows, hd, dtype=F32),
            vm(PAIR, PAIR * rows, KEY_TILE, dtype=F32),
            vm(PAIR * model, WIDE),
            vm(SLOTS, GROUP * rows, model),
            vm(chunks, 3 * rows, model),
            vm(chunks, rows, model),
            vm(PAIR, *state[1:], dtype=F32),
            vm(GROUP, 1, PAIR * hd, dtype=F32),
            vm(PAIR * ffn // WIDE, 1, WIDE, dtype=F32),
            *(vm(*b.shape) for b in biases),
            *(dma(chunks, 6) for _ in range(8)),
            dma(),
            dma(),
            dma(chunks),
            dma(chunks),
            dma(layers, 6),
            dma(layers, 6),
            dma(GROUP),
            dma(GROUP),
            *few,
            pltpu.SemaphoreType.REGULAR,
        ],
        compiler_params=pltpu.CompilerParams(vmem_limit_bytes=VMEM_LIMIT, collective_id=0, has_side_effects=True),
        name="step",
    )(scal, tokens, norms, cos, sin, *weights, *biases, *biases, *caches, w_o, w_up, w_down, b_o, b_down)


def copy_kernel(scal, *refs):
    hidden, kv, h_out, k_out, v_out, p_out, h_s, kv_s, in_sem, out_sem = refs
    window = k_out.shape[1]
    cut = window // GROUP
    part = hidden.shape[0] // GROUP
    moves = [(hidden.at[pl.ds(n * part, part)], h_s.at[pl.ds(n * part, part)], h_out.at[pl.ds(n * part, part)]) for n in range(GROUP)]
    for layer in range(k_out.shape[0]):
        for k, out in enumerate((k_out, v_out)):
            for n in range(GROUP):
                at = pl.ds((layer * PAIR + k) * window + n * cut, cut)
                moves.append((kv.at[at], kv_s.at[at], out.at[layer, pl.ds(n * cut, cut)]))
    for n, (src, mid, _) in enumerate(moves):
        pltpu.make_async_copy(src, mid, in_sem.at[n]).start()
    start_pos = scal[0]
    ahead = lax.broadcasted_iota(jnp.int32, p_out.shape, 1) + (window - lax.rem(start_pos, window))
    p_out[...] = start_pos + jnp.where(ahead >= window, ahead - window, ahead)
    for n, (src, mid, dst) in enumerate(moves):
        pltpu.make_async_copy(src, mid, in_sem.at[n]).wait()
        pltpu.make_async_copy(mid, dst, out_sem.at[n]).start()
    for n, (_, mid, dst) in enumerate(moves):
        pltpu.make_async_copy(mid, dst, out_sem.at[n]).wait()


def run_copy(scal, hidden, kv, layers, window):
    hd = kv.shape[1]
    planes = jax.ShapeDtypeStruct((layers, window, hd), BF16)
    count = GROUP + PAIR * GROUP * layers
    return pl.pallas_call(
        copy_kernel,
        out_shape=(jax.ShapeDtypeStruct(hidden.shape, BF16), planes, planes, jax.ShapeDtypeStruct((1, window), jnp.int32)),
        in_specs=[SMEM, ANY, ANY],
        out_specs=(ANY, ANY, ANY, VMEM),
        scratch_shapes=[vm(*hidden.shape), vm(*kv.shape), dma(count), dma(count)],
        compiler_params=pltpu.CompilerParams(vmem_limit_bytes=VMEM_LIMIT),
        name="copy_out",
    )(scal, hidden, kv)


def solution(mesh):
    row_spec = P('dp', 'tp', None)
    cache_spec = P(None, 'dp', None, 'tp', None)
    col_spec = P(None, None, 'tp')
    bias_spec = P(None, 'tp')
    in_specs = (row_spec, P('dp'), P('dp', None, None), P('dp', None, None), cache_spec, cache_spec, P('dp', None), P(), col_spec, bias_spec, col_spec, bias_spec, col_spec, bias_spec, P(None, 'tp', None), P(), col_spec, bias_spec, P(None, 'tp', None), P())
    out_specs = (row_spec, cache_spec, cache_spec, P('dp', None))

    def device_step(tokens, start_pos, cos_tab, sin_tab, key_cache, value_cache, slot_pos, norm_params, w_q, b_q, w_k, b_k, w_v, b_v, w_o, b_o, w_up, b_up, w_down, b_down):
        layers, _, window, _, hd = key_cache.shape
        caches = tuple(cache.reshape(layers, window, hd) for cache in (key_cache, value_cache))
        made = run_step(CHUNKS, start_pos, tokens[0], norm_params, cos_tab[0], sin_tab[0], (w_q, w_k, w_v), (b_q, b_k, b_v, b_up), caches, w_o, w_up, w_down, b_o, b_down)
        hidden, key_out, value_out, pos_out = run_copy(start_pos, made[0], made[1], layers, window)
        return hidden[None], key_out.reshape(key_cache.shape), value_out.reshape(value_cache.shape), pos_out

    return jax.shard_map(device_step, mesh=mesh, in_specs=in_specs, out_specs=out_specs, check_vma=False)
```

```python
import functools

import jax
import jax.numpy as jnp
from jax import lax
from jax.experimental import pallas as pl
from jax.experimental.pallas import tpu as pltpu
from jax.sharding import PartitionSpec as P

NORM_EPS = 1e-5
LOG2E = 1.4426950408889634
CHUNKS = 4
KEY_TILE = 512
LANES = 128
WIDE = 512
ROW_BLOCK = 16
PAIR = 2
GROUP = 4
WEIGHT_SLOTS = 3
SLOTS = 5
ROLL_ROWS = 256
ROLL_SLOTS = 4
EARLY = 7
LOWEST = -3.3e38
VMEM_LIMIT = 67_043_328
BF16 = jnp.bfloat16
F32 = jnp.float32
MESH = pl.DeviceIdType.MESH

ANY = pl.BlockSpec(memory_space=pl.ANY)
SMEM = pl.BlockSpec(memory_space=pltpu.SMEM)
VMEM = pl.BlockSpec(memory_space=pltpu.VMEM)
DMA = pltpu.SemaphoreType.DMA


def vm(*shape, dtype=BF16):
    return pltpu.VMEM(shape, dtype)


def dma(*shape):
    return DMA(shape) if shape else DMA


def whole(ref, sem):
    pltpu.make_async_copy(ref, ref, sem).wait()


def one_row(ref, n):
    return ref[pl.ds(n, 1), :].astype(F32)


def gelu_tanh(x):
    inner = 0.7978845608028654 * (x + 0.044715 * (x * x * x))
    return 0.5 * x * (1.0 + jnp.tanh(inner))


def normalized(values, gain, shift):
    centered = values - jnp.mean(values, axis=-1, keepdims=True)
    variance = jnp.mean(centered * centered, axis=-1, keepdims=True)
    return (centered * lax.rsqrt(variance + NORM_EPS) * gain + shift).astype(BF16)


def rotate(planes, put, window, shift, first, last):
    def tile(n, carry):
        want = lax.broadcasted_iota(jnp.int32, (ROLL_ROWS, 1), 0) + (n * ROLL_ROWS + shift)
        want = jnp.where(want >= window, want - window, want)
        pick = jnp.where(lax.broadcasted_iota(jnp.int32, (1, window), 1) == want, 1.0, 0.0).astype(BF16)
        put(n, [jnp.dot(pick, plane(), preferred_element_type=F32).astype(BF16) for plane in planes])
        return carry

    lax.fori_loop(first, last, tile, 0)


def reset_state(st_s, w):
    for g in range(PAIR):
        st_s[w, g, :, 0:LANES] = jnp.full((st_s.shape[2], LANES), LOWEST, F32)
        st_s[w, g, :, LANES:] = jnp.zeros((st_s.shape[2], st_s.shape[3] - LANES), F32)


def flash_step(st_s, w, s_s, scale, mask, values, next_scores, width=KEY_TILE):
    for g in range(PAIR):
        s = s_s[g, :, :width] * scale
        if mask is not None:
            s = jnp.where(mask, s, -jnp.inf)
        s_next = next_scores(g)
        m_prev = st_s[w, g, :, 0:LANES]
        m_next = jnp.maximum(m_prev, jnp.max(s, axis=1, keepdims=True))
        e = jnp.exp2(s - jnp.concatenate([m_next] * (s.shape[1] // LANES), axis=1))
        alpha = jnp.exp2(m_prev - m_next)
        total = st_s[w, g, :, LANES:2 * LANES] * alpha
        for k in range(s.shape[1] // LANES):
            total = total + e[:, k * LANES:(k + 1) * LANES]
        st_s[w, g, :, LANES:2 * LANES] = total
        st_s[w, g, :, 0:LANES] = m_next
        mixed = jnp.dot(e.astype(BF16), values(g), preferred_element_type=F32)
        st_s[w, g, :, 2 * LANES:] = st_s[w, g, :, 2 * LANES:] * jnp.concatenate([alpha] * (mixed.shape[1] // LANES), axis=1) + mixed
        s_s[g, :, :s_next.shape[1]] = s_next


def score_tile(queries, keys):
    return lax.dot_general(queries, keys, (((1,), (1,)), ((), ())), preferred_element_type=F32)


class Place:
    def __init__(self):
        me = lax.axis_index('tp')
        self.core = lax.rem(me, 2)
        self.xb = lax.rem(lax.div(me, 2), 2)
        self.yb = lax.div(me, 4)
        self.peer = me + 1 - 2 * self.core
        self.x = me + 2 - 4 * self.xb
        self.y = me + 4 - 8 * self.yb

    def member(self, i):
        xb = self.xb + lax.rem(i, 2) * (1 - 2 * self.xb)
        yb = self.yb + lax.div(i, 2) * (1 - 2 * self.yb)
        return yb * 2 + xb

    def barrier(self, others):
        sem = pltpu.get_barrier_semaphore()
        for other in others:
            pl.semaphore_signal(sem, inc=1, device_id={'tp': other}, device_id_type=MESH)
        pl.semaphore_wait(sem, len(others))


def remote(src, dst, send_sem, recv_sem, other):
    return pltpu.make_async_remote_copy(src_ref=src, dst_ref=dst, send_sem=send_sem, recv_sem=recv_sem, device_id={'tp': other}, device_id_type=MESH)


class Gather:
    def __init__(self, place, x_s, slot, send, recv, rows):
        self.place, self.x_s, self.slot, self.send, self.recv, self.rows = place, x_s, slot, send, recv, rows

    def copy(self, c, kind):
        r, h = self.rows, self.rows // 2
        x, y = self.place.x, self.place.y
        src, dst, other = ((0, r, x), (h, 2 * r + h, y), (h, r + h, x), (0, 2 * r, y), (r, 3 * r, y), (2 * r + h, 3 * r + h, x))[kind]
        slot = self.slot(c)
        return remote(self.x_s.at[slot, pl.ds(src, h)], self.x_s.at[slot, pl.ds(dst, h)], self.send.at[c, kind], self.recv.at[c, kind], other)

    def start(self, c):
        for kind in range(4):
            self.copy(c, kind).start()

    def forward(self, c):
        for kind in range(2):
            self.copy(c, kind).wait_recv()
            self.copy(c, kind + 4).start()

    def near(self, c):
        for kind in (2, 3):
            self.copy(c, kind).wait_recv()

    def finish(self, c):
        for kind in (4, 5):
            self.copy(c, kind).wait_recv()

    def drain(self, c):
        for kind in range(6):
            self.copy(c, kind).wait_send()


class Scatter:
    def __init__(self, place, out_s, slot, land_s, send, recv, rows):
        self.place, self.out_s, self.slot, self.land_s, self.send, self.recv, self.rows = place, out_s, slot, land_s, send, recv, rows

    def copy(self, c, kind):
        r, h = self.rows, self.rows // 2
        x, y = self.place.x, self.place.y
        src, dst, other = ((3 * r, 2 * r, x), (3 * r + h, 2 * r + h, y), (r, 0, x), (2 * r + h, r + h, y), (r + h, h, x), (2 * r, r, y))[kind]
        return remote(self.out_s.at[self.slot(c), pl.ds(src, h)], self.land_s.at[c, pl.ds(dst, h)], self.send.at[c, kind], self.recv.at[c, kind], other)

    def start(self, c):
        for kind in range(GROUP):
            self.copy(c, kind).start()

    def relay(self, c, settled):
        r, h = self.rows, self.rows // 2
        slot = self.slot(c)
        for kind, src, dst in ((0, 2 * r, 2 * r), (1, 2 * r + h, r + h)):
            self.copy(c, kind).wait_recv()

            def block(n, carry):
                at = pl.multiple_of(n * ROW_BLOCK, ROW_BLOCK)
                mine = self.out_s[slot, pl.ds(dst + at, ROW_BLOCK), :].astype(F32)
                came = self.land_s[c, pl.ds(src + at, ROW_BLOCK), :].astype(F32)
                self.out_s[slot, pl.ds(dst + at, ROW_BLOCK), :] = (mine + came).astype(BF16)
                return carry

            lax.fori_loop(0, h // ROW_BLOCK, block, 0)

        if settled is not None:
            @pl.when(settled >= 0)
            def _():
                self.drain(settled)

        self.copy(c, 5).start()
        self.copy(c, 4).start()

    def finish(self, c):
        for kind in range(2, 6):
            self.copy(c, kind).wait_recv()

    def drain(self, c):
        for kind in range(6):
            self.copy(c, kind).wait_send()

    def total(self, c, at):
        own = self.out_s[self.slot(c), pl.ds(at, ROW_BLOCK), :].astype(F32)
        came = [self.land_s[c, pl.ds(k * self.rows + at, ROW_BLOCK), :].astype(F32) for k in range(PAIR)]
        return own + came[0] + came[1]


def step_kernel(dims, scal, *refs):
    layers, chunks, rows, model, hd, window, ffn = dims
    (tokens, norms, cos, sin, wq, wk, wv, bq, bk, bv, bu, bq_push, bk_push, bv_push, bu_push, kc, vc, wo, up, down, b_o, b_down,
     h_out, kv_rolled, q_hbm, state, qkv_peer, wo_peer, up_peer, down_peer,
     big_s, q_s, t_s, s_s, wo_s, xo_s, land_s, mid_s, st_s, ba_s, bm_s, bq_s, bk_s, bv_s, bu_s,
     a1_send, a1_recv, a2_send, a2_recv, r1_send, r1_recv, r2_send, r2_recv, old_send, old_recv, kv_send, kv_recv, p_send, p_recv, b_send, b_recv,
     h_sem, t_sem, raw_sem, wa_sem, wo_sem, wm_sem, q_sem, st_sem, f_sem, ready) = refs
    place = Place()
    start_pos = scal[0]
    first_slot = lax.rem(start_pos, window)
    floor = window - 1 - start_pos
    block = rows * chunks
    tall = PAIR * rows
    tile = KEY_TILE
    tiles = window // tile
    scale = LOG2E * hd ** -0.5
    deep = GROUP * hd
    q_rows = PAIR * GROUP * tall
    last_chunk = chunks - 1
    roll_tiles = window // ROLL_ROWS

    def here(rows_from, count):
        return pl.ds(pl.multiple_of(rows_from, rows), count)

    def position(c, i):
        return (place.member(i) * PAIR + place.core) * block + c * rows

    def region(g, new):
        return jnp.where(new, (3 - g) * window, g * window)

    def q_row(c, g, i):
        return ((lax.rem(c, PAIR) * PAIR + g) * GROUP + i) * tall

    def tile_of(g, new, at, kv):
        return big_s[pl.ds(pl.multiple_of(region(g, new) + at, tile), tile), kv * hd:(kv + 1) * hd]

    def scores(c, i, g, new, at):
        return score_tile(q_s[here(q_row(c, g, i), tall), :], tile_of(g, new, at, 0))

    def row_blocks(body, first=0, last=rows):
        def one(n, carry):
            body(pl.ds(pl.multiple_of(n * ROW_BLOCK, ROW_BLOCK), ROW_BLOCK), n * ROW_BLOCK)
            return carry

        lax.fori_loop(first // ROW_BLOCK, last // ROW_BLOCK, one, 0)

    def q_move(c, out):
        inner, outer = q_s.at[here(lax.rem(c, PAIR) * q_rows, q_rows)], q_hbm.at[here(c * q_rows, q_rows)]
        sem = q_sem.at[lax.rem(c, PAIR)]
        return pltpu.make_async_copy(inner, outer, sem) if out else pltpu.make_async_copy(outer, inner, sem)

    def raw_copy(layer, k):
        return pltpu.make_async_copy((kc, vc)[k].at[layer], q_s, raw_sem)

    def table_copies(c):
        return [pltpu.make_async_copy(tab.at[here(position(c, i), rows)], t_s.at[k, pl.ds(i * rows, rows)], t_sem) for i in range(GROUP) for k, tab in enumerate((cos, sin))]

    def pushes(layer, some=slice(None)):
        pairs = ((wk, qkv_peer.at[layer, :, pl.ds(PAIR * hd, hd)]), (wv, qkv_peer.at[layer, :, pl.ds(3 * hd, hd)]), (wq, qkv_peer.at[layer, :, pl.ds(0, PAIR * hd)]),
                 (wo, wo_peer.at[layer]), (up, up_peer.at[layer]), (down, down_peer.at[layer]))
        return [remote(src.at[layer], dst, p_send.at[layer, k], p_recv.at[layer, k], place.peer) for k, (src, dst) in list(enumerate(pairs))[some]]

    def norm_into(layer, which, c, slot, *span):
        gain, shift = one_row(norms.at[layer], which), one_row(norms.at[layer], which + 1)

        def body(at, _):
            xo_s[slot, at, :] = normalized(mid_s[c, at, :].astype(F32), gain, shift)

        row_blocks(body, *span)

    def slot_of(layer, ahead):
        return lambda c: lax.rem(c + (SLOTS - layer + ahead), SLOTS)

    spot = [slot_of(layer, 0) for layer in range(layers)]
    spare = [(SLOTS - 1 - layer) % SLOTS for layer in range(layers)]
    gather1 = [Gather(place, xo_s, spot[layer], a1_send, a1_recv, rows) for layer in range(layers)]
    h_loads = [pltpu.make_async_copy(tokens.at[pl.ds(c * rows, rows)], mid_s.at[c], h_sem.at[c]) for c in range(chunks)]
    for copy in h_loads:
        copy.start()
    raw_copy(0, 0).start()
    place.barrier((place.x, place.y, place.peer))

    def lead(layer, c):
        if layer == 0:
            h_loads[c].wait()
        if layer == 0 and c == 0:
            for k in range(PAIR):
                norm_into(0, 0, c, spot[0](c), k * rows // PAIR, (k + 1) * rows // PAIR)
                for kind in (k, 3 - k):
                    gather1[0].copy(c, kind).start()
            return
        if layer == 0:
            norm_into(0, 0, c, spot[0](c))
        gather1[layer].start(c)

    lead(0, 0)
    lead(0, 1)
    b_copies = [remote(src, dst, b_send.at[k], b_recv.at[k], place.peer) for k, (src, dst) in enumerate(((bq_push, bq_s), (bk_push, bk_s), (bv_push, bv_s), (bu_push, bu_s)))]
    for copy in b_copies + pushes(0):
        copy.start()
    for copy in b_copies:
        copy.wait_recv()

    def pick(k):
        return jnp.where(k == 0, 3, jnp.where(k == 3, 0, k))

    def state_out(n, c, i):
        return pltpu.make_async_copy(st_s.at[lax.rem(n, PAIR)], state.at[c * GROUP + i], st_sem.at[lax.rem(n, PAIR)])

    def state_in(b):
        slot = lax.rem(b, PAIR)
        return pltpu.make_async_copy(state.at[lax.div(b, GROUP) * GROUP + pick(lax.rem(b, GROUP))], st_s.at[slot], st_sem.at[slot])

    def project_phase(layer):
        gather = gather1[layer]
        old_push = remote(big_s.at[pl.ds(0, window)], big_s.at[pl.ds(window, window)], old_send, old_recv, place.peer)
        n_passes = chunks + 1

        def wa_fetch(n):
            t = lax.rem(n, GROUP)
            slot = lax.rem(n, PAIR)
            dst = pl.ds(pl.multiple_of(slot * model, tile), model)
            sem = wa_sem.at[slot]
            sources = (((wk.at[layer], 0, hd), (wv.at[layer], hd, hd)), ((qkv_peer.at[layer, :, pl.ds(PAIR * hd, PAIR * hd)], 0, PAIR * hd),),
                       ((wq.at[layer], 0, PAIR * hd),), ((qkv_peer.at[layer, :, pl.ds(0, PAIR * hd)], 0, PAIR * hd),))
            for k, made in enumerate(sources):
                @pl.when(jnp.logical_and(t == k, n < n_passes * GROUP))
                def _():
                    for src, at, width in made:
                        pltpu.make_async_copy(src, wo_s.at[dst, pl.ds(at, width)], sem).start()

        def wa_landed(n):
            slot = lax.rem(n, PAIR)
            at = pl.ds(pl.multiple_of(slot * model, tile), model)
            whole(wo_s.at[at], wa_sem.at[slot])
            return at

        def kv_copy(c, i, g):
            at = position(c, i)
            return remote(big_s.at[here(region(g, True) + at, rows)], big_s.at[here(region(1 - g, True) + at, rows)], kv_send.at[c], kv_recv.at[c], place.peer)

        whole_chunk = big_s.at[pl.ds(0, PAIR * GROUP * rows)]
        kv_all = [remote(whole_chunk, whole_chunk, kv_send.at[c], kv_recv.at[c], place.peer) for c in range(chunks)]
        wa_fetch(jnp.int32(0))
        for copy in table_copies(0):
            copy.start()

        def put_old(k):
            def put(n, turned):
                big_s[pl.ds(pl.multiple_of(n * ROLL_ROWS, ROLL_ROWS), ROLL_ROWS), k * hd:(k + 1) * hd] = turned[0]

            return put

        raw = [lambda: q_s[...]]
        raw_copy(layer, 0).wait()
        rotate(raw, put_old(0), window, first_slot, 0, roll_tiles)
        raw_copy(layer, 1).start()
        gather.forward(0)
        lead(layer, 2)
        raw_copy(layer, 1).wait()
        rotate(raw, put_old(1), window, first_slot, 0, roll_tiles)
        if layer > 0:
            pl.semaphore_wait(ready, 1)
        old_push.start()
        gather.forward(1)
        for g, (for_q, for_k, for_v) in enumerate(((bq, bk, bv), (bq_s, bk_s, bv_s))):
            ba_s[PAIR * g] = one_row(for_q, layer)
            ba_s[PAIR * g + 1, :, :hd] = one_row(for_k, layer)
            ba_s[PAIR * g + 1, :, hd:] = one_row(for_v, layer)
        for copy in pushes(layer, slice(0, 3)):
            copy.wait_recv()
        wa_fetch(jnp.int32(1))

        def attend_old(c, i):
            b = c * (GROUP - 1) + i
            w = lax.rem(b, PAIR)
            j0 = position(c, i)
            diag = lax.div(j0, tile)
            i_next = jnp.minimum(i + 1, GROUP - 1)
            diag_next = lax.div(position(c, i_next), tile)

            @pl.when(b >= PAIR)
            def _():
                state_out(b - PAIR, c, i).wait()

            reset_state(st_s, w)

            def step(t, by_row):
                at = t * tile
                last = t + 1 == tiles
                at_next = jnp.where(last, diag_next, t + 1) * tile
                n_i = jnp.where(last, i_next, i)
                age = lax.broadcasted_iota(jnp.int32, (1, tile), 1) + at
                if by_row:
                    row = lax.rem(lax.broadcasted_iota(jnp.int32, (tall, 1), 0), rows) + j0
                    mask = age > jnp.maximum(row, floor)
                else:
                    mask = age > floor
                flash_step(st_s, w, s_s, scale, mask, lambda g: tile_of(g, False, at, 1), lambda g: scores(c, n_i, g, False, at_next))

            step(diag, True)

            def younger(t, carry):
                @pl.when(t > diag)
                def _():
                    step(t, False)

                return carry

            lax.fori_loop(1, tiles, younger, 0)
            state_out(b, c, i).start()

        def one_pass(p, carry):
            c = jnp.minimum(p, last_chunk)
            upper = p != n_passes - 1
            lower = p != n_passes - PAIR

            @pl.when(upper)
            def _():
                whole(t_s, t_sem)
                gather.near(c)

            @pl.when(lower)
            def _():
                gather.finish(c)

            slot = spot[layer](c)

            def rope(u, i):
                turned = jnp.concatenate([-u[:, hd // 2:], u[:, :hd // 2]], axis=1)
                return (u * t_s[0, i * rows:(i + 1) * rows, :] + turned * t_s[1, i * rows:(i + 1) * rows, :]).astype(BF16)

            parts = ((upper, 0, GROUP - 1), (lower, GROUP - 1, 1))

            def keys_values(g, inner):
                at = wa_landed(p * GROUP + g)
                for wanted, i0, count in parts:
                    @pl.when(wanted)
                    def _():
                        r0, n = i0 * rows, count * rows
                        u = jnp.dot(xo_s[slot, r0:r0 + n, :], wo_s[at, :], preferred_element_type=F32) + ba_s[PAIR * g + 1]
                        for i in range(count):
                            to = here(region(g, True) + position(c, i0 + i), rows)
                            part = u[i * rows:(i + 1) * rows]
                            big_s[to, :hd] = rope(part[:, :hd], i0 + i)
                            big_s[to, hd:] = part[:, hd:].astype(BF16)
                        for i in range(i0, i0 + count):
                            kv_copy(c, i, g).start()
                wa_fetch(p * GROUP + g + PAIR)
                return inner

            lax.fori_loop(0, PAIR, keys_values, 0)

            @pl.when(jnp.logical_and(upper, c >= PAIR))
            def _():
                q_move(c - PAIR, True).wait()

            def for_queries(g, inner):
                at = wa_landed(p * GROUP + PAIR + g)
                for wanted, i0, count in parts:
                    @pl.when(wanted)
                    def _():
                        r0, n = i0 * rows, count * rows
                        u = jnp.dot(xo_s[slot, r0:r0 + n, :], wo_s[at, :], preferred_element_type=F32) + ba_s[PAIR * g]
                        for h in range(PAIR):
                            for i in range(count):
                                part = u[i * rows:(i + 1) * rows, h * hd:(h + 1) * hd]
                                q_s[here(q_row(c, g, i0 + i) + h * rows, rows), :] = rope(part, i0 + i)
                wa_fetch(p * GROUP + g + PAIR + PAIR)
                return inner

            lax.fori_loop(0, PAIR, for_queries, 0)

            @pl.when(lower)
            def _():
                q_move(c, True).start()

            @pl.when(c < last_chunk)
            def _():
                for copy in table_copies(c + 1):
                    copy.start()

            @pl.when(p == 0)
            def _():
                old_push.wait_recv()

            @pl.when(jnp.logical_or(p == 0, p == 2))
            def _():
                early = lax.div(p, 2)
                for g in range(PAIR):
                    s_s[g] = scores(early, early, g, False, lax.div(position(early, early), tile) * tile)

                @pl.when(p == 2)
                def _():
                    gather.forward(3)

                def one(i, inner):
                    @pl.when(i >= early)
                    def _():
                        attend_old(early, i)

                    return inner

                lax.fori_loop(0, GROUP, one, 0)

            @pl.when(p == 0)
            def _():
                gather.forward(2)
                lead(layer, 3)

            @pl.when(p == 2)
            def _():
                q_move(2, True).wait()
                q_move(0, False).start()
                for b in range(PAIR):
                    state_out(jnp.int32(EARLY - PAIR + b), 0, 0).wait()
                for b in range(PAIR):
                    state_in(jnp.int32(b)).start()

            @pl.when(p == 3)
            def _():
                for copy in kv_all[:3]:
                    copy.wait_recv()
                q_move(0, False).wait()
                state_in(jnp.int32(0)).wait()
                diag = lax.div(position(0, 3), tile)
                width = 3 * rows

                def keys(g, t, kv):
                    return big_s[here(region(g, True) + t * tile, width), kv * hd:(kv + 1) * hd]

                def score(g, t):
                    return score_tile(q_s[here(q_row(0, g, 3), tall), :], keys(g, t, 0))

                for g in range(PAIR):
                    s_s[g, :, :width] = score(g, 0)

                def earlier(t, inner):
                    @pl.when(t < diag)
                    def _():
                        after = jnp.minimum(t + 1, tiles - 1)
                        flash_step(st_s, 0, s_s, scale, None, lambda g: keys(g, t, 1), lambda g: score(g, after), width)

                    return inner

                lax.fori_loop(0, tiles - 1, earlier, 0)

            return carry

        lax.fori_loop(0, n_passes, one_pass, 0)
        kv_all[3].wait_recv()
        for c in range(chunks):
            gather.drain(c)
        return kv_all + [old_push]

    def block_phase(layer, sent):
        onward = layer + 1 < layers
        gather = Gather(place, xo_s, spot[layer], a2_send, a2_recv, rows)
        first = Scatter(place, xo_s, slot_of(layer, 1), land_s, r1_send, r1_recv, rows)
        second = Scatter(place, xo_s, spot[layer], land_s, r2_send, r2_recv, rows)
        pushes(layer, slice(3, 4))[0].wait_recv()
        n_out = model // WIDE
        for n in range(n_out):
            for k, src in enumerate((wo, wo_peer)):
                pltpu.make_async_copy(src.at[layer, :, pl.ds(n * WIDE, WIDE)], wo_s.at[pl.ds(n * deep + k * PAIR * hd, PAIR * hd)], wo_sem).start()
        if onward:
            for copy in pushes(layer + 1):
                copy.start()

        def tile_at(diag, n):
            is_new = jnp.logical_or(n == 0, jnp.logical_and(n >= 2, n - 2 < diag))
            t = jnp.where(n < 2, diag, jnp.where(is_new, n - 2, n - 1))
            return is_new, t * tile

        for g in range(PAIR):
            s_s[g] = scores(jnp.int32(0), 3, g, True, lax.div(position(0, 3), tile) * tile)

        def attend(c, k):
            i = pick(k)
            b = c * GROUP + k
            w = lax.rem(b, PAIR)
            late = b >= EARLY
            j0 = position(c, i)
            diag = lax.div(j0, tile)
            count = jnp.where(b == 0, 2, jnp.where(late, tiles + 1, diag + 2))
            end = k == 3
            c_next = jnp.minimum(jnp.where(end, c + 1, c), last_chunk)
            i_next = pick(jnp.where(end, 0, k + 1))
            next_at = lax.div(position(c_next, i_next), tile) * tile

            @pl.when(late)
            def _():
                reset_state(st_s, w)

            @pl.when(jnp.logical_and(jnp.logical_not(late), b > 0))
            def _():
                state_in(b).wait()

            def step(n):
                is_new, at = tile_at(diag, n)
                following = jnp.where(jnp.logical_and(n == 0, jnp.logical_not(late)), 2, n + 1)
                last = following == count
                new_next, at_next = tile_at(diag, following)
                new_next = jnp.logical_or(last, new_next)
                at_next = jnp.where(last, next_at, at_next)
                nc = jnp.where(last, c_next, c)
                ni = jnp.where(last, i_next, i)
                col = lax.broadcasted_iota(jnp.int32, (1, tile), 1) + at
                row = lax.rem(lax.broadcasted_iota(jnp.int32, (tall, 1), 0), rows) + j0
                if not isinstance(n, int):
                    mask = col > jnp.where(is_new, -1, floor)
                elif n == 0:
                    mask = col <= row
                else:
                    mask = col > jnp.maximum(row, floor)
                flash_step(st_s, w, s_s, scale, mask, lambda g: tile_of(g, is_new, at, 1), lambda g: scores(nc, ni, g, new_next, at_next))

            step(0)

            @pl.when(late)
            def _():
                step(1)

            def last_keys(u, carry):
                @pl.when(jnp.logical_and(b == 0, u * GROUP < diag))
                def _():
                    def gathered(g, kv):
                        cols = slice(kv * hd, (kv + 1) * hd)
                        return jnp.concatenate([big_s[here(region(g, True) + (u * GROUP + n + 1) * tile - rows, rows), cols] for n in range(GROUP)], axis=0)

                    for g in range(PAIR):
                        s_s[g] = score_tile(q_s[here(q_row(c, g, i), tall), :], gathered(g, 0))
                    seen = lax.broadcasted_iota(jnp.int32, (1, tile), 1) < (diag - u * GROUP) * rows
                    flash_step(st_s, w, s_s, scale, seen, lambda g: gathered(g, 1), lambda g: scores(c_next, i_next, g, True, next_at))

                return carry

            lax.fori_loop(0, PAIR, last_keys, 0)

            def further(n, carry):
                @pl.when(n < count)
                def _():
                    step(n)

                return carry

            lax.fori_loop(2, tiles + 1, further, 0)
            slot = first.slot(c)
            for g in range(PAIR):
                total = jnp.sum(st_s[w, g, :, LANES:PAIR * LANES], axis=1, keepdims=True)
                out = (st_s[w, g, :, PAIR * LANES:] / total).astype(BF16)
                for h in range(PAIR):
                    n = PAIR * g + h
                    xo_s[slot, :rows, n * hd:(n + 1) * hd] = out[h * rows:(h + 1) * rows]

            @pl.when(b + PAIR < EARLY)
            def _():
                state_in(b + PAIR).start()

            @pl.when(b == 0)
            def _():
                whole(wo_s, wo_sem)

            to = here(i * rows, rows)

            def summed(n):
                return jnp.dot(xo_s[slot, :rows, :deep], wo_s[n * deep:(n + 1) * deep, :], preferred_element_type=F32).astype(BF16)

            held = deep // WIDE
            for n in range(held, n_out):
                xo_s[slot, to, n * WIDE:(n + 1) * WIDE] = summed(n)
            for n, part in enumerate([summed(n) for n in range(held)]):
                xo_s[slot, to, n * WIDE:(n + 1) * WIDE] = part

            @pl.when(i == 3)
            def _():
                first.copy(c, 0).start()
                first.copy(c, 1).start()

            for kind in (2, 3):
                @pl.when(i == kind - 1)
                def _():
                    first.copy(c, kind).start()

        bias_o, bias_d = one_row(b_o, layer), one_row(b_down, layer)

        def open_mlp(c):
            first.finish(c)

            def body(at, n):
                mid_s[c, at, :] = (mid_s[c, at, :].astype(F32) + first.total(c, n) + bias_o).astype(BF16)

            row_blocks(body)
            norm_into(layer, 2, c, spot[layer](c))
            gather.start(c)

        def attend_chunk(c, carry):
            def one(k, inner):
                @pl.when(jnp.logical_and(k == 3, c + 1 < chunks))
                def _():
                    q_move(c + 1, False).wait()

                attend(c, k)

                @pl.when(jnp.logical_and(c == 0, k == 1))
                def _():
                    q_move(last_chunk, True).wait()
                    q_move(1, False).start()

                @pl.when(jnp.where(c == 0, k == 3, jnp.logical_and(c >= 2, k == 0)))
                def _():
                    first.relay(jnp.maximum(c - 1, 0), c - 2)

                return inner

            lax.fori_loop(0, GROUP, one, 0)

            @pl.when(c + PAIR < chunks)
            def _():
                q_move(c + PAIR, False).start()

            @pl.when(c >= 2)
            def _():
                open_mlp(c - 2)

            return carry

        lax.fori_loop(0, chunks, attend_chunk, 0)
        for copy in sent:
            copy.wait_send()
        if onward:
            raw_copy(layer + 1, 0).start()
        for copy in pushes(layer, slice(4, None)):
            copy.wait_recv()
        n_up = PAIR * ffn // WIDE
        n_tiles = n_up + n_out
        sub = WIDE // PAIR
        n_sub = ffn // sub
        act = xo_s.at[spare[layer]]

        def slot_at(c, k):
            slot = lax.rem(c * n_tiles + k, WEIGHT_SLOTS)
            return slot, pl.multiple_of(slot * model, WIDE)

        def fetch(c, k):
            over = k >= n_tiles
            k = jnp.where(over, k - n_tiles, k)
            c = jnp.where(over, c + 1, c)
            slot, base = slot_at(c, k)

            @pl.when(c < chunks)
            def _():
                for part in range(PAIR):
                    n = PAIR * k + part
                    for side, src in enumerate((up, up_peer)):
                        @pl.when(jnp.logical_and(n >= side * n_sub, n < (side + 1) * n_sub))
                        def _():
                            at = pl.multiple_of((n - side * n_sub) * sub, sub)
                            pltpu.make_async_copy(src.at[layer, :, pl.ds(at, sub)], big_s.at[pl.ds(base, model), pl.ds(part * sub, sub)], wm_sem.at[slot]).start()

                @pl.when(k >= n_up)
                def _():
                    at = pl.multiple_of((k - n_up) * WIDE, WIDE)
                    for side, src in enumerate((down, down_peer)):
                        dst = big_s.at[pl.ds(pl.multiple_of(base + side * ffn, sub), ffn)]
                        pltpu.make_async_copy(src.at[layer, :, pl.ds(at, WIDE)], dst, wm_sem.at[slot]).start()

        def landed(c, k):
            slot, base = slot_at(c, k)
            whole(big_s.at[pl.ds(base, model)], wm_sem.at[slot])
            fetch(c, k + WEIGHT_SLOTS - 1)
            return pl.ds(base, model)

        for k in range(WEIGHT_SLOTS - 1):
            fetch(jnp.int32(0), jnp.int32(k))
        stage = WEIGHT_SLOTS * model

        def stage_at(n):
            slot = lax.rem(n, ROLL_SLOTS)
            return slot, pl.ds(pl.multiple_of(stage + slot * ROLL_ROWS, ROLL_ROWS), ROLL_ROWS)

        def staged(n):
            slot, at = stage_at(n)
            whole(big_s.at[at], f_sem.at[slot])

        def put_new(n, turned):
            slot, at = stage_at(n)

            @pl.when(n >= ROLL_SLOTS)
            def _():
                staged(n)

            for k in range(PAIR):
                cols = slice(k * hd, (k + 1) * hd)
                big_s[at, cols] = turned[k]
                dst = pl.ds(pl.multiple_of((layer * PAIR + k) * window + n * ROLL_ROWS, ROLL_ROWS), ROLL_ROWS)
                pltpu.make_async_copy(big_s.at[at, cols], kv_rolled.at[dst], f_sem.at[slot]).start()

        fresh = [lambda k=k: big_s[3 * window:, k * hd:(k + 1) * hd] for k in range(PAIR)]
        rotate(fresh, put_new, window, window - first_slot, 0, roll_tiles // PAIR)
        gather.forward(0)
        rotate(fresh, put_new, window, window - first_slot, roll_tiles // PAIR, roll_tiles)
        for n in range(PAIR * n_sub):
            src = bu if n < n_sub else bu_s
            at = n % n_sub * sub
            bm_s[n // PAIR, :, n % PAIR * sub:(n % PAIR + 1) * sub] = one_row(src, layer)[:, at:at + sub]
        first.relay(last_chunk, last_chunk - 1)
        open_mlp(2)
        gather.forward(1)
        open_mlp(3)
        first.drain(last_chunk)
        for n in range(ROLL_SLOTS):
            staged(n)

        def mlp_chunk(c, carry):
            gather.near(c)
            gather.finish(c)
            slot = spot[layer](c)

            def up_step(k, inner):
                at = landed(c, k)
                for top in range(PAIR):
                    r0 = top * tall
                    lifted = jnp.dot(xo_s[slot, r0:r0 + tall, :], big_s[at, :], preferred_element_type=F32) + bm_s[k]
                    act[r0:r0 + tall, pl.ds(pl.multiple_of(k * WIDE, WIDE), WIDE)] = gelu_tanh(lifted).astype(BF16)
                return inner

            lax.fori_loop(0, n_up, up_step, 0)

            @pl.when(c + 2 < chunks)
            def _():
                gather.forward(c + 2)

            gather.drain(c)

            @pl.when(c >= 2)
            def _():
                second.relay(c - 2, c - 3 if onward else None)

            def down_step(k, inner):
                at = landed(c, k)
                xo_s[slot, :, pl.ds(pl.multiple_of((k - n_up) * WIDE, WIDE), WIDE)] = jnp.dot(act[...], big_s[at, :], preferred_element_type=F32).astype(BF16)
                return inner

            lax.fori_loop(n_up, n_tiles, down_step, 0)
            second.start(c)
            return carry

        lax.fori_loop(0, chunks, mlp_chunk, 0)
        if onward:
            pl.semaphore_signal(ready, inc=1, device_id={'tp': place.peer}, device_id_type=MESH)

        def o_copy(c):
            return pltpu.make_async_copy(mid_s.at[c], h_out.at[here(c * rows, rows)], h_sem.at[c])

        second.relay(2, 1 if onward else None)
        second.relay(3, 2 if onward else None)

        def close(c, carry):
            second.finish(c)

            def body(at, n):
                mid_s[c, at, :] = (mid_s[c, at, :].astype(F32) + second.total(c, n) + bias_d).astype(BF16)

            row_blocks(body)
            if onward:
                norm_into(layer + 1, 0, c, spot[layer + 1](c))

                @pl.when(c < 2)
                def _():
                    lead(layer + 1, c)
            else:
                o_copy(c).start()
            return carry

        lax.fori_loop(0, chunks, close, 0)
        if onward:
            second.drain(last_chunk)
        else:
            for c in range(chunks):
                second.drain(c)
                o_copy(c).wait()

    for layer in range(layers):
        block_phase(layer, project_phase(layer))
    for copy in b_copies:
        copy.wait_send()
    for layer in range(layers):
        for copy in pushes(layer):
            copy.wait_send()


def run_step(chunks, scal, tokens, norms, cos, sin, weights, biases, caches, w_o, w_up, w_down, b_o, b_down):
    model = tokens.shape[1]
    rows = tokens.shape[0] // chunks
    layers, window, hd = caches[0].shape
    ffn = w_up.shape[2]
    dims = (layers, chunks, rows, model, hd, window, ffn)
    state = (PAIR * GROUP, PAIR, PAIR * rows, PAIR * LANES + hd)
    out = [tokens.shape, (layers * PAIR * window, hd), (chunks * PAIR * GROUP * PAIR * rows, hd), (layers, model, GROUP * hd), w_o.shape, w_up.shape, w_down.shape]
    out = [jax.ShapeDtypeStruct(o, BF16) for o in out]
    out.insert(3, jax.ShapeDtypeStruct(state, F32))
    few = [dma(*n) for n in ((chunks,), (), (), (PAIR,), (), (WEIGHT_SLOTS,), (PAIR,), (PAIR,), (ROLL_SLOTS,))]
    return pl.pallas_call(
        functools.partial(step_kernel, dims),
        out_shape=tuple(out),
        in_specs=[SMEM, ANY, VMEM] + [ANY] * 5 + [VMEM] * 4 + [ANY] * 9 + [VMEM] * 2,
        out_specs=(ANY,) * len(out),
        scratch_shapes=[
            vm(PAIR * PAIR * window, WIDE),
            vm(window, hd),
            vm(PAIR, GROUP * rows, hd, dtype=F32),
            vm(PAIR, PAIR * rows, KEY_TILE, dtype=F32),
            vm(PAIR * model, WIDE),
            vm(SLOTS, GROUP * rows, model),
            vm(chunks, 3 * rows, model),
            vm(chunks, rows, model),
            vm(PAIR, *state[1:], dtype=F32),
            vm(GROUP, 1, PAIR * hd, dtype=F32),
            vm(PAIR * ffn // WIDE, 1, WIDE, dtype=F32),
            *(vm(*b.shape) for b in biases),
            *(dma(chunks, 6) for _ in range(8)),
            dma(),
            dma(),
            dma(chunks),
            dma(chunks),
            dma(layers, 6),
            dma(layers, 6),
            dma(GROUP),
            dma(GROUP),
            *few,
            pltpu.SemaphoreType.REGULAR,
        ],
        compiler_params=pltpu.CompilerParams(vmem_limit_bytes=VMEM_LIMIT, collective_id=0, has_side_effects=True),
        name="step",
    )(scal, tokens, norms, cos, sin, *weights, *biases, *biases, *caches, w_o, w_up, w_down, b_o, b_down)


def copy_kernel(scal, *refs):
    hidden, kv, h_out, k_out, v_out, p_out, h_s, kv_s, in_sem, out_sem = refs
    window = k_out.shape[1]
    cut = window // GROUP
    part = hidden.shape[0] // GROUP
    moves = [(hidden.at[pl.ds(n * part, part)], h_s.at[pl.ds(n * part, part)], h_out.at[pl.ds(n * part, part)]) for n in range(GROUP)]
    for layer in range(k_out.shape[0]):
        for k, out in enumerate((k_out, v_out)):
            for n in range(GROUP):
                at = pl.ds((layer * PAIR + k) * window + n * cut, cut)
                moves.append((kv.at[at], kv_s.at[at], out.at[layer, pl.ds(n * cut, cut)]))
    for n, (src, mid, _) in enumerate(moves):
        pltpu.make_async_copy(src, mid, in_sem.at[n]).start()
    start_pos = scal[0]
    ahead = lax.broadcasted_iota(jnp.int32, p_out.shape, 1) + (window - lax.rem(start_pos, window))
    p_out[...] = start_pos + jnp.where(ahead >= window, ahead - window, ahead)
    for n, (src, mid, dst) in enumerate(moves):
        pltpu.make_async_copy(src, mid, in_sem.at[n]).wait()
        pltpu.make_async_copy(mid, dst, out_sem.at[n]).start()
    for n, (_, mid, dst) in enumerate(moves):
        pltpu.make_async_copy(mid, dst, out_sem.at[n]).wait()


def run_copy(scal, hidden, kv, layers, window):
    hd = kv.shape[1]
    planes = jax.ShapeDtypeStruct((layers, window, hd), BF16)
    count = GROUP + PAIR * GROUP * layers
    return pl.pallas_call(
        copy_kernel,
        out_shape=(jax.ShapeDtypeStruct(hidden.shape, BF16), planes, planes, jax.ShapeDtypeStruct((1, window), jnp.int32)),
        in_specs=[SMEM, ANY, ANY],
        out_specs=(ANY, ANY, ANY, VMEM),
        scratch_shapes=[vm(*hidden.shape), vm(*kv.shape), dma(count), dma(count)],
        compiler_params=pltpu.CompilerParams(vmem_limit_bytes=VMEM_LIMIT),
        name="copy_out",
    )(scal, hidden, kv)


def solution(mesh):
    row_spec = P('dp', 'tp', None)
    cache_spec = P(None, 'dp', None, 'tp', None)
    col_spec = P(None, None, 'tp')
    bias_spec = P(None, 'tp')
    in_specs = (row_spec, P('dp'), P('dp', None, None), P('dp', None, None), cache_spec, cache_spec, P('dp', None), P(), col_spec, bias_spec, col_spec, bias_spec, col_spec, bias_spec, P(None, 'tp', None), P(), col_spec, bias_spec, P(None, 'tp', None), P())
    out_specs = (row_spec, cache_spec, cache_spec, P('dp', None))

    def device_step(tokens, start_pos, cos_tab, sin_tab, key_cache, value_cache, slot_pos, norm_params, w_q, b_q, w_k, b_k, w_v, b_v, w_o, b_o, w_up, b_up, w_down, b_down):
        layers, _, window, _, hd = key_cache.shape
        caches = tuple(cache.reshape(layers, window, hd) for cache in (key_cache, value_cache))
        made = run_step(CHUNKS, start_pos, tokens[0], norm_params, cos_tab[0], sin_tab[0], (w_q, w_k, w_v), (b_q, b_k, b_v, b_up), caches, w_o, w_up, w_down, b_o, b_down)
        hidden, key_out, value_out, pos_out = run_copy(start_pos, made[0], made[1], layers, window)
        return hidden[None], key_out.reshape(key_cache.shape), value_out.reshape(value_cache.shape), pos_out

    return jax.shard_map(device_step, mesh=mesh, in_specs=in_specs, out_specs=out_specs, check_vma=False)
```

```python
import functools

import jax
import jax.numpy as jnp
from jax import lax
from jax.experimental import pallas as pl
from jax.experimental.pallas import tpu as pltpu
from jax.sharding import PartitionSpec as P

NORM_EPS = 1e-5
LOG2E = 1.4426950408889634
CHUNKS = 4
KEY_TILE = 512
LANES = 128
WIDE = 512
ROW_BLOCK = 32
PAIR = 2
GROUP = 4
WEIGHT_SLOTS = 3
SLOTS = 5
ROLL_ROWS = 256
ROLL_SLOTS = 4
EARLY = 7
LOWEST = -3.3e38
VMEM_LIMIT = 67_043_328
BF16 = jnp.bfloat16
F32 = jnp.float32
MESH = pl.DeviceIdType.MESH

ANY = pl.BlockSpec(memory_space=pl.ANY)
SMEM = pl.BlockSpec(memory_space=pltpu.SMEM)
VMEM = pl.BlockSpec(memory_space=pltpu.VMEM)
DMA = pltpu.SemaphoreType.DMA


def vm(*shape, dtype=BF16):
    return pltpu.VMEM(shape, dtype)


def dma(*shape):
    return DMA(shape) if shape else DMA


def whole(ref, sem):
    pltpu.make_async_copy(ref, ref, sem).wait()


def one_row(ref, n):
    return ref[pl.ds(n, 1), :].astype(F32)


def gelu_tanh(x):
    inner = 0.7978845608028654 * (x + 0.044715 * (x * x * x))
    return 0.5 * x * (1.0 + jnp.tanh(inner))


def normalized(values, gain, shift):
    centered = values - jnp.mean(values, axis=-1, keepdims=True)
    variance = jnp.mean(centered * centered, axis=-1, keepdims=True)
    return (centered * lax.rsqrt(variance + NORM_EPS) * gain + shift).astype(BF16)


def rotate(planes, put, window, shift, first, last):
    def tile(n, carry):
        want = lax.broadcasted_iota(jnp.int32, (ROLL_ROWS, 1), 0) + (n * ROLL_ROWS + shift)
        want = jnp.where(want >= window, want - window, want)
        pick = jnp.where(lax.broadcasted_iota(jnp.int32, (1, window), 1) == want, 1.0, 0.0).astype(BF16)
        put(n, [jnp.dot(pick, plane(), preferred_element_type=F32).astype(BF16) for plane in planes])
        return carry

    lax.fori_loop(first, last, tile, 0)


def reset_state(st_s, w):
    for g in range(PAIR):
        st_s[w, g, :, 0:LANES] = jnp.full((st_s.shape[2], LANES), LOWEST, F32)
        st_s[w, g, :, LANES:] = jnp.zeros((st_s.shape[2], st_s.shape[3] - LANES), F32)


def flash_step(st_s, w, s_s, scale, mask, values, next_scores, width=KEY_TILE):
    for g in range(PAIR):
        s = s_s[g, :, :width] * scale
        if mask is not None:
            s = jnp.where(mask, s, -jnp.inf)
        s_next = next_scores(g)
        m_prev = st_s[w, g, :, 0:LANES]
        m_next = jnp.maximum(m_prev, jnp.max(s, axis=1, keepdims=True))
        e = jnp.exp2(s - jnp.concatenate([m_next] * (s.shape[1] // LANES), axis=1))
        alpha = jnp.exp2(m_prev - m_next)
        total = st_s[w, g, :, LANES:2 * LANES] * alpha
        for k in range(s.shape[1] // LANES):
            total = total + e[:, k * LANES:(k + 1) * LANES]
        st_s[w, g, :, LANES:2 * LANES] = total
        st_s[w, g, :, 0:LANES] = m_next
        mixed = jnp.dot(e.astype(BF16), values(g), preferred_element_type=F32)
        st_s[w, g, :, 2 * LANES:] = st_s[w, g, :, 2 * LANES:] * jnp.concatenate([alpha] * (mixed.shape[1] // LANES), axis=1) + mixed
        s_s[g, :, :s_next.shape[1]] = s_next


def score_tile(queries, keys):
    return lax.dot_general(queries, keys, (((1,), (1,)), ((), ())), preferred_element_type=F32)


class Place:
    def __init__(self):
        me = lax.axis_index('tp')
        self.core = lax.rem(me, 2)
        self.xb = lax.rem(lax.div(me, 2), 2)
        self.yb = lax.div(me, 4)
        self.peer = me + 1 - 2 * self.core
        self.x = me + 2 - 4 * self.xb
        self.y = me + 4 - 8 * self.yb

    def member(self, i):
        xb = self.xb + lax.rem(i, 2) * (1 - 2 * self.xb)
        yb = self.yb + lax.div(i, 2) * (1 - 2 * self.yb)
        return yb * 2 + xb

    def arrive(self, others):
        sem = pltpu.get_barrier_semaphore()
        for other in others:
            pl.semaphore_signal(sem, inc=1, device_id={'tp': other}, device_id_type=MESH)


def remote(src, dst, send_sem, recv_sem, other):
    return pltpu.make_async_remote_copy(src_ref=src, dst_ref=dst, send_sem=send_sem, recv_sem=recv_sem, device_id={'tp': other}, device_id_type=MESH)


class Gather:
    def __init__(self, place, x_s, slot, send, recv, rows):
        self.place, self.x_s, self.slot, self.send, self.recv, self.rows = place, x_s, slot, send, recv, rows

    def copy(self, c, kind):
        r, h = self.rows, self.rows // 2
        x, y = self.place.x, self.place.y
        src, dst, other = ((0, r, x), (h, 2 * r + h, y), (h, r + h, x), (0, 2 * r, y), (r, 3 * r, y), (2 * r + h, 3 * r + h, x))[kind]
        slot = self.slot(c)
        return remote(self.x_s.at[slot, pl.ds(src, h)], self.x_s.at[slot, pl.ds(dst, h)], self.send.at[c, kind], self.recv.at[c, kind], other)

    def start(self, c):
        for kind in range(4):
            self.copy(c, kind).start()

    def forward(self, c):
        for kind in range(2):
            self.copy(c, kind).wait_recv()
            self.copy(c, kind + 4).start()

    def near(self, c):
        for kind in (2, 3):
            self.copy(c, kind).wait_recv()

    def finish(self, c):
        for kind in (4, 5):
            self.copy(c, kind).wait_recv()

    def drain(self, c):
        for kind in range(6):
            self.copy(c, kind).wait_send()


class Scatter:
    def __init__(self, place, out_s, slot, land_s, send, recv, rows):
        self.place, self.out_s, self.slot, self.land_s, self.send, self.recv, self.rows = place, out_s, slot, land_s, send, recv, rows

    def copy(self, c, kind):
        r, h = self.rows, self.rows // 2
        x, y = self.place.x, self.place.y
        src, dst, other = ((3 * r, 2 * r, x), (3 * r + h, 2 * r + h, y), (r, 0, x), (2 * r + h, r + h, y), (r + h, h, x), (2 * r, r, y))[kind]
        return remote(self.out_s.at[self.slot(c), pl.ds(src, h)], self.land_s.at[c, pl.ds(dst, h)], self.send.at[c, kind], self.recv.at[c, kind], other)

    def start(self, c):
        for kind in range(GROUP):
            self.copy(c, kind).start()

    def relay(self, c, settled):
        r, h = self.rows, self.rows // 2
        slot = self.slot(c)
        for kind, src, dst in ((0, 2 * r, 2 * r), (1, 2 * r + h, r + h)):
            self.copy(c, kind).wait_recv()

            def block(n, carry):
                at = pl.multiple_of(n * ROW_BLOCK, ROW_BLOCK)
                mine = self.out_s[slot, pl.ds(dst + at, ROW_BLOCK), :].astype(F32)
                came = self.land_s[c, pl.ds(src + at, ROW_BLOCK), :].astype(F32)
                self.out_s[slot, pl.ds(dst + at, ROW_BLOCK), :] = (mine + came).astype(BF16)
                return carry

            lax.fori_loop(0, h // ROW_BLOCK, block, 0)

        if settled is not None:
            @pl.when(settled >= 0)
            def _():
                self.drain(settled)

        self.copy(c, 5).start()
        self.copy(c, 4).start()

    def finish(self, c):
        for kind in range(2, 6):
            self.copy(c, kind).wait_recv()

    def drain(self, c):
        for kind in range(6):
            self.copy(c, kind).wait_send()

    def total(self, c, at):
        own = self.out_s[self.slot(c), pl.ds(at, ROW_BLOCK), :].astype(F32)
        came = [self.land_s[c, pl.ds(k * self.rows + at, ROW_BLOCK), :].astype(F32) for k in range(PAIR)]
        return own + came[0] + came[1]


def step_kernel(dims, scal, *refs):
    layers, chunks, rows, model, hd, window, ffn = dims
    (tokens, norms, cos, sin, wq, wk, wv, bq, bk, bv, bu, bq_push, bk_push, bv_push, bu_push, kc, vc, wo, up, down, b_o, b_down,
     h_out, kv_rolled, q_hbm, state, qkv_peer, wo_peer, up_peer, down_peer,
     big_s, q_s, t_s, s_s, wo_s, xo_s, land_s, mid_s, st_s, ba_s, bm_s, bq_s, bk_s, bv_s, bu_s,
     a1_send, a1_recv, a2_send, a2_recv, r1_send, r1_recv, r2_send, r2_recv, old_send, old_recv, kv_send, kv_recv, p_send, p_recv, b_send, b_recv,
     h_sem, t_sem, raw_sem, wa_sem, wo_sem, wm_sem, q_sem, st_sem, f_sem, ready) = refs
    place = Place()
    start_pos = scal[0]
    first_slot = lax.rem(start_pos, window)
    floor = window - 1 - start_pos
    block = rows * chunks
    tall = PAIR * rows
    tile = KEY_TILE
    tiles = window // tile
    scale = LOG2E * hd ** -0.5
    deep = GROUP * hd
    q_rows = PAIR * GROUP * tall
    last_chunk = chunks - 1
    roll_tiles = window // ROLL_ROWS

    def here(rows_from, count):
        return pl.ds(pl.multiple_of(rows_from, rows), count)

    def position(c, i):
        return (place.member(i) * PAIR + place.core) * block + c * rows

    def region(g, new):
        return jnp.where(new, (3 - g) * window, g * window)

    def q_row(c, g, i):
        return ((lax.rem(c, PAIR) * PAIR + g) * GROUP + i) * tall

    def tile_of(g, new, at, kv):
        return big_s[pl.ds(pl.multiple_of(region(g, new) + at, tile), tile), kv * hd:(kv + 1) * hd]

    def scores(c, i, g, new, at):
        return score_tile(q_s[here(q_row(c, g, i), tall), :], tile_of(g, new, at, 0))

    def row_blocks(body, first=0, last=rows):
        def one(n, carry):
            body(pl.ds(pl.multiple_of(n * ROW_BLOCK, ROW_BLOCK), ROW_BLOCK), n * ROW_BLOCK)
            return carry

        lax.fori_loop(first // ROW_BLOCK, last // ROW_BLOCK, one, 0)

    def q_move(c, out):
        inner, outer = q_s.at[here(lax.rem(c, PAIR) * q_rows, q_rows)], q_hbm.at[here(c * q_rows, q_rows)]
        sem = q_sem.at[lax.rem(c, PAIR)]
        return pltpu.make_async_copy(inner, outer, sem) if out else pltpu.make_async_copy(outer, inner, sem)

    def raw_copy(layer, k):
        return pltpu.make_async_copy((kc, vc)[k].at[layer], q_s, raw_sem)

    def table_copies(c):
        return [pltpu.make_async_copy(tab.at[here(position(c, i), rows)], t_s.at[k, pl.ds(i * rows, rows)], t_sem) for i in range(GROUP) for k, tab in enumerate((cos, sin))]

    def pushes(layer, some=slice(None)):
        pairs = ((wk, qkv_peer.at[layer, :, pl.ds(PAIR * hd, hd)]), (wv, qkv_peer.at[layer, :, pl.ds(3 * hd, hd)]), (wq, qkv_peer.at[layer, :, pl.ds(0, PAIR * hd)]),
                 (wo, wo_peer.at[layer]), (up, up_peer.at[layer]), (down, down_peer.at[layer]))
        return [remote(src.at[layer], dst, p_send.at[layer, k], p_recv.at[layer, k], place.peer) for k, (src, dst) in list(enumerate(pairs))[some]]

    def norm_into(layer, which, c, slot, *span):
        gain, shift = one_row(norms.at[layer], which), one_row(norms.at[layer], which + 1)

        def body(at, _):
            xo_s[slot, at, :] = normalized(mid_s[c, at, :].astype(F32), gain, shift)

        row_blocks(body, *span)

    def slot_of(layer, ahead):
        return lambda c: lax.rem(c + (SLOTS - layer + ahead), SLOTS)

    spot = [slot_of(layer, 0) for layer in range(layers)]
    spare = [(SLOTS - 1 - layer) % SLOTS for layer in range(layers)]
    gather1 = [Gather(place, xo_s, spot[layer], a1_send, a1_recv, rows) for layer in range(layers)]
    h_loads = [pltpu.make_async_copy(tokens.at[pl.ds(c * rows, rows)], mid_s.at[c], h_sem.at[c]) for c in range(chunks)]
    near = (place.x, place.y, place.peer)
    place.arrive(near)
    for copy in h_loads:
        copy.start()
    raw_copy(0, 0).start()

    def lead(layer, c):
        if layer == 0:
            h_loads[c].wait()
        if layer == 0 and c == 0:
            for k in range(PAIR):
                norm_into(0, 0, c, spot[0](c), k * rows // PAIR, (k + 1) * rows // PAIR)
                if k == 0:
                    pl.semaphore_wait(pltpu.get_barrier_semaphore(), len(near))
                for kind in (k, 3 - k):
                    gather1[0].copy(c, kind).start()
            return
        if layer == 0:
            norm_into(0, 0, c, spot[0](c))
        gather1[layer].start(c)

    lead(0, 0)
    lead(0, 1)
    b_copies = [remote(src, dst, b_send.at[k], b_recv.at[k], place.peer) for k, (src, dst) in enumerate(((bq_push, bq_s), (bk_push, bk_s), (bv_push, bv_s), (bu_push, bu_s)))]
    for copy in b_copies + pushes(0):
        copy.start()
    for copy in b_copies:
        copy.wait_recv()

    def pick(k):
        return jnp.where(k == 0, 3, jnp.where(k == 3, 0, k))

    def state_out(n, c, i):
        return pltpu.make_async_copy(st_s.at[lax.rem(n, PAIR)], state.at[c * GROUP + i], st_sem.at[lax.rem(n, PAIR)])

    def state_in(b):
        slot = lax.rem(b, PAIR)
        return pltpu.make_async_copy(state.at[lax.div(b, GROUP) * GROUP + pick(lax.rem(b, GROUP))], st_s.at[slot], st_sem.at[slot])

    def project_phase(layer):
        gather = gather1[layer]
        old_push = remote(big_s.at[pl.ds(0, window)], big_s.at[pl.ds(window, window)], old_send, old_recv, place.peer)
        n_passes = chunks + 1

        def wa_fetch(n):
            t = lax.rem(n, GROUP)
            slot = lax.rem(n, PAIR)
            dst = pl.ds(pl.multiple_of(slot * model, tile), model)
            sem = wa_sem.at[slot]
            sources = (((wk.at[layer], 0, hd), (wv.at[layer], hd, hd)), ((qkv_peer.at[layer, :, pl.ds(PAIR * hd, PAIR * hd)], 0, PAIR * hd),),
                       ((wq.at[layer], 0, PAIR * hd),), ((qkv_peer.at[layer, :, pl.ds(0, PAIR * hd)], 0, PAIR * hd),))
            for k, made in enumerate(sources):
                @pl.when(jnp.logical_and(t == k, n < n_passes * GROUP))
                def _():
                    for src, at, width in made:
                        pltpu.make_async_copy(src, wo_s.at[dst, pl.ds(at, width)], sem).start()

        def wa_landed(n):
            slot = lax.rem(n, PAIR)
            at = pl.ds(pl.multiple_of(slot * model, tile), model)
            whole(wo_s.at[at], wa_sem.at[slot])
            return at

        def kv_copy(c, i, g):
            at = position(c, i)
            return remote(big_s.at[here(region(g, True) + at, rows)], big_s.at[here(region(1 - g, True) + at, rows)], kv_send.at[c], kv_recv.at[c], place.peer)

        whole_chunk = big_s.at[pl.ds(0, PAIR * GROUP * rows)]
        kv_all = [remote(whole_chunk, whole_chunk, kv_send.at[c], kv_recv.at[c], place.peer) for c in range(chunks)]
        wa_fetch(jnp.int32(0))
        for copy in table_copies(0):
            copy.start()

        def put_old(k):
            def put(n, turned):
                big_s[pl.ds(pl.multiple_of(n * ROLL_ROWS, ROLL_ROWS), ROLL_ROWS), k * hd:(k + 1) * hd] = turned[0]

            return put

        raw = [lambda: q_s[...]]
        raw_copy(layer, 0).wait()
        rotate(raw, put_old(0), window, first_slot, 0, roll_tiles)
        raw_copy(layer, 1).start()
        gather.forward(0)
        lead(layer, 2)
        raw_copy(layer, 1).wait()
        rotate(raw, put_old(1), window, first_slot, 0, roll_tiles)
        if layer > 0:
            pl.semaphore_wait(ready, 1)
        old_push.start()
        gather.forward(1)
        for g, (for_q, for_k, for_v) in enumerate(((bq, bk, bv), (bq_s, bk_s, bv_s))):
            ba_s[PAIR * g] = one_row(for_q, layer)
            ba_s[PAIR * g + 1, :, :hd] = one_row(for_k, layer)
            ba_s[PAIR * g + 1, :, hd:] = one_row(for_v, layer)
        for copy in pushes(layer, slice(0, 3)):
            copy.wait_recv()
        wa_fetch(jnp.int32(1))

        def attend_old(c, i):
            b = c * (GROUP - 1) + i
            w = lax.rem(b, PAIR)
            j0 = position(c, i)
            diag = lax.div(j0, tile)
            i_next = jnp.minimum(i + 1, GROUP - 1)
            diag_next = lax.div(position(c, i_next), tile)

            @pl.when(b >= PAIR)
            def _():
                state_out(b - PAIR, c, i).wait()

            reset_state(st_s, w)

            def step(t, by_row):
                at = t * tile
                last = t + 1 == tiles
                at_next = jnp.where(last, diag_next, t + 1) * tile
                n_i = jnp.where(last, i_next, i)
                age = lax.broadcasted_iota(jnp.int32, (1, tile), 1) + at
                if by_row:
                    row = lax.rem(lax.broadcasted_iota(jnp.int32, (tall, 1), 0), rows) + j0
                    mask = age > jnp.maximum(row, floor)
                else:
                    mask = age > floor
                flash_step(st_s, w, s_s, scale, mask, lambda g: tile_of(g, False, at, 1), lambda g: scores(c, n_i, g, False, at_next))

            step(diag, True)

            def younger(t, carry):
                @pl.when(t > diag)
                def _():
                    step(t, False)

                return carry

            lax.fori_loop(1, tiles, younger, 0)
            state_out(b, c, i).start()

        def one_pass(p, carry):
            c = jnp.minimum(p, last_chunk)
            upper = p != n_passes - 1
            lower = p != n_passes - PAIR

            @pl.when(upper)
            def _():
                whole(t_s, t_sem)
                gather.near(c)

            @pl.when(lower)
            def _():
                gather.finish(c)

            slot = spot[layer](c)

            def rope(u, i):
                turned = jnp.concatenate([-u[:, hd // 2:], u[:, :hd // 2]], axis=1)
                return (u * t_s[0, i * rows:(i + 1) * rows, :] + turned * t_s[1, i * rows:(i + 1) * rows, :]).astype(BF16)

            parts = ((upper, 0, GROUP - 1), (lower, GROUP - 1, 1))

            def keys_values(g, inner):
                at = wa_landed(p * GROUP + g)
                for wanted, i0, count in parts:
                    @pl.when(wanted)
                    def _():
                        r0, n = i0 * rows, count * rows
                        u = jnp.dot(xo_s[slot, r0:r0 + n, :], wo_s[at, :], preferred_element_type=F32) + ba_s[PAIR * g + 1]
                        for i in range(count):
                            to = here(region(g, True) + position(c, i0 + i), rows)
                            part = u[i * rows:(i + 1) * rows]
                            big_s[to, :hd] = rope(part[:, :hd], i0 + i)
                            big_s[to, hd:] = part[:, hd:].astype(BF16)
                        for i in range(i0, i0 + count):
                            kv_copy(c, i, g).start()
                wa_fetch(p * GROUP + g + PAIR)
                return inner

            lax.fori_loop(0, PAIR, keys_values, 0)

            @pl.when(jnp.logical_and(upper, c >= PAIR))
            def _():
                q_move(c - PAIR, True).wait()

            def for_queries(g, inner):
                at = wa_landed(p * GROUP + PAIR + g)
                for wanted, i0, count in parts:
                    @pl.when(wanted)
                    def _():
                        r0, n = i0 * rows, count * rows
                        u = jnp.dot(xo_s[slot, r0:r0 + n, :], wo_s[at, :], preferred_element_type=F32) + ba_s[PAIR * g]
                        for h in range(PAIR):
                            for i in range(count):
                                part = u[i * rows:(i + 1) * rows, h * hd:(h + 1) * hd]
                                q_s[here(q_row(c, g, i0 + i) + h * rows, rows), :] = rope(part, i0 + i)
                wa_fetch(p * GROUP + g + PAIR + PAIR)
                return inner

            lax.fori_loop(0, PAIR, for_queries, 0)

            @pl.when(lower)
            def _():
                q_move(c, True).start()

            @pl.when(c < last_chunk)
            def _():
                for copy in table_copies(c + 1):
                    copy.start()

            @pl.when(p == 0)
            def _():
                old_push.wait_recv()

            @pl.when(jnp.logical_or(p == 0, p == 2))
            def _():
                early = lax.div(p, 2)
                for g in range(PAIR):
                    s_s[g] = scores(early, early, g, False, lax.div(position(early, early), tile) * tile)

                @pl.when(p == 2)
                def _():
                    gather.forward(3)

                def one(i, inner):
                    @pl.when(i >= early)
                    def _():
                        attend_old(early, i)

                    return inner

                lax.fori_loop(0, GROUP, one, 0)

            @pl.when(p == 0)
            def _():
                gather.forward(2)
                lead(layer, 3)

            @pl.when(p == 2)
            def _():
                q_move(2, True).wait()
                q_move(0, False).start()
                for b in range(PAIR):
                    state_out(jnp.int32(EARLY - PAIR + b), 0, 0).wait()
                for b in range(PAIR):
                    state_in(jnp.int32(b)).start()

            @pl.when(p == 3)
            def _():
                for copy in kv_all[:3]:
                    copy.wait_recv()
                q_move(0, False).wait()
                state_in(jnp.int32(0)).wait()
                diag = lax.div(position(0, 3), tile)
                width = 3 * rows

                def keys(g, t, kv):
                    return big_s[here(region(g, True) + t * tile, width), kv * hd:(kv + 1) * hd]

                def score(g, t):
                    return score_tile(q_s[here(q_row(0, g, 3), tall), :], keys(g, t, 0))

                for g in range(PAIR):
                    s_s[g, :, :width] = score(g, 0)

                def earlier(t, inner):
                    @pl.when(t < diag)
                    def _():
                        after = jnp.minimum(t + 1, tiles - 1)
                        flash_step(st_s, 0, s_s, scale, None, lambda g: keys(g, t, 1), lambda g: score(g, after), width)

                    return inner

                lax.fori_loop(0, tiles - 1, earlier, 0)

            return carry

        lax.fori_loop(0, n_passes, one_pass, 0)
        kv_all[3].wait_recv()
        for c in range(chunks):
            gather.drain(c)
        return kv_all + [old_push]

    def block_phase(layer, sent):
        onward = layer + 1 < layers
        gather = Gather(place, xo_s, spot[layer], a2_send, a2_recv, rows)
        first = Scatter(place, xo_s, slot_of(layer, 1), land_s, r1_send, r1_recv, rows)
        second = Scatter(place, xo_s, spot[layer], land_s, r2_send, r2_recv, rows)
        pushes(layer, slice(3, 4))[0].wait_recv()
        n_out = model // WIDE
        for n in range(n_out):
            for k, src in enumerate((wo, wo_peer)):
                pltpu.make_async_copy(src.at[layer, :, pl.ds(n * WIDE, WIDE)], wo_s.at[pl.ds(n * deep + k * PAIR * hd, PAIR * hd)], wo_sem).start()
        if onward:
            for copy in pushes(layer + 1):
                copy.start()

        def tile_at(diag, n):
            is_new = jnp.logical_or(n == 0, jnp.logical_and(n >= 2, n - 2 < diag))
            t = jnp.where(n < 2, diag, jnp.where(is_new, n - 2, n - 1))
            return is_new, t * tile

        for g in range(PAIR):
            s_s[g] = scores(jnp.int32(0), 3, g, True, lax.div(position(0, 3), tile) * tile)

        def attend(c, k):
            i = pick(k)
            b = c * GROUP + k
            w = lax.rem(b, PAIR)
            late = b >= EARLY
            j0 = position(c, i)
            diag = lax.div(j0, tile)
            count = jnp.where(b == 0, 2, jnp.where(late, tiles + 1, diag + 2))
            end = k == 3
            c_next = jnp.minimum(jnp.where(end, c + 1, c), last_chunk)
            i_next = pick(jnp.where(end, 0, k + 1))
            next_at = lax.div(position(c_next, i_next), tile) * tile

            @pl.when(late)
            def _():
                reset_state(st_s, w)

            @pl.when(jnp.logical_and(jnp.logical_not(late), b > 0))
            def _():
                state_in(b).wait()

            def step(n):
                is_new, at = tile_at(diag, n)
                following = jnp.where(jnp.logical_and(n == 0, jnp.logical_not(late)), 2, n + 1)
                last = following == count
                new_next, at_next = tile_at(diag, following)
                new_next = jnp.logical_or(last, new_next)
                at_next = jnp.where(last, next_at, at_next)
                nc = jnp.where(last, c_next, c)
                ni = jnp.where(last, i_next, i)
                col = lax.broadcasted_iota(jnp.int32, (1, tile), 1) + at
                row = lax.rem(lax.broadcasted_iota(jnp.int32, (tall, 1), 0), rows) + j0
                if not isinstance(n, int):
                    mask = col > jnp.where(is_new, -1, floor)
                elif n == 0:
                    mask = col <= row
                else:
                    mask = col > jnp.maximum(row, floor)
                flash_step(st_s, w, s_s, scale, mask, lambda g: tile_of(g, is_new, at, 1), lambda g: scores(nc, ni, g, new_next, at_next))

            step(0)

            @pl.when(late)
            def _():
                step(1)

            def last_keys(u, carry):
                @pl.when(jnp.logical_and(b == 0, u * GROUP < diag))
                def _():
                    def gathered(g, kv):
                        cols = slice(kv * hd, (kv + 1) * hd)
                        return jnp.concatenate([big_s[here(region(g, True) + (u * GROUP + n + 1) * tile - rows, rows), cols] for n in range(GROUP)], axis=0)

                    for g in range(PAIR):
                        s_s[g] = score_tile(q_s[here(q_row(c, g, i), tall), :], gathered(g, 0))
                    seen = lax.broadcasted_iota(jnp.int32, (1, tile), 1) < (diag - u * GROUP) * rows
                    flash_step(st_s, w, s_s, scale, seen, lambda g: gathered(g, 1), lambda g: scores(c_next, i_next, g, True, next_at))

                return carry

            lax.fori_loop(0, PAIR, last_keys, 0)

            def further(n, carry):
                @pl.when(n < count)
                def _():
                    step(n)

                return carry

            lax.fori_loop(2, tiles + 1, further, 0)
            slot = first.slot(c)
            for g in range(PAIR):
                total = jnp.sum(st_s[w, g, :, LANES:PAIR * LANES], axis=1, keepdims=True)
                out = (st_s[w, g, :, PAIR * LANES:] / total).astype(BF16)
                for h in range(PAIR):
                    n = PAIR * g + h
                    xo_s[slot, :rows, n * hd:(n + 1) * hd] = out[h * rows:(h + 1) * rows]

            @pl.when(b + PAIR < EARLY)
            def _():
                state_in(b + PAIR).start()

            @pl.when(b == 0)
            def _():
                whole(wo_s, wo_sem)

            to = here(i * rows, rows)

            def summed(n):
                return jnp.dot(xo_s[slot, :rows, :deep], wo_s[n * deep:(n + 1) * deep, :], preferred_element_type=F32).astype(BF16)

            held = deep // WIDE
            for n in range(held, n_out):
                xo_s[slot, to, n * WIDE:(n + 1) * WIDE] = summed(n)
            for n, part in enumerate([summed(n) for n in range(held)]):
                xo_s[slot, to, n * WIDE:(n + 1) * WIDE] = part

            @pl.when(i == 3)
            def _():
                first.copy(c, 0).start()
                first.copy(c, 1).start()

            for kind in (2, 3):
                @pl.when(i == kind - 1)
                def _():
                    first.copy(c, kind).start()

        bias_o, bias_d = one_row(b_o, layer), one_row(b_down, layer)

        def open_mlp(c):
            first.finish(c)

            def body(at, n):
                mid_s[c, at, :] = (mid_s[c, at, :].astype(F32) + first.total(c, n) + bias_o).astype(BF16)

            row_blocks(body)
            norm_into(layer, 2, c, spot[layer](c))
            gather.start(c)

        def attend_chunk(c, carry):
            def one(k, inner):
                @pl.when(jnp.logical_and(k == 3, c + 1 < chunks))
                def _():
                    q_move(c + 1, False).wait()

                attend(c, k)

                @pl.when(jnp.logical_and(c == 0, k == 1))
                def _():
                    q_move(last_chunk, True).wait()
                    q_move(1, False).start()

                @pl.when(jnp.where(c == 0, k == 3, jnp.logical_and(c >= 2, k == 0)))
                def _():
                    first.relay(jnp.maximum(c - 1, 0), c - 2)

                return inner

            lax.fori_loop(0, GROUP, one, 0)

            @pl.when(c + PAIR < chunks)
            def _():
                q_move(c + PAIR, False).start()

            @pl.when(c >= 2)
            def _():
                open_mlp(c - 2)

            return carry

        lax.fori_loop(0, chunks, attend_chunk, 0)
        for copy in sent:
            copy.wait_send()
        if onward:
            raw_copy(layer + 1, 0).start()
        for copy in pushes(layer, slice(4, None)):
            copy.wait_recv()
        n_up = PAIR * ffn // WIDE
        n_tiles = n_up + n_out
        sub = WIDE // PAIR
        n_sub = ffn // sub
        act = xo_s.at[spare[layer]]

        def slot_at(c, k):
            slot = lax.rem(c * n_tiles + k, WEIGHT_SLOTS)
            return slot, pl.multiple_of(slot * model, WIDE)

        def fetch(c, k):
            over = k >= n_tiles
            k = jnp.where(over, k - n_tiles, k)
            c = jnp.where(over, c + 1, c)
            slot, base = slot_at(c, k)

            @pl.when(c < chunks)
            def _():
                for part in range(PAIR):
                    n = PAIR * k + part
                    for side, src in enumerate((up, up_peer)):
                        @pl.when(jnp.logical_and(n >= side * n_sub, n < (side + 1) * n_sub))
                        def _():
                            at = pl.multiple_of((n - side * n_sub) * sub, sub)
                            pltpu.make_async_copy(src.at[layer, :, pl.ds(at, sub)], big_s.at[pl.ds(base, model), pl.ds(part * sub, sub)], wm_sem.at[slot]).start()

                @pl.when(k >= n_up)
                def _():
                    at = pl.multiple_of((k - n_up) * WIDE, WIDE)
                    for side, src in enumerate((down, down_peer)):
                        dst = big_s.at[pl.ds(pl.multiple_of(base + side * ffn, sub), ffn)]
                        pltpu.make_async_copy(src.at[layer, :, pl.ds(at, WIDE)], dst, wm_sem.at[slot]).start()

        def landed(c, k):
            slot, base = slot_at(c, k)
            whole(big_s.at[pl.ds(base, model)], wm_sem.at[slot])
            fetch(c, k + WEIGHT_SLOTS - 1)
            return pl.ds(base, model)

        for k in range(WEIGHT_SLOTS - 1):
            fetch(jnp.int32(0), jnp.int32(k))
        stage = WEIGHT_SLOTS * model

        def stage_at(n):
            slot = lax.rem(n, ROLL_SLOTS)
            return slot, pl.ds(pl.multiple_of(stage + slot * ROLL_ROWS, ROLL_ROWS), ROLL_ROWS)

        def staged(n):
            slot, at = stage_at(n)
            whole(big_s.at[at], f_sem.at[slot])

        def put_new(n, turned):
            slot, at = stage_at(n)

            @pl.when(n >= ROLL_SLOTS)
            def _():
                staged(n)

            for k in range(PAIR):
                cols = slice(k * hd, (k + 1) * hd)
                big_s[at, cols] = turned[k]
                dst = pl.ds(pl.multiple_of((layer * PAIR + k) * window + n * ROLL_ROWS, ROLL_ROWS), ROLL_ROWS)
                pltpu.make_async_copy(big_s.at[at, cols], kv_rolled.at[dst], f_sem.at[slot]).start()

        fresh = [lambda k=k: big_s[3 * window:, k * hd:(k + 1) * hd] for k in range(PAIR)]
        rotate(fresh, put_new, window, window - first_slot, 0, roll_tiles // PAIR)
        gather.forward(0)
        rotate(fresh, put_new, window, window - first_slot, roll_tiles // PAIR, roll_tiles)
        for n in range(PAIR * n_sub):
            src = bu if n < n_sub else bu_s
            at = n % n_sub * sub
            bm_s[n // PAIR, :, n % PAIR * sub:(n % PAIR + 1) * sub] = one_row(src, layer)[:, at:at + sub]
        first.relay(last_chunk, last_chunk - 1)
        open_mlp(2)
        gather.forward(1)
        open_mlp(3)
        first.drain(last_chunk)
        for n in range(ROLL_SLOTS):
            staged(n)

        def mlp_chunk(c, carry):
            gather.near(c)
            gather.finish(c)
            slot = spot[layer](c)

            def up_step(k, inner):
                at = landed(c, k)
                for top in range(PAIR):
                    r0 = top * tall
                    lifted = jnp.dot(xo_s[slot, r0:r0 + tall, :], big_s[at, :], preferred_element_type=F32) + bm_s[k]
                    act[r0:r0 + tall, pl.ds(pl.multiple_of(k * WIDE, WIDE), WIDE)] = gelu_tanh(lifted).astype(BF16)
                return inner

            lax.fori_loop(0, n_up, up_step, 0)

            @pl.when(c + 2 < chunks)
            def _():
                gather.forward(c + 2)

            gather.drain(c)

            @pl.when(c >= 2)
            def _():
                second.relay(c - 2, c - 3 if onward else None)

            def down_step(k, inner):
                at = landed(c, k)
                xo_s[slot, :, pl.ds(pl.multiple_of((k - n_up) * WIDE, WIDE), WIDE)] = jnp.dot(act[...], big_s[at, :], preferred_element_type=F32).astype(BF16)
                return inner

            lax.fori_loop(n_up, n_tiles, down_step, 0)
            second.start(c)
            return carry

        lax.fori_loop(0, chunks, mlp_chunk, 0)
        if onward:
            pl.semaphore_signal(ready, inc=1, device_id={'tp': place.peer}, device_id_type=MESH)

        def o_copy(c):
            return pltpu.make_async_copy(mid_s.at[c], h_out.at[here(c * rows, rows)], h_sem.at[c])

        second.relay(2, None)
        second.relay(3, None)
        if onward:
            second.drain(1)

        def close(c, carry):
            second.finish(c)

            def body(at, n):
                mid_s[c, at, :] = (mid_s[c, at, :].astype(F32) + second.total(c, n) + bias_d).astype(BF16)

            row_blocks(body)
            if onward:
                norm_into(layer + 1, 0, c, spot[layer + 1](c))

                @pl.when(c < 2)
                def _():
                    lead(layer + 1, c)
            else:
                o_copy(c).start()
            return carry

        lax.fori_loop(0, chunks, close, 0)
        if onward:
            second.drain(2)
            second.drain(last_chunk)
        else:
            for c in range(chunks):
                second.drain(c)
                o_copy(c).wait()

    for layer in range(layers):
        block_phase(layer, project_phase(layer))
    for copy in b_copies:
        copy.wait_send()
    for layer in range(layers):
        for copy in pushes(layer):
            copy.wait_send()


def run_step(chunks, scal, tokens, norms, cos, sin, weights, biases, caches, w_o, w_up, w_down, b_o, b_down):
    model = tokens.shape[1]
    rows = tokens.shape[0] // chunks
    layers, window, hd = caches[0].shape
    ffn = w_up.shape[2]
    dims = (layers, chunks, rows, model, hd, window, ffn)
    state = (PAIR * GROUP, PAIR, PAIR * rows, PAIR * LANES + hd)
    out = [tokens.shape, (layers * PAIR * window, hd), (chunks * PAIR * GROUP * PAIR * rows, hd), (layers, model, GROUP * hd), w_o.shape, w_up.shape, w_down.shape]
    out = [jax.ShapeDtypeStruct(o, BF16) for o in out]
    out.insert(3, jax.ShapeDtypeStruct(state, F32))
    few = [dma(*n) for n in ((chunks,), (), (), (PAIR,), (), (WEIGHT_SLOTS,), (PAIR,), (PAIR,), (ROLL_SLOTS,))]
    return pl.pallas_call(
        functools.partial(step_kernel, dims),
        out_shape=tuple(out),
        in_specs=[SMEM, ANY, VMEM] + [ANY] * 5 + [VMEM] * 4 + [ANY] * 9 + [VMEM] * 2,
        out_specs=(ANY,) * len(out),
        scratch_shapes=[
            vm(PAIR * PAIR * window, WIDE),
            vm(window, hd),
            vm(PAIR, GROUP * rows, hd, dtype=F32),
            vm(PAIR, PAIR * rows, KEY_TILE, dtype=F32),
            vm(PAIR * model, WIDE),
            vm(SLOTS, GROUP * rows, model),
            vm(chunks, 3 * rows, model),
            vm(chunks, rows, model),
            vm(PAIR, *state[1:], dtype=F32),
            vm(GROUP, 1, PAIR * hd, dtype=F32),
            vm(PAIR * ffn // WIDE, 1, WIDE, dtype=F32),
            *(vm(*b.shape) for b in biases),
            *(dma(chunks, 6) for _ in range(8)),
            dma(),
            dma(),
            dma(chunks),
            dma(chunks),
            dma(layers, 6),
            dma(layers, 6),
            dma(GROUP),
            dma(GROUP),
            *few,
            pltpu.SemaphoreType.REGULAR,
        ],
        compiler_params=pltpu.CompilerParams(vmem_limit_bytes=VMEM_LIMIT, collective_id=0, has_side_effects=True),
        name="step",
    )(scal, tokens, norms, cos, sin, *weights, *biases, *biases, *caches, w_o, w_up, w_down, b_o, b_down)


def copy_kernel(scal, *refs):
    hidden, kv, h_out, k_out, v_out, p_out, h_s, kv_s, in_sem, out_sem = refs
    window = k_out.shape[1]
    cut = window // GROUP
    part = hidden.shape[0] // GROUP
    moves = [(hidden.at[pl.ds(n * part, part)], h_s.at[pl.ds(n * part, part)], h_out.at[pl.ds(n * part, part)]) for n in range(GROUP)]
    for layer in range(k_out.shape[0]):
        for k, out in enumerate((k_out, v_out)):
            for n in range(GROUP):
                at = pl.ds((layer * PAIR + k) * window + n * cut, cut)
                moves.append((kv.at[at], kv_s.at[at], out.at[layer, pl.ds(n * cut, cut)]))
    for n, (src, mid, _) in enumerate(moves):
        pltpu.make_async_copy(src, mid, in_sem.at[n]).start()
    start_pos = scal[0]
    ahead = lax.broadcasted_iota(jnp.int32, p_out.shape, 1) + (window - lax.rem(start_pos, window))
    p_out[...] = start_pos + jnp.where(ahead >= window, ahead - window, ahead)
    for n, (src, mid, dst) in enumerate(moves):
        pltpu.make_async_copy(src, mid, in_sem.at[n]).wait()
        pltpu.make_async_copy(mid, dst, out_sem.at[n]).start()
    for n, (_, mid, dst) in enumerate(moves):
        pltpu.make_async_copy(mid, dst, out_sem.at[n]).wait()


def run_copy(scal, hidden, kv, layers, window):
    hd = kv.shape[1]
    planes = jax.ShapeDtypeStruct((layers, window, hd), BF16)
    count = GROUP + PAIR * GROUP * layers
    return pl.pallas_call(
        copy_kernel,
        out_shape=(jax.ShapeDtypeStruct(hidden.shape, BF16), planes, planes, jax.ShapeDtypeStruct((1, window), jnp.int32)),
        in_specs=[SMEM, ANY, ANY],
        out_specs=(ANY, ANY, ANY, VMEM),
        scratch_shapes=[vm(*hidden.shape), vm(*kv.shape), dma(count), dma(count)],
        compiler_params=pltpu.CompilerParams(vmem_limit_bytes=VMEM_LIMIT),
        name="copy_out",
    )(scal, hidden, kv)


def solution(mesh):
    row_spec = P('dp', 'tp', None)
    cache_spec = P(None, 'dp', None, 'tp', None)
    col_spec = P(None, None, 'tp')
    bias_spec = P(None, 'tp')
    in_specs = (row_spec, P('dp'), P('dp', None, None), P('dp', None, None), cache_spec, cache_spec, P('dp', None), P(), col_spec, bias_spec, col_spec, bias_spec, col_spec, bias_spec, P(None, 'tp', None), P(), col_spec, bias_spec, P(None, 'tp', None), P())
    out_specs = (row_spec, cache_spec, cache_spec, P('dp', None))

    def device_step(tokens, start_pos, cos_tab, sin_tab, key_cache, value_cache, slot_pos, norm_params, w_q, b_q, w_k, b_k, w_v, b_v, w_o, b_o, w_up, b_up, w_down, b_down):
        layers, _, window, _, hd = key_cache.shape
        caches = tuple(cache.reshape(layers, window, hd) for cache in (key_cache, value_cache))
        made = run_step(CHUNKS, start_pos, tokens[0], norm_params, cos_tab[0], sin_tab[0], (w_q, w_k, w_v), (b_q, b_k, b_v, b_up), caches, w_o, w_up, w_down, b_o, b_down)
        hidden, key_out, value_out, pos_out = run_copy(start_pos, made[0], made[1], layers, window)
        return hidden[None], key_out.reshape(key_cache.shape), value_out.reshape(value_cache.shape), pos_out

    return jax.shard_map(device_step, mesh=mesh, in_specs=in_specs, out_specs=out_specs, check_vma=False)
```

```python
import functools

import jax
import jax.numpy as jnp
from jax import lax
from jax.experimental import pallas as pl
from jax.experimental.pallas import tpu as pltpu
from jax.sharding import PartitionSpec as P

NORM_EPS = 1e-5
LOG2E = 1.4426950408889634
CHUNKS = 4
KEY_TILE = 512
LANES = 128
WIDE = 512
ROW_BLOCK = 32
PAIR = 2
GROUP = 4
WEIGHT_SLOTS = 3
SLOTS = 5
ROLL_ROWS = 256
ROLL_SLOTS = 4
EARLY = 6
LOWEST = -3.3e38
VMEM_LIMIT = 67_043_328
BF16 = jnp.bfloat16
F32 = jnp.float32
MESH = pl.DeviceIdType.MESH

ANY = pl.BlockSpec(memory_space=pl.ANY)
SMEM = pl.BlockSpec(memory_space=pltpu.SMEM)
VMEM = pl.BlockSpec(memory_space=pltpu.VMEM)
DMA = pltpu.SemaphoreType.DMA


def vm(*shape, dtype=BF16):
    return pltpu.VMEM(shape, dtype)


def dma(*shape):
    return DMA(shape) if shape else DMA


def whole(ref, sem):
    pltpu.make_async_copy(ref, ref, sem).wait()


def one_row(ref, n):
    return ref[pl.ds(n, 1), :].astype(F32)


def gelu_tanh(x):
    inner = 0.7978845608028654 * (x + 0.044715 * (x * x * x))
    return 0.5 * x * (1.0 + jnp.tanh(inner))


def normalized(values, gain, shift):
    centered = values - jnp.mean(values, axis=-1, keepdims=True)
    variance = jnp.mean(centered * centered, axis=-1, keepdims=True)
    return (centered * lax.rsqrt(variance + NORM_EPS) * gain + shift).astype(BF16)


def rotate(planes, put, window, shift, first, last):
    def tile(n, carry):
        want = lax.broadcasted_iota(jnp.int32, (ROLL_ROWS, 1), 0) + (n * ROLL_ROWS + shift)
        want = jnp.where(want >= window, want - window, want)
        pick = jnp.where(lax.broadcasted_iota(jnp.int32, (1, window), 1) == want, 1.0, 0.0).astype(BF16)
        put(n, [jnp.dot(pick, plane(), preferred_element_type=F32).astype(BF16) for plane in planes])
        return carry

    lax.fori_loop(first, last, tile, 0)


def reset_state(st_s, w):
    for g in range(PAIR):
        st_s[w, g, :, 0:LANES] = jnp.full((st_s.shape[2], LANES), LOWEST, F32)
        st_s[w, g, :, LANES:] = jnp.zeros((st_s.shape[2], st_s.shape[3] - LANES), F32)


def flash_step(st_s, w, s_s, scale, mask, values, next_scores, width=KEY_TILE):
    for g in range(PAIR):
        s = s_s[g, :, :width] * scale
        if mask is not None:
            s = jnp.where(mask, s, -jnp.inf)
        s_next = next_scores(g)
        m_prev = st_s[w, g, :, 0:LANES]
        m_next = jnp.maximum(m_prev, jnp.max(s, axis=1, keepdims=True))
        e = jnp.exp2(s - jnp.concatenate([m_next] * (s.shape[1] // LANES), axis=1))
        alpha = jnp.exp2(m_prev - m_next)
        total = st_s[w, g, :, LANES:2 * LANES] * alpha
        for k in range(s.shape[1] // LANES):
            total = total + e[:, k * LANES:(k + 1) * LANES]
        st_s[w, g, :, LANES:2 * LANES] = total
        st_s[w, g, :, 0:LANES] = m_next
        mixed = jnp.dot(e.astype(BF16), values(g), preferred_element_type=F32)
        st_s[w, g, :, 2 * LANES:] = st_s[w, g, :, 2 * LANES:] * jnp.concatenate([alpha] * (mixed.shape[1] // LANES), axis=1) + mixed
        s_s[g, :, :s_next.shape[1]] = s_next


def score_tile(queries, keys):
    return lax.dot_general(queries, keys, (((1,), (1,)), ((), ())), preferred_element_type=F32)


class Place:
    def __init__(self):
        me = lax.axis_index('tp')
        self.core = lax.rem(me, 2)
        self.xb = lax.rem(lax.div(me, 2), 2)
        self.yb = lax.div(me, 4)
        self.peer = me + 1 - 2 * self.core
        self.x = me + 2 - 4 * self.xb
        self.y = me + 4 - 8 * self.yb

    def member(self, i):
        xb = self.xb + lax.rem(i, 2) * (1 - 2 * self.xb)
        yb = self.yb + lax.div(i, 2) * (1 - 2 * self.yb)
        return yb * 2 + xb

    def arrive(self, others):
        sem = pltpu.get_barrier_semaphore()
        for other in others:
            pl.semaphore_signal(sem, inc=1, device_id={'tp': other}, device_id_type=MESH)


def remote(src, dst, send_sem, recv_sem, other):
    return pltpu.make_async_remote_copy(src_ref=src, dst_ref=dst, send_sem=send_sem, recv_sem=recv_sem, device_id={'tp': other}, device_id_type=MESH)


class Gather:
    def __init__(self, place, x_s, slot, send, recv, rows):
        self.place, self.x_s, self.slot, self.send, self.recv, self.rows = place, x_s, slot, send, recv, rows

    def copy(self, c, kind):
        r, h = self.rows, self.rows // 2
        x, y = self.place.x, self.place.y
        src, dst, other = ((0, r, x), (h, 2 * r + h, y), (h, r + h, x), (0, 2 * r, y), (r, 3 * r, y), (2 * r + h, 3 * r + h, x))[kind]
        slot = self.slot(c)
        return remote(self.x_s.at[slot, pl.ds(src, h)], self.x_s.at[slot, pl.ds(dst, h)], self.send.at[c, kind], self.recv.at[c, kind], other)

    def start(self, c):
        for kind in range(4):
            self.copy(c, kind).start()

    def forward(self, c):
        for kind in range(2):
            self.copy(c, kind).wait_recv()
            self.copy(c, kind + 4).start()

    def near(self, c):
        for kind in (2, 3):
            self.copy(c, kind).wait_recv()

    def finish(self, c):
        for kind in (4, 5):
            self.copy(c, kind).wait_recv()

    def drain(self, c):
        for kind in range(6):
            self.copy(c, kind).wait_send()


class Scatter:
    def __init__(self, place, out_s, slot, land_s, send, recv, rows):
        self.place, self.out_s, self.slot, self.land_s, self.send, self.recv, self.rows = place, out_s, slot, land_s, send, recv, rows

    def copy(self, c, kind):
        r, h = self.rows, self.rows // 2
        x, y = self.place.x, self.place.y
        src, dst, other = ((3 * r, 2 * r, x), (3 * r + h, 2 * r + h, y), (r, 0, x), (2 * r + h, r + h, y), (r + h, h, x), (2 * r, r, y))[kind]
        return remote(self.out_s.at[self.slot(c), pl.ds(src, h)], self.land_s.at[c, pl.ds(dst, h)], self.send.at[c, kind], self.recv.at[c, kind], other)

    def start(self, c):
        for kind in range(GROUP):
            self.copy(c, kind).start()

    def relay(self, c, settled):
        r, h = self.rows, self.rows // 2
        slot = self.slot(c)
        for kind, src, dst in ((0, 2 * r, 2 * r), (1, 2 * r + h, r + h)):
            self.copy(c, kind).wait_recv()

            def block(n, carry):
                at = pl.multiple_of(n * ROW_BLOCK, ROW_BLOCK)
                mine = self.out_s[slot, pl.ds(dst + at, ROW_BLOCK), :].astype(F32)
                came = self.land_s[c, pl.ds(src + at, ROW_BLOCK), :].astype(F32)
                self.out_s[slot, pl.ds(dst + at, ROW_BLOCK), :] = (mine + came).astype(BF16)
                return carry

            lax.fori_loop(0, h // ROW_BLOCK, block, 0)

        if settled is not None:
            @pl.when(settled >= 0)
            def _():
                self.drain(settled)

        self.copy(c, 5).start()
        self.copy(c, 4).start()

    def finish(self, c):
        for kind in range(2, 6):
            self.copy(c, kind).wait_recv()

    def drain(self, c):
        for kind in range(6):
            self.copy(c, kind).wait_send()

    def total(self, c, at):
        own = self.out_s[self.slot(c), pl.ds(at, ROW_BLOCK), :].astype(F32)
        came = [self.land_s[c, pl.ds(k * self.rows + at, ROW_BLOCK), :].astype(F32) for k in range(PAIR)]
        return own + came[0] + came[1]


def step_kernel(dims, scal, *refs):
    layers, chunks, rows, model, hd, window, ffn = dims
    (tokens, norms, cos, sin, wq, wk, wv, bq, bk, bv, bu, bq_push, bk_push, bv_push, bu_push, kc, vc, wo, up, down, b_o, b_down,
     h_out, kv_rolled, q_hbm, state, qkv_peer, wo_peer, up_peer, down_peer,
     big_s, q_s, t_s, s_s, wo_s, xo_s, land_s, mid_s, st_s, ba_s, bm_s, bq_s, bk_s, bv_s, bu_s,
     a1_send, a1_recv, a2_send, a2_recv, r1_send, r1_recv, r2_send, r2_recv, old_send, old_recv, kv_send, kv_recv, p_send, p_recv, b_send, b_recv,
     h_sem, t_sem, raw_sem, wa_sem, wo_sem, wm_sem, q_sem, st_sem, f_sem, ready) = refs
    place = Place()
    start_pos = scal[0]
    first_slot = lax.rem(start_pos, window)
    floor = window - 1 - start_pos
    block = rows * chunks
    tall = PAIR * rows
    tile = KEY_TILE
    tiles = window // tile
    scale = LOG2E * hd ** -0.5
    deep = GROUP * hd
    q_rows = PAIR * GROUP * tall
    last_chunk = chunks - 1
    roll_tiles = window // ROLL_ROWS

    def here(rows_from, count):
        return pl.ds(pl.multiple_of(rows_from, rows), count)

    def position(c, i):
        return (place.member(i) * PAIR + place.core) * block + c * rows

    def region(g, new):
        return jnp.where(new, (3 - g) * window, g * window)

    def q_row(c, g, i):
        return ((lax.rem(c, PAIR) * PAIR + g) * GROUP + i) * tall

    def tile_of(g, new, at, kv):
        return big_s[pl.ds(pl.multiple_of(region(g, new) + at, tile), tile), kv * hd:(kv + 1) * hd]

    def scores(c, i, g, new, at):
        return score_tile(q_s[here(q_row(c, g, i), tall), :], tile_of(g, new, at, 0))

    def row_blocks(body, first=0, last=rows):
        def one(n, carry):
            body(pl.ds(pl.multiple_of(n * ROW_BLOCK, ROW_BLOCK), ROW_BLOCK), n * ROW_BLOCK)
            return carry

        lax.fori_loop(first // ROW_BLOCK, last // ROW_BLOCK, one, 0)

    def q_move(c, out):
        inner, outer = q_s.at[here(lax.rem(c, PAIR) * q_rows, q_rows)], q_hbm.at[here(c * q_rows, q_rows)]
        sem = q_sem.at[lax.rem(c, PAIR)]
        return pltpu.make_async_copy(inner, outer, sem) if out else pltpu.make_async_copy(outer, inner, sem)

    def raw_copy(layer, k):
        return pltpu.make_async_copy((kc, vc)[k].at[layer], q_s, raw_sem)

    def table_copies(c):
        return [pltpu.make_async_copy(tab.at[here(position(c, i), rows)], t_s.at[k, pl.ds(i * rows, rows)], t_sem) for i in range(GROUP) for k, tab in enumerate((cos, sin))]

    def pushes(layer, some=slice(None)):
        pairs = ((wk, qkv_peer.at[layer, :, pl.ds(PAIR * hd, hd)]), (wv, qkv_peer.at[layer, :, pl.ds(3 * hd, hd)]), (wq, qkv_peer.at[layer, :, pl.ds(0, PAIR * hd)]),
                 (wo, wo_peer.at[layer]), (up, up_peer.at[layer]), (down, down_peer.at[layer]))
        return [remote(src.at[layer], dst, p_send.at[layer, k], p_recv.at[layer, k], place.peer) for k, (src, dst) in list(enumerate(pairs))[some]]

    def norm_into(layer, which, c, slot, *span):
        gain, shift = one_row(norms.at[layer], which), one_row(norms.at[layer], which + 1)

        def body(at, _):
            xo_s[slot, at, :] = normalized(mid_s[c, at, :].astype(F32), gain, shift)

        row_blocks(body, *span)

    def slot_of(layer, ahead):
        return lambda c: lax.rem(c + (SLOTS - layer + ahead), SLOTS)

    spot = [slot_of(layer, 0) for layer in range(layers)]
    spare = [(SLOTS - 1 - layer) % SLOTS for layer in range(layers)]
    gather1 = [Gather(place, xo_s, spot[layer], a1_send, a1_recv, rows) for layer in range(layers)]
    h_loads = [pltpu.make_async_copy(tokens.at[pl.ds(c * rows, rows)], mid_s.at[c], h_sem.at[c]) for c in range(chunks)]
    near = (place.x, place.y, place.peer)
    place.arrive(near)
    for copy in h_loads:
        copy.start()
    raw_copy(0, 0).start()

    def lead(layer, c):
        if layer == 0:
            h_loads[c].wait()
        if layer == 0 and c == 0:
            for k in range(PAIR):
                norm_into(0, 0, c, spot[0](c), k * rows // PAIR, (k + 1) * rows // PAIR)
                if k == 0:
                    pl.semaphore_wait(pltpu.get_barrier_semaphore(), len(near))
                for kind in (k, 3 - k):
                    gather1[0].copy(c, kind).start()
            return
        if layer == 0:
            norm_into(0, 0, c, spot[0](c))
        gather1[layer].start(c)

    lead(0, 0)
    lead(0, 1)
    b_copies = [remote(src, dst, b_send.at[k], b_recv.at[k], place.peer) for k, (src, dst) in enumerate(((bq_push, bq_s), (bk_push, bk_s), (bv_push, bv_s), (bu_push, bu_s)))]
    for copy in b_copies + pushes(0):
        copy.start()
    for copy in b_copies:
        copy.wait_recv()

    def pick(k):
        return jnp.where(k == 0, 3, jnp.where(k == 3, 0, k))

    def state_out(n, c, i):
        return pltpu.make_async_copy(st_s.at[lax.rem(n, PAIR)], state.at[c * GROUP + i], st_sem.at[lax.rem(n, PAIR)])

    def state_in(b):
        slot = lax.rem(b, PAIR)
        return pltpu.make_async_copy(state.at[lax.div(b, GROUP) * GROUP + pick(lax.rem(b, GROUP))], st_s.at[slot], st_sem.at[slot])

    def project_phase(layer):
        gather = gather1[layer]
        old_push = remote(big_s.at[pl.ds(0, window)], big_s.at[pl.ds(window, window)], old_send, old_recv, place.peer)
        n_passes = chunks + 1

        def wa_fetch(n):
            t = lax.rem(n, GROUP)
            slot = lax.rem(n, PAIR)
            dst = pl.ds(pl.multiple_of(slot * model, tile), model)
            sem = wa_sem.at[slot]
            sources = (((wk.at[layer], 0, hd), (wv.at[layer], hd, hd)), ((qkv_peer.at[layer, :, pl.ds(PAIR * hd, PAIR * hd)], 0, PAIR * hd),),
                       ((wq.at[layer], 0, PAIR * hd),), ((qkv_peer.at[layer, :, pl.ds(0, PAIR * hd)], 0, PAIR * hd),))
            for k, made in enumerate(sources):
                @pl.when(jnp.logical_and(t == k, n < n_passes * GROUP))
                def _():
                    for src, at, width in made:
                        pltpu.make_async_copy(src, wo_s.at[dst, pl.ds(at, width)], sem).start()

        def wa_landed(n):
            slot = lax.rem(n, PAIR)
            at = pl.ds(pl.multiple_of(slot * model, tile), model)
            whole(wo_s.at[at], wa_sem.at[slot])
            return at

        def kv_copy(c, i, g):
            at = position(c, i)
            return remote(big_s.at[here(region(g, True) + at, rows)], big_s.at[here(region(1 - g, True) + at, rows)], kv_send.at[c], kv_recv.at[c], place.peer)

        whole_chunk = big_s.at[pl.ds(0, PAIR * GROUP * rows)]
        kv_all = [remote(whole_chunk, whole_chunk, kv_send.at[c], kv_recv.at[c], place.peer) for c in range(chunks)]
        wa_fetch(jnp.int32(0))
        for copy in table_copies(0):
            copy.start()

        def put_old(k):
            def put(n, turned):
                big_s[pl.ds(pl.multiple_of(n * ROLL_ROWS, ROLL_ROWS), ROLL_ROWS), k * hd:(k + 1) * hd] = turned[0]

            return put

        raw = [lambda: q_s[...]]
        raw_copy(layer, 0).wait()
        rotate(raw, put_old(0), window, first_slot, 0, roll_tiles)
        raw_copy(layer, 1).start()
        gather.forward(0)
        lead(layer, 2)
        raw_copy(layer, 1).wait()
        rotate(raw, put_old(1), window, first_slot, 0, roll_tiles)
        if layer > 0:
            pl.semaphore_wait(ready, 1)
        old_push.start()
        gather.forward(1)
        for g, (for_q, for_k, for_v) in enumerate(((bq, bk, bv), (bq_s, bk_s, bv_s))):
            ba_s[PAIR * g] = one_row(for_q, layer)
            ba_s[PAIR * g + 1, :, :hd] = one_row(for_k, layer)
            ba_s[PAIR * g + 1, :, hd:] = one_row(for_v, layer)
        for copy in pushes(layer, slice(0, 3)):
            copy.wait_recv()
        wa_fetch(jnp.int32(1))

        def attend_old(c, i):
            b = jnp.where(c == 0, i, GROUP + lax.div(i, 2))
            w = lax.rem(b, PAIR)
            j0 = position(c, i)
            diag = lax.div(j0, tile)
            i_next = jnp.where(c == 0, jnp.minimum(i + 1, GROUP - 1), GROUP - 1)
            diag_next = lax.div(position(c, i_next), tile)

            @pl.when(b >= PAIR)
            def _():
                state_out(b - PAIR, c, i).wait()

            reset_state(st_s, w)

            def step(t, by_row):
                at = t * tile
                last = t + 1 == tiles
                at_next = jnp.where(last, diag_next, t + 1) * tile
                n_i = jnp.where(last, i_next, i)
                age = lax.broadcasted_iota(jnp.int32, (1, tile), 1) + at
                if by_row:
                    row = lax.rem(lax.broadcasted_iota(jnp.int32, (tall, 1), 0), rows) + j0
                    mask = age > jnp.maximum(row, floor)
                else:
                    mask = age > floor
                flash_step(st_s, w, s_s, scale, mask, lambda g: tile_of(g, False, at, 1), lambda g: scores(c, n_i, g, False, at_next))

            step(diag, True)

            def younger(t, carry):
                @pl.when(t > diag)
                def _():
                    step(t, False)

                return carry

            lax.fori_loop(1, tiles, younger, 0)
            state_out(b, c, i).start()

        def one_pass(p, carry):
            c = jnp.minimum(p, last_chunk)
            upper = p != n_passes - 1
            lower = p != n_passes - PAIR

            @pl.when(upper)
            def _():
                whole(t_s, t_sem)
                gather.near(c)

            @pl.when(lower)
            def _():
                gather.finish(c)

            slot = spot[layer](c)

            def rope(u, i):
                turned = jnp.concatenate([-u[:, hd // 2:], u[:, :hd // 2]], axis=1)
                return (u * t_s[0, i * rows:(i + 1) * rows, :] + turned * t_s[1, i * rows:(i + 1) * rows, :]).astype(BF16)

            parts = ((upper, 0, GROUP - 1), (lower, GROUP - 1, 1))

            def keys_values(g, inner):
                at = wa_landed(p * GROUP + g)
                for wanted, i0, count in parts:
                    @pl.when(wanted)
                    def _():
                        r0, n = i0 * rows, count * rows
                        u = jnp.dot(xo_s[slot, r0:r0 + n, :], wo_s[at, :], preferred_element_type=F32) + ba_s[PAIR * g + 1]
                        for i in range(count):
                            to = here(region(g, True) + position(c, i0 + i), rows)
                            part = u[i * rows:(i + 1) * rows]
                            big_s[to, :hd] = rope(part[:, :hd], i0 + i)
                            big_s[to, hd:] = part[:, hd:].astype(BF16)
                        for i in range(i0, i0 + count):
                            kv_copy(c, i, g).start()
                wa_fetch(p * GROUP + g + PAIR)
                return inner

            lax.fori_loop(0, PAIR, keys_values, 0)

            @pl.when(jnp.logical_and(upper, c >= PAIR))
            def _():
                q_move(c - PAIR, True).wait()

            def for_queries(g, inner):
                at = wa_landed(p * GROUP + PAIR + g)
                for wanted, i0, count in parts:
                    @pl.when(wanted)
                    def _():
                        r0, n = i0 * rows, count * rows
                        u = jnp.dot(xo_s[slot, r0:r0 + n, :], wo_s[at, :], preferred_element_type=F32) + ba_s[PAIR * g]
                        for h in range(PAIR):
                            for i in range(count):
                                part = u[i * rows:(i + 1) * rows, h * hd:(h + 1) * hd]
                                q_s[here(q_row(c, g, i0 + i) + h * rows, rows), :] = rope(part, i0 + i)
                wa_fetch(p * GROUP + g + PAIR + PAIR)
                return inner

            lax.fori_loop(0, PAIR, for_queries, 0)

            @pl.when(lower)
            def _():
                q_move(c, True).start()

            @pl.when(c < last_chunk)
            def _():
                for copy in table_copies(c + 1):
                    copy.start()

            @pl.when(p == 0)
            def _():
                old_push.wait_recv()

            @pl.when(jnp.logical_or(p == 0, p == 2))
            def _():
                early = lax.div(p, 2)
                for g in range(PAIR):
                    s_s[g] = scores(early, early, g, False, lax.div(position(early, early), tile) * tile)

                @pl.when(p == 2)
                def _():
                    gather.forward(3)

                def one(i, inner):
                    @pl.when(jnp.logical_or(early == 0, lax.rem(i, 2) == 1))
                    def _():
                        attend_old(early, i)

                    return inner

                lax.fori_loop(0, GROUP, one, 0)

            @pl.when(p == 0)
            def _():
                gather.forward(2)
                lead(layer, 3)

            @pl.when(p == 2)
            def _():
                q_move(2, True).wait()
                q_move(0, False).start()
                for b in range(PAIR):
                    state_out(jnp.int32(EARLY - PAIR + b), 0, 0).wait()
                for b in range(PAIR):
                    state_in(jnp.int32(b)).start()

            @pl.when(p == 3)
            def _():
                for copy in kv_all[:3]:
                    copy.wait_recv()
                q_move(0, False).wait()
                state_in(jnp.int32(0)).wait()
                diag = lax.div(position(0, 3), tile)
                width = 3 * rows

                def keys(g, t, kv):
                    return big_s[here(region(g, True) + t * tile, width), kv * hd:(kv + 1) * hd]

                def score(g, t):
                    return score_tile(q_s[here(q_row(0, g, 3), tall), :], keys(g, t, 0))

                for g in range(PAIR):
                    s_s[g, :, :width] = score(g, 0)

                def earlier(t, inner):
                    @pl.when(t < diag)
                    def _():
                        after = jnp.minimum(t + 1, tiles - 1)
                        flash_step(st_s, 0, s_s, scale, None, lambda g: keys(g, t, 1), lambda g: score(g, after), width)

                    return inner

                lax.fori_loop(0, tiles - 1, earlier, 0)

            return carry

        lax.fori_loop(0, n_passes, one_pass, 0)
        kv_all[3].wait_recv()
        for c in range(chunks):
            gather.drain(c)
        return kv_all + [old_push]

    def block_phase(layer, sent):
        onward = layer + 1 < layers
        gather = Gather(place, xo_s, spot[layer], a2_send, a2_recv, rows)
        first = Scatter(place, xo_s, slot_of(layer, 1), land_s, r1_send, r1_recv, rows)
        second = Scatter(place, xo_s, spot[layer], land_s, r2_send, r2_recv, rows)
        pushes(layer, slice(3, 4))[0].wait_recv()
        n_out = model // WIDE
        for n in range(n_out):
            for k, src in enumerate((wo, wo_peer)):
                pltpu.make_async_copy(src.at[layer, :, pl.ds(n * WIDE, WIDE)], wo_s.at[pl.ds(n * deep + k * PAIR * hd, PAIR * hd)], wo_sem).start()
        if onward:
            for copy in pushes(layer + 1):
                copy.start()

        def tile_at(diag, n):
            is_new = jnp.logical_or(n == 0, jnp.logical_and(n >= 2, n - 2 < diag))
            t = jnp.where(n < 2, diag, jnp.where(is_new, n - 2, n - 1))
            return is_new, t * tile

        for g in range(PAIR):
            s_s[g] = scores(jnp.int32(0), 3, g, True, lax.div(position(0, 3), tile) * tile)

        def attend(c, k):
            i = pick(k)
            b = c * GROUP + k
            w = lax.rem(b, PAIR)
            late = b >= EARLY
            j0 = position(c, i)
            diag = lax.div(j0, tile)
            count = jnp.where(b == 0, 2, jnp.where(late, tiles + 1, diag + 2))
            end = k == 3
            c_next = jnp.minimum(jnp.where(end, c + 1, c), last_chunk)
            i_next = pick(jnp.where(end, 0, k + 1))
            next_at = lax.div(position(c_next, i_next), tile) * tile

            @pl.when(late)
            def _():
                reset_state(st_s, w)

            @pl.when(jnp.logical_and(jnp.logical_not(late), b > 0))
            def _():
                state_in(b).wait()

            def step(n):
                is_new, at = tile_at(diag, n)
                following = jnp.where(jnp.logical_and(n == 0, jnp.logical_not(late)), 2, n + 1)
                last = following == count
                new_next, at_next = tile_at(diag, following)
                new_next = jnp.logical_or(last, new_next)
                at_next = jnp.where(last, next_at, at_next)
                nc = jnp.where(last, c_next, c)
                ni = jnp.where(last, i_next, i)
                col = lax.broadcasted_iota(jnp.int32, (1, tile), 1) + at
                row = lax.rem(lax.broadcasted_iota(jnp.int32, (tall, 1), 0), rows) + j0
                if not isinstance(n, int):
                    mask = col > jnp.where(is_new, -1, floor)
                elif n == 0:
                    mask = col <= row
                else:
                    mask = col > jnp.maximum(row, floor)
                flash_step(st_s, w, s_s, scale, mask, lambda g: tile_of(g, is_new, at, 1), lambda g: scores(nc, ni, g, new_next, at_next))

            step(0)

            @pl.when(late)
            def _():
                step(1)

            def last_keys(u, carry):
                @pl.when(jnp.logical_and(b == 0, u * GROUP < diag))
                def _():
                    def gathered(g, kv):
                        cols = slice(kv * hd, (kv + 1) * hd)
                        return jnp.concatenate([big_s[here(region(g, True) + (u * GROUP + n + 1) * tile - rows, rows), cols] for n in range(GROUP)], axis=0)

                    for g in range(PAIR):
                        s_s[g] = score_tile(q_s[here(q_row(c, g, i), tall), :], gathered(g, 0))
                    seen = lax.broadcasted_iota(jnp.int32, (1, tile), 1) < (diag - u * GROUP) * rows
                    flash_step(st_s, w, s_s, scale, seen, lambda g: gathered(g, 1), lambda g: scores(c_next, i_next, g, True, next_at))

                return carry

            lax.fori_loop(0, PAIR, last_keys, 0)

            def further(n, carry):
                @pl.when(n < count)
                def _():
                    step(n)

                return carry

            lax.fori_loop(2, tiles + 1, further, 0)
            slot = first.slot(c)
            for g in range(PAIR):
                total = jnp.sum(st_s[w, g, :, LANES:PAIR * LANES], axis=1, keepdims=True)
                out = (st_s[w, g, :, PAIR * LANES:] / total).astype(BF16)
                for h in range(PAIR):
                    n = PAIR * g + h
                    xo_s[slot, :rows, n * hd:(n + 1) * hd] = out[h * rows:(h + 1) * rows]

            @pl.when(b + PAIR < EARLY)
            def _():
                state_in(b + PAIR).start()

            @pl.when(b == 0)
            def _():
                whole(wo_s, wo_sem)

            to = here(i * rows, rows)

            def summed(n):
                return jnp.dot(xo_s[slot, :rows, :deep], wo_s[n * deep:(n + 1) * deep, :], preferred_element_type=F32).astype(BF16)

            held = deep // WIDE
            for n in range(held, n_out):
                xo_s[slot, to, n * WIDE:(n + 1) * WIDE] = summed(n)
            for n, part in enumerate([summed(n) for n in range(held)]):
                xo_s[slot, to, n * WIDE:(n + 1) * WIDE] = part

            @pl.when(i == 3)
            def _():
                first.copy(c, 0).start()
                first.copy(c, 1).start()

            for kind in (2, 3):
                @pl.when(i == kind - 1)
                def _():
                    first.copy(c, kind).start()

        bias_o, bias_d = one_row(b_o, layer), one_row(b_down, layer)

        def open_mlp(c):
            first.finish(c)

            def body(at, n):
                mid_s[c, at, :] = (mid_s[c, at, :].astype(F32) + first.total(c, n) + bias_o).astype(BF16)

            row_blocks(body)
            norm_into(layer, 2, c, spot[layer](c))
            gather.start(c)

        def attend_chunk(c, carry):
            def one(k, inner):
                @pl.when(jnp.logical_and(k == 3, c + 1 < chunks))
                def _():
                    q_move(c + 1, False).wait()

                attend(c, k)

                @pl.when(jnp.logical_and(c == 0, k == 1))
                def _():
                    q_move(last_chunk, True).wait()
                    q_move(1, False).start()

                @pl.when(jnp.where(c == 0, k == 3, jnp.logical_and(c >= 2, k == 0)))
                def _():
                    first.relay(jnp.maximum(c - 1, 0), c - 2)

                return inner

            lax.fori_loop(0, GROUP, one, 0)

            @pl.when(c + PAIR < chunks)
            def _():
                q_move(c + PAIR, False).start()

            @pl.when(c >= 2)
            def _():
                open_mlp(c - 2)

            return carry

        lax.fori_loop(0, chunks, attend_chunk, 0)
        for copy in sent:
            copy.wait_send()
        if onward:
            raw_copy(layer + 1, 0).start()
        for copy in pushes(layer, slice(4, None)):
            copy.wait_recv()
        n_up = PAIR * ffn // WIDE
        n_tiles = n_up + n_out
        sub = WIDE // PAIR
        n_sub = ffn // sub
        act = xo_s.at[spare[layer]]

        def slot_at(c, k):
            slot = lax.rem(c * n_tiles + k, WEIGHT_SLOTS)
            return slot, pl.multiple_of(slot * model, WIDE)

        def fetch(c, k):
            over = k >= n_tiles
            k = jnp.where(over, k - n_tiles, k)
            c = jnp.where(over, c + 1, c)
            slot, base = slot_at(c, k)

            @pl.when(c < chunks)
            def _():
                for part in range(PAIR):
                    n = PAIR * k + part
                    for side, src in enumerate((up, up_peer)):
                        @pl.when(jnp.logical_and(n >= side * n_sub, n < (side + 1) * n_sub))
                        def _():
                            at = pl.multiple_of((n - side * n_sub) * sub, sub)
                            pltpu.make_async_copy(src.at[layer, :, pl.ds(at, sub)], big_s.at[pl.ds(base, model), pl.ds(part * sub, sub)], wm_sem.at[slot]).start()

                @pl.when(k >= n_up)
                def _():
                    at = pl.multiple_of((k - n_up) * WIDE, WIDE)
                    for side, src in enumerate((down, down_peer)):
                        dst = big_s.at[pl.ds(pl.multiple_of(base + side * ffn, sub), ffn)]
                        pltpu.make_async_copy(src.at[layer, :, pl.ds(at, WIDE)], dst, wm_sem.at[slot]).start()

        def landed(c, k):
            slot, base = slot_at(c, k)
            whole(big_s.at[pl.ds(base, model)], wm_sem.at[slot])
            fetch(c, k + WEIGHT_SLOTS - 1)
            return pl.ds(base, model)

        for k in range(WEIGHT_SLOTS - 1):
            fetch(jnp.int32(0), jnp.int32(k))
        stage = WEIGHT_SLOTS * model

        def stage_at(n):
            slot = lax.rem(n, ROLL_SLOTS)
            return slot, pl.ds(pl.multiple_of(stage + slot * ROLL_ROWS, ROLL_ROWS), ROLL_ROWS)

        def staged(n):
            slot, at = stage_at(n)
            whole(big_s.at[at], f_sem.at[slot])

        def put_new(n, turned):
            slot, at = stage_at(n)

            @pl.when(n >= ROLL_SLOTS)
            def _():
                staged(n)

            for k in range(PAIR):
                cols = slice(k * hd, (k + 1) * hd)
                big_s[at, cols] = turned[k]
                dst = pl.ds(pl.multiple_of((layer * PAIR + k) * window + n * ROLL_ROWS, ROLL_ROWS), ROLL_ROWS)
                pltpu.make_async_copy(big_s.at[at, cols], kv_rolled.at[dst], f_sem.at[slot]).start()

        fresh = [lambda k=k: big_s[3 * window:, k * hd:(k + 1) * hd] for k in range(PAIR)]
        rotate(fresh, put_new, window, window - first_slot, 0, roll_tiles // PAIR)
        gather.forward(0)
        rotate(fresh, put_new, window, window - first_slot, roll_tiles // PAIR, roll_tiles)
        for n in range(PAIR * n_sub):
            src = bu if n < n_sub else bu_s
            at = n % n_sub * sub
            bm_s[n // PAIR, :, n % PAIR * sub:(n % PAIR + 1) * sub] = one_row(src, layer)[:, at:at + sub]
        first.relay(last_chunk, last_chunk - 1)
        open_mlp(2)
        gather.forward(1)
        open_mlp(3)
        first.drain(last_chunk)
        for n in range(ROLL_SLOTS):
            staged(n)

        def mlp_chunk(c, carry):
            gather.near(c)
            gather.finish(c)
            slot = spot[layer](c)

            def up_step(k, inner):
                at = landed(c, k)
                for top in range(PAIR):
                    r0 = top * tall
                    lifted = jnp.dot(xo_s[slot, r0:r0 + tall, :], big_s[at, :], preferred_element_type=F32) + bm_s[k]
                    act[r0:r0 + tall, pl.ds(pl.multiple_of(k * WIDE, WIDE), WIDE)] = gelu_tanh(lifted).astype(BF16)
                return inner

            lax.fori_loop(0, n_up, up_step, 0)

            @pl.when(c + 2 < chunks)
            def _():
                gather.forward(c + 2)

            gather.drain(c)

            @pl.when(c >= 2)
            def _():
                second.relay(c - 2, c - 3 if onward else None)

            def down_step(k, inner):
                at = landed(c, k)
                xo_s[slot, :, pl.ds(pl.multiple_of((k - n_up) * WIDE, WIDE), WIDE)] = jnp.dot(act[...], big_s[at, :], preferred_element_type=F32).astype(BF16)
                return inner

            lax.fori_loop(n_up, n_tiles, down_step, 0)
            second.start(c)
            return carry

        lax.fori_loop(0, chunks, mlp_chunk, 0)
        if onward:
            pl.semaphore_signal(ready, inc=1, device_id={'tp': place.peer}, device_id_type=MESH)

        def o_copy(c):
            return pltpu.make_async_copy(mid_s.at[c], h_out.at[here(c * rows, rows)], h_sem.at[c])

        second.relay(2, None)
        second.relay(3, None)
        if onward:
            second.drain(1)

        def close(c, carry):
            second.finish(c)

            def body(at, n):
                mid_s[c, at, :] = (mid_s[c, at, :].astype(F32) + second.total(c, n) + bias_d).astype(BF16)

            row_blocks(body)
            if onward:
                norm_into(layer + 1, 0, c, spot[layer + 1](c))

                @pl.when(c < 2)
                def _():
                    lead(layer + 1, c)
            else:
                o_copy(c).start()
            return carry

        lax.fori_loop(0, chunks, close, 0)
        if onward:
            second.drain(2)
            second.drain(last_chunk)
        else:
            for c in range(chunks):
                second.drain(c)
                o_copy(c).wait()

    for layer in range(layers):
        block_phase(layer, project_phase(layer))
    for copy in b_copies:
        copy.wait_send()
    for layer in range(layers):
        for copy in pushes(layer):
            copy.wait_send()


def run_step(chunks, scal, tokens, norms, cos, sin, weights, biases, caches, w_o, w_up, w_down, b_o, b_down):
    model = tokens.shape[1]
    rows = tokens.shape[0] // chunks
    layers, window, hd = caches[0].shape
    ffn = w_up.shape[2]
    dims = (layers, chunks, rows, model, hd, window, ffn)
    state = (PAIR * GROUP, PAIR, PAIR * rows, PAIR * LANES + hd)
    out = [tokens.shape, (layers * PAIR * window, hd), (chunks * PAIR * GROUP * PAIR * rows, hd), (layers, model, GROUP * hd), w_o.shape, w_up.shape, w_down.shape]
    out = [jax.ShapeDtypeStruct(o, BF16) for o in out]
    out.insert(3, jax.ShapeDtypeStruct(state, F32))
    few = [dma(*n) for n in ((chunks,), (), (), (PAIR,), (), (WEIGHT_SLOTS,), (PAIR,), (PAIR,), (ROLL_SLOTS,))]
    return pl.pallas_call(
        functools.partial(step_kernel, dims),
        out_shape=tuple(out),
        in_specs=[SMEM, ANY, VMEM] + [ANY] * 5 + [VMEM] * 4 + [ANY] * 9 + [VMEM] * 2,
        out_specs=(ANY,) * len(out),
        scratch_shapes=[
            vm(PAIR * PAIR * window, WIDE),
            vm(window, hd),
            vm(PAIR, GROUP * rows, hd, dtype=F32),
            vm(PAIR, PAIR * rows, KEY_TILE, dtype=F32),
            vm(PAIR * model, WIDE),
            vm(SLOTS, GROUP * rows, model),
            vm(chunks, 3 * rows, model),
            vm(chunks, rows, model),
            vm(PAIR, *state[1:], dtype=F32),
            vm(GROUP, 1, PAIR * hd, dtype=F32),
            vm(PAIR * ffn // WIDE, 1, WIDE, dtype=F32),
            *(vm(*b.shape) for b in biases),
            *(dma(chunks, 6) for _ in range(8)),
            dma(),
            dma(),
            dma(chunks),
            dma(chunks),
            dma(layers, 6),
            dma(layers, 6),
            dma(GROUP),
            dma(GROUP),
            *few,
            pltpu.SemaphoreType.REGULAR,
        ],
        compiler_params=pltpu.CompilerParams(vmem_limit_bytes=VMEM_LIMIT, collective_id=0, has_side_effects=True),
        name="step",
    )(scal, tokens, norms, cos, sin, *weights, *biases, *biases, *caches, w_o, w_up, w_down, b_o, b_down)


def copy_kernel(scal, *refs):
    hidden, kv, h_out, k_out, v_out, p_out, h_s, kv_s, in_sem, out_sem = refs
    window = k_out.shape[1]
    cut = window // GROUP
    part = hidden.shape[0] // GROUP
    moves = [(hidden.at[pl.ds(n * part, part)], h_s.at[pl.ds(n * part, part)], h_out.at[pl.ds(n * part, part)]) for n in range(GROUP)]
    for layer in range(k_out.shape[0]):
        for k, out in enumerate((k_out, v_out)):
            for n in range(GROUP):
                at = pl.ds((layer * PAIR + k) * window + n * cut, cut)
                moves.append((kv.at[at], kv_s.at[at], out.at[layer, pl.ds(n * cut, cut)]))
    for n, (src, mid, _) in enumerate(moves):
        pltpu.make_async_copy(src, mid, in_sem.at[n]).start()
    start_pos = scal[0]
    ahead = lax.broadcasted_iota(jnp.int32, p_out.shape, 1) + (window - lax.rem(start_pos, window))
    p_out[...] = start_pos + jnp.where(ahead >= window, ahead - window, ahead)
    for n, (src, mid, dst) in enumerate(moves):
        pltpu.make_async_copy(src, mid, in_sem.at[n]).wait()
        pltpu.make_async_copy(mid, dst, out_sem.at[n]).start()
    for n, (_, mid, dst) in enumerate(moves):
        pltpu.make_async_copy(mid, dst, out_sem.at[n]).wait()


def run_copy(scal, hidden, kv, layers, window):
    hd = kv.shape[1]
    planes = jax.ShapeDtypeStruct((layers, window, hd), BF16)
    count = GROUP + PAIR * GROUP * layers
    return pl.pallas_call(
        copy_kernel,
        out_shape=(jax.ShapeDtypeStruct(hidden.shape, BF16), planes, planes, jax.ShapeDtypeStruct((1, window), jnp.int32)),
        in_specs=[SMEM, ANY, ANY],
        out_specs=(ANY, ANY, ANY, VMEM),
        scratch_shapes=[vm(*hidden.shape), vm(*kv.shape), dma(count), dma(count)],
        compiler_params=pltpu.CompilerParams(vmem_limit_bytes=VMEM_LIMIT),
        name="copy_out",
    )(scal, hidden, kv)


def solution(mesh):
    row_spec = P('dp', 'tp', None)
    cache_spec = P(None, 'dp', None, 'tp', None)
    col_spec = P(None, None, 'tp')
    bias_spec = P(None, 'tp')
    in_specs = (row_spec, P('dp'), P('dp', None, None), P('dp', None, None), cache_spec, cache_spec, P('dp', None), P(), col_spec, bias_spec, col_spec, bias_spec, col_spec, bias_spec, P(None, 'tp', None), P(), col_spec, bias_spec, P(None, 'tp', None), P())
    out_specs = (row_spec, cache_spec, cache_spec, P('dp', None))

    def device_step(tokens, start_pos, cos_tab, sin_tab, key_cache, value_cache, slot_pos, norm_params, w_q, b_q, w_k, b_k, w_v, b_v, w_o, b_o, w_up, b_up, w_down, b_down):
        layers, _, window, _, hd = key_cache.shape
        caches = tuple(cache.reshape(layers, window, hd) for cache in (key_cache, value_cache))
        made = run_step(CHUNKS, start_pos, tokens[0], norm_params, cos_tab[0], sin_tab[0], (w_q, w_k, w_v), (b_q, b_k, b_v, b_up), caches, w_o, w_up, w_down, b_o, b_down)
        hidden, key_out, value_out, pos_out = run_copy(start_pos, made[0], made[1], layers, window)
        return hidden[None], key_out.reshape(key_cache.shape), value_out.reshape(value_cache.shape), pos_out

    return jax.shard_map(device_step, mesh=mesh, in_specs=in_specs, out_specs=out_specs, check_vma=False)
```

```python
import functools

import jax
import jax.numpy as jnp
from jax import lax
from jax.experimental import pallas as pl
from jax.experimental.pallas import tpu as pltpu
from jax.sharding import PartitionSpec as P

NORM_EPS = 1e-5
LOG2E = 1.4426950408889634
CHUNKS = 4
KEY_TILE = 512
LANES = 128
WIDE = 512
ROW_BLOCK = 32
PAIR = 2
GROUP = 4
WEIGHT_SLOTS = 3
SLOTS = 5
ROLL_ROWS = 256
ROLL_SLOTS = 4
EARLY = 6
LOWEST = -3.3e38
VMEM_LIMIT = 67_043_328
BF16 = jnp.bfloat16
F32 = jnp.float32
MESH = pl.DeviceIdType.MESH

ANY = pl.BlockSpec(memory_space=pl.ANY)
SMEM = pl.BlockSpec(memory_space=pltpu.SMEM)
VMEM = pl.BlockSpec(memory_space=pltpu.VMEM)
DMA = pltpu.SemaphoreType.DMA


def vm(*shape, dtype=BF16):
    return pltpu.VMEM(shape, dtype)


def dma(*shape):
    return DMA(shape) if shape else DMA


def whole(ref, sem):
    pltpu.make_async_copy(ref, ref, sem).wait()


def one_row(ref, n):
    return ref[pl.ds(n, 1), :].astype(F32)


def gelu_tanh(x):
    inner = 0.7978845608028654 * (x + 0.044715 * (x * x * x))
    return 0.5 * x * (1.0 + jnp.tanh(inner))


def normalized(values, gain, shift):
    centered = values - jnp.mean(values, axis=-1, keepdims=True)
    variance = jnp.mean(centered * centered, axis=-1, keepdims=True)
    return (centered * lax.rsqrt(variance + NORM_EPS) * gain + shift).astype(BF16)


def rotate(planes, put, window, shift, first, last):
    def tile(n, carry):
        want = lax.broadcasted_iota(jnp.int32, (ROLL_ROWS, 1), 0) + (n * ROLL_ROWS + shift)
        want = jnp.where(want >= window, want - window, want)
        pick = jnp.where(lax.broadcasted_iota(jnp.int32, (1, window), 1) == want, 1.0, 0.0).astype(BF16)
        put(n, [jnp.dot(pick, plane(), preferred_element_type=F32).astype(BF16) for plane in planes])
        return carry

    lax.fori_loop(first, last, tile, 0)


def reset_state(st_s, w):
    for g in range(PAIR):
        st_s[w, g, :, 0:LANES] = jnp.full((st_s.shape[2], LANES), LOWEST, F32)
        st_s[w, g, :, LANES:] = jnp.zeros((st_s.shape[2], st_s.shape[3] - LANES), F32)


def flash_step(st_s, w, s_s, scale, mask, values, next_scores, width=KEY_TILE):
    for g in range(PAIR):
        s = s_s[g, :, :width] * scale
        if mask is not None:
            s = jnp.where(mask, s, -jnp.inf)
        s_next = next_scores(g)
        m_prev = st_s[w, g, :, 0:LANES]
        m_next = jnp.maximum(m_prev, jnp.max(s, axis=1, keepdims=True))
        e = jnp.exp2(s - jnp.concatenate([m_next] * (s.shape[1] // LANES), axis=1))
        alpha = jnp.exp2(m_prev - m_next)
        total = st_s[w, g, :, LANES:2 * LANES] * alpha
        for k in range(s.shape[1] // LANES):
            total = total + e[:, k * LANES:(k + 1) * LANES]
        st_s[w, g, :, LANES:2 * LANES] = total
        st_s[w, g, :, 0:LANES] = m_next
        mixed = jnp.dot(e.astype(BF16), values(g), preferred_element_type=F32)
        st_s[w, g, :, 2 * LANES:] = st_s[w, g, :, 2 * LANES:] * jnp.concatenate([alpha] * (mixed.shape[1] // LANES), axis=1) + mixed
        s_s[g, :, :s_next.shape[1]] = s_next


def score_tile(queries, keys):
    return lax.dot_general(queries, keys, (((1,), (1,)), ((), ())), preferred_element_type=F32)


class Place:
    def __init__(self):
        me = lax.axis_index('tp')
        self.core = lax.rem(me, 2)
        self.xb = lax.rem(lax.div(me, 2), 2)
        self.yb = lax.div(me, 4)
        self.peer = me + 1 - 2 * self.core
        self.x = me + 2 - 4 * self.xb
        self.y = me + 4 - 8 * self.yb

    def member(self, i):
        xb = self.xb + lax.rem(i, 2) * (1 - 2 * self.xb)
        yb = self.yb + lax.div(i, 2) * (1 - 2 * self.yb)
        return yb * 2 + xb

    def arrive(self, others):
        sem = pltpu.get_barrier_semaphore()
        for other in others:
            pl.semaphore_signal(sem, inc=1, device_id={'tp': other}, device_id_type=MESH)


def remote(src, dst, send_sem, recv_sem, other):
    return pltpu.make_async_remote_copy(src_ref=src, dst_ref=dst, send_sem=send_sem, recv_sem=recv_sem, device_id={'tp': other}, device_id_type=MESH)


class Gather:
    def __init__(self, place, x_s, slot, send, recv, rows):
        self.place, self.x_s, self.slot, self.send, self.recv, self.rows = place, x_s, slot, send, recv, rows

    def copy(self, c, kind):
        r, h = self.rows, self.rows // 2
        x, y = self.place.x, self.place.y
        src, dst, other = ((0, r, x), (h, 2 * r + h, y), (h, r + h, x), (0, 2 * r, y), (r, 3 * r, y), (2 * r + h, 3 * r + h, x))[kind]
        slot = self.slot(c)
        return remote(self.x_s.at[slot, pl.ds(src, h)], self.x_s.at[slot, pl.ds(dst, h)], self.send.at[c, kind], self.recv.at[c, kind], other)

    def start(self, c):
        for kind in range(4):
            self.copy(c, kind).start()

    def forward(self, c):
        for kind in range(2):
            self.copy(c, kind).wait_recv()
            self.copy(c, kind + 4).start()

    def near(self, c):
        for kind in (2, 3):
            self.copy(c, kind).wait_recv()

    def finish(self, c):
        for kind in (4, 5):
            self.copy(c, kind).wait_recv()

    def drain(self, c):
        for kind in range(6):
            self.copy(c, kind).wait_send()


class Scatter:
    def __init__(self, place, out_s, slot, land_s, send, recv, rows):
        self.place, self.out_s, self.slot, self.land_s, self.send, self.recv, self.rows = place, out_s, slot, land_s, send, recv, rows

    def copy(self, c, kind):
        r, h = self.rows, self.rows // 2
        x, y = self.place.x, self.place.y
        src, dst, other = ((3 * r, 2 * r, x), (3 * r + h, 2 * r + h, y), (r, 0, x), (2 * r + h, r + h, y), (r + h, h, x), (2 * r, r, y))[kind]
        return remote(self.out_s.at[self.slot(c), pl.ds(src, h)], self.land_s.at[c, pl.ds(dst, h)], self.send.at[c, kind], self.recv.at[c, kind], other)

    def start(self, c):
        for kind in range(GROUP):
            self.copy(c, kind).start()

    def relay(self, c, settled):
        r, h = self.rows, self.rows // 2
        slot = self.slot(c)
        for kind, src, dst in ((0, 2 * r, 2 * r), (1, 2 * r + h, r + h)):
            self.copy(c, kind).wait_recv()

            def block(n, carry):
                at = pl.multiple_of(n * ROW_BLOCK, ROW_BLOCK)
                mine = self.out_s[slot, pl.ds(dst + at, ROW_BLOCK), :].astype(F32)
                came = self.land_s[c, pl.ds(src + at, ROW_BLOCK), :].astype(F32)
                self.out_s[slot, pl.ds(dst + at, ROW_BLOCK), :] = (mine + came).astype(BF16)
                return carry

            lax.fori_loop(0, h // ROW_BLOCK, block, 0)

        if settled is not None:
            @pl.when(settled >= 0)
            def _():
                self.drain(settled)

        self.copy(c, 5).start()
        self.copy(c, 4).start()

    def finish(self, c):
        for kind in range(2, 6):
            self.copy(c, kind).wait_recv()

    def drain(self, c):
        for kind in range(6):
            self.copy(c, kind).wait_send()

    def total(self, c, at):
        own = self.out_s[self.slot(c), pl.ds(at, ROW_BLOCK), :].astype(F32)
        came = [self.land_s[c, pl.ds(k * self.rows + at, ROW_BLOCK), :].astype(F32) for k in range(PAIR)]
        return own + came[0] + came[1]


def step_kernel(dims, scal, *refs):
    layers, chunks, rows, model, hd, window, ffn = dims
    (tokens, norms, cos, sin, wq, wk, wv, bq, bk, bv, bu, bq_push, bk_push, bv_push, bu_push, kc, vc, wo, up, down, b_o, b_down,
     h_out, kv_rolled, q_hbm, state, qkv_peer, wo_peer, up_peer, down_peer,
     big_s, q_s, t_s, s_s, wo_s, xo_s, land_s, mid_s, st_s, ba_s, bm_s, bq_s, bk_s, bv_s, bu_s,
     a1_send, a1_recv, a2_send, a2_recv, r1_send, r1_recv, r2_send, r2_recv, old_send, old_recv, kv_send, kv_recv, p_send, p_recv, b_send, b_recv,
     h_sem, t_sem, raw_sem, wa_sem, wo_sem, wm_sem, q_sem, st_sem, f_sem, ready) = refs
    place = Place()
    start_pos = scal[0]
    first_slot = lax.rem(start_pos, window)
    floor = window - 1 - start_pos
    block = rows * chunks
    tall = PAIR * rows
    tile = KEY_TILE
    tiles = window // tile
    scale = LOG2E * hd ** -0.5
    deep = GROUP * hd
    q_rows = PAIR * GROUP * tall
    last_chunk = chunks - 1
    roll_tiles = window // ROLL_ROWS

    def here(rows_from, count):
        return pl.ds(pl.multiple_of(rows_from, rows), count)

    def position(c, i):
        return (place.member(i) * PAIR + place.core) * block + c * rows

    def region(g, new):
        return jnp.where(new, (3 - g) * window, g * window)

    def q_row(c, g, i):
        return ((lax.rem(c, PAIR) * PAIR + g) * GROUP + i) * tall

    def tile_of(g, new, at, kv):
        return big_s[pl.ds(pl.multiple_of(region(g, new) + at, tile), tile), kv * hd:(kv + 1) * hd]

    def scores(c, i, g, new, at):
        return score_tile(q_s[here(q_row(c, g, i), tall), :], tile_of(g, new, at, 0))

    def row_blocks(body, first=0, last=rows):
        def one(n, carry):
            body(pl.ds(pl.multiple_of(n * ROW_BLOCK, ROW_BLOCK), ROW_BLOCK), n * ROW_BLOCK)
            return carry

        lax.fori_loop(first // ROW_BLOCK, last // ROW_BLOCK, one, 0)

    def q_move(c, out):
        inner, outer = q_s.at[here(lax.rem(c, PAIR) * q_rows, q_rows)], q_hbm.at[here(c * q_rows, q_rows)]
        sem = q_sem.at[lax.rem(c, PAIR)]
        return pltpu.make_async_copy(inner, outer, sem) if out else pltpu.make_async_copy(outer, inner, sem)

    def raw_copy(layer, k):
        return pltpu.make_async_copy((kc, vc)[k].at[layer], q_s, raw_sem)

    def table_copies(c):
        return [pltpu.make_async_copy(tab.at[here(position(c, i), rows)], t_s.at[k, pl.ds(i * rows, rows)], t_sem) for i in range(GROUP) for k, tab in enumerate((cos, sin))]

    def pushes(layer, some=slice(None)):
        pairs = ((wk, qkv_peer.at[layer, :, pl.ds(PAIR * hd, hd)]), (wv, qkv_peer.at[layer, :, pl.ds(3 * hd, hd)]), (wq, qkv_peer.at[layer, :, pl.ds(0, PAIR * hd)]),
                 (wo, wo_peer.at[layer]), (up, up_peer.at[layer]), (down, down_peer.at[layer]))
        return [remote(src.at[layer], dst, p_send.at[layer, k], p_recv.at[layer, k], place.peer) for k, (src, dst) in list(enumerate(pairs))[some]]

    def norm_into(layer, which, c, slot, *span):
        gain, shift = one_row(norms.at[layer], which), one_row(norms.at[layer], which + 1)

        def body(at, _):
            xo_s[slot, at, :] = normalized(mid_s[c, at, :].astype(F32), gain, shift)

        row_blocks(body, *span)

    def slot_of(layer, ahead):
        return lambda c: lax.rem(c + (SLOTS - layer + ahead), SLOTS)

    spot = [slot_of(layer, 0) for layer in range(layers)]
    spare = [(SLOTS - 1 - layer) % SLOTS for layer in range(layers)]
    gather1 = [Gather(place, xo_s, spot[layer], a1_send, a1_recv, rows) for layer in range(layers)]
    h_loads = [pltpu.make_async_copy(tokens.at[pl.ds(c * rows, rows)], mid_s.at[c], h_sem.at[c]) for c in range(chunks)]
    near = (place.x, place.y, place.peer)
    place.arrive(near)
    for copy in h_loads:
        copy.start()
    raw_copy(0, 0).start()

    def lead(layer, c):
        if layer == 0:
            h_loads[c].wait()
        if layer == 0 and c == 0:
            for k in range(PAIR):
                norm_into(0, 0, c, spot[0](c), k * rows // PAIR, (k + 1) * rows // PAIR)
                if k == 0:
                    pl.semaphore_wait(pltpu.get_barrier_semaphore(), len(near))
                for kind in (k, 3 - k):
                    gather1[0].copy(c, kind).start()
            return
        if layer == 0:
            norm_into(0, 0, c, spot[0](c))
        gather1[layer].start(c)

    lead(0, 0)
    lead(0, 1)
    b_copies = [remote(src, dst, b_send.at[k], b_recv.at[k], place.peer) for k, (src, dst) in enumerate(((bq_push, bq_s), (bk_push, bk_s), (bv_push, bv_s), (bu_push, bu_s)))]
    for copy in b_copies + pushes(0):
        copy.start()
    for copy in b_copies:
        copy.wait_recv()

    def pick(k):
        return jnp.where(k == 0, 3, jnp.where(k == 3, 0, k))

    def state_out(n, c, i):
        return pltpu.make_async_copy(st_s.at[lax.rem(n, PAIR)], state.at[c * GROUP + i], st_sem.at[lax.rem(n, PAIR)])

    def state_in(b):
        slot = lax.rem(b, PAIR)
        return pltpu.make_async_copy(state.at[lax.div(b, GROUP) * GROUP + pick(lax.rem(b, GROUP))], st_s.at[slot], st_sem.at[slot])

    def project_phase(layer):
        gather = gather1[layer]
        old_push = remote(big_s.at[pl.ds(0, window)], big_s.at[pl.ds(window, window)], old_send, old_recv, place.peer)
        n_passes = chunks + 1

        def wa_fetch(n):
            t = lax.rem(n, GROUP)
            slot = lax.rem(n, PAIR)
            dst = pl.ds(pl.multiple_of(slot * model, tile), model)
            sem = wa_sem.at[slot]
            sources = (((wk.at[layer], 0, hd), (wv.at[layer], hd, hd)), ((qkv_peer.at[layer, :, pl.ds(PAIR * hd, PAIR * hd)], 0, PAIR * hd),),
                       ((wq.at[layer], 0, PAIR * hd),), ((qkv_peer.at[layer, :, pl.ds(0, PAIR * hd)], 0, PAIR * hd),))
            for k, made in enumerate(sources):
                @pl.when(jnp.logical_and(t == k, n < n_passes * GROUP))
                def _():
                    for src, at, width in made:
                        pltpu.make_async_copy(src, wo_s.at[dst, pl.ds(at, width)], sem).start()

        def wa_landed(n):
            slot = lax.rem(n, PAIR)
            at = pl.ds(pl.multiple_of(slot * model, tile), model)
            whole(wo_s.at[at], wa_sem.at[slot])
            return at

        def kv_copy(c, i, g):
            at = position(c, i)
            return remote(big_s.at[here(region(g, True) + at, rows)], big_s.at[here(region(1 - g, True) + at, rows)], kv_send.at[c], kv_recv.at[c], place.peer)

        whole_chunk = big_s.at[pl.ds(0, PAIR * GROUP * rows)]
        kv_all = [remote(whole_chunk, whole_chunk, kv_send.at[c], kv_recv.at[c], place.peer) for c in range(chunks)]
        wa_fetch(jnp.int32(0))
        for copy in table_copies(0):
            copy.start()

        def put_old(k):
            def put(n, turned):
                big_s[pl.ds(pl.multiple_of(n * ROLL_ROWS, ROLL_ROWS), ROLL_ROWS), k * hd:(k + 1) * hd] = turned[0]

            return put

        raw = [lambda: q_s[...]]
        raw_copy(layer, 0).wait()
        rotate(raw, put_old(0), window, first_slot, 0, roll_tiles)
        raw_copy(layer, 1).start()
        gather.forward(0)
        lead(layer, 2)
        raw_copy(layer, 1).wait()
        rotate(raw, put_old(1), window, first_slot, 0, roll_tiles)
        if layer > 0:
            pl.semaphore_wait(ready, 1)
        old_push.start()
        gather.forward(1)
        for g, (for_q, for_k, for_v) in enumerate(((bq, bk, bv), (bq_s, bk_s, bv_s))):
            ba_s[PAIR * g] = one_row(for_q, layer)
            ba_s[PAIR * g + 1, :, :hd] = one_row(for_k, layer)
            ba_s[PAIR * g + 1, :, hd:] = one_row(for_v, layer)
        for copy in pushes(layer, slice(0, 3)):
            copy.wait_recv()
        wa_fetch(jnp.int32(1))

        def attend_old(c, i):
            b = jnp.where(c == 0, i, GROUP + lax.div(i, 2))
            w = lax.rem(b, PAIR)
            j0 = position(c, i)
            diag = lax.div(j0, tile)
            i_next = jnp.where(c == 0, jnp.minimum(i + 1, GROUP - 1), GROUP - 1)
            diag_next = lax.div(position(c, i_next), tile)

            @pl.when(b >= PAIR)
            def _():
                state_out(b - PAIR, c, i).wait()

            reset_state(st_s, w)

            def step(t, by_row):
                at = t * tile
                last = t + 1 == tiles
                at_next = jnp.where(last, diag_next, t + 1) * tile
                n_i = jnp.where(last, i_next, i)
                age = lax.broadcasted_iota(jnp.int32, (1, tile), 1) + at
                if by_row:
                    row = lax.rem(lax.broadcasted_iota(jnp.int32, (tall, 1), 0), rows) + j0
                    mask = age > jnp.maximum(row, floor)
                else:
                    mask = age > floor
                flash_step(st_s, w, s_s, scale, mask, lambda g: tile_of(g, False, at, 1), lambda g: scores(c, n_i, g, False, at_next))

            step(diag, True)

            def younger(t, carry):
                @pl.when(t > diag)
                def _():
                    step(t, False)

                return carry

            lax.fori_loop(1, tiles, younger, 0)
            state_out(b, c, i).start()

        def one_pass(p, carry):
            c = jnp.minimum(p, last_chunk)
            upper = p != n_passes - 1
            lower = p != n_passes - PAIR

            @pl.when(upper)
            def _():
                whole(t_s, t_sem)
                gather.near(c)

            @pl.when(lower)
            def _():
                gather.finish(c)

            slot = spot[layer](c)

            def rope(u, i):
                turned = jnp.concatenate([-u[:, hd // 2:], u[:, :hd // 2]], axis=1)
                return (u * t_s[0, i * rows:(i + 1) * rows, :] + turned * t_s[1, i * rows:(i + 1) * rows, :]).astype(BF16)

            parts = ((upper, 0, GROUP - 1), (lower, GROUP - 1, 1))

            def keys_values(g, inner):
                at = wa_landed(p * GROUP + g)
                for wanted, i0, count in parts:
                    @pl.when(wanted)
                    def _():
                        r0, n = i0 * rows, count * rows
                        u = jnp.dot(xo_s[slot, r0:r0 + n, :], wo_s[at, :], preferred_element_type=F32) + ba_s[PAIR * g + 1]
                        for i in range(count):
                            to = here(region(g, True) + position(c, i0 + i), rows)
                            part = u[i * rows:(i + 1) * rows]
                            big_s[to, :hd] = rope(part[:, :hd], i0 + i)
                            big_s[to, hd:] = part[:, hd:].astype(BF16)
                        for i in range(i0, i0 + count):
                            kv_copy(c, i, g).start()
                wa_fetch(p * GROUP + g + PAIR)
                return inner

            lax.fori_loop(0, PAIR, keys_values, 0)

            @pl.when(jnp.logical_and(upper, c >= PAIR))
            def _():
                q_move(c - PAIR, True).wait()

            def for_queries(g, inner):
                at = wa_landed(p * GROUP + PAIR + g)
                for wanted, i0, count in parts:
                    @pl.when(wanted)
                    def _():
                        r0, n = i0 * rows, count * rows
                        u = jnp.dot(xo_s[slot, r0:r0 + n, :], wo_s[at, :], preferred_element_type=F32) + ba_s[PAIR * g]
                        for h in range(PAIR):
                            for i in range(count):
                                part = u[i * rows:(i + 1) * rows, h * hd:(h + 1) * hd]
                                q_s[here(q_row(c, g, i0 + i) + h * rows, rows), :] = rope(part, i0 + i)
                wa_fetch(p * GROUP + g + PAIR + PAIR)
                return inner

            lax.fori_loop(0, PAIR, for_queries, 0)

            @pl.when(lower)
            def _():
                q_move(c, True).start()

            @pl.when(c < last_chunk)
            def _():
                for copy in table_copies(c + 1):
                    copy.start()

            @pl.when(p == 0)
            def _():
                old_push.wait_recv()

            @pl.when(jnp.logical_or(p == 0, p == 2))
            def _():
                early = lax.div(p, 2)
                for g in range(PAIR):
                    s_s[g] = scores(early, early, g, False, lax.div(position(early, early), tile) * tile)

                @pl.when(p == 2)
                def _():
                    gather.forward(3)

                def one(i, inner):
                    @pl.when(jnp.logical_or(early == 0, lax.rem(i, 2) == 1))
                    def _():
                        attend_old(early, i)

                    return inner

                lax.fori_loop(0, GROUP, one, 0)

            @pl.when(p == 0)
            def _():
                gather.forward(2)
                lead(layer, 3)

            @pl.when(p == 2)
            def _():
                q_move(2, True).wait()
                q_move(0, False).start()
                for b in range(PAIR):
                    state_out(jnp.int32(EARLY - PAIR + b), 0, 0).wait()
                for b in range(PAIR):
                    state_in(jnp.int32(b)).start()

            @pl.when(p == 3)
            def _():
                for copy in kv_all[:3]:
                    copy.wait_recv()
                q_move(0, False).wait()
                state_in(jnp.int32(0)).wait()
                diag = lax.div(position(0, 3), tile)
                width = 3 * rows

                def keys(g, t, kv):
                    return big_s[here(region(g, True) + t * tile, width), kv * hd:(kv + 1) * hd]

                def score(g, t):
                    return score_tile(q_s[here(q_row(0, g, 3), tall), :], keys(g, t, 0))

                row = lax.rem(lax.broadcasted_iota(jnp.int32, (tall, 1), 0), rows) + position(0, 3)
                col = lax.broadcasted_iota(jnp.int32, (1, width), 1)
                for g in range(PAIR):
                    s_s[g, :, :width] = score(g, 0)

                def earlier(t, inner):
                    @pl.when(t <= diag)
                    def _():
                        after = jnp.minimum(t + 1, tiles - 1)
                        flash_step(st_s, 0, s_s, scale, col + t * tile <= row, lambda g: keys(g, t, 1), lambda g: score(g, after), width)

                    return inner

                lax.fori_loop(0, tiles, earlier, 0)

            return carry

        lax.fori_loop(0, n_passes, one_pass, 0)
        kv_all[3].wait_recv()
        for c in range(chunks):
            gather.drain(c)
        return kv_all + [old_push]

    def block_phase(layer, sent):
        onward = layer + 1 < layers
        gather = Gather(place, xo_s, spot[layer], a2_send, a2_recv, rows)
        first = Scatter(place, xo_s, slot_of(layer, 1), land_s, r1_send, r1_recv, rows)
        second = Scatter(place, xo_s, spot[layer], land_s, r2_send, r2_recv, rows)
        pushes(layer, slice(3, 4))[0].wait_recv()
        n_out = model // WIDE
        for n in range(n_out):
            for k, src in enumerate((wo, wo_peer)):
                pltpu.make_async_copy(src.at[layer, :, pl.ds(n * WIDE, WIDE)], wo_s.at[pl.ds(n * deep + k * PAIR * hd, PAIR * hd)], wo_sem).start()
        if onward:
            for copy in pushes(layer + 1):
                copy.start()

        def tile_at(diag, n):
            is_new = jnp.logical_or(n == 0, jnp.logical_and(n >= 2, n - 2 < diag))
            t = jnp.where(n < 2, diag, jnp.where(is_new, n - 2, n - 1))
            return is_new, t * tile

        @pl.when(lax.div(position(0, 3), tile) == 0)
        def _():
            for g in range(PAIR):
                s_s[g] = scores(jnp.int32(0), 1, g, True, lax.div(position(0, 1), tile) * tile)

        def attend(c, k):
            i = pick(k)
            b = c * GROUP + k
            w = lax.rem(b, PAIR)
            late = b >= EARLY
            j0 = position(c, i)
            diag = lax.div(j0, tile)
            count = jnp.where(b == 0, 0, jnp.where(late, tiles + 1, diag + 2))
            end = k == 3
            c_next = jnp.minimum(jnp.where(end, c + 1, c), last_chunk)
            i_next = pick(jnp.where(end, 0, k + 1))
            next_at = lax.div(position(c_next, i_next), tile) * tile

            @pl.when(late)
            def _():
                reset_state(st_s, w)

            @pl.when(jnp.logical_and(jnp.logical_not(late), b > 0))
            def _():
                state_in(b).wait()

            def step(n):
                is_new, at = tile_at(diag, n)
                following = jnp.where(jnp.logical_and(n == 0, jnp.logical_not(late)), 2, n + 1)
                last = following == count
                new_next, at_next = tile_at(diag, following)
                new_next = jnp.logical_or(last, new_next)
                at_next = jnp.where(last, next_at, at_next)
                nc = jnp.where(last, c_next, c)
                ni = jnp.where(last, i_next, i)
                col = lax.broadcasted_iota(jnp.int32, (1, tile), 1) + at
                row = lax.rem(lax.broadcasted_iota(jnp.int32, (tall, 1), 0), rows) + j0
                if not isinstance(n, int):
                    mask = col > jnp.where(is_new, -1, floor)
                elif n == 0:
                    mask = col <= row
                else:
                    mask = col > jnp.maximum(row, floor)
                flash_step(st_s, w, s_s, scale, mask, lambda g: tile_of(g, is_new, at, 1), lambda g: scores(nc, ni, g, new_next, at_next))

            @pl.when(b > 0)
            def _():
                step(0)

            @pl.when(late)
            def _():
                step(1)

            def last_keys(u, carry):
                @pl.when(jnp.logical_and(b == 0, u * GROUP < diag))
                def _():
                    def gathered(g, kv):
                        cols = slice(kv * hd, (kv + 1) * hd)
                        return jnp.concatenate([big_s[here(region(g, True) + (u * GROUP + n + 1) * tile - rows, rows), cols] for n in range(GROUP)], axis=0)

                    for g in range(PAIR):
                        s_s[g] = score_tile(q_s[here(q_row(c, g, i), tall), :], gathered(g, 0))
                    seen = lax.broadcasted_iota(jnp.int32, (1, tile), 1) < (diag - u * GROUP) * rows
                    flash_step(st_s, w, s_s, scale, seen, lambda g: gathered(g, 1), lambda g: scores(c_next, i_next, g, True, next_at))

                return carry

            lax.fori_loop(0, PAIR, last_keys, 0)

            def further(n, carry):
                @pl.when(n < count)
                def _():
                    step(n)

                return carry

            lax.fori_loop(2, tiles + 1, further, 0)
            slot = first.slot(c)
            for g in range(PAIR):
                total = jnp.sum(st_s[w, g, :, LANES:PAIR * LANES], axis=1, keepdims=True)
                out = (st_s[w, g, :, PAIR * LANES:] / total).astype(BF16)
                for h in range(PAIR):
                    n = PAIR * g + h
                    xo_s[slot, :rows, n * hd:(n + 1) * hd] = out[h * rows:(h + 1) * rows]

            @pl.when(b + PAIR < EARLY)
            def _():
                state_in(b + PAIR).start()

            @pl.when(b == 0)
            def _():
                whole(wo_s, wo_sem)

            to = here(i * rows, rows)

            def summed(n):
                return jnp.dot(xo_s[slot, :rows, :deep], wo_s[n * deep:(n + 1) * deep, :], preferred_element_type=F32).astype(BF16)

            held = deep // WIDE
            for n in range(held, n_out):
                xo_s[slot, to, n * WIDE:(n + 1) * WIDE] = summed(n)
            for n, part in enumerate([summed(n) for n in range(held)]):
                xo_s[slot, to, n * WIDE:(n + 1) * WIDE] = part

            @pl.when(i == 3)
            def _():
                first.copy(c, 0).start()
                first.copy(c, 1).start()

            for kind in (2, 3):
                @pl.when(i == kind - 1)
                def _():
                    first.copy(c, kind).start()

        bias_o, bias_d = one_row(b_o, layer), one_row(b_down, layer)

        def open_mlp(c):
            first.finish(c)

            def body(at, n):
                mid_s[c, at, :] = (mid_s[c, at, :].astype(F32) + first.total(c, n) + bias_o).astype(BF16)

            row_blocks(body)
            norm_into(layer, 2, c, spot[layer](c))
            gather.start(c)

        def attend_chunk(c, carry):
            def one(k, inner):
                @pl.when(jnp.logical_and(k == 3, c + 1 < chunks))
                def _():
                    q_move(c + 1, False).wait()

                attend(c, k)

                @pl.when(jnp.logical_and(c == 0, k == 1))
                def _():
                    q_move(last_chunk, True).wait()
                    q_move(1, False).start()

                @pl.when(jnp.where(c == 0, k == 3, jnp.logical_and(c >= 2, k == 0)))
                def _():
                    first.relay(jnp.maximum(c - 1, 0), c - 2)

                return inner

            lax.fori_loop(0, GROUP, one, 0)

            @pl.when(c + PAIR < chunks)
            def _():
                q_move(c + PAIR, False).start()

            @pl.when(c >= 2)
            def _():
                open_mlp(c - 2)

            return carry

        lax.fori_loop(0, chunks, attend_chunk, 0)
        for copy in sent:
            copy.wait_send()
        if onward:
            raw_copy(layer + 1, 0).start()
        for copy in pushes(layer, slice(4, None)):
            copy.wait_recv()
        n_up = PAIR * ffn // WIDE
        n_tiles = n_up + n_out
        sub = WIDE // PAIR
        n_sub = ffn // sub
        act = xo_s.at[spare[layer]]

        def slot_at(c, k):
            slot = lax.rem(c * n_tiles + k, WEIGHT_SLOTS)
            return slot, pl.multiple_of(slot * model, WIDE)

        def fetch(c, k):
            over = k >= n_tiles
            k = jnp.where(over, k - n_tiles, k)
            c = jnp.where(over, c + 1, c)
            slot, base = slot_at(c, k)

            @pl.when(c < chunks)
            def _():
                for part in range(PAIR):
                    n = PAIR * k + part
                    for side, src in enumerate((up, up_peer)):
                        @pl.when(jnp.logical_and(n >= side * n_sub, n < (side + 1) * n_sub))
                        def _():
                            at = pl.multiple_of((n - side * n_sub) * sub, sub)
                            pltpu.make_async_copy(src.at[layer, :, pl.ds(at, sub)], big_s.at[pl.ds(base, model), pl.ds(part * sub, sub)], wm_sem.at[slot]).start()

                @pl.when(k >= n_up)
                def _():
                    at = pl.multiple_of((k - n_up) * WIDE, WIDE)
                    for side, src in enumerate((down, down_peer)):
                        dst = big_s.at[pl.ds(pl.multiple_of(base + side * ffn, sub), ffn)]
                        pltpu.make_async_copy(src.at[layer, :, pl.ds(at, WIDE)], dst, wm_sem.at[slot]).start()

        def landed(c, k):
            slot, base = slot_at(c, k)
            whole(big_s.at[pl.ds(base, model)], wm_sem.at[slot])
            fetch(c, k + WEIGHT_SLOTS - 1)
            return pl.ds(base, model)

        for k in range(WEIGHT_SLOTS - 1):
            fetch(jnp.int32(0), jnp.int32(k))
        stage = WEIGHT_SLOTS * model

        def stage_at(n):
            slot = lax.rem(n, ROLL_SLOTS)
            return slot, pl.ds(pl.multiple_of(stage + slot * ROLL_ROWS, ROLL_ROWS), ROLL_ROWS)

        def staged(n):
            slot, at = stage_at(n)
            whole(big_s.at[at], f_sem.at[slot])

        def put_new(n, turned):
            slot, at = stage_at(n)

            @pl.when(n >= ROLL_SLOTS)
            def _():
                staged(n)

            for k in range(PAIR):
                cols = slice(k * hd, (k + 1) * hd)
                big_s[at, cols] = turned[k]
                dst = pl.ds(pl.multiple_of((layer * PAIR + k) * window + n * ROLL_ROWS, ROLL_ROWS), ROLL_ROWS)
                pltpu.make_async_copy(big_s.at[at, cols], kv_rolled.at[dst], f_sem.at[slot]).start()

        fresh = [lambda k=k: big_s[3 * window:, k * hd:(k + 1) * hd] for k in range(PAIR)]
        rotate(fresh, put_new, window, window - first_slot, 0, roll_tiles // PAIR)
        gather.forward(0)
        rotate(fresh, put_new, window, window - first_slot, roll_tiles // PAIR, roll_tiles)
        for n in range(PAIR * n_sub):
            src = bu if n < n_sub else bu_s
            at = n % n_sub * sub
            bm_s[n // PAIR, :, n % PAIR * sub:(n % PAIR + 1) * sub] = one_row(src, layer)[:, at:at + sub]
        first.relay(last_chunk, last_chunk - 1)
        open_mlp(2)
        gather.forward(1)
        open_mlp(3)
        first.drain(last_chunk)
        for n in range(ROLL_SLOTS):
            staged(n)

        def mlp_chunk(c, carry):
            gather.near(c)
            gather.finish(c)
            slot = spot[layer](c)

            def up_step(k, inner):
                at = landed(c, k)
                for top in range(PAIR):
                    r0 = top * tall
                    lifted = jnp.dot(xo_s[slot, r0:r0 + tall, :], big_s[at, :], preferred_element_type=F32) + bm_s[k]
                    act[r0:r0 + tall, pl.ds(pl.multiple_of(k * WIDE, WIDE), WIDE)] = gelu_tanh(lifted).astype(BF16)
                return inner

            lax.fori_loop(0, n_up, up_step, 0)

            @pl.when(c + 2 < chunks)
            def _():
                gather.forward(c + 2)

            gather.drain(c)

            @pl.when(c >= 2)
            def _():
                second.relay(c - 2, c - 3 if onward else None)

            def down_step(k, inner):
                at = landed(c, k)
                xo_s[slot, :, pl.ds(pl.multiple_of((k - n_up) * WIDE, WIDE), WIDE)] = jnp.dot(act[...], big_s[at, :], preferred_element_type=F32).astype(BF16)
                return inner

            lax.fori_loop(n_up, n_tiles, down_step, 0)
            second.start(c)
            return carry

        lax.fori_loop(0, chunks, mlp_chunk, 0)
        if onward:
            pl.semaphore_signal(ready, inc=1, device_id={'tp': place.peer}, device_id_type=MESH)

        def o_copy(c):
            return pltpu.make_async_copy(mid_s.at[c], h_out.at[here(c * rows, rows)], h_sem.at[c])

        second.relay(2, None)
        second.relay(3, None)
        if onward:
            second.drain(1)

        def close(c, carry):
            second.finish(c)

            def body(at, n):
                mid_s[c, at, :] = (mid_s[c, at, :].astype(F32) + second.total(c, n) + bias_d).astype(BF16)

            row_blocks(body)
            if onward:
                norm_into(layer + 1, 0, c, spot[layer + 1](c))

                @pl.when(c < 2)
                def _():
                    lead(layer + 1, c)
            else:
                o_copy(c).start()
            return carry

        lax.fori_loop(0, chunks, close, 0)
        if onward:
            second.drain(2)
            second.drain(last_chunk)
        else:
            for c in range(chunks):
                second.drain(c)
                o_copy(c).wait()

    for layer in range(layers):
        block_phase(layer, project_phase(layer))
    for copy in b_copies:
        copy.wait_send()
    for layer in range(layers):
        for copy in pushes(layer):
            copy.wait_send()


def run_step(chunks, scal, tokens, norms, cos, sin, weights, biases, caches, w_o, w_up, w_down, b_o, b_down):
    model = tokens.shape[1]
    rows = tokens.shape[0] // chunks
    layers, window, hd = caches[0].shape
    ffn = w_up.shape[2]
    dims = (layers, chunks, rows, model, hd, window, ffn)
    state = (PAIR * GROUP, PAIR, PAIR * rows, PAIR * LANES + hd)
    out = [tokens.shape, (layers * PAIR * window, hd), (chunks * PAIR * GROUP * PAIR * rows, hd), (layers, model, GROUP * hd), w_o.shape, w_up.shape, w_down.shape]
    out = [jax.ShapeDtypeStruct(o, BF16) for o in out]
    out.insert(3, jax.ShapeDtypeStruct(state, F32))
    few = [dma(*n) for n in ((chunks,), (), (), (PAIR,), (), (WEIGHT_SLOTS,), (PAIR,), (PAIR,), (ROLL_SLOTS,))]
    return pl.pallas_call(
        functools.partial(step_kernel, dims),
        out_shape=tuple(out),
        in_specs=[SMEM, ANY, VMEM] + [ANY] * 5 + [VMEM] * 4 + [ANY] * 9 + [VMEM] * 2,
        out_specs=(ANY,) * len(out),
        scratch_shapes=[
            vm(PAIR * PAIR * window, WIDE),
            vm(window, hd),
            vm(PAIR, GROUP * rows, hd, dtype=F32),
            vm(PAIR, PAIR * rows, KEY_TILE, dtype=F32),
            vm(PAIR * model, WIDE),
            vm(SLOTS, GROUP * rows, model),
            vm(chunks, 3 * rows, model),
            vm(chunks, rows, model),
            vm(PAIR, *state[1:], dtype=F32),
            vm(GROUP, 1, PAIR * hd, dtype=F32),
            vm(PAIR * ffn // WIDE, 1, WIDE, dtype=F32),
            *(vm(*b.shape) for b in biases),
            *(dma(chunks, 6) for _ in range(8)),
            dma(),
            dma(),
            dma(chunks),
            dma(chunks),
            dma(layers, 6),
            dma(layers, 6),
            dma(GROUP),
            dma(GROUP),
            *few,
            pltpu.SemaphoreType.REGULAR,
        ],
        compiler_params=pltpu.CompilerParams(vmem_limit_bytes=VMEM_LIMIT, collective_id=0, has_side_effects=True),
        name="step",
    )(scal, tokens, norms, cos, sin, *weights, *biases, *biases, *caches, w_o, w_up, w_down, b_o, b_down)


def copy_kernel(scal, *refs):
    hidden, kv, h_out, k_out, v_out, p_out, h_s, kv_s, in_sem, out_sem = refs
    window = k_out.shape[1]
    cut = window // GROUP
    part = hidden.shape[0] // GROUP
    moves = [(hidden.at[pl.ds(n * part, part)], h_s.at[pl.ds(n * part, part)], h_out.at[pl.ds(n * part, part)]) for n in range(GROUP)]
    for layer in range(k_out.shape[0]):
        for k, out in enumerate((k_out, v_out)):
            for n in range(GROUP):
                at = pl.ds((layer * PAIR + k) * window + n * cut, cut)
                moves.append((kv.at[at], kv_s.at[at], out.at[layer, pl.ds(n * cut, cut)]))
    for n, (src, mid, _) in enumerate(moves):
        pltpu.make_async_copy(src, mid, in_sem.at[n]).start()
    start_pos = scal[0]
    ahead = lax.broadcasted_iota(jnp.int32, p_out.shape, 1) + (window - lax.rem(start_pos, window))
    p_out[...] = start_pos + jnp.where(ahead >= window, ahead - window, ahead)
    for n, (src, mid, dst) in enumerate(moves):
        pltpu.make_async_copy(src, mid, in_sem.at[n]).wait()
        pltpu.make_async_copy(mid, dst, out_sem.at[n]).start()
    for n, (_, mid, dst) in enumerate(moves):
        pltpu.make_async_copy(mid, dst, out_sem.at[n]).wait()


def run_copy(scal, hidden, kv, layers, window):
    hd = kv.shape[1]
    planes = jax.ShapeDtypeStruct((layers, window, hd), BF16)
    count = GROUP + PAIR * GROUP * layers
    return pl.pallas_call(
        copy_kernel,
        out_shape=(jax.ShapeDtypeStruct(hidden.shape, BF16), planes, planes, jax.ShapeDtypeStruct((1, window), jnp.int32)),
        in_specs=[SMEM, ANY, ANY],
        out_specs=(ANY, ANY, ANY, VMEM),
        scratch_shapes=[vm(*hidden.shape), vm(*kv.shape), dma(count), dma(count)],
        compiler_params=pltpu.CompilerParams(vmem_limit_bytes=VMEM_LIMIT),
        name="copy_out",
    )(scal, hidden, kv)


def solution(mesh):
    row_spec = P('dp', 'tp', None)
    cache_spec = P(None, 'dp', None, 'tp', None)
    col_spec = P(None, None, 'tp')
    bias_spec = P(None, 'tp')
    in_specs = (row_spec, P('dp'), P('dp', None, None), P('dp', None, None), cache_spec, cache_spec, P('dp', None), P(), col_spec, bias_spec, col_spec, bias_spec, col_spec, bias_spec, P(None, 'tp', None), P(), col_spec, bias_spec, P(None, 'tp', None), P())
    out_specs = (row_spec, cache_spec, cache_spec, P('dp', None))

    def device_step(tokens, start_pos, cos_tab, sin_tab, key_cache, value_cache, slot_pos, norm_params, w_q, b_q, w_k, b_k, w_v, b_v, w_o, b_o, w_up, b_up, w_down, b_down):
        layers, _, window, _, hd = key_cache.shape
        caches = tuple(cache.reshape(layers, window, hd) for cache in (key_cache, value_cache))
        made = run_step(CHUNKS, start_pos, tokens[0], norm_params, cos_tab[0], sin_tab[0], (w_q, w_k, w_v), (b_q, b_k, b_v, b_up), caches, w_o, w_up, w_down, b_o, b_down)
        hidden, key_out, value_out, pos_out = run_copy(start_pos, made[0], made[1], layers, window)
        return hidden[None], key_out.reshape(key_cache.shape), value_out.reshape(value_cache.shape), pos_out

    return jax.shard_map(device_step, mesh=mesh, in_specs=in_specs, out_specs=out_specs, check_vma=False)
```
